8 devices in a mesh: batch: 1 (over z), src: 2 (over y), graph: 4 (over x, core).
Axes of the slice: x: 2, y: 2, z: 1, core: 2. Of those that a mesh axis runs over, the one named last changes fastest.
Arguments:
- adj: bfloat16 [16384, 16384], P(('batch', 'graph'))
- sources: int32 [512], P(('batch', 'src'))
- level_weight: float32 [11], replicated
Outputs:
- output: float32 [16384], P(('batch', 'graph'))
All inputs are finite; a program needn't handle non-finite values.
Results may differ from the reference program's by a relative error of at most 0.001.
Values are sent between devices in bfloat16 or wider.
A program may use at most 1 GiB of HBM per device.

```python
import jax
import jax.numpy as jnp
from jax import lax

GRID_X = 128
GRID_Y = 128
GRID_Z = 1
NUM_SOURCES = 512
LEVELS = 12


def setup_inputs(seed: int = 0, part: int = 0) -> dict:
    vertex_count = GRID_X * GRID_Y * GRID_Z
    base_key = jax.random.key(seed)
    shared_key, part_root = jax.random.split(base_key)
    part_key = jax.random.fold_in(part_root, part)
    graph_key, source_key = jax.random.split(part_key)
    hidden = jax.random.permutation(graph_key, vertex_count)
    coord_x = hidden % GRID_X
    coord_y = (hidden // GRID_X) % GRID_Y
    coord_z = hidden // (GRID_X * GRID_Y)
    manhattan = (jnp.abs(coord_x[:, None] - coord_x[None, :])
                 + jnp.abs(coord_y[:, None] - coord_y[None, :])
                 + jnp.abs(coord_z[:, None] - coord_z[None, :]))
    adj = jnp.where(manhattan == 1, 1.0, 0.0).astype(jnp.float32).astype(jnp.bfloat16)
    sources = jax.random.permutation(source_key, vertex_count)[:NUM_SOURCES].astype(jnp.int32)
    level_weight = jax.random.uniform(shared_key, (LEVELS - 1,), jnp.float32, 0.5, 1.5)
    return {"adj": adj, "sources": sources, "level_weight": level_weight}


def reference(adj, sources, level_weight):
    vertex_count = GRID_X * GRID_Y * GRID_Z
    row_block = vertex_count // 8
    adj_blocks = adj.reshape(8, row_block, vertex_count)
    vertex_ids = jnp.arange(vertex_count, dtype=jnp.int32)
    sigma_zero = jnp.where(vertex_ids[:, None] == sources[None, :], 1.0, 0.0).astype(jnp.float32)

    def push_forward(sigma):
        sigma_blocks = sigma.reshape(8, row_block, NUM_SOURCES)

        def accumulate(acc, pair):
            adj_blk, sig_blk = pair
            return acc + jnp.dot(adj_blk.astype(jnp.float32).T, sig_blk, preferred_element_type=jnp.float32), None

        result, _ = lax.scan(accumulate, jnp.zeros_like(sigma), (adj_blocks, sigma_blocks))
        return result

    def pull_back(weights):
        def block_product(adj_blk):
            return jnp.dot(adj_blk.astype(jnp.float32), weights, preferred_element_type=jnp.float32)

        return lax.map(block_product, adj_blocks).reshape(vertex_count, NUM_SOURCES)

    def forward_step(carry, unused):
        sigma, seen = carry
        sigma_next = push_forward(sigma) * (1.0 - seen)
        seen_next = jnp.maximum(seen, jnp.where(sigma_next > 0, 1.0, 0.0))
        return (sigma_next, seen_next), sigma_next

    _, sigmas = lax.scan(forward_step, (sigma_zero, sigma_zero), None, length=LEVELS)
    uppers = sigmas[1:][::-1]
    lowers = sigmas[:-1][::-1]
    weights_by_level = level_weight[::-1]

    def backward_step(carry, level_inputs):
        delta, total = carry
        sig_upper, sig_lower, weight = level_inputs
        reached = sig_upper > 0
        weights = jnp.where(reached, (weight + delta) / jnp.where(reached, sig_upper, 1.0), 0.0)
        delta_next = sig_lower * pull_back(weights)
        return (delta_next, total + delta_next), None

    zero_mat = jnp.zeros_like(sigma_zero)
    (_, total), _ = lax.scan(backward_step, (zero_mat, zero_mat), (uppers, lowers, weights_by_level))
    scale = vertex_count / (NUM_SOURCES * LEVELS ** 3)
    return jnp.sum(total, axis=1) * scale
```

```python
import functools

import jax
import jax.numpy as jnp
from jax import lax
from jax.experimental import pallas as pl
from jax.experimental.pallas import tpu as pltpu
from jax.sharding import PartitionSpec as P

MESH = pl.DeviceIdType.MESH
exact_precision = lax.Precision.HIGHEST
f32 = jnp.float32

LANES = 128
WIDE = 256
DEG = 8
EMPTY = -2.0
FULL = 32767.0
HALF = 64
SLOTS = 8
WINDOW = 64
CAP = 1024
TURN = (((1,), (1,)), ((), ()))


def extract_kernel(half_ref, a_ref, o_ref, tops_ref, seen_ref, *, group=4, step=8):
    block, vertices = a_ref.shape
    chunks = vertices // WIDE
    height = 8 * group

    def scan_rows(t, carry):
        rows = pl.ds(pl.multiple_of(t * height, height), height)

        def scan_chunks(g, state):
            top, low, seen, value = state
            for k in range(step):
                a = a_ref[rows, pl.ds(pl.multiple_of((g * step + k) * WIDE, WIDE), WIDE)]
                x = a * value
                low = jnp.maximum(low, jnp.minimum(top, x))
                top = jnp.maximum(top, x)
                seen = seen + a
                value = value + 1
            return top, low, seen, value

        zero = jnp.zeros((height, WIDE), jnp.bfloat16)
        top, low, seen, _ = lax.fori_loop(0, chunks // step, scan_chunks, (zero, zero, zero, zero + 1))
        tops_ref[0, rows, :] = top
        tops_ref[1, rows, :] = low
        seen_ref[rows, :] = seen
        return carry

    lax.fori_loop(0, block // height, scan_rows, 0)

    ones = jnp.ones((8, WIDE), jnp.bfloat16)
    degree = lax.dot_general(ones, seen_ref[...], TURN, preferred_element_type=jnp.float32)
    crowd = jnp.max(seen_ref[...].astype(jnp.float32)) > 2.0
    simple = jnp.logical_and(jnp.logical_not(crowd), jnp.max(degree) <= DEG // 2)

    @pl.when(crowd)
    def _():
        def scan_chunk(c, carry):
            a = a_ref[:, pl.ds(pl.multiple_of(c * WIDE, WIDE), WIDE)]
            x = a.astype(jnp.float32) * (c + 1).astype(jnp.float32)
            for s in range(DEG):
                top = tops_ref[s].astype(jnp.float32)
                tops_ref[s] = jnp.maximum(top, x).astype(jnp.bfloat16)
                x = jnp.minimum(top, x)
            return carry

        tops_ref[...] = jnp.zeros_like(tops_ref)
        lax.fori_loop(0, chunks, scan_chunk, 0)

    @pl.when(jnp.logical_not(crowd))
    def _():
        tops_ref[2:] = jnp.zeros((DEG - 2, block, WIDE), jnp.bfloat16)

    row_i = lax.broadcasted_iota(jnp.int32, (WIDE, WIDE), 0)
    col_i = lax.broadcasted_iota(jnp.int32, (WIDE, WIDE), 1)
    eye = jnp.where(row_i == col_i, 1.0, 0.0).astype(jnp.bfloat16)
    lane_id = lax.broadcasted_iota(jnp.int32, (8, block), 0).astype(jnp.float32)

    def place(plane, lists):
        flipped = lax.dot_general(eye, tops_ref[plane], TURN, preferred_element_type=jnp.float32)
        lists = list(lists)
        for g in range(WIDE // 8):
            c = flipped[g * 8:(g + 1) * 8]
            x = jnp.where(c > 0, c * WIDE + (lane_id + float(g * 8 - WIDE)), EMPTY)
            for s in range(len(lists)):
                hi = jnp.maximum(lists[s], x)
                x = jnp.minimum(lists[s], x)
                lists[s] = hi
        return lists

    def merge(lists):
        size = len(lists)
        for shift in (4, 2, 1):
            other = [pltpu.roll(v, shift, 0) for v in lists]
            lists = [jnp.maximum(lists[s], other[size - 1 - s]) for s in range(size)]
            gap = size // 2
            while gap:
                for s in range(size):
                    if not s & gap:
                        lists[s], lists[s + gap] = jnp.maximum(lists[s], lists[s + gap]), jnp.minimum(lists[s], lists[s + gap])
                gap //= 2
        sub = lax.broadcasted_iota(jnp.int32, (8, block), 0)
        out = jnp.full((8, block), EMPTY, jnp.float32)
        for s in range(size):
            out = jnp.where(sub == s, lists[s], out)
        return out

    empty = jnp.full((8, block), EMPTY, jnp.float32)

    @pl.when(simple)
    def _():
        lists = [empty] * (DEG // 2)
        for plane in range(2):
            lists = place(plane, lists)
        o_ref[...] = merge(lists)

    @pl.when(jnp.logical_not(simple))
    def _():
        lists = lax.fori_loop(0, DEG, lambda plane, lists: tuple(place(plane, lists)), (empty,) * DEG)
        o_ref[...] = jnp.where(degree > DEG, FULL, merge(list(lists)))


def extract(adj_slab, half, rows, block=128, **kw):
    vertices = adj_slab.shape[1]
    steps = rows // block
    return pl.pallas_call(
        functools.partial(extract_kernel, **kw),
        grid_spec=pltpu.PrefetchScalarGridSpec(
            num_scalar_prefetch=1,
            grid=(steps,),
            in_specs=[pl.BlockSpec((block, vertices), lambda i, h: (h[0] * steps + i, 0))],
            out_specs=pl.BlockSpec((8, block), lambda i, h: (0, i)),
            scratch_shapes=[pltpu.VMEM((DEG, block, WIDE), jnp.bfloat16), pltpu.VMEM((block, WIDE), jnp.bfloat16)],
        ),
        out_shape=jax.ShapeDtypeStruct((DEG, rows), jnp.float32),
        name="extract",
    )(half, adj_slab)


def walk_kernel(lists_ref, src_ref, weight_ref, out_ref,
                table, queue, sigma, ratio, delta, cand, ids, near, bins, ids_s, meta, sem, *, levels, vertices, scale):
    parts, _, width = lists_ref.shape
    dummy = vertices
    lane = lax.broadcasted_iota(jnp.int32, (8, LANES), 1)
    sub = lax.broadcasted_iota(jnp.int32, (8, LANES), 0)
    upper = lane >= HALF
    lane_row = lax.broadcasted_iota(jnp.int32, (1, LANES), 1)
    group_odd = ((lane_row // 32) % 2) == 1
    lane32 = lane_row % 32

    srow = lax.broadcasted_iota(jnp.int32, (2 * DEG, LANES), 0)
    slane = lax.broadcasted_iota(jnp.int32, (2 * DEG, LANES), 1)

    def spread(quad):
        mine = (srow % DEG) == (slane // 32 + 4 * quad)
        return jnp.where(mine, jnp.where(srow < DEG, float(LANES), 1.0), 0.0).astype(jnp.bfloat16)

    def fill(quad):
        pick = spread(quad)
        blocks = width // LANES

        def body(b, most):
            for k in range(4):
                bb = b * 4 + k
                d, c = bb // blocks, bb % blocks
                x = lists_ref[d, :, pl.ds(pl.multiple_of(c * LANES, LANES), LANES)]
                hi = jnp.floor(x * (1.0 / LANES))
                lo = x - hi * LANES
                both = jnp.concatenate([hi, lo], axis=0).astype(jnp.bfloat16)
                rows = lax.dot_general(both, pick, (((0,), (0,)), ((), ())), preferred_element_type=f32)
                table[quad, pl.ds(pl.multiple_of(bb * LANES, LANES), LANES), :] = rows
                most = jnp.maximum(most, x)
            return most

        most = lax.fori_loop(0, parts * blocks // 4, body, jnp.full((DEG, LANES), EMPTY, f32))
        table[quad, vertices:, :] = jnp.full((8, LANES), EMPTY, f32)
        return most

    most = fill(0)
    top = jnp.max(most)
    wide = jnp.max(jnp.where(sub >= 4, most, EMPTY)) >= 0
    quads = jnp.where(wide, 2, 1)

    @pl.when(wide)
    def _():
        fill(1)

    bad = top > vertices
    meta[2, 0] = bad.astype(jnp.int32)

    rows_all = queue.shape[0]

    def clear(t, carry):
        rows = pl.ds(pl.multiple_of(t * 8, 8), 8)
        queue[rows, :] = jnp.full((8, LANES), -1.0, f32)
        sigma[rows, :] = jnp.zeros((8, LANES), f32)
        delta[rows, :] = jnp.zeros((8, LANES), f32)
        ids[rows, :] = jnp.full((8, LANES), dummy, jnp.int32)
        return carry

    lax.fori_loop(0, rows_all // 8, clear, 0)
    bins[...] = jnp.zeros_like(bins)

    def window_rows(base, group):
        return [pl.ds(pl.multiple_of(base + group * WINDOW + 8 * t, 8), 8) for t in range(WINDOW // 8)]

    def gather(slot, row, quad):
        acc = [jnp.full((1, LANES), EMPTY, f32)] * 2
        for j in range(32):
            hit = lane32 == j
            for b in range(2):
                v = ids_s[slot, b * 32 + j]
                acc[b] = jnp.where(hit, table[quad, pl.ds(v, 1), :], acc[b])
        c0 = jnp.where(group_odd, acc[1], acc[0])
        c1 = pltpu.roll(jnp.where(group_odd, acc[0], acc[1]), LANES - 32, 1)
        cand[2 * quad, pl.ds(row, 1), :] = c0
        cand[2 * quad + 1, pl.ds(row, 1), :] = c1

    def bits(x):
        return jnp.where(x, 1, 0)

    def place(c0, c1, near0, near1, tail):
        c0r, c1r = pltpu.roll(c0, HALF, 1), pltpu.roll(c1, HALF, 1)
        both = near0 + 2 * near1
        for shift in (4, 2, 1):
            both = both | pltpu.roll(both, shift, 0)
        both = both | bits(c0 < 0) | (2 * bits(c1 < 0))
        other = pltpu.roll(both, HALF, 1)
        n0, n1 = 1 - (both & 1), 1 - (both >> 1)
        r0, r1 = 1 - (other & 1), 1 - (other >> 1)
        mid = tail + n0 + r0
        d0 = jnp.where(n0 > 0, tail + jnp.where(upper, r0, 0), -1)
        e0 = jnp.where(r0 > 0, tail + jnp.where(upper, 0, n0), -1)
        d1 = jnp.where(n1 > 0, mid + jnp.where(upper, r1, 0), -1)
        e1 = jnp.where(r1 > 0, mid + jnp.where(upper, 0, n1), -1)
        return c0r, c1r, d0, e0, d1, e1, mid + n1 + r1

    def look(c0, c1, q, s, sig, near0, near1):
        m0, m1 = q == c0, q == c1
        return (jnp.where(m0, 1, near0), jnp.where(m1, 1, near1), jnp.where(m0 | m1, s + sig, s))

    def put(pos, q, s, sig, c0, c1, c0r, c1r, d0, e0, d1, e1):
        a, b, c, d = pos == d0, pos == e0, pos == d1, pos == e1
        q = jnp.where(a, c0, jnp.where(b, c0r, jnp.where(c, c1, jnp.where(d, c1r, q))))
        return q, jnp.where(a | c, sig, s)

    def wide_row(ref, row):
        return jnp.broadcast_to(ref[pl.ds(row, 1), :], (8, LANES))

    def wide_cand(which, row):
        return jnp.broadcast_to(cand[which, pl.ds(row, 1), :], (8, LANES))

    def level_step(level, carry):
        base, count = meta[0, level], meta[1, level]
        following = base + (count + 7) // 8 * 8

        def chunk_step(ch, tail):
            first = base + ch * WINDOW
            copy = pltpu.make_async_copy(ids.at[pl.ds(pl.multiple_of(first, 8), WINDOW)], ids_s, sem)
            copy.start()
            copy.wait()
            here = jnp.minimum(count - ch * WINDOW, WINDOW)

            def quad_step(quad, tail):
                for i in range(SLOTS):
                    gather(i, first + i, quad)

                def batch_step(bt, tail):
                    row = first + bt * SLOTS

                    cs = [wide_cand(2 * quad + h, row + i) for i in range(SLOTS) for h in range(2)]

                    def prefix(t, marks):
                        marks = list(marks)
                        for rows in window_rows(0, t):
                            q = queue[rows, :]
                            for m in range(2 * SLOTS):
                                marks[m] = jnp.where(q == cs[m], 1, marks[m])
                        return tuple(marks)

                    marks = lax.fori_loop(0, (following + WINDOW - 1) // WINDOW, prefix,
                                          (jnp.zeros((8, LANES), jnp.int32),) * (2 * SLOTS))
                    for m in range(2 * SLOTS):
                        near[m] = marks[m]

                    slots = window_rows(jnp.minimum(following, CAP), 0)
                    qs = [queue[r, :] for r in slots]
                    ss = [sigma[r, :] for r in slots]
                    newtail = tail
                    for i in range(SLOTS):
                        gather(jnp.minimum(bt * SLOTS + SLOTS + i, WINDOW - 1), row + SLOTS + i, quad)
                        c0, c1 = wide_cand(2 * quad, row + i), wide_cand(2 * quad + 1, row + i)
                        sig = wide_row(sigma, row + i)
                        n0, n1 = near[2 * i], near[2 * i + 1]
                        for t in range(WINDOW // 8):
                            n0, n1, ss[t] = look(c0, c1, qs[t], ss[t], sig, n0, n1)
                        c0r, c1r, d0, e0, d1, e1, newtail = place(c0, c1, n0, n1, newtail)
                        for t in range(WINDOW // 8):
                            qs[t], ss[t] = put(sub + 8 * t, qs[t], ss[t], sig, c0, c1, c0r, c1r, d0, e0, d1, e1)
                    length = jnp.max(newtail)
                    short = jnp.logical_and(length <= WINDOW, following <= CAP)

                    @pl.when(short)
                    def _():
                        for t, r in enumerate(slots):
                            queue[r, :] = qs[t]
                            sigma[r, :] = ss[t]

                    def long_batch(tail):
                        groups = (length + WINDOW - 1) // WINDOW
                        fits = following + groups * WINDOW <= CAP
                        groups = jnp.where(fits, groups, 0)

                        @pl.when(jnp.logical_not(fits))
                        def _():
                            meta[2, 0] = 1

                        def slot_step(i, tail):
                            c0, c1 = wide_cand(2 * quad, row + i), wide_cand(2 * quad + 1, row + i)
                            sig = wide_row(sigma, row + i)

                            def seek(g, marks):
                                n0, n1 = marks
                                for r in window_rows(following, g):
                                    n0, n1, sigma[r, :] = look(c0, c1, queue[r, :], sigma[r, :], sig, n0, n1)
                                return n0, n1

                            n0, n1 = lax.fori_loop(0, groups, seek, (near[2 * i], near[2 * i + 1]))
                            c0r, c1r, d0, e0, d1, e1, tail = place(c0, c1, n0, n1, tail)

                            def insert(g, carry):
                                for t, r in enumerate(window_rows(following, g)):
                                    queue[r, :], sigma[r, :] = put(sub + (g * WINDOW + 8 * t), queue[r, :], sigma[r, :], sig,
                                                                   c0, c1, c0r, c1r, d0, e0, d1, e1)
                                return carry

                            lax.fori_loop(0, groups, insert, 0)
                            return tail

                        return lax.fori_loop(0, SLOTS, slot_step, tail)

                    return lax.cond(short, lambda t: newtail, long_batch, tail)

                return lax.fori_loop(0, (here + SLOTS - 1) // SLOTS, batch_step, tail)

            return lax.fori_loop(0, quads, quad_step, tail)

        tail = lax.fori_loop(0, (count + WINDOW - 1) // WINDOW, chunk_step, jnp.zeros((8, LANES), jnp.int32))
        found = jnp.where(meta[2, 0] == 0, jnp.max(tail), 0)
        meta[0, level + 1] = following
        meta[1, level + 1] = found

        def settle(g, carry):
            for r in window_rows(following, g):
                q = queue[r, :]
                ids[r, :] = jnp.where(q < 0, dummy, q.astype(jnp.int32))
            for r in window_rows(following, g):
                s = sigma[r, :]
                sigma[r, :] = s + pltpu.roll(s, HALF, 1)
            return carry

        lax.fori_loop(0, (found + WINDOW - 1) // WINDOW, settle, 0)
        return carry

    @pl.when(jnp.logical_not(bad))
    def _():
        queue[0:1, :] = src_ref[...]
        sigma[0:1, :] = jnp.ones((1, LANES), f32)
        ids[0:1, :] = src_ref[...].astype(jnp.int32)
        meta[0, 0] = 0
        meta[1, 0] = 1
        lax.fori_loop(0, levels, level_step, 0)

    good = meta[2, 0] == 0

    @pl.when(good)
    def _():
        last = meta[0, levels]
        g_last = weight_ref[levels - 2]

        def seed(g, carry):
            for r in window_rows(last, g):
                s = sigma[r, :]
                ratio[r, :] = jnp.where(s > 0, g_last / jnp.where(s > 0, s, 1.0), 0.0)
            return carry

        lax.fori_loop(0, (meta[1, levels] + WINDOW - 1) // WINDOW, seed, 0)

        def back_step(k, carry):
            level = levels - 1 - k
            base, count = meta[0, level], meta[1, level]
            nbase, ncount = meta[0, level + 1], meta[1, level + 1]
            g_here = weight_ref[jnp.maximum(level - 2, 0)]

            def batch_step(bt, carry):
                row = pl.multiple_of(base + bt * SLOTS, 8)

                def pull(m, acc):
                    quad, g = m % quads, m // quads
                    acc = list(acc)
                    slots = window_rows(nbase, g)
                    qs = [queue[r, :] for r in slots]
                    ws = [ratio[r, :] for r in slots]
                    for i in range(SLOTS):
                        c0, c1 = wide_cand(2 * quad, row + i), wide_cand(2 * quad + 1, row + i)
                        for t in range(WINDOW // 8):
                            acc[i] = acc[i] + jnp.where((qs[t] == c0) | (qs[t] == c1), ws[t], 0.0)
                    return tuple(acc)

                acc = lax.fori_loop(0, quads * ((ncount + WINDOW - 1) // WINDOW), pull,
                                    (jnp.zeros((8, LANES), f32),) * SLOTS)
                pulled = jnp.concatenate([jnp.sum(a, axis=0, keepdims=True) for a in acc], axis=0)
                pulled = pulled + pltpu.roll(pulled, HALF, 1)
                here = pl.ds(row, SLOTS)
                s = sigma[here, :]
                d = s * pulled
                delta[here, :] = d
                ratio[here, :] = jnp.where(s > 0, (g_here + d) / jnp.where(s > 0, s, 1.0), 0.0)
                return carry

            lax.fori_loop(0, (count + SLOTS - 1) // SLOTS, batch_step, 0)
            return carry

        lax.fori_loop(0, levels - 1, back_step, 0)

        tall = lax.broadcasted_iota(jnp.int32, (LANES, 2 * LANES), 0).astype(f32)
        start = meta[0, 1]

        def tally(t, carry):
            a = pl.ds(pl.multiple_of(start + t * 16, 8), 8)
            b = pl.ds(pl.multiple_of(start + t * 16 + 8, 8), 8)
            v = jnp.where(upper, queue[b, :], queue[a, :])
            d = jnp.where(upper, delta[b, :], delta[a, :])
            hi = jnp.floor(v * (1.0 / LANES))
            lo = v - hi * LANES
            d_hi = d.astype(jnp.bfloat16).astype(f32)
            d_mid = (d - d_hi).astype(jnp.bfloat16).astype(f32)
            d_lo = d - d_hi - d_mid
            for p in range(0, 8, 2):
                def pair(x):
                    return jnp.concatenate([x[p:p + 1], x[p + 1:p + 2]], axis=1)
                rowhot = jnp.where(tall == pair(hi), 1.0, 0.0).astype(jnp.bfloat16)
                match = tall == pair(lo)
                colhot = jnp.concatenate([jnp.where(match, pair(x), 0.0).astype(jnp.bfloat16) for x in (d_hi, d_mid, d_lo)], axis=0)
                bins[...] += lax.dot_general(rowhot, colhot, TURN, preferred_element_type=f32)
            return carry

        lax.fori_loop(0, (last - start + 15) // 16, tally, 0)

    blocks = out_ref.shape[0]
    high = LANES // blocks
    total = (bins[:, :LANES] + bins[:, LANES:2 * LANES] + bins[:, 2 * LANES:]) * scale
    flag = jnp.where(good, 0.0, 1.0)
    for b in range(blocks):
        out_ref[b, 0:high, :] = total[b * high:(b + 1) * high]
        out_ref[b, high:, :] = jnp.full((8, LANES), flag, f32)


def walk(lists, src_row, weights, *, blocks, vertices, scale):
    levels = weights.shape[0] + 1
    rows = CAP + WINDOW + 2 * SLOTS
    high = LANES // blocks + 8
    vm = pltpu.VMEM
    return pl.pallas_call(
        functools.partial(walk_kernel, levels=levels, vertices=vertices, scale=scale),
        in_specs=[pl.BlockSpec(memory_space=pltpu.VMEM), pl.BlockSpec(memory_space=pltpu.VMEM), pl.BlockSpec(memory_space=pltpu.SMEM)],
        out_specs=pl.BlockSpec(memory_space=pltpu.VMEM),
        out_shape=jax.ShapeDtypeStruct((blocks, high, LANES), f32),
        scratch_shapes=[
            vm((2, vertices + 8, LANES), f32),
            vm((rows, LANES), f32), vm((rows, LANES), f32), vm((rows, LANES), f32), vm((rows, LANES), f32),
            vm((4, rows, LANES), f32), vm((rows, LANES), jnp.int32),
            vm((2 * SLOTS, 8, LANES), jnp.int32), vm((LANES, 3 * LANES), f32),
            pltpu.SMEM((WINDOW, LANES), jnp.int32), pltpu.SMEM((3, 16), jnp.int32), pltpu.SemaphoreType.DMA,
        ],
        compiler_params=pltpu.CompilerParams(vmem_limit_bytes=48 * 1024 * 1024),
        name="walk",
    )(lists, src_row, weights)


def everyone(src, graph):
    return [(y, g) for y in range(src) for g in range(graph)]


def meet(peers):
    barrier = pltpu.get_barrier_semaphore()
    for y, g in peers:
        pl.semaphore_signal(barrier, inc=1, device_id={"src": y, "graph": g}, device_id_type=MESH)
    pl.semaphore_wait(barrier, len(peers))


def share_kernel(src, graph, x_ref, o_ref, own_sem, send_sem, recv_sem):
    y, g = lax.axis_index("src"), lax.axis_index("graph")
    others = [((y + i) % src, (g + k) % graph) for i, k in everyone(src, graph)][1:]
    meet(others)
    mine = g * src + y
    own = pltpu.make_async_copy(x_ref, o_ref.at[mine], own_sem)
    own.start()
    copies = []
    for n, (py, pg) in enumerate(others):
        copies.append(pltpu.make_async_remote_copy(
            src_ref=x_ref, dst_ref=o_ref.at[mine], send_sem=send_sem.at[n], recv_sem=recv_sem.at[n],
            device_id={"src": py, "graph": pg}, device_id_type=MESH))
        copies[-1].start()
    own.wait()
    for c in copies:
        c.wait()


def share(x, src, graph):
    n = src * graph
    return pl.pallas_call(
        functools.partial(share_kernel, src, graph),
        in_specs=[pl.BlockSpec(memory_space=pltpu.VMEM)],
        out_specs=pl.BlockSpec(memory_space=pltpu.VMEM),
        out_shape=jax.ShapeDtypeStruct((n,) + x.shape, x.dtype),
        scratch_shapes=[pltpu.SemaphoreType.DMA, pltpu.SemaphoreType.DMA((n - 1,)), pltpu.SemaphoreType.DMA((n - 1,))],
        compiler_params=pltpu.CompilerParams(collective_id=0, has_side_effects=True),
        name="share",
    )(x)


def total_kernel(src, graph, x_ref, o_ref, got, own_sem, send_sem, recv_sem):
    y, g = lax.axis_index("src"), lax.axis_index("graph")
    others = [((y + i) % src, (g + k) % graph) for i, k in everyone(src, graph)][1:]
    meet(others)
    mine = g * src + y
    own = pltpu.make_async_copy(x_ref.at[g], got.at[mine], own_sem)
    own.start()
    copies = []
    for n, (py, pg) in enumerate(others):
        copies.append(pltpu.make_async_remote_copy(
            src_ref=x_ref.at[pg], dst_ref=got.at[mine], send_sem=send_sem.at[n], recv_sem=recv_sem.at[n],
            device_id={"src": py, "graph": pg}, device_id_type=MESH))
        copies[-1].start()
    own.wait()
    for c in copies:
        c.wait()
    acc = got[0]
    for n in range(1, src * graph):
        acc = acc + got[n]
    o_ref[...] = acc


def total(x, src, graph):
    n = src * graph
    return pl.pallas_call(
        functools.partial(total_kernel, src, graph),
        in_specs=[pl.BlockSpec(memory_space=pltpu.VMEM)],
        out_specs=pl.BlockSpec(memory_space=pltpu.VMEM),
        out_shape=jax.ShapeDtypeStruct(x.shape[1:], x.dtype),
        scratch_shapes=[pltpu.VMEM((n,) + x.shape[1:], x.dtype), pltpu.SemaphoreType.DMA,
                        pltpu.SemaphoreType.DMA((n - 1,)), pltpu.SemaphoreType.DMA((n - 1,))],
        compiler_params=pltpu.CompilerParams(collective_id=1, has_side_effects=True),
        name="total",
    )(x)


def dense(adj_slab, src_local, level_weight, src, graph):
    slab_rows, vertex_count = adj_slab.shape
    src_count = src_local.shape[0]
    levels = level_weight.shape[0] + 1
    row_start = lax.axis_index("graph") * slab_rows
    vertex_ids = row_start + lax.broadcasted_iota(jnp.int32, (slab_rows, 1), 0)
    first = jnp.where(vertex_ids == src_local[None, :], 1.0, 0.0).astype(f32)

    def forward(carry, unused):
        sigma, seen = carry
        partial = jnp.einsum("uv,us->vs", adj_slab, sigma, preferred_element_type=f32, precision=exact_precision)
        parts = lax.all_to_all(partial.reshape(graph, slab_rows, src_count), "graph", 0, 0)
        sigma = jnp.sum(parts, axis=0) * (1.0 - seen)
        seen = jnp.maximum(seen, jnp.where(sigma > 0, 1.0, 0.0))
        return (sigma, seen), sigma

    _, sigmas = lax.scan(forward, (first, first), None, length=levels)

    def backward(carry, xs):
        delta, acc = carry
        upper, lower, weight = xs
        reached = upper > 0
        ratio = jnp.where(reached, (weight + delta) / jnp.where(reached, upper, 1.0), 0.0)
        gathered = lax.all_to_all(jnp.broadcast_to(ratio[None], (graph,) + ratio.shape), "graph", 0, 0)
        pulled = jnp.einsum("uv,vs->us", adj_slab, gathered.reshape(vertex_count, src_count),
                            preferred_element_type=f32, precision=exact_precision)
        delta = lower * pulled
        return (delta, acc + delta), None

    zero = jnp.zeros_like(first)
    (_, acc), _ = lax.scan(backward, (zero, zero), (sigmas[1:][::-1], sigmas[:-1][::-1], level_weight[::-1]))
    scale = vertex_count / (src_count * src * levels ** 3)
    mine = jnp.sum(acc, axis=1) * scale
    both = lax.all_to_all(jnp.broadcast_to(mine.reshape(1, -1, LANES), (src, slab_rows // LANES, LANES)), "src", 0, 0)
    return jnp.sum(both, axis=0).reshape(slab_rows)


def solution(mesh):
    src, graph = mesh.shape["src"], mesh.shape["graph"]

    def device_program(adj_slab, src_local, level_weight):
        slab_rows, vertex_count = adj_slab.shape
        levels = level_weight.shape[0] + 1
        half = lax.axis_index("src").astype(jnp.int32).reshape(1)
        lists = share(extract(adj_slab, half, slab_rows // src), src, graph)
        mine = lax.dynamic_slice(src_local, (lax.axis_index("graph") * HALF,), (HALF,)).astype(f32)
        scale = vertex_count / (HALF * src * graph * levels ** 3)
        parts = walk(lists, jnp.concatenate([mine, mine])[None], level_weight, blocks=graph, vertices=vertex_count, scale=scale)
        summed = total(parts, src, graph)
        high = slab_rows // LANES
        return lax.cond(summed[high, 0] > 0,
                        lambda: dense(adj_slab, src_local, level_weight, src, graph),
                        lambda: summed[:high].reshape(slab_rows))

    return jax.shard_map(device_program, mesh=mesh,
                         in_specs=(P(("batch", "graph"), None), P(("batch", "src")), P(None)),
                         out_specs=P(("batch", "graph")), check_vma=False)
```

```python
import functools

import jax
import jax.numpy as jnp
from jax import lax
from jax.experimental import pallas as pl
from jax.experimental.pallas import tpu as pltpu
from jax.sharding import PartitionSpec as P

MESH = pl.DeviceIdType.MESH
exact_precision = lax.Precision.HIGHEST
f32 = jnp.float32

LANES = 128
WIDE = 256
DEG = 8
EMPTY = -2.0
FULL = 32767.0
TURN = (((1,), (1,)), ((), ()))
BLOCK = 128
READS = 4
HALF = 64
SLOTS = 8
WINDOW = 48
SCAN = 32
CAP = 1024
SPREAD = 1024


def extract_kernel(half_ref, a_ref, o_ref, bufs, top_ref, low_ref, third_ref, seen_ref, planes, flags, sems, *, group=4, step=16):
    rows, vertices = o_ref.shape[1], a_ref.shape[1]
    blocks, chunks = rows // BLOCK, vertices // WIDE
    first = half_ref[0] * rows
    height = 8 * group

    def fetch(i, slot):
        return pltpu.make_async_copy(a_ref.at[pl.ds(pl.multiple_of(first + i * BLOCK, BLOCK), BLOCK)], bufs.at[slot], sems.at[slot])

    row_i = lax.broadcasted_iota(jnp.int32, (WIDE, WIDE), 0)
    col_i = lax.broadcasted_iota(jnp.int32, (WIDE, WIDE), 1)
    eye = jnp.where(row_i == col_i, float(WIDE), 0.0).astype(jnp.bfloat16)
    ones = jnp.ones((8, WIDE), jnp.bfloat16)
    sub = lax.broadcasted_iota(jnp.int32, (8, BLOCK), 0)
    lane_id = sub.astype(f32)
    none = jnp.zeros((8, BLOCK), f32)

    def place(plane, lists):
        lists = list(lists)
        flipped = lax.dot_general(eye, plane, TURN, preferred_element_type=f32)
        for g in range(WIDE // 8):
            x = flipped[g * 8:(g + 1) * 8] + (lane_id + float(g * 8))
            for s in range(len(lists)):
                hi = jnp.maximum(lists[s], x)
                if s < len(lists) - 1:
                    x = jnp.minimum(lists[s], x)
                lists[s] = hi
        return lists

    def sort(lists):
        gap = len(lists) // 2
        while gap:
            for s in range(len(lists)):
                if not s & gap:
                    lists[s], lists[s + gap] = jnp.maximum(lists[s], lists[s + gap]), jnp.minimum(lists[s], lists[s + gap])
            gap //= 2
        return lists

    def over_sublanes(lists):
        size = len(lists)
        for shift in (4, 2, 1):
            other = [pltpu.roll(v, shift, 0) for v in lists]
            lists = sort([jnp.maximum(lists[s], other[size - 1 - s]) for s in range(size)])
        out = jnp.full((8, BLOCK), EMPTY, f32)
        for s in range(size):
            out = jnp.where(sub == s, jnp.where(lists[s] >= WIDE, lists[s] - WIDE, EMPTY), out)
        return out

    for i in range(READS - 1):
        fetch(i, i).start()

    def block_step(i, carry):
        slot = i % READS

        @pl.when(i + READS - 1 < blocks)
        def _():
            fetch(i + READS - 1, (i + READS - 1) % READS).start()

        fetch(i, slot).wait()

        def scan_rows(t, carry):
            here = pl.ds(pl.multiple_of(t * height, height), height)

            def scan_chunks(g, state):
                top, low, seen, sums, value = state
                for k in range(step):
                    a = bufs[slot, here, pl.ds(pl.multiple_of((g * step + k) * WIDE, WIDE), WIDE)]
                    x = a * value
                    low = jnp.maximum(low, jnp.minimum(top, x))
                    top = jnp.maximum(top, x)
                    seen = seen + a
                    sums = sums + x
                    value = value + 1
                return top, low, seen, sums, value

            zero = jnp.zeros((height, WIDE), jnp.bfloat16)
            top, low, seen, sums, _ = lax.fori_loop(0, chunks // step, scan_chunks, (zero, zero, zero, zero, zero + 1))
            top_ref[here, :] = top
            low_ref[here, :] = low
            third_ref[here, :] = (sums - top) - low
            seen_ref[here, :] = seen
            return carry

        lax.fori_loop(0, BLOCK // height, scan_rows, 0)

        seen = seen_ref[...]
        degree = lax.dot_general(ones, seen, TURN, preferred_element_type=f32)
        crowd = seen[0:8]
        for g in range(1, BLOCK // 8):
            crowd = jnp.maximum(crowd, seen[g * 8:(g + 1) * 8])
        crowd = crowd.astype(f32)
        crowd = jnp.maximum(crowd[:, :LANES], crowd[:, LANES:])
        flags[i] = jnp.where((crowd > 3) | (degree > 4), 1.0, 0.0)
        a = place(top_ref[...], [none] * 4)
        b = place(low_ref[...], [none] * 2)
        c = place(third_ref[...], [none])
        rest = [jnp.maximum(b[0], c[0]), jnp.minimum(b[0], c[0])]
        rest = [rest[0], jnp.maximum(b[1], rest[1]), jnp.minimum(b[1], rest[1])]
        lists = sort([a[0], jnp.maximum(a[1], rest[2]), jnp.maximum(a[2], rest[1]), jnp.maximum(a[3], rest[0])])
        o_ref[:, pl.ds(pl.multiple_of(i * BLOCK, BLOCK), BLOCK)] = over_sublanes(lists)
        return carry

    lax.fori_loop(0, blocks, block_step, 0)

    most = flags[0]
    for i in range(1, blocks):
        most = jnp.maximum(most, flags[i])

    @pl.when(jnp.max(most) > 0)
    def _():
        def again(i, carry):
            @pl.when(jnp.max(flags[i]) > 0)
            def _():
                fetch(i, 0).start()
                fetch(i, 0).wait()
                planes[...] = jnp.zeros_like(planes)
                seen_ref[...] = jnp.zeros_like(seen_ref)

                def scan_chunk(c, carry):
                    a = bufs[0, :, pl.ds(pl.multiple_of(c * WIDE, WIDE), WIDE)]
                    seen_ref[...] = seen_ref[...] + a
                    x = a.astype(f32) * (c + 1).astype(f32)
                    for s in range(DEG):
                        top = planes[s].astype(f32)
                        planes[s] = jnp.maximum(top, x).astype(jnp.bfloat16)
                        x = jnp.minimum(top, x)
                    return carry

                lax.fori_loop(0, chunks, scan_chunk, 0)
                degree = lax.dot_general(ones, seen_ref[...], TURN, preferred_element_type=f32)
                lists = lax.fori_loop(0, DEG, lambda p, lists: tuple(place(planes[p], lists)), (none,) * DEG)
                o_ref[:, pl.ds(pl.multiple_of(i * BLOCK, BLOCK), BLOCK)] = jnp.where(degree > DEG, FULL, over_sublanes(list(lists)))

            return carry

        lax.fori_loop(0, blocks, again, 0)


def extract(adj_slab, half, rows):
    vertices = adj_slab.shape[1]
    tile = pltpu.VMEM((BLOCK, WIDE), jnp.bfloat16)
    return pl.pallas_call(
        extract_kernel,
        in_specs=[pl.BlockSpec(memory_space=pltpu.SMEM), pl.BlockSpec(memory_space=pl.ANY)],
        out_specs=pl.BlockSpec(memory_space=pltpu.VMEM),
        out_shape=jax.ShapeDtypeStruct((DEG, rows), f32),
        scratch_shapes=[pltpu.VMEM((READS, BLOCK, vertices), jnp.bfloat16), tile, tile, tile, tile,
                        pltpu.VMEM((DEG, BLOCK, WIDE), jnp.bfloat16), pltpu.VMEM((rows // BLOCK, 8, BLOCK), f32),
                        pltpu.SemaphoreType.DMA((READS,))],
        compiler_params=pltpu.CompilerParams(vmem_limit_bytes=40 * 1024 * 1024),
        name="extract",
    )(half, adj_slab)


def walk_kernel(lists_ref, src_ref, weight_ref, out_ref,
                table, queue, sigma, ratio, delta, cand, ids, turned, dest, tail_ref, rowhot, colhot, bins,
                ids_a, ids_b, meta, sems, *, levels, vertices, scale):
    parts, _, width = lists_ref.shape
    pitch = vertices + 8
    lane = lax.broadcasted_iota(jnp.int32, (8, LANES), 1)
    sub = lax.broadcasted_iota(jnp.int32, (8, LANES), 0)
    upper = lane >= HALF
    lane_row = lax.broadcasted_iota(jnp.int32, (1, LANES), 1)
    group_odd = ((lane_row // 32) % 2) == 1
    lane32 = lane_row % 32
    rows_all = queue.shape[0]

    def eight(row):
        return pl.ds(pl.multiple_of(row, 8), 8)

    def spread_row(ref, *index):
        return jnp.broadcast_to(ref[(*index[:-1], pl.ds(index[-1], 1), slice(None))], (8, LANES))

    srow = lax.broadcasted_iota(jnp.int32, (2 * DEG, LANES), 0)
    slane = lax.broadcasted_iota(jnp.int32, (2 * DEG, LANES), 1)

    def fill(quad):
        mine = (srow % DEG) == (slane // 32 + 4 * quad)
        pick = jnp.where(mine, jnp.where(srow < DEG, float(LANES), 1.0), 0.0).astype(jnp.bfloat16)
        per = width // SPREAD

        def body(b, most):
            x = lists_ref[b // per, :, pl.ds(pl.multiple_of(b % per * SPREAD, SPREAD), SPREAD)]
            hi = jnp.floor(x * (1.0 / LANES))
            lo = x - hi * LANES
            both = jnp.concatenate([hi, lo], axis=0).astype(jnp.bfloat16)
            table[pl.ds(pl.multiple_of(quad * pitch + b * SPREAD, 8), SPREAD), :] = lax.dot_general(
                both, pick, (((0,), (0,)), ((), ())), preferred_element_type=f32)
            for k in range(SPREAD // LANES):
                most = jnp.maximum(most, x[:, k * LANES:(k + 1) * LANES])
            return most

        most = lax.fori_loop(0, parts * per, body, jnp.full((DEG, LANES), EMPTY, f32))
        table[quad * pitch + vertices:(quad + 1) * pitch, :] = jnp.full((8, LANES), EMPTY, f32)
        return most

    most = fill(0)
    top = jnp.max(most)
    wide = jnp.max(jnp.where(sub >= 4, most, EMPTY)) >= 0
    quads = jnp.where(wide, 2, 1)

    @pl.when(wide)
    def _():
        fill(1)

    bad = top > vertices
    meta[2, 0] = bad.astype(jnp.int32)

    def clear(t, carry):
        rows = eight(t * 8)
        queue[rows, :] = jnp.full((8, LANES), -1.0, f32)
        sigma[rows, :] = jnp.zeros((8, LANES), f32)
        delta[rows, :] = jnp.zeros((8, LANES), f32)
        ids[0, rows, :] = jnp.full((8, LANES), vertices, jnp.int32)
        ids[1, rows, :] = jnp.full((8, LANES), vertices + pitch, jnp.int32)
        return carry

    lax.fori_loop(0, rows_all // 8, clear, 0)
    bins[...] = jnp.zeros_like(bins)

    def fetch(quad, row, to, which):
        return pltpu.make_async_copy(ids.at[quad, eight(row)], to, sems.at[which])

    for to, which in ((ids_a, 0), (ids_b, 1)):
        fetch(0, rows_all - 8, to, which).start()
        fetch(0, rows_all - 8, to, which).wait()

    def gather(ids_s, quad, row):
        acc = [[jnp.full((1, LANES), EMPTY, f32)] * 2 for _ in range(SLOTS)]
        for j in range(32):
            hit = lane32 == j
            for i in range(SLOTS):
                for b in range(2):
                    acc[i][b] = jnp.where(hit, table[pl.ds(ids_s[i, b * 32 + j], 1), :], acc[i][b])
        for i in range(SLOTS):
            a, b = acc[i]
            cand[2 * quad, pl.ds(row + i, 1), :] = jnp.where(group_odd, b, a)
            cand[2 * quad + 1, pl.ds(row + i, 1), :] = pltpu.roll(jnp.where(group_odd, a, b), LANES - 32, 1)

    def flag(x):
        return jnp.where(x, 1, 0)

    def level_step(level, carry):
        base, count = meta[0, level], meta[1, level]
        following = base + (count + 7) // 8 * 8
        batches = jnp.where(following <= CAP, (count + SLOTS - 1) // SLOTS, 0)
        units = batches * quads

        def at(m):
            quad = jnp.where(m >= batches, 1, 0)
            return quad, base + (m - quad * batches) * SLOTS

        def start(m, to, which):
            @pl.when(m < units)
            def _():
                fetch(*at(m), to, which).start()

        def await_(m, to, which):
            @pl.when(m < units)
            def _():
                fetch(*at(m), to, which).wait()

        def unit_step(m, to, which):
            quad, row = at(m)
            x = [cand[2 * quad + h, eight(row), :] for h in range(2)]

            def search(t, marks):
                marks = list(marks)
                for k in range(SCAN):
                    q = spread_row(queue, t * SCAN + k)
                    for h in range(2):
                        n = 2 * h + k % 2
                        marks[n] = jnp.where(x[h] == q, 1, marks[n])
                return tuple(marks)

            reach = following + meta[3, 0]
            marks = lax.fori_loop(0, (reach + SCAN - 1) // SCAN, search, (jnp.zeros((8, LANES), jnp.int32),) * 4)
            await_(m + 1, to, which)
            near = [marks[0] | marks[1] | flag(x[0] < 0), marks[2] | marks[3] | flag(x[1] < 0)]

            xr = [pltpu.roll(v, HALF, 1) for v in x]
            turns = [[(pltpu.roll(x[h], s, 0), pltpu.roll(xr[h], s, 0)) if s else (x[h], xr[h]) for s in range(8)] for h in range(2)]
            for s in range(8):
                a, b = turns[0][s]
                near[1] = jnp.where((x[1] == a) | (x[1] == b), 1, near[1])
                if s:
                    after = sub >= s
                    near[0] = jnp.where(((x[0] == a) | (x[0] == b)) & after, 1, near[0])
                    a, b = turns[1][s]
                    near[1] = jnp.where(((x[1] == a) | (x[1] == b)) & after, 1, near[1])

            new = [1 - near[0], 1 - near[1]]
            other = pltpu.roll(new[0] + 256 * new[1], HALF, 1)
            far = [other & 255, other >> 8]
            both = new[0] + 256 * new[1] + other
            run, whole = both, both
            for s in (1, 2, 4):
                run = run + jnp.where(sub >= s, pltpu.roll(run, s, 0), 0)
                whole = whole + pltpu.roll(whole, s, 0)
            run = run - both
            tail = tail_ref[...]
            begin = [tail + (run & 255), tail + (whole & 255) + (run >> 8)]
            for h in range(2):
                dest[8 * h:8 * h + 8, :] = jnp.where(new[h] > 0, begin[h] + jnp.where(upper, far[h], 0), -1)
                dest[16 + 8 * h:24 + 8 * h, :] = jnp.where(far[h] > 0, begin[h] + jnp.where(upper, 0, new[h]), -1)
                turned[8 * h:8 * h + 8, :] = xr[h]
            tail = tail + (whole & 255) + (whole >> 8)
            tail_ref[...] = tail
            length = jnp.max(tail.astype(f32)).astype(jnp.int32)

            quad2, row2 = at(jnp.minimum(m + 1, units - 1))
            gather(to, quad2, jnp.where(m + 1 < units, row2, rows_all - 8))
            start(m + 3, to, which)

            groups = (length + WINDOW - 1) // WINDOW
            fits = following + groups * WINDOW <= CAP + WINDOW
            meta[3, 0] = jnp.where(fits, length, 0)

            @pl.when(jnp.logical_not(fits))
            def _():
                meta[2, 0] = 1

            def insert(g, carry):
                slots = [eight(following + g * WINDOW + 8 * t) for t in range(WINDOW // 8)]
                qs = [queue[r, :] for r in slots]
                ss = [sigma[r, :] for r in slots]
                pos = [sub + (g * WINDOW + 8 * t) for t in range(WINDOW // 8)]
                for h in range(2):
                    for i in range(8):
                        d, e = spread_row(dest, 8 * h + i), spread_row(dest, 16 + 8 * h + i)
                        v, w = spread_row(cand, 2 * quad + h, row + i), spread_row(turned, 8 * h + i)
                        for t in range(WINDOW // 8):
                            qs[t] = jnp.where(pos[t] == d, v, jnp.where(pos[t] == e, w, qs[t]))
                for t, r in enumerate(slots):
                    queue[r, :] = qs[t]
                for i in range(8):
                    v, w = spread_row(cand, 2 * quad, row + i), spread_row(cand, 2 * quad + 1, row + i)
                    sig = spread_row(sigma, row + i)
                    for t in range(WINDOW // 8):
                        ss[t] = ss[t] + jnp.where((qs[t] == v) | (qs[t] == w), sig, 0.0)
                for t, r in enumerate(slots):
                    sigma[r, :] = ss[t]
                return carry

            lax.fori_loop(0, jnp.where(fits, groups, 0), insert, 0)

        tail_ref[...] = jnp.zeros_like(tail_ref)
        meta[3, 0] = 0
        start(0, ids_a, 0)
        start(1, ids_b, 1)

        @pl.when(units > 0)
        def _():
            fetch(0, base, ids_a, 0).wait()
            gather(ids_a, 0, base)

        start(2, ids_a, 0)

        def pair_step(p, carry):
            unit_step(2 * p, ids_b, 1)

            @pl.when(2 * p + 1 < units)
            def _():
                unit_step(2 * p + 1, ids_a, 0)

            return carry

        lax.fori_loop(0, (units + 1) // 2, pair_step, 0)

        @pl.when(following > CAP)
        def _():
            meta[2, 0] = 1

        found = jnp.where(meta[2, 0] == 0, meta[3, 0], 0)
        meta[0, level + 1] = following
        meta[1, level + 1] = found

        def settle(g, carry):
            slots = [eight(following + g * WINDOW + 8 * t) for t in range(WINDOW // 8)]
            for r in slots:
                q = queue[r, :]
                v = jnp.where(q < 0, vertices, q.astype(jnp.int32))
                ids[0, r, :] = v
                ids[1, r, :] = v + pitch
            for r in slots:
                s = sigma[r, :]
                sigma[r, :] = s + pltpu.roll(s, HALF, 1)
            return carry

        lax.fori_loop(0, (found + WINDOW - 1) // WINDOW, settle, 0)
        return carry

    @pl.when(jnp.logical_not(bad))
    def _():
        queue[0:1, :] = src_ref[...]
        sigma[0:1, :] = jnp.ones((1, LANES), f32)
        first = src_ref[...].astype(jnp.int32)
        ids[0, 0:1, :] = first
        ids[1, 0:1, :] = first + pitch
        meta[0, 0] = 0
        meta[1, 0] = 1
        lax.fori_loop(0, levels, level_step, 0)

    good = meta[2, 0] == 0

    @pl.when(good)
    def _():
        last = meta[0, levels]
        g_last = weight_ref[levels - 2]

        def seed(g, carry):
            for t in range(WINDOW // 8):
                r = eight(last + g * WINDOW + 8 * t)
                s = sigma[r, :]
                ratio[r, :] = jnp.where(s > 0, g_last / jnp.where(s > 0, s, 1.0), 0.0)
            return carry

        lax.fori_loop(0, (meta[1, levels] + WINDOW - 1) // WINDOW, seed, 0)

        def back_step(k, carry):
            level = levels - 1 - k
            base, count = meta[0, level], meta[1, level]
            nbase, ncount = meta[0, level + 1], meta[1, level + 1]
            g_here = weight_ref[jnp.maximum(level - 2, 0)]
            chunks = (ncount + 15) // 16

            def pull_batch(bt, carry):
                here = eight(base + bt * SLOTS)

                def pull_quad(quad, acc):
                    x = [cand[2 * quad + h, here, :] for h in range(2)]

                    def pull(c, acc):
                        acc = list(acc)
                        for n in range(16):
                            q = spread_row(queue, nbase + c * 16 + n)
                            w = spread_row(ratio, nbase + c * 16 + n)
                            acc[n % 2] = acc[n % 2] + jnp.where((x[0] == q) | (x[1] == q), w, 0.0)
                        return tuple(acc)

                    return lax.fori_loop(0, chunks, pull, acc)

                acc = lax.fori_loop(0, quads, pull_quad, (jnp.zeros((8, LANES), f32),) * 2)
                delta[here, :] = acc[0] + acc[1]
                return carry

            lax.fori_loop(0, (count + SLOTS - 1) // SLOTS, pull_batch, 0)

            def finish(g, carry):
                slots = [eight(base + g * WINDOW + 8 * t) for t in range(WINDOW // 8)]
                for t, r in enumerate(slots):
                    inside = g * WINDOW + 8 * t < count
                    part, s = delta[r, :], sigma[r, :]
                    d = s * (part + pltpu.roll(part, HALF, 1))
                    w = jnp.where(s > 0, (g_here + d) / jnp.where(s > 0, s, 1.0), 0.0)
                    delta[r, :] = jnp.where(inside, d, part)
                    ratio[r, :] = jnp.where(inside, w, ratio[r, :])
                return carry

            lax.fori_loop(0, (count + WINDOW - 1) // WINDOW, finish, 0)
            return carry

        lax.fori_loop(0, levels - 1, back_step, 0)

        tall = lax.broadcasted_iota(jnp.int32, (LANES, LANES), 0).astype(f32)
        start = meta[0, 1]

        def tally(t, carry):
            a, b = eight(start + t * 16), eight(start + t * 16 + 8)
            v = jnp.where(upper, queue[b, :], queue[a, :])
            d = jnp.where(upper, delta[b, :], delta[a, :])
            hi = jnp.floor(v * (1.0 / LANES))
            lo = v - hi * LANES
            d_hi = d.astype(jnp.bfloat16).astype(f32)
            d_mid = (d - d_hi).astype(jnp.bfloat16).astype(f32)
            d_lo = d - d_hi - d_mid
            for p in range(8):
                cols = slice(p * LANES, (p + 1) * LANES)
                rowhot[:, cols] = jnp.where(tall == hi[p:p + 1], 1.0, 0.0).astype(jnp.bfloat16)
                match = tall == lo[p:p + 1]
                for n, x in enumerate((d_hi, d_mid, d_lo)):
                    colhot[n * LANES:(n + 1) * LANES, cols] = jnp.where(match, x[p:p + 1], 0.0).astype(jnp.bfloat16)
            bins[...] += lax.dot_general(rowhot[...], colhot[...], TURN, preferred_element_type=f32)
            return carry

        lax.fori_loop(0, (last - start + 15) // 16, tally, 0)

    blocks = out_ref.shape[0]
    high = LANES // blocks
    total = (bins[:, :LANES] + bins[:, LANES:2 * LANES] + bins[:, 2 * LANES:]) * scale
    fault = jnp.where(good, 0.0, 1.0)
    for b in range(blocks):
        out_ref[b, 0:high, :] = total[b * high:(b + 1) * high]
        out_ref[b, high:, :] = jnp.full((8, LANES), fault, f32)


def walk(lists, src_row, weights, *, blocks, vertices, scale):
    levels = weights.shape[0] + 1
    rows = CAP + 4 * WINDOW
    high = LANES // blocks + 8
    vm = pltpu.VMEM
    queue = vm((rows, LANES), f32)
    return pl.pallas_call(
        functools.partial(walk_kernel, levels=levels, vertices=vertices, scale=scale),
        in_specs=[pl.BlockSpec(memory_space=pltpu.VMEM), pl.BlockSpec(memory_space=pltpu.VMEM), pl.BlockSpec(memory_space=pltpu.SMEM)],
        out_specs=pl.BlockSpec(memory_space=pltpu.VMEM),
        out_shape=jax.ShapeDtypeStruct((blocks, high, LANES), f32),
        scratch_shapes=[
            vm((2 * (vertices + 8), LANES), f32), queue, queue, queue, queue,
            vm((4, rows, LANES), f32), vm((2, rows, LANES), jnp.int32),
            vm((16, LANES), f32), vm((32, LANES), jnp.int32), vm((8, LANES), jnp.int32),
            vm((LANES, 8 * LANES), jnp.bfloat16), vm((3 * LANES, 8 * LANES), jnp.bfloat16), vm((LANES, 3 * LANES), f32),
            pltpu.SMEM((SLOTS, LANES), jnp.int32), pltpu.SMEM((SLOTS, LANES), jnp.int32), pltpu.SMEM((4, 16), jnp.int32),
            pltpu.SemaphoreType.DMA((2,)),
        ],
        compiler_params=pltpu.CompilerParams(vmem_limit_bytes=48 * 1024 * 1024),
        name="walk",
    )(lists, src_row, weights)


def everyone(src, graph):
    return [(y, g) for y in range(src) for g in range(graph)]


def meet(peers):
    barrier = pltpu.get_barrier_semaphore()
    for y, g in peers:
        pl.semaphore_signal(barrier, inc=1, device_id={"src": y, "graph": g}, device_id_type=MESH)
    pl.semaphore_wait(barrier, len(peers))


def share_kernel(src, graph, x_ref, o_ref, own_sem, send_sem, recv_sem):
    y, g = lax.axis_index("src"), lax.axis_index("graph")
    others = [((y + i) % src, (g + k) % graph) for i, k in everyone(src, graph)][1:]
    meet(others)
    mine = g * src + y
    own = pltpu.make_async_copy(x_ref, o_ref.at[mine], own_sem)
    own.start()
    copies = []
    for n, (py, pg) in enumerate(others):
        copies.append(pltpu.make_async_remote_copy(
            src_ref=x_ref, dst_ref=o_ref.at[mine], send_sem=send_sem.at[n], recv_sem=recv_sem.at[n],
            device_id={"src": py, "graph": pg}, device_id_type=MESH))
        copies[-1].start()
    own.wait()
    for c in copies:
        c.wait()


def share(x, src, graph):
    n = src * graph
    return pl.pallas_call(
        functools.partial(share_kernel, src, graph),
        in_specs=[pl.BlockSpec(memory_space=pltpu.VMEM)],
        out_specs=pl.BlockSpec(memory_space=pltpu.VMEM),
        out_shape=jax.ShapeDtypeStruct((n,) + x.shape, x.dtype),
        scratch_shapes=[pltpu.SemaphoreType.DMA, pltpu.SemaphoreType.DMA((n - 1,)), pltpu.SemaphoreType.DMA((n - 1,))],
        compiler_params=pltpu.CompilerParams(collective_id=0, has_side_effects=True),
        name="share",
    )(x)


def total_kernel(src, graph, x_ref, o_ref, got, own_sem, send_sem, recv_sem):
    y, g = lax.axis_index("src"), lax.axis_index("graph")
    others = [((y + i) % src, (g + k) % graph) for i, k in everyone(src, graph)][1:]
    meet(others)
    mine = g * src + y
    own = pltpu.make_async_copy(x_ref.at[g], got.at[mine], own_sem)
    own.start()
    copies = []
    for n, (py, pg) in enumerate(others):
        copies.append(pltpu.make_async_remote_copy(
            src_ref=x_ref.at[pg], dst_ref=got.at[mine], send_sem=send_sem.at[n], recv_sem=recv_sem.at[n],
            device_id={"src": py, "graph": pg}, device_id_type=MESH))
        copies[-1].start()
    own.wait()
    for c in copies:
        c.wait()
    acc = got[0]
    for n in range(1, src * graph):
        acc = acc + got[n]
    o_ref[...] = acc


def total(x, src, graph):
    n = src * graph
    return pl.pallas_call(
        functools.partial(total_kernel, src, graph),
        in_specs=[pl.BlockSpec(memory_space=pltpu.VMEM)],
        out_specs=pl.BlockSpec(memory_space=pltpu.VMEM),
        out_shape=jax.ShapeDtypeStruct(x.shape[1:], x.dtype),
        scratch_shapes=[pltpu.VMEM((n,) + x.shape[1:], x.dtype), pltpu.SemaphoreType.DMA,
                        pltpu.SemaphoreType.DMA((n - 1,)), pltpu.SemaphoreType.DMA((n - 1,))],
        compiler_params=pltpu.CompilerParams(collective_id=1, has_side_effects=True),
        name="total",
    )(x)


def dense(adj_slab, src_local, level_weight, src, graph):
    slab_rows, vertex_count = adj_slab.shape
    src_count = src_local.shape[0]
    levels = level_weight.shape[0] + 1
    row_start = lax.axis_index("graph") * slab_rows
    vertex_ids = row_start + lax.broadcasted_iota(jnp.int32, (slab_rows, 1), 0)
    first = jnp.where(vertex_ids == src_local[None, :], 1.0, 0.0).astype(f32)

    def forward(carry, unused):
        sigma, seen = carry
        partial = jnp.einsum("uv,us->vs", adj_slab, sigma, preferred_element_type=f32, precision=exact_precision)
        parts = lax.all_to_all(partial.reshape(graph, slab_rows, src_count), "graph", 0, 0)
        sigma = jnp.sum(parts, axis=0) * (1.0 - seen)
        seen = jnp.maximum(seen, jnp.where(sigma > 0, 1.0, 0.0))
        return (sigma, seen), sigma

    _, sigmas = lax.scan(forward, (first, first), None, length=levels)

    def backward(carry, xs):
        delta, acc = carry
        upper, lower, weight = xs
        reached = upper > 0
        ratio = jnp.where(reached, (weight + delta) / jnp.where(reached, upper, 1.0), 0.0)
        gathered = lax.all_to_all(jnp.broadcast_to(ratio[None], (graph,) + ratio.shape), "graph", 0, 0)
        pulled = jnp.einsum("uv,vs->us", adj_slab, gathered.reshape(vertex_count, src_count),
                            preferred_element_type=f32, precision=exact_precision)
        delta = lower * pulled
        return (delta, acc + delta), None

    zero = jnp.zeros_like(first)
    (_, acc), _ = lax.scan(backward, (zero, zero), (sigmas[1:][::-1], sigmas[:-1][::-1], level_weight[::-1]))
    scale = vertex_count / (src_count * src * levels ** 3)
    mine = jnp.sum(acc, axis=1) * scale
    both = lax.all_to_all(jnp.broadcast_to(mine.reshape(1, -1, LANES), (src, slab_rows // LANES, LANES)), "src", 0, 0)
    return jnp.sum(both, axis=0).reshape(slab_rows)


def solution(mesh):
    src, graph = mesh.shape["src"], mesh.shape["graph"]

    def device_program(adj_slab, src_local, level_weight):
        slab_rows, vertex_count = adj_slab.shape
        levels = level_weight.shape[0] + 1
        half = lax.axis_index("src").astype(jnp.int32).reshape(1)
        lists = share(extract(adj_slab, half, slab_rows // src), src, graph)
        mine = lax.dynamic_slice(src_local, (lax.axis_index("graph") * HALF,), (HALF,)).astype(f32)
        scale = vertex_count / (HALF * src * graph * levels ** 3)
        parts = walk(lists, jnp.concatenate([mine, mine])[None], level_weight, blocks=graph, vertices=vertex_count, scale=scale)
        summed = total(parts, src, graph)
        high = slab_rows // LANES
        return lax.cond(summed[high, 0] > 0,
                        lambda: dense(adj_slab, src_local, level_weight, src, graph),
                        lambda: summed[:high].reshape(slab_rows))

    return jax.shard_map(device_program, mesh=mesh,
                         in_specs=(P(("batch", "graph"), None), P(("batch", "src")), P(None)),
                         out_specs=P(("batch", "graph")), check_vma=False)
```

```python
import functools

import jax
import jax.numpy as jnp
from jax import lax
from jax.experimental import pallas as pl
from jax.experimental.pallas import tpu as pltpu
from jax.sharding import PartitionSpec as P

MESH = pl.DeviceIdType.MESH
exact_precision = lax.Precision.HIGHEST
f32, bf16 = jnp.float32, jnp.bfloat16

LANES, SUB = 128, 8
WIDE = 256
DEG, FEW = 8, 4
EMPTY = -2.0
FULL = 32767.0
TURN = (((1,), (1,)), ((), ()))
BLOCK = 128
READS = 4
STEP = 16
HALF = 64
SLOTS = 8
WINDOW = 48
SCAN = 32
CAP = 1024
TALLY = 64
PAIR = (0, 1)
BYTE = 256
BASE, COUNT, FAULT, LENGTH, EARLY = 0, 1, (2, 0), (3, 0), (3, 1)


def everyone(src, graph):
    return [(y, g) for y in range(src) for g in range(graph)]


def hello(peers):
    for y, g in peers:
        pl.semaphore_signal(pltpu.get_barrier_semaphore(), inc=1, device_id={"src": y, "graph": g}, device_id_type=MESH)


def await_hello(peers):
    pl.semaphore_wait(pltpu.get_barrier_semaphore(), len(peers))


def sublane():
    return lax.broadcasted_iota(jnp.int32, (SUB, BLOCK), 0)


def place(plane, lists):
    lists = list(lists)
    row_i = lax.broadcasted_iota(jnp.int32, (WIDE, WIDE), 0)
    col_i = lax.broadcasted_iota(jnp.int32, (WIDE, WIDE), 1)
    eye = jnp.where(row_i == col_i, float(WIDE), 0.0).astype(bf16)
    flipped = lax.dot_general(eye, plane, TURN, preferred_element_type=f32)
    lane_id = sublane().astype(f32)
    for g in range(WIDE // SUB):
        x = flipped[g * SUB:(g + 1) * SUB] + (lane_id + float(g * SUB))
        for s in range(len(lists)):
            hi = jnp.maximum(lists[s], x)
            if s < len(lists) - 1:
                x = jnp.minimum(lists[s], x)
            lists[s] = hi
    return lists


def sort(lists):
    gap = len(lists) // 2
    while gap:
        for s in range(len(lists)):
            if not s & gap:
                lists[s], lists[s + gap] = jnp.maximum(lists[s], lists[s + gap]), jnp.minimum(lists[s], lists[s + gap])
        gap //= 2
    return lists


def over_sublanes(lists):
    size = len(lists)
    for shift in (4, 2, 1):
        other = [pltpu.roll(v, shift, 0) for v in lists]
        lists = sort([jnp.maximum(lists[s], other[size - 1 - s]) for s in range(size)])
    out = jnp.full((SUB, BLOCK), EMPTY, f32)
    for s in range(size):
        out = jnp.where(sublane() == s, jnp.where(lists[s] >= WIDE, lists[s] - WIDE, EMPTY), out)
    return out


def degree_of(seen):
    return lax.dot_general(jnp.ones((SUB, WIDE), bf16), seen, TURN, preferred_element_type=f32)


def collect_kernel(src, graph, a_ref, o_ref, bufs, tops, mine, sems, own_sem, send_sems, recv_sems):
    vertices = a_ref.shape[1]
    pairs, chunks = mine.shape[1] // LANES, vertices // WIDE
    blocks = 2 * pairs
    y, g = lax.axis_index("src"), lax.axis_index("graph")
    others = [((y + i) % src, (g + k) % graph) for i, k in everyone(src, graph)][1:]
    me = g * src + y
    height = 4 * SUB

    def fetch(i):
        rows = pl.ds(pl.multiple_of((y * blocks + i) * BLOCK, BLOCK), BLOCK)
        return pltpu.make_async_copy(a_ref.at[rows], bufs.at[i % READS], sems.at[i % READS])

    def send(n, cols):
        py, pg = others[n]
        return pltpu.make_async_remote_copy(
            src_ref=mine.at[:, cols], dst_ref=o_ref.at[me, :, cols], send_sem=send_sems.at[n], recv_sem=recv_sems.at[n],
            device_id={"src": py, "graph": pg}, device_id_type=MESH)

    def send_pair(p):
        for n in range(len(others)):
            send(n, pl.ds(pl.multiple_of(p * LANES, LANES), LANES)).start()

    hello(others)
    for i in range(READS - 1):
        fetch(i).start()
    none = jnp.zeros((SUB, BLOCK), f32)

    def block_lists(i):
        @pl.when(i + READS - 1 < blocks)
        def _():
            fetch(i + READS - 1).start()

        fetch(i).wait()

        def scan_rows(t, carry):
            here = pl.ds(pl.multiple_of(t * height, height), height)

            def scan_chunks(c, state):
                top, low, seen, sums, value = state
                for k in range(STEP):
                    a = bufs[i % READS, here, pl.ds(pl.multiple_of((c * STEP + k) * WIDE, WIDE), WIDE)]
                    x = a * value
                    low = jnp.maximum(low, jnp.minimum(top, x))
                    top = jnp.maximum(top, x)
                    seen = seen + a
                    sums = sums + x
                    value = value + 1
                return top, low, seen, sums, value

            zero = jnp.zeros((height, WIDE), bf16)
            top, low, seen, sums, _ = lax.fori_loop(0, chunks // STEP, scan_chunks, (zero,) * 4 + (zero + 1,))
            for n, v in enumerate((top, low, (sums - top) - low, seen)):
                tops[n, here, :] = v
            return carry

        lax.fori_loop(0, BLOCK // height, scan_rows, 0)
        seen = tops[3]
        crowd = seen[:SUB]
        for k in range(1, BLOCK // SUB):
            crowd = jnp.maximum(crowd, seen[k * SUB:(k + 1) * SUB])
        crowd = crowd.astype(f32)
        crowd = jnp.maximum(crowd[:, :LANES], crowd[:, LANES:])
        crowd = jnp.max(crowd, axis=0, keepdims=True)
        a, b, c = place(tops[0], (none,) * 4), place(tops[1], (none,) * 2), place(tops[2], (none,))
        rest = [jnp.maximum(b[0], c[0]), jnp.minimum(b[0], c[0])]
        rest = [rest[0], jnp.maximum(b[1], rest[1]), jnp.minimum(b[1], rest[1])]
        lists = sort([a[0]] + [jnp.maximum(a[s + 1], rest[2 - s]) for s in range(3)])
        return jnp.where((crowd > 3) | (degree_of(seen) > 4), FULL, over_sublanes(lists))

    def pair_step(p, carry):
        even = block_lists(2 * p)
        odd = block_lists(2 * p + 1)
        mine[:, pl.ds(pl.multiple_of(p * LANES, LANES), LANES)] = jnp.where(sublane() < 4, even, pltpu.roll(odd, 4, 0))

        @pl.when(p == 1)
        def _():
            await_hello(others)

        @pl.when(p > 0)
        def _():
            send_pair(p - 1)

        return carry

    lax.fori_loop(0, pairs, pair_step, 0)
    own = pltpu.make_async_copy(mine, o_ref.at[me], own_sem)
    send_pair(pairs - 1)
    own.start()
    own.wait()
    for n in range(len(others)):
        send(n, slice(None)).wait()


def collect(adj_slab, src, graph):
    rows, vertices = adj_slab.shape
    n = src * graph
    mine = (SUB, rows // src // 2)
    return pl.pallas_call(
        functools.partial(collect_kernel, src, graph),
        in_specs=[pl.BlockSpec(memory_space=pl.ANY)],
        out_specs=pl.BlockSpec(memory_space=pltpu.VMEM),
        out_shape=jax.ShapeDtypeStruct((n,) + mine, f32),
        scratch_shapes=[pltpu.VMEM((READS, BLOCK, vertices), bf16), pltpu.VMEM((4, BLOCK, WIDE), bf16), pltpu.VMEM(mine, f32),
                        pltpu.SemaphoreType.DMA((READS,)), pltpu.SemaphoreType.DMA,
                        pltpu.SemaphoreType.DMA((n - 1,)), pltpu.SemaphoreType.DMA((n - 1,))],
        compiler_params=pltpu.CompilerParams(collective_id=0, has_side_effects=True, vmem_limit_bytes=40 * 1024 * 1024),
        name="collect",
    )(adj_slab)


def extract_kernel(half_ref, a_ref, o_ref, block, seen, planes, sem):
    vertices = a_ref.shape[1]

    def block_step(i, carry):
        copy = pltpu.make_async_copy(
            a_ref.at[pl.ds(pl.multiple_of(half_ref[0] * o_ref.shape[1] + i * BLOCK, BLOCK), BLOCK)], block, sem)
        copy.start()
        copy.wait()
        planes[...] = jnp.zeros_like(planes)
        seen[...] = jnp.zeros_like(seen)

        def scan_chunk(c, carry):
            a = block[:, pl.ds(pl.multiple_of(c * WIDE, WIDE), WIDE)]
            seen[...] = seen[...] + a
            x = a.astype(f32) * (c + 1).astype(f32)
            for s in range(DEG):
                top = planes[s].astype(f32)
                planes[s] = jnp.maximum(top, x).astype(bf16)
                x = jnp.minimum(top, x)
            return carry

        lax.fori_loop(0, vertices // WIDE, scan_chunk, 0)
        lists = lax.fori_loop(0, DEG, lambda p, lists: tuple(place(planes[p], lists)), (jnp.zeros((SUB, BLOCK), f32),) * DEG)
        o_ref[:, pl.ds(pl.multiple_of(i * BLOCK, BLOCK), BLOCK)] = jnp.where(
            degree_of(seen[...]) > DEG, FULL, over_sublanes(list(lists)))
        return carry

    lax.fori_loop(0, o_ref.shape[1] // BLOCK, block_step, 0)


def extract(adj_slab, half, rows):
    vertices = adj_slab.shape[1]
    return pl.pallas_call(
        extract_kernel,
        in_specs=[pl.BlockSpec(memory_space=pltpu.SMEM), pl.BlockSpec(memory_space=pl.ANY)],
        out_specs=pl.BlockSpec(memory_space=pltpu.VMEM),
        out_shape=jax.ShapeDtypeStruct((DEG, rows), f32),
        scratch_shapes=[pltpu.VMEM((BLOCK, vertices), bf16), pltpu.VMEM((BLOCK, WIDE), bf16),
                        pltpu.VMEM((DEG, BLOCK, WIDE), bf16), pltpu.SemaphoreType.DMA],
        name="extract",
    )(half, adj_slab)


def walk_kernel(which_ref, src_ref, weight_ref, lists_ref, out_ref,
                table, queue, sigma, ratio, delta, cand, ids, now, dest, tail_ref, held, rowhot, colhot, bins,
                ids_a, ids_b, meta, sems, *, levels, vertices, scale, compact):
    parts, _, width = lists_ref.shape
    pitch = vertices + SUB
    lane = lax.broadcasted_iota(jnp.int32, (SUB, LANES), 1)
    sub = lax.broadcasted_iota(jnp.int32, (SUB, LANES), 0)
    upper = lane >= HALF
    lane_row = lax.broadcasted_iota(jnp.int32, (1, LANES), 1)
    group_odd = ((lane_row // 32) % 2) == 1
    lane32 = lane_row % 32
    rows_all = queue.shape[0]
    high = vertices // WIDE

    def eight(row):
        return pl.ds(pl.multiple_of(row, SUB), SUB)

    def spread_row(ref, *index):
        return jnp.broadcast_to(ref[(*index[:-1], pl.ds(index[-1], 1), slice(None))], (SUB, LANES))

    def clear(t, carry):
        rows = eight(t * SUB)
        queue[rows, :] = jnp.full((SUB, LANES), -1.0, f32)
        sigma[rows, :] = jnp.zeros((SUB, LANES), f32)
        delta[rows, :] = jnp.zeros((SUB, LANES), f32)
        ids[0, rows, :] = jnp.full((SUB, LANES), vertices, jnp.int32)
        ids[1, rows, :] = jnp.full((SUB, LANES), vertices + pitch, jnp.int32)
        return carry

    lax.fori_loop(0, rows_all // SUB, clear, 0)
    bins[...] = jnp.zeros_like(bins)

    srow = lax.broadcasted_iota(jnp.int32, (2 * SUB, LANES), 0)
    slane = lax.broadcasted_iota(jnp.int32, (2 * SUB, LANES), 1)

    def fill(halves, target):
        picks = [jnp.where((srow % SUB) == (slane // 32 + FEW * h), jnp.where(srow < SUB, float(LANES), 1.0), 0.0).astype(bf16)
                 for h in halves]

        def body(b, most):
            x = lists_ref[b]
            hi = jnp.floor(x * (1.0 / LANES))
            lo = x - hi * LANES
            both = jnp.concatenate([hi, lo], axis=0).astype(bf16)
            for h, pick in zip(halves, picks):
                rows = lax.dot_general(both, pick, (((0,), (0,)), ((), ())), preferred_element_type=f32)
                for k in range(width // LANES):
                    table[pl.ds(pl.multiple_of(target(h, b, k * LANES), SUB), LANES), :] = rows[k * LANES:(k + 1) * LANES]
            for k in range(width // LANES):
                most = jnp.maximum(most, x[:, k * LANES:(k + 1) * LANES])
            return most

        return lax.fori_loop(0, parts, body, jnp.full((SUB, LANES), EMPTY, f32))

    table[vertices:pitch, :] = jnp.full((SUB, LANES), EMPTY, f32)
    if compact:
        most = fill((0, 1), lambda h, b, col: (b * width + col) * 2 + h * LANES)
        quads = 1
    else:
        table[pitch + vertices:, :] = jnp.full((SUB, LANES), EMPTY, f32)
        most = fill((0,), lambda h, b, col: b * width + col)
        wide = jnp.max(jnp.where(sub >= FEW, most, EMPTY)) >= 0
        quads = jnp.where(wide, 2, 1)

        @pl.when(wide)
        def _():
            fill((1,), lambda h, b, col: pitch + b * width + col)

    bad = jnp.max(most) > vertices
    meta[FAULT] = bad.astype(jnp.int32)

    def fetch(quad, row, to, which):
        return pltpu.make_async_copy(ids.at[quad, eight(row)], to, sems.at[which])

    for to, which in ((ids_a, 0), (ids_b, 1)):
        fetch(0, rows_all - SUB, to, which).start()
        fetch(0, rows_all - SUB, to, which).wait()

    def gather(ids_s):
        acc = [[jnp.full((1, LANES), EMPTY, f32)] * 2 for _ in range(SLOTS)]
        for j in range(32):
            hit = lane32 == j
            for i in range(SLOTS):
                for b in PAIR:
                    acc[i][b] = jnp.where(hit, table[pl.ds(ids_s[i, b * 32 + j], 1), :], acc[i][b])
        return [(jnp.where(group_odd, b, a), pltpu.roll(jnp.where(group_odd, a, b), LANES - 32, 1)) for a, b in acc]

    def keep(rows, quad, row):
        for i, pair in enumerate(rows):
            for h in PAIR:
                cand[2 * quad + h, pl.ds(row + i, 1), :] = pair[h]

    def name(row, q):
        v = jnp.where(q < 0, vertices, q.astype(jnp.int32))
        ids[0, eight(row), :] = v
        ids[1, eight(row), :] = v + pitch

    def flag(x):
        return jnp.where(x, 1, 0)

    def level_step(level, carry):
        base, count = meta[BASE, level], meta[COUNT, level]
        following = base + (count + 7) // SUB * SUB
        batches = jnp.where(following <= CAP, (count + SLOTS - 1) // SLOTS, 0)
        units = batches * quads

        def at(m):
            quad = jnp.where(m >= batches, 1, 0)
            return quad, base + (m - quad * batches) * SLOTS

        def start(m, to, which):
            @pl.when(m < units)
            def _():
                fetch(*at(m), to, which).start()

        def unit_step(unit, to, which, other, other_which):
            quad, row = at(unit)
            x = [cand[2 * quad + h, eight(row), :] for h in PAIR]

            def search(t, marks):
                marks = list(marks)
                for k in range(SCAN):
                    q = spread_row(queue, t * SCAN + k)
                    for h in PAIR:
                        n = 2 * h + k % 2
                        marks[n] = jnp.where(x[h] == q, 1, marks[n])
                return tuple(marks)

            reach = following + meta[LENGTH]
            marks = lax.fori_loop(0, (reach + SCAN - 1) // SCAN, search, (jnp.zeros((SUB, LANES), jnp.int32),) * 4)
            ahead = unit + 1 < units
            soon = jnp.logical_and(unit + 1 == units, meta[EARLY] > 0)

            @pl.when(jnp.logical_or(ahead, soon))
            def _():
                fetch(0, base, to, which).wait()

            even, odd = x
            m, n, k, l = marks
            near_even, near_odd = m | n | flag(even < 0), k | l | flag(odd < 0)

            xr = [pltpu.roll(v, HALF, 1) for v in x]
            turns = [[[pltpu.roll(v, s, 0) if s else v for v in (x[h], xr[h])] for s in range(SUB)] for h in PAIR]
            for s, ((a, b), (c, d)) in enumerate(zip(*turns)):
                near_odd = jnp.where((odd == a) | (odd == b), 1, near_odd)
                if s:
                    after = sub >= s
                    near_even = jnp.where(((even == a) | (even == b)) & after, 1, near_even)
                    near_odd = jnp.where(((odd == c) | (odd == d)) & after, 1, near_odd)

            new = [1 - near_even, 1 - near_odd]
            packed = new[0] + BYTE * new[1]
            across = pltpu.roll(packed, HALF, 1)
            far = [across & (BYTE - 1), across >> SUB]
            both = packed + across
            run, whole = both, both
            for s in (1, 2, 4):
                run = run + jnp.where(sub >= s, pltpu.roll(run, s, 0), 0)
                whole = whole + pltpu.roll(whole, s, 0)
            run = run - both
            tail = tail_ref[...]
            evens = whole & (BYTE - 1)
            begin = [tail + (run & (BYTE - 1)), tail + evens + (run >> SUB)]
            for h in PAIR:
                dest[SUB * h:SUB * h + SUB, :] = jnp.where(new[h] > 0, begin[h] + jnp.where(upper, far[h], 0), -1)
                dest[16 + SUB * h:24 + SUB * h, :] = jnp.where(far[h] > 0, begin[h] + jnp.where(upper, 0, new[h]), -1)
                now[SUB * h:SUB * h + SUB, :] = x[h]
                now[16 + SUB * h:24 + SUB * h, :] = xr[h]
            now[32:40, :] = sigma[eight(row), :]
            tail = tail + evens + (whole >> SUB)
            tail_ref[...] = tail
            passed = SLOTS * (unit + 1 - (quads - 1) * batches)
            open_ = (tail < SLOTS) & (held[...] > passed)
            most = jnp.max(jnp.where(sub == 0, tail, flag(open_)).astype(f32), axis=1, keepdims=True)
            length = most[0, 0].astype(jnp.int32)
            ready = most[1, 0] == 0

            def insert(g):
                slots = [eight(following + g * WINDOW + SUB * t) for t in range(WINDOW // SUB)]
                qs = [queue[r, :] for r in slots]
                ss = [sigma[r, :] for r in slots]
                pos = [sub + (g * WINDOW + SUB * t) for t in range(WINDOW // SUB)]
                for h in PAIR:
                    for i in range(SUB):
                        d, e = spread_row(dest, SUB * h + i), spread_row(dest, 16 + SUB * h + i)
                        v, w = spread_row(now, SUB * h + i), spread_row(now, 16 + SUB * h + i)
                        for t in range(WINDOW // SUB):
                            qs[t] = jnp.where(pos[t] == d, v, jnp.where(pos[t] == e, w, qs[t]))
                for i in range(SUB):
                    v, w, sig = spread_row(now, i), spread_row(now, SUB + i), spread_row(now, 32 + i)
                    for t in range(WINDOW // SUB):
                        ss[t] = ss[t] + jnp.where((qs[t] == v) | (qs[t] == w), sig, 0.0)
                for t, r in enumerate(slots):
                    queue[r, :] = qs[t]
                    sigma[r, :] = ss[t]
                return qs[0]

            quad2, row2 = at(jnp.minimum(unit + 1, units - 1))
            rows = gather(to)
            name(following, insert(0))
            keep(rows, jnp.where(ahead, quad2, 0), jnp.where(ahead, row2, jnp.where(soon, following, rows_all - SUB)))
            start(unit + 3, to, which)
            early = jnp.logical_and(ready, meta[EARLY] == 0)

            @pl.when(jnp.logical_and(early, unit + 3 == units))
            def _():
                fetch(0, following, to, which).start()
                meta[EARLY] = 1

            @pl.when(jnp.logical_and(early, unit + 2 == units))
            def _():
                fetch(0, following, other, other_which).start()
                meta[EARLY] = 1

            groups = (length + WINDOW - 1) // WINDOW
            fits = following + groups * WINDOW <= CAP + WINDOW
            meta[LENGTH] = jnp.where(fits, length, 0)

            @pl.when(jnp.logical_not(fits))
            def _():
                meta[FAULT] = 1

            def more(g, carry):
                insert(g)
                return carry

            lax.fori_loop(1, jnp.where(fits, groups, 0), more, 0)

        cold = jnp.logical_and(units > 0, meta[EARLY] == 0)

        @pl.when(cold)
        def _():
            fetch(0, base, ids_a, 0).start()

        tail_ref[...] = jnp.zeros_like(tail_ref)
        meta[LENGTH] = 0
        meta[EARLY] = 0
        start(1, ids_b, 1)

        @pl.when(cold)
        def _():
            fetch(0, base, ids_a, 0).wait()
            keep(gather(ids_a), 0, base)

        start(2, ids_a, 0)

        def pair_step(p, carry):
            unit_step(2 * p, ids_b, 1, ids_a, 0)

            @pl.when(2 * p + 1 < units)
            def _():
                unit_step(2 * p + 1, ids_a, 0, ids_b, 1)

            return carry

        lax.fori_loop(0, (units + 1) // 2, pair_step, 0)

        @pl.when(following > CAP)
        def _():
            meta[FAULT] = 1

        found = jnp.where(meta[FAULT] == 0, meta[LENGTH], 0)
        meta[BASE, level + 1] = following
        meta[COUNT, level + 1] = found

        def settle(g, carry):
            slots = [eight(following + g * WINDOW + SUB * t) for t in range(WINDOW // SUB)]
            for r in slots:
                name(r.start, queue[r, :])
            for r in slots:
                s = sigma[r, :]
                sigma[r, :] = s + pltpu.roll(s, HALF, 1)
            return carry

        lax.fori_loop(0, (found + WINDOW - 1) // WINDOW, settle, 0)
        held[...] = tail_ref[...]
        return carry

    @pl.when(jnp.logical_not(bad))
    def _():
        first = jnp.zeros((1, LANES), jnp.int32)
        for j in range(HALF):
            first = jnp.where(lane_row % HALF == j, src_ref[which_ref[0] * HALF + j], first)
        queue[0:1, :] = first.astype(f32)
        sigma[0:1, :] = jnp.ones((1, LANES), f32)
        name(0, queue[0:SUB, :])
        held[...] = jnp.ones_like(held)
        meta[BASE, 0] = 0
        meta[COUNT, 0] = 1
        meta[EARLY] = 0
        lax.fori_loop(0, levels, level_step, 0)

    good = meta[FAULT] == 0

    @pl.when(good)
    def _():
        last = meta[BASE, levels]
        g_last = weight_ref[levels - 2]

        def seed(g, carry):
            for t in range(WINDOW // SUB):
                r = eight(last + g * WINDOW + SUB * t)
                s = sigma[r, :]
                ratio[r, :] = jnp.where(s > 0, g_last / jnp.where(s > 0, s, 1.0), 0.0)
            return carry

        lax.fori_loop(0, (meta[COUNT, levels] + WINDOW - 1) // WINDOW, seed, 0)

        def back_step(k, carry):
            level = levels - 1 - k
            base, count = meta[BASE, level], meta[COUNT, level]
            nbase, ncount = meta[BASE, level + 1], meta[COUNT, level + 1]
            g_here = weight_ref[jnp.maximum(level - 2, 0)]
            chunks = (ncount + 15) // 16

            def pull_batch(bt, carry):
                here = eight(base + bt * SLOTS)

                def pull_quad(quad, acc):
                    x = [cand[2 * quad + h, here, :] for h in PAIR]

                    def pull(c, acc):
                        acc = list(acc)
                        for n in range(16):
                            q = spread_row(queue, nbase + c * 16 + n)
                            w = spread_row(ratio, nbase + c * 16 + n)
                            acc[n % 2] = acc[n % 2] + jnp.where((x[0] == q) | (x[1] == q), w, 0.0)
                        return tuple(acc)

                    return lax.fori_loop(0, chunks, pull, acc)

                acc = lax.fori_loop(0, quads, pull_quad, (jnp.zeros((SUB, LANES), f32),) * 2)
                delta[here, :] = acc[0] + acc[1]
                return carry

            lax.fori_loop(0, (count + SLOTS - 1) // SLOTS, pull_batch, 0)

            def finish(g, carry):
                slots = [eight(base + g * WINDOW + SUB * t) for t in range(WINDOW // SUB)]
                for t, r in enumerate(slots):
                    inside = g * WINDOW + SUB * t < count
                    part, s = delta[r, :], sigma[r, :]
                    d = s * (part + pltpu.roll(part, HALF, 1))
                    w = jnp.where(s > 0, (g_here + d) / jnp.where(s > 0, s, 1.0), 0.0)
                    delta[r, :] = jnp.where(inside, d, part)
                    ratio[r, :] = jnp.where(inside, w, ratio[r, :])
                return carry

            lax.fori_loop(0, (count + WINDOW - 1) // WINDOW, finish, 0)
            return carry

        lax.fori_loop(0, levels - 1, back_step, 0)

        tall = lax.broadcasted_iota(jnp.int32, (WIDE, WIDE), 0).astype(f32).astype(bf16)
        zero = jnp.zeros((WIDE, WIDE), bf16)
        one = zero + 1
        start = meta[BASE, 1]

        def tally(t, carry):
            for u in range(TALLY // 16):
                a, b = eight(start + t * TALLY + u * 16), eight(start + t * TALLY + u * 16 + SUB)
                v = jnp.where(upper, queue[b, :], queue[a, :])
                d = jnp.where(upper, delta[b, :], delta[a, :])
                hi = jnp.floor(v * (1.0 / WIDE))
                lo = v - hi * WIDE
                d_hi = d.astype(bf16).astype(f32)
                d_mid = (d - d_hi).astype(bf16).astype(f32)
                d_lo = d - d_hi - d_mid
                for p in range(0, SUB, 2):
                    cols = slice((u * SUB + p) * LANES, (u * SUB + p + 2) * LANES)

                    def pair(x):
                        return jnp.concatenate([x[p:p + 1], x[p + 1:p + 2]], axis=1).astype(bf16)

                    colhot[:, cols] = jnp.where(tall == pair(lo), one, zero)
                    match = tall[:high] == pair(hi)
                    for n, x in enumerate((d_hi, d_mid, d_lo)):
                        rowhot[n * high:(n + 1) * high, cols] = jnp.where(match, pair(x), zero[:high])
            bins[...] += lax.dot_general(rowhot[...], colhot[...], TURN, preferred_element_type=f32)
            return carry

        lax.fori_loop(0, (last - start + TALLY - 1) // TALLY, tally, 0)

    blocks = out_ref.shape[0]
    per = high // blocks
    total = (bins[:high] + bins[high:2 * high] + bins[2 * high:]) * scale
    fault = jnp.where(good, 0.0, 1.0)
    for b in range(blocks):
        for n in PAIR:
            out_ref[b, n * per:(n + 1) * per, :] = total[b * per:(b + 1) * per, n * LANES:(n + 1) * LANES]
        out_ref[b, 2 * per:, :] = jnp.full((SUB, LANES), fault, f32)


def walk(which, sources, weights, lists, *, blocks, vertices, scale, compact):
    levels = weights.shape[0] + 1
    rows = CAP + 4 * WINDOW
    high = LANES // blocks + SUB
    vm = pltpu.VMEM
    queue = vm((rows, LANES), f32)
    parts = 3 * (vertices // WIDE)
    return pl.pallas_call(
        functools.partial(walk_kernel, levels=levels, vertices=vertices, scale=scale, compact=compact),
        in_specs=[pl.BlockSpec(memory_space=pltpu.SMEM)] * 3 + [pl.BlockSpec(memory_space=pltpu.VMEM)],
        out_specs=pl.BlockSpec(memory_space=pltpu.VMEM),
        out_shape=jax.ShapeDtypeStruct((blocks, high, LANES), f32),
        scratch_shapes=[
            vm(((1 if compact else 2) * (vertices + SUB), LANES), f32), queue, queue, queue, queue,
            vm((4, rows, LANES), f32), vm((2, rows, LANES), jnp.int32),
            vm((40, LANES), f32), vm((32, LANES), jnp.int32), vm((SUB, LANES), jnp.int32), vm((SUB, LANES), jnp.int32),
            vm((parts, TALLY // 2 * LANES), bf16), vm((WIDE, TALLY // 2 * LANES), bf16), vm((parts, WIDE), f32),
            pltpu.SMEM((SLOTS, LANES), jnp.int32), pltpu.SMEM((SLOTS, LANES), jnp.int32), pltpu.SMEM((4, 16), jnp.int32),
            pltpu.SemaphoreType.DMA((2,)),
        ],
        compiler_params=pltpu.CompilerParams(
            vmem_limit_bytes=48 * 1024 * 1024),
        name="walk",
    )(which, sources, weights, lists)


def share_kernel(src, graph, x_ref, o_ref, own_sem, send_sem, recv_sem):
    y, g = lax.axis_index("src"), lax.axis_index("graph")
    others = [((y + i) % src, (g + k) % graph) for i, k in everyone(src, graph)][1:]
    hello(others)
    await_hello(others)
    mine = g * src + y
    own = pltpu.make_async_copy(x_ref, o_ref.at[mine], own_sem)
    own.start()
    copies = []
    for n, (py, pg) in enumerate(others):
        copies.append(pltpu.make_async_remote_copy(
            src_ref=x_ref, dst_ref=o_ref.at[mine], send_sem=send_sem.at[n], recv_sem=recv_sem.at[n],
            device_id={"src": py, "graph": pg}, device_id_type=MESH))
        copies[-1].start()
    own.wait()
    for c in copies:
        c.wait()


def share(x, src, graph):
    n = src * graph
    return pl.pallas_call(
        functools.partial(share_kernel, src, graph),
        in_specs=[pl.BlockSpec(memory_space=pltpu.VMEM)],
        out_specs=pl.BlockSpec(memory_space=pltpu.VMEM),
        out_shape=jax.ShapeDtypeStruct((n,) + x.shape, x.dtype),
        scratch_shapes=[pltpu.SemaphoreType.DMA, pltpu.SemaphoreType.DMA((n - 1,)), pltpu.SemaphoreType.DMA((n - 1,))],
        compiler_params=pltpu.CompilerParams(collective_id=2, has_side_effects=True),
        name="share",
    )(x)


def total_kernel(src, graph, x_ref, o_ref, got, own_sem, send_sem, recv_sem):
    y, g = lax.axis_index("src"), lax.axis_index("graph")
    others = [((y + i) % src, (g + k) % graph) for i, k in everyone(src, graph)][1:]
    hello(others)
    mine = g * src + y
    own = pltpu.make_async_copy(x_ref.at[g], got.at[mine], own_sem)
    own.start()
    await_hello(others)
    copies = []
    for n, (py, pg) in enumerate(others):
        copies.append(pltpu.make_async_remote_copy(
            src_ref=x_ref.at[pg], dst_ref=got.at[mine], send_sem=send_sem.at[n], recv_sem=recv_sem.at[n],
            device_id={"src": py, "graph": pg}, device_id_type=MESH))
        copies[-1].start()
    own.wait()
    for c in copies:
        c.wait()
    acc = got[0]
    for n in range(1, src * graph):
        acc = acc + got[n]
    o_ref[...] = acc


def total(x, src, graph, collective_id):
    n = src * graph
    return pl.pallas_call(
        functools.partial(total_kernel, src, graph),
        in_specs=[pl.BlockSpec(memory_space=pl.ANY)],
        out_specs=pl.BlockSpec(memory_space=pltpu.VMEM),
        out_shape=jax.ShapeDtypeStruct(x.shape[1:], x.dtype),
        scratch_shapes=[pltpu.VMEM((n,) + x.shape[1:], x.dtype), pltpu.SemaphoreType.DMA,
                        pltpu.SemaphoreType.DMA((n - 1,)), pltpu.SemaphoreType.DMA((n - 1,))],
        compiler_params=pltpu.CompilerParams(collective_id=collective_id, has_side_effects=True),
        name="total",
    )(x)


def dense(adj_slab, src_local, level_weight, src, graph):
    slab_rows, vertex_count = adj_slab.shape
    src_count = src_local.shape[0]
    levels = level_weight.shape[0] + 1
    row_start = lax.axis_index("graph") * slab_rows
    vertex_ids = row_start + lax.broadcasted_iota(jnp.int32, (slab_rows, 1), 0)
    first = jnp.where(vertex_ids == src_local[None, :], 1.0, 0.0).astype(f32)

    def forward(carry, unused):
        sigma, seen = carry
        partial = jnp.einsum("uv,us->vs", adj_slab, sigma, preferred_element_type=f32, precision=exact_precision)
        parts = lax.all_to_all(partial.reshape(graph, slab_rows, src_count), "graph", 0, 0)
        sigma = jnp.sum(parts, axis=0) * (1.0 - seen)
        seen = jnp.maximum(seen, jnp.where(sigma > 0, 1.0, 0.0))
        return (sigma, seen), sigma

    _, sigmas = lax.scan(forward, (first, first), None, length=levels)

    def backward(carry, xs):
        delta, acc = carry
        upper, lower, weight = xs
        reached = upper > 0
        ratio = jnp.where(reached, (weight + delta) / jnp.where(reached, upper, 1.0), 0.0)
        gathered = lax.all_to_all(jnp.broadcast_to(ratio[None], (graph,) + ratio.shape), "graph", 0, 0)
        pulled = jnp.einsum("uv,vs->us", adj_slab, gathered.reshape(vertex_count, src_count),
                            preferred_element_type=f32, precision=exact_precision)
        delta = lower * pulled
        return (delta, acc + delta), None

    zero = jnp.zeros_like(first)
    (_, acc), _ = lax.scan(backward, (zero, zero), (sigmas[1:][::-1], sigmas[:-1][::-1], level_weight[::-1]))
    scale = vertex_count / (src_count * src * levels ** 3)
    mine = jnp.sum(acc, axis=1) * scale
    both = lax.all_to_all(jnp.broadcast_to(mine.reshape(1, -1, LANES), (src, slab_rows // LANES, LANES)), "src", 0, 0)
    return jnp.sum(both, axis=0).reshape(slab_rows)


def solution(mesh):
    src, graph = mesh.shape["src"], mesh.shape["graph"]

    def device_program(adj_slab, src_local, level_weight):
        slab_rows, vertex_count = adj_slab.shape
        levels = level_weight.shape[0] + 1
        scale = vertex_count / (HALF * src * graph * levels ** 3)
        which = lax.axis_index("graph").astype(jnp.int32).reshape(1)
        flag_row = slab_rows // LANES

        def finish(lists, compact, collective_id, other):
            parts = walk(which, src_local, level_weight, lists, blocks=graph, vertices=vertex_count, scale=scale, compact=compact)
            summed = total(parts, src, graph, collective_id)

            def plain():
                return summed[:flag_row].reshape(2, -1, LANES).transpose(1, 0, 2).reshape(slab_rows)

            return lax.cond(summed[flag_row, 0] > 0, other, plain)

        def dense_path():
            return dense(adj_slab, src_local, level_weight, src, graph)

        def general_path():
            half = lax.axis_index("src").astype(jnp.int32).reshape(1)
            return finish(share(extract(adj_slab, half, slab_rows // src), src, graph), False, 3, dense_path)

        return finish(collect(adj_slab, src, graph), True, 1, general_path)

    return jax.shard_map(device_program, mesh=mesh,
                         in_specs=(P(("batch", "graph"), None), P(("batch", "src")), P(None)),
                         out_specs=P(("batch", "graph")), check_vma=False)
```

```python
import functools

import jax
import jax.numpy as jnp
from jax import lax
from jax.experimental import pallas as pl
from jax.experimental.pallas import tpu as pltpu
from jax.sharding import PartitionSpec as P

MESH = pl.DeviceIdType.MESH
exact_precision = lax.Precision.HIGHEST
f32, bf16 = jnp.float32, jnp.bfloat16

LANES, SUB = 128, 8
WIDE = 256
DEG, FEW = 8, 4
EMPTY = -2.0
FULL = 32767.0
TURN = (((1,), (1,)), ((), ()))
BLOCK = 128
READS = 4
STEP = 32
HALF = 64
SLOTS = 8
WINDOW = 48
SCAN = 32
CAP = 1024
TALLY = 64
PAIR = (0, 1)
BYTE = 256
BASE, COUNT = 0, 1
FAULT, LENGTH, GOT, PARITY, AWAIT0, AWAIT1 = ((2, n) for n in range(6))


def everyone(src, graph):
    return [(y, g) for y in range(src) for g in range(graph)]


def hello(peers):
    for y, g in peers:
        pl.semaphore_signal(pltpu.get_barrier_semaphore(), inc=1, device_id={"src": y, "graph": g}, device_id_type=MESH)


def await_hello(peers):
    pl.semaphore_wait(pltpu.get_barrier_semaphore(), len(peers))


def place(plane, lists):
    lists = list(lists)
    row_i = lax.broadcasted_iota(jnp.int32, (WIDE, WIDE), 0)
    col_i = lax.broadcasted_iota(jnp.int32, (WIDE, WIDE), 1)
    eye = jnp.where(row_i == col_i, float(WIDE), 0.0).astype(bf16)
    flipped = lax.dot_general(eye, plane, TURN, preferred_element_type=f32)
    lane_id = lax.broadcasted_iota(jnp.int32, (SUB, flipped.shape[1]), 0).astype(f32)
    for g in range(WIDE // SUB):
        x = flipped[g * SUB:(g + 1) * SUB] + (lane_id + float(g * SUB))
        for s in range(len(lists)):
            hi = jnp.maximum(lists[s], x)
            if s < len(lists) - 1:
                x = jnp.minimum(lists[s], x)
            lists[s] = hi
    return lists


def sort(lists):
    gap = len(lists) // 2
    while gap:
        for s in range(len(lists)):
            if not s & gap:
                lists[s], lists[s + gap] = jnp.maximum(lists[s], lists[s + gap]), jnp.minimum(lists[s], lists[s + gap])
        gap //= 2
    return lists


def over_sublanes(lists):
    size = len(lists)
    for shift in (4, 2, 1):
        other = [pltpu.roll(v, shift, 0) for v in lists]
        lists = sort([jnp.maximum(lists[s], other[size - 1 - s]) for s in range(size)])
    out = jnp.full(lists[0].shape, EMPTY, f32)
    sub = lax.broadcasted_iota(jnp.int32, out.shape, 0)
    for s in range(size):
        out = jnp.where(sub == s, jnp.where(lists[s] >= WIDE, lists[s] - WIDE, EMPTY), out)
    return out


def degree_of(seen):
    return lax.dot_general(jnp.ones((SUB, WIDE), bf16), seen, TURN, preferred_element_type=f32)


def collect_kernel(src, graph, a_ref, o_ref, bufs, tops, mine, sems, own_sem, send_sems, recv_sems):
    vertices = a_ref.shape[1]
    pairs, chunks = mine.shape[1] // LANES, vertices // WIDE
    blocks = 2 * pairs
    y, g = lax.axis_index("src"), lax.axis_index("graph")
    others = [((y + i) % src, (g + k) % graph) for i, k in everyone(src, graph)][1:]
    me = g * src + y
    height = 4 * SUB
    pieces = BLOCK // height

    def fetch(i, t):
        rows = pl.ds(pl.multiple_of((y * blocks + i) * BLOCK + t * height, height), height)
        here = pl.ds(pl.multiple_of(t * height, height), height)
        return pltpu.make_async_copy(a_ref.at[rows], bufs.at[i % READS, here], sems.at[i % READS, t])

    def send(n, cols):
        py, pg = others[n]
        return pltpu.make_async_remote_copy(
            src_ref=mine.at[:, cols], dst_ref=o_ref.at[me, :, cols], send_sem=send_sems.at[n], recv_sem=recv_sems.at[n],
            device_id={"src": py, "graph": pg}, device_id_type=MESH)

    def send_pair(p):
        for n in range(len(others)):
            send(n, pl.ds(pl.multiple_of(p * LANES, LANES), LANES)).start()

    hello(others)
    for i in range(READS - 1):
        for t in range(pieces):
            fetch(i, t).start()
    none = jnp.zeros((SUB, 2 * BLOCK), f32)

    def scan(i, first):
        @pl.when(i + READS - 1 < blocks)
        def _():
            for t in range(pieces):
                fetch(i + READS - 1, t).start()

        def scan_rows(t, carry):
            fetch(i, t).wait()
            here = pl.ds(pl.multiple_of(t * height, height), height)

            def scan_chunks(c, state):
                top, low, seen, sums, value = state
                for k in range(STEP):
                    a = bufs[i % READS, here, pl.ds(pl.multiple_of((c * STEP + k) * WIDE, WIDE), WIDE)]
                    x = a * value
                    low = jnp.maximum(low, jnp.minimum(top, x))
                    top = jnp.maximum(top, x)
                    seen = seen + a
                    sums = sums + x
                    value = value + 1
                return top, low, seen, sums, value

            zero = jnp.zeros((height, WIDE), bf16)
            top, low, seen, sums, _ = lax.fori_loop(0, chunks // STEP, scan_chunks, (zero,) * 4 + (zero + 1,))
            for n, v in enumerate((top, low, (sums - top) - low, seen)):
                tops[n, pl.ds(pl.multiple_of(first + t * height, height), height), :] = v
            return carry

        lax.fori_loop(0, pieces, scan_rows, 0)

    def pair_step(p, carry):
        for h in range(2):
            scan(2 * p + h, h * BLOCK)
        seen = tops[3]
        crowd = seen[:SUB]
        for k in range(1, 2 * BLOCK // SUB):
            crowd = jnp.maximum(crowd, seen[k * SUB:(k + 1) * SUB])
        crowd = jnp.max(crowd.astype(f32), axis=0, keepdims=True)
        a, b, c = place(tops[0], (none,) * 4), place(tops[1], (none,) * 2), place(tops[2], (none,))
        rest = [jnp.maximum(b[0], c[0]), jnp.minimum(b[0], c[0])]
        rest = [rest[0], jnp.maximum(b[1], rest[1]), jnp.minimum(b[1], rest[1])]
        lists = over_sublanes(sort([a[0]] + [jnp.maximum(a[s + 1], rest[2 - s]) for s in range(3)]))
        lists = jnp.where((crowd > 3) | (degree_of(seen) > 4), FULL, lists)
        even, odd = lists[:, :BLOCK], lists[:, BLOCK:]
        sub = lax.broadcasted_iota(jnp.int32, even.shape, 0)
        mine[:, pl.ds(pl.multiple_of(p * LANES, LANES), LANES)] = jnp.where(sub < 4, even, pltpu.roll(odd, 4, 0))

        @pl.when(p == 1)
        def _():
            await_hello(others)

        @pl.when(p > 0)
        def _():
            send_pair(p - 1)

        return carry

    lax.fori_loop(0, pairs, pair_step, 0)
    own = pltpu.make_async_copy(mine, o_ref.at[me], own_sem)
    send_pair(pairs - 1)
    own.start()
    own.wait()
    for n in range(len(others)):
        send(n, slice(None)).wait()


def collect(adj_slab, src, graph):
    rows, vertices = adj_slab.shape
    n = src * graph
    mine = (SUB, rows // src // 2)
    return pl.pallas_call(
        functools.partial(collect_kernel, src, graph),
        in_specs=[pl.BlockSpec(memory_space=pl.ANY)],
        out_specs=pl.BlockSpec(memory_space=pltpu.VMEM),
        out_shape=jax.ShapeDtypeStruct((n,) + mine, f32),
        scratch_shapes=[pltpu.VMEM((READS, BLOCK, vertices), bf16), pltpu.VMEM((4, 2 * BLOCK, WIDE), bf16), pltpu.VMEM(mine, f32),
                        pltpu.SemaphoreType.DMA((READS, BLOCK // (4 * SUB))), pltpu.SemaphoreType.DMA,
                        pltpu.SemaphoreType.DMA((n - 1,)), pltpu.SemaphoreType.DMA((n - 1,))],
        compiler_params=pltpu.CompilerParams(collective_id=0, has_side_effects=True, vmem_limit_bytes=40 * 1024 * 1024),
        name="collect",
    )(adj_slab)


def extract_kernel(half_ref, a_ref, o_ref, block, seen, planes, sem):
    vertices = a_ref.shape[1]

    def block_step(i, carry):
        copy = pltpu.make_async_copy(
            a_ref.at[pl.ds(pl.multiple_of(half_ref[0] * o_ref.shape[1] + i * BLOCK, BLOCK), BLOCK)], block, sem)
        copy.start()
        copy.wait()
        planes[...] = jnp.zeros_like(planes)
        seen[...] = jnp.zeros_like(seen)

        def scan_chunk(c, carry):
            a = block[:, pl.ds(pl.multiple_of(c * WIDE, WIDE), WIDE)]
            seen[...] = seen[...] + a
            x = a.astype(f32) * (c + 1).astype(f32)
            for s in range(DEG):
                top = planes[s].astype(f32)
                planes[s] = jnp.maximum(top, x).astype(bf16)
                x = jnp.minimum(top, x)
            return carry

        lax.fori_loop(0, vertices // WIDE, scan_chunk, 0)
        lists = lax.fori_loop(0, DEG, lambda p, lists: tuple(place(planes[p], lists)), (jnp.zeros((SUB, BLOCK), f32),) * DEG)
        o_ref[:, pl.ds(pl.multiple_of(i * BLOCK, BLOCK), BLOCK)] = jnp.where(
            degree_of(seen[...]) > DEG, FULL, over_sublanes(list(lists)))
        return carry

    lax.fori_loop(0, o_ref.shape[1] // BLOCK, block_step, 0)


def extract(adj_slab, half, rows):
    vertices = adj_slab.shape[1]
    return pl.pallas_call(
        extract_kernel,
        in_specs=[pl.BlockSpec(memory_space=pltpu.SMEM), pl.BlockSpec(memory_space=pl.ANY)],
        out_specs=pl.BlockSpec(memory_space=pltpu.VMEM),
        out_shape=jax.ShapeDtypeStruct((DEG, rows), f32),
        scratch_shapes=[pltpu.VMEM((BLOCK, vertices), bf16), pltpu.VMEM((BLOCK, WIDE), bf16),
                        pltpu.VMEM((DEG, BLOCK, WIDE), bf16), pltpu.SemaphoreType.DMA],
        name="extract",
    )(half, adj_slab)


def walk_kernel(which_ref, src_ref, weight_ref, lists_ref, out_ref,
                table, queue, sigma, ratio, delta, cand, ids, now, dest, tail_ref, held, rowhot, colhot, bins,
                ids_a, ids_b, meta, sems, *, levels, vertices, scale, compact):
    parts, _, width = lists_ref.shape
    pitch = vertices + SUB
    lane = lax.broadcasted_iota(jnp.int32, (SUB, LANES), 1)
    sub = lax.broadcasted_iota(jnp.int32, (SUB, LANES), 0)
    upper = lane >= HALF
    lane_row = lax.broadcasted_iota(jnp.int32, (1, LANES), 1)
    group_odd = ((lane_row // 32) % 2) == 1
    lane32 = lane_row % 32
    rows_all = queue.shape[0]
    high = vertices // WIDE

    def eight(row):
        return pl.ds(pl.multiple_of(row, SUB), SUB)

    def spread_row(ref, *index):
        return jnp.broadcast_to(ref[(*index[:-1], pl.ds(index[-1], 1), slice(None))], (SUB, LANES))

    def clear(t, carry):
        for k in range(SUB):
            rows = eight((t * SUB + k) * SUB)
            queue[rows, :] = jnp.full((SUB, LANES), -1.0, f32)
            sigma[rows, :] = jnp.zeros((SUB, LANES), f32)
        return carry

    lax.fori_loop(0, rows_all // (SUB * SUB), clear, 0)
    bins[...] = jnp.zeros_like(bins)

    def fetch(quad, row, buf):
        return pltpu.make_async_copy(ids.at[quad, eight(row)], buf[0], sems.at[buf[1]])

    def name(row, q):
        v = jnp.where(q < 0, vertices, q.astype(jnp.int32))
        ids[0, eight(row), :] = v
        ids[1, eight(row), :] = v + pitch

    first = jnp.zeros((1, LANES), jnp.int32)
    for j in range(HALF):
        first = jnp.where(lane_row % HALF == j, src_ref[which_ref[0] * HALF + j], first)
    queue[0:1, :] = first.astype(f32)
    sigma[0:1, :] = jnp.ones((1, LANES), f32)
    held[...] = jnp.ones_like(held)
    name(0, queue[eight(0), :])
    name(SUB, queue[eight(SUB), :])
    for place_, value in ((meta_at, 0) for meta_at in (FAULT, GOT, PARITY)):
        meta[place_] = value
    meta[BASE, 0] = 0
    meta[COUNT, 0] = 1
    meta[AWAIT0] = 1
    meta[AWAIT1] = 1
    bufs = (ids_a, 0), (ids_b, 1)
    for n, buf in enumerate(bufs):
        fetch(0, n * SUB, buf).start()

    srow = lax.broadcasted_iota(jnp.int32, (2 * SUB, LANES), 0)
    slane = lax.broadcasted_iota(jnp.int32, (2 * SUB, LANES), 1)

    def fill(halves, target):
        picks = [jnp.where((srow % SUB) == (slane // 32 + FEW * h), jnp.where(srow < SUB, float(LANES), 1.0), 0.0).astype(bf16)
                 for h in halves]

        def body(b, most):
            x = lists_ref[b]
            hi = jnp.floor(x * (1.0 / LANES))
            lo = x - hi * LANES
            both = jnp.concatenate([hi, lo], axis=0).astype(bf16)
            for h, pick in zip(halves, picks):
                rows = lax.dot_general(both, pick, (((0,), (0,)), ((), ())), preferred_element_type=f32)
                for k in range(width // LANES):
                    table[pl.ds(pl.multiple_of(target(h, b, k * LANES), SUB), LANES), :] = rows[k * LANES:(k + 1) * LANES]
            for k in range(width // LANES):
                most = jnp.maximum(most, x[:, k * LANES:(k + 1) * LANES])
            return most

        return lax.fori_loop(0, parts, body, jnp.full((SUB, LANES), EMPTY, f32))

    table[vertices:pitch, :] = jnp.full((SUB, LANES), EMPTY, f32)
    if compact:
        most = fill((0, 1), lambda h, b, col: (b * width + col) * 2 + h * LANES)
        quads = 1
    else:
        table[pitch + vertices:, :] = jnp.full((SUB, LANES), EMPTY, f32)
        most = fill((0,), lambda h, b, col: b * width + col)
        wide = jnp.max(jnp.where(sub >= FEW, most, EMPTY)) >= 0
        quads = jnp.where(wide, 2, 1)

        @pl.when(wide)
        def _():
            fill((1,), lambda h, b, col: pitch + b * width + col)
            fetch(0, SUB, bufs[1]).wait()
            fetch(1, 0, bufs[1]).start()

    bad = jnp.max(most) > vertices
    meta[FAULT] = bad.astype(jnp.int32)

    def gather(ids_s):
        acc = [[jnp.full((1, LANES), EMPTY, f32)] * 2 for _ in range(SLOTS)]
        for j in range(32):
            hit = lane32 == j
            for i in range(SLOTS):
                for b in PAIR:
                    acc[i][b] = jnp.where(hit, table[pl.ds(ids_s[i, b * 32 + j], 1), :], acc[i][b])
        return [(jnp.where(group_odd, b, a), pltpu.roll(jnp.where(group_odd, a, b), LANES - 32, 1)) for a, b in acc]

    def keep(rows, quad, row):
        for i, pair in enumerate(rows):
            for h in PAIR:
                cand[2 * quad + h, pl.ds(row + i, 1), :] = pair[h]

    def flag(x):
        return jnp.where(x, 1, 0)

    def level_step(level, carry):
        base, count = meta[BASE, level], meta[COUNT, level]
        following = base + (count + 7) // SUB * SUB
        batches = jnp.where(following <= CAP, (count + SLOTS - 1) // SLOTS, 0)
        units = batches * quads
        parity = meta[PARITY]

        def at(unit, origin):
            return unit & (quads - 1), origin + (unit >> (quads - 1)) * SUB

        def on_parity(n, f):
            for k in PAIR:
                @pl.when(n & 1 == k)
                def _():
                    f(bufs[k], bufs[1 - k])

        def unit_step(unit, other, to):
            quad, row = at(unit, base)
            x = [cand[2 * quad + h, eight(row), :] for h in PAIR]

            def search(t, marks):
                marks = list(marks)
                for k in range(SCAN):
                    q = spread_row(queue, t * SCAN + k)
                    for h in PAIR:
                        n = 2 * h + k % 2
                        marks[n] = jnp.where(x[h] == q, 1, marks[n])
                return tuple(marks)

            reach = following + meta[LENGTH]
            marks = lax.fori_loop(0, (reach + SCAN - 1) // SCAN, search, (jnp.zeros((SUB, LANES), jnp.int32),) * 4)
            ahead = unit + 1 < units
            final_unit = unit + 1 == units
            soon = jnp.logical_and(final_unit, meta[AWAIT0] > 0)

            @pl.when(jnp.logical_or(ahead, soon))
            def _():
                fetch(0, base, to).wait()

            even, odd = x
            m, n, k, l = marks
            near_even, near_odd = m | n | flag(even < 0), k | l | flag(odd < 0)

            xr = [pltpu.roll(v, HALF, 1) for v in x]
            turns = [[[pltpu.roll(v, s, 0) if s else v for v in (x[h], xr[h])] for s in range(SUB)] for h in PAIR]
            for s, ((a, b), (c, d)) in enumerate(zip(*turns)):
                near_odd = jnp.where((odd == a) | (odd == b), 1, near_odd)
                if s:
                    after = sub >= s
                    near_even = jnp.where(((even == a) | (even == b)) & after, 1, near_even)
                    near_odd = jnp.where(((odd == c) | (odd == d)) & after, 1, near_odd)

            new = [1 - near_even, 1 - near_odd]
            packed = new[0] + BYTE * new[1]
            across = pltpu.roll(packed, HALF, 1)
            far = [across & (BYTE - 1), across >> SUB]
            both = packed + across
            run, whole = both, both
            for s in (1, 2, 4):
                run = run + jnp.where(sub >= s, pltpu.roll(run, s, 0), 0)
                whole = whole + pltpu.roll(whole, s, 0)
            run = run - both
            tail = tail_ref[...]
            evens = whole & (BYTE - 1)
            begin = [tail + (run & (BYTE - 1)), tail + evens + (run >> SUB)]
            for h in PAIR:
                dest[SUB * h:SUB * h + SUB, :] = jnp.where(new[h] > 0, begin[h] + jnp.where(upper, far[h], 0), -1)
                dest[16 + SUB * h:24 + SUB * h, :] = jnp.where(far[h] > 0, begin[h] + jnp.where(upper, 0, new[h]), -1)
                now[SUB * h:SUB * h + SUB, :] = x[h]
                now[16 + SUB * h:24 + SUB * h, :] = xr[h]
            now[32:40, :] = sigma[eight(row), :]
            tail = tail + evens + (whole >> SUB)
            tail_ref[...] = tail
            passed = SLOTS * ((unit + 1) >> (quads - 1))
            second = SUB + SUB * (1 >> (quads - 1))
            need = jnp.where(sub == 1, SUB, second)
            short = (tail < need) & (held[...] > passed)
            most = jnp.max(jnp.where(sub == 0, tail, flag(short)).astype(f32), axis=1, keepdims=True)
            length = most[0, 0].astype(jnp.int32)
            ready = [most[1, 0] == 0, most[2, 0] == 0]

            def insert(g):
                slots = [eight(following + g * WINDOW + SUB * t) for t in range(WINDOW // SUB)]
                qs = [queue[r, :] for r in slots]
                ss = [sigma[r, :] for r in slots]
                pos = [sub + (g * WINDOW + SUB * t) for t in range(WINDOW // SUB)]
                for h in PAIR:
                    for i in range(SUB):
                        d, e = spread_row(dest, SUB * h + i), spread_row(dest, 16 + SUB * h + i)
                        v, w = spread_row(now, SUB * h + i), spread_row(now, 16 + SUB * h + i)
                        for t in range(WINDOW // SUB):
                            qs[t] = jnp.where(pos[t] == d, v, jnp.where(pos[t] == e, w, qs[t]))
                for i in range(SUB):
                    v, w, sig = spread_row(now, i), spread_row(now, SUB + i), spread_row(now, 32 + i)
                    for t in range(WINDOW // SUB):
                        ss[t] = ss[t] + jnp.where((qs[t] == v) | (qs[t] == w), sig, 0.0)
                for t, r in enumerate(slots):
                    queue[r, :] = qs[t]
                    sigma[r, :] = ss[t]
                return qs

            quad2, row2 = at(unit + 1, base)
            rows = gather(to[0])
            qs = insert(0)
            for n in PAIR:
                name(following + n * SUB, qs[n])
            keep(rows, jnp.where(ahead, quad2, 0), jnp.where(ahead, row2, jnp.where(soon, following, rows_all - SUB)))

            @pl.when(unit + 3 < units)
            def _():
                fetch(*at(unit + 3, base), to).start()

            @pl.when(soon)
            def _():
                meta[GOT] = 1

            def first_of_next(n, when, buf):
                @pl.when(jnp.logical_and(when, meta[(AWAIT0, AWAIT1)[n]] == 0))
                def _():
                    fetch(*at(n, following), buf).start()
                    meta[(AWAIT0, AWAIT1)[n]] = 1

            first_of_next(0, jnp.logical_and(ready[0], unit + 3 == units), to)
            first_of_next(0, jnp.logical_and(ready[0], unit + 2 == units), other)
            first_of_next(1, jnp.logical_and(ready[1], unit + 2 == units), to)
            first_of_next(0, final_unit, to)
            first_of_next(1, final_unit, other)

            groups = (length + WINDOW - 1) // WINDOW
            fits = following + groups * WINDOW <= CAP + WINDOW
            meta[LENGTH] = jnp.where(fits, length, 0)

            @pl.when(jnp.logical_not(fits))
            def _():
                meta[FAULT] = 1

            def more(g, carry):
                insert(g)
                return carry

            lax.fori_loop(1, jnp.where(fits, groups, 0), more, 0)

        tail_ref[...] = jnp.zeros_like(tail_ref)
        meta[LENGTH] = 0

        def open_level(mine, other):
            @pl.when(jnp.logical_and(meta[GOT] == 0, meta[AWAIT0] > 0))
            def _():
                fetch(0, base, mine).wait()
                keep(gather(mine[0]), 0, base)

            @pl.when(jnp.logical_and(units < 2, meta[AWAIT1] > 0))
            def _():
                fetch(0, base, other).wait()

            @pl.when(units > 2)
            def _():
                fetch(*at(2, base), mine).start()

        on_parity(parity, open_level)
        for place_ in (GOT, AWAIT0, AWAIT1):
            meta[place_] = 0

        def any_unit(unit, carry):
            on_parity(parity + unit, functools.partial(unit_step, unit))
            return carry

        lax.fori_loop(0, units, any_unit, 0)
        meta[PARITY] = parity + units

        @pl.when(following > CAP)
        def _():
            meta[FAULT] = 1

        found = jnp.where(meta[FAULT] == 0, meta[LENGTH], 0)
        meta[BASE, level + 1] = following
        meta[COUNT, level + 1] = found

        def settle(g, carry):
            slots = [eight(following + g * WINDOW + SUB * t) for t in range(WINDOW // SUB)]
            @pl.when(g > 0)
            def _():
                for r in slots[:2]:
                    name(r.start, queue[r, :])

            for r in slots[2:]:
                name(r.start, queue[r, :])
            for r in slots:
                s = sigma[r, :]
                sigma[r, :] = s + pltpu.roll(s, HALF, 1)
            return carry

        lax.fori_loop(0, (found + WINDOW - 1) // WINDOW, settle, 0)
        held[...] = tail_ref[...]
        return carry

    @pl.when(jnp.logical_not(bad))
    def _():
        lax.fori_loop(0, levels, level_step, 0)

    def drain(n, buf):
        @pl.when(meta[(AWAIT0, AWAIT1)[n]] > 0)
        def _():
            fetch(0, 0, buf).wait()

    for k in PAIR:
        @pl.when(meta[PARITY] & 1 == k)
        def _():
            @pl.when(meta[GOT] == 0)
            def _():
                drain(0, bufs[k])

            drain(1, bufs[1 - k])

    good = meta[FAULT] == 0

    @pl.when(good)
    def _():
        last = meta[BASE, levels]
        g_last = weight_ref[levels - 2]

        def seed(g, carry):
            for t in range(WINDOW // SUB):
                r = eight(last + g * WINDOW + SUB * t)
                s = sigma[r, :]
                ratio[r, :] = jnp.where(s > 0, g_last / jnp.where(s > 0, s, 1.0), 0.0)
            return carry

        lax.fori_loop(0, (meta[COUNT, levels] + WINDOW - 1) // WINDOW, seed, 0)

        def back_step(k, carry):
            level = levels - 1 - k
            base, count = meta[BASE, level], meta[COUNT, level]
            nbase, ncount = meta[BASE, level + 1], meta[COUNT, level + 1]
            g_here = weight_ref[jnp.maximum(level - 2, 0)]

            def pull_batch(bt, carry):
                here = eight(base + bt * SLOTS)

                def pull_quad(quad, acc):
                    x = [cand[2 * quad + h, here, :] for h in PAIR]

                    def pull(c, acc):
                        acc = list(acc)
                        for n in range(WINDOW):
                            q = spread_row(queue, nbase + c * WINDOW + n)
                            w = spread_row(ratio, nbase + c * WINDOW + n)
                            acc[n % 2] = acc[n % 2] + jnp.where((x[0] == q) | (x[1] == q), w, 0.0)
                        return tuple(acc)

                    return lax.fori_loop(0, (ncount + WINDOW - 1) // WINDOW, pull, acc)

                acc = lax.fori_loop(0, quads, pull_quad, (jnp.zeros((SUB, LANES), f32),) * 2)
                delta[here, :] = acc[0] + acc[1]
                return carry

            lax.fori_loop(0, (count + SLOTS - 1) // SLOTS, pull_batch, 0)

            def finish(g, carry):
                slots = [eight(base + g * WINDOW + SUB * t) for t in range(WINDOW // SUB)]
                for t, r in enumerate(slots):
                    inside = g * WINDOW + SUB * t < count
                    part, s = delta[r, :], sigma[r, :]
                    d = s * (part + pltpu.roll(part, HALF, 1))
                    w = jnp.where(s > 0, (g_here + d) / jnp.where(s > 0, s, 1.0), 0.0)
                    delta[r, :] = jnp.where(inside, d, part)
                    ratio[r, :] = jnp.where(inside, w, ratio[r, :])
                return carry

            lax.fori_loop(0, (count + WINDOW - 1) // WINDOW, finish, 0)
            return carry

        lax.fori_loop(0, levels - 1, back_step, 0)

        tall = lax.broadcasted_iota(jnp.int32, (WIDE, WIDE), 0).astype(f32).astype(bf16)
        zero = jnp.zeros((WIDE, WIDE), bf16)
        one = zero + 1
        start = meta[BASE, 1]

        def tally(t, carry):
            for u in range(TALLY // 16):
                a, b = eight(start + t * TALLY + u * 16), eight(start + t * TALLY + u * 16 + SUB)
                v = jnp.where(upper, queue[b, :], queue[a, :])
                d = jnp.where(upper, delta[b, :], delta[a, :])
                hi = jnp.floor(v * (1.0 / WIDE))
                lo = v - hi * WIDE
                d_hi = d.astype(bf16).astype(f32)
                d_mid = (d - d_hi).astype(bf16).astype(f32)
                d_lo = d - d_hi - d_mid
                for p in range(0, SUB, 2):
                    cols = slice((u * SUB + p) * LANES, (u * SUB + p + 2) * LANES)

                    def pair(x):
                        return jnp.concatenate([x[p:p + 1], x[p + 1:p + 2]], axis=1).astype(bf16)

                    colhot[:, cols] = jnp.where(tall == pair(lo), one, zero)
                    match = tall[:high] == pair(hi)
                    for n, x in enumerate((d_hi, d_mid, d_lo)):
                        rowhot[n * high:(n + 1) * high, cols] = jnp.where(match, pair(x), zero[:high])
            bins[...] += lax.dot_general(rowhot[...], colhot[...], TURN, preferred_element_type=f32)
            return carry

        for t in range(TALLY // SUB):
            delta[eight(last + t * SUB), :] = jnp.zeros((SUB, LANES), f32)
        lax.fori_loop(0, (last - start + TALLY - 1) // TALLY, tally, 0)

    blocks = out_ref.shape[0]
    per = high // blocks
    total = (bins[:high] + bins[high:2 * high] + bins[2 * high:]) * scale
    fault = jnp.where(good, 0.0, 1.0)
    for b in range(blocks):
        for n in PAIR:
            out_ref[b, n * per:(n + 1) * per, :] = total[b * per:(b + 1) * per, n * LANES:(n + 1) * LANES]
        out_ref[b, 2 * per:, :] = jnp.full((SUB, LANES), fault, f32)


def walk(which, sources, weights, lists, *, blocks, vertices, scale, compact):
    levels = weights.shape[0] + 1
    rows = CAP + 4 * WINDOW
    high = LANES // blocks + SUB
    vm = pltpu.VMEM
    queue = vm((rows, LANES), f32)
    parts = 3 * (vertices // WIDE)
    return pl.pallas_call(
        functools.partial(walk_kernel, levels=levels, vertices=vertices, scale=scale, compact=compact),
        in_specs=[pl.BlockSpec(memory_space=pltpu.SMEM)] * 3 + [pl.BlockSpec(memory_space=pltpu.VMEM)],
        out_specs=pl.BlockSpec(memory_space=pltpu.VMEM),
        out_shape=jax.ShapeDtypeStruct((blocks, high, LANES), f32),
        scratch_shapes=[
            vm(((1 if compact else 2) * (vertices + SUB), LANES), f32), queue, queue, queue, queue,
            vm((4, rows, LANES), f32), vm((2, rows, LANES), jnp.int32),
            vm((40, LANES), f32), vm((32, LANES), jnp.int32), vm((SUB, LANES), jnp.int32), vm((SUB, LANES), jnp.int32),
            vm((parts, TALLY // 2 * LANES), bf16), vm((WIDE, TALLY // 2 * LANES), bf16), vm((parts, WIDE), f32),
            pltpu.SMEM((SLOTS, LANES), jnp.int32), pltpu.SMEM((SLOTS, LANES), jnp.int32), pltpu.SMEM((3, 16), jnp.int32),
            pltpu.SemaphoreType.DMA((2,)),
        ],
        compiler_params=pltpu.CompilerParams(
            vmem_limit_bytes=48 * 1024 * 1024),
        name="walk",
    )(which, sources, weights, lists)


def share_kernel(src, graph, x_ref, o_ref, own_sem, send_sem, recv_sem):
    y, g = lax.axis_index("src"), lax.axis_index("graph")
    others = [((y + i) % src, (g + k) % graph) for i, k in everyone(src, graph)][1:]
    hello(others)
    await_hello(others)
    mine = g * src + y
    own = pltpu.make_async_copy(x_ref, o_ref.at[mine], own_sem)
    own.start()
    copies = []
    for n, (py, pg) in enumerate(others):
        copies.append(pltpu.make_async_remote_copy(
            src_ref=x_ref, dst_ref=o_ref.at[mine], send_sem=send_sem.at[n], recv_sem=recv_sem.at[n],
            device_id={"src": py, "graph": pg}, device_id_type=MESH))
        copies[-1].start()
    own.wait()
    for c in copies:
        c.wait()


def share(x, src, graph):
    n = src * graph
    return pl.pallas_call(
        functools.partial(share_kernel, src, graph),
        in_specs=[pl.BlockSpec(memory_space=pltpu.VMEM)],
        out_specs=pl.BlockSpec(memory_space=pltpu.VMEM),
        out_shape=jax.ShapeDtypeStruct((n,) + x.shape, x.dtype),
        scratch_shapes=[pltpu.SemaphoreType.DMA, pltpu.SemaphoreType.DMA((n - 1,)), pltpu.SemaphoreType.DMA((n - 1,))],
        compiler_params=pltpu.CompilerParams(collective_id=2, has_side_effects=True),
        name="share",
    )(x)


def total_kernel(src, graph, x_ref, o_ref, flag_ref, got, own_sem, send_sem, recv_sem):
    y, g = lax.axis_index("src"), lax.axis_index("graph")
    others = [((y + i) % src, (g + k) % graph) for i, k in everyone(src, graph)][1:]
    hello(others)
    mine = g * src + y
    own = pltpu.make_async_copy(x_ref.at[g], got.at[mine], own_sem)
    own.start()
    await_hello(others)
    copies = []
    for n, (py, pg) in enumerate(others):
        copies.append(pltpu.make_async_remote_copy(
            src_ref=x_ref.at[pg], dst_ref=got.at[mine], send_sem=send_sem.at[n], recv_sem=recv_sem.at[n],
            device_id={"src": py, "graph": pg}, device_id_type=MESH))
        copies[-1].start()
    own.wait()
    for c in copies:
        c.wait()
    acc = got[0]
    for n in range(1, src * graph):
        acc = acc + got[n]
    half = o_ref.shape[0] // 2
    for n in PAIR:
        o_ref[pl.ds(n, half, 2), :] = acc[n * half:(n + 1) * half]
    flag_ref[...] = acc[2 * half:]


def total(x, src, graph, collective_id):
    n = src * graph
    return pl.pallas_call(
        functools.partial(total_kernel, src, graph),
        in_specs=[pl.BlockSpec(memory_space=pl.ANY)],
        out_specs=[pl.BlockSpec(memory_space=pltpu.VMEM)] * 2,
        out_shape=[jax.ShapeDtypeStruct((rows, LANES), f32) for rows in (x.shape[1] - SUB, SUB)],
        scratch_shapes=[pltpu.VMEM((n,) + x.shape[1:], x.dtype), pltpu.SemaphoreType.DMA,
                        pltpu.SemaphoreType.DMA((n - 1,)), pltpu.SemaphoreType.DMA((n - 1,))],
        compiler_params=pltpu.CompilerParams(collective_id=collective_id, has_side_effects=True),
        name="total",
    )(x)


def dense(adj_slab, src_local, level_weight, src, graph):
    slab_rows, vertex_count = adj_slab.shape
    src_count = src_local.shape[0]
    levels = level_weight.shape[0] + 1
    row_start = lax.axis_index("graph") * slab_rows
    vertex_ids = row_start + lax.broadcasted_iota(jnp.int32, (slab_rows, 1), 0)
    first = jnp.where(vertex_ids == src_local[None, :], 1.0, 0.0).astype(f32)

    def forward(carry, unused):
        sigma, seen = carry
        partial = jnp.einsum("uv,us->vs", adj_slab, sigma, preferred_element_type=f32, precision=exact_precision)
        parts = lax.all_to_all(partial.reshape(graph, slab_rows, src_count), "graph", 0, 0)
        sigma = jnp.sum(parts, axis=0) * (1.0 - seen)
        seen = jnp.maximum(seen, jnp.where(sigma > 0, 1.0, 0.0))
        return (sigma, seen), sigma

    _, sigmas = lax.scan(forward, (first, first), None, length=levels)

    def backward(carry, xs):
        delta, acc = carry
        upper, lower, weight = xs
        reached = upper > 0
        ratio = jnp.where(reached, (weight + delta) / jnp.where(reached, upper, 1.0), 0.0)
        gathered = lax.all_to_all(jnp.broadcast_to(ratio[None], (graph,) + ratio.shape), "graph", 0, 0)
        pulled = jnp.einsum("uv,vs->us", adj_slab, gathered.reshape(vertex_count, src_count),
                            preferred_element_type=f32, precision=exact_precision)
        delta = lower * pulled
        return (delta, acc + delta), None

    zero = jnp.zeros_like(first)
    (_, acc), _ = lax.scan(backward, (zero, zero), (sigmas[1:][::-1], sigmas[:-1][::-1], level_weight[::-1]))
    scale = vertex_count / (src_count * src * levels ** 3)
    mine = jnp.sum(acc, axis=1) * scale
    both = lax.all_to_all(jnp.broadcast_to(mine.reshape(1, -1, LANES), (src, slab_rows // LANES, LANES)), "src", 0, 0)
    return jnp.sum(both, axis=0).reshape(slab_rows)


def solution(mesh):
    src, graph = mesh.shape["src"], mesh.shape["graph"]

    def device_program(adj_slab, src_local, level_weight):
        slab_rows, vertex_count = adj_slab.shape
        levels = level_weight.shape[0] + 1
        scale = vertex_count / (HALF * src * graph * levels ** 3)
        which = lax.axis_index("graph").astype(jnp.int32).reshape(1)

        def finish(lists, compact, collective_id, other):
            parts = walk(which, src_local, level_weight, lists, blocks=graph, vertices=vertex_count, scale=scale, compact=compact)
            summed, flag = total(parts, src, graph, collective_id)
            return lax.cond(flag[0, 0] > 0, other, lambda: summed.reshape(slab_rows))

        def dense_path():
            return dense(adj_slab, src_local, level_weight, src, graph)

        def general_path():
            half = lax.axis_index("src").astype(jnp.int32).reshape(1)
            return finish(share(extract(adj_slab, half, slab_rows // src), src, graph), False, 3, dense_path)

        return finish(collect(adj_slab, src, graph), True, 1, general_path)

    return jax.shard_map(device_program, mesh=mesh,
                         in_specs=(P(("batch", "graph"), None), P(("batch", "src")), P(None)),
                         out_specs=P(("batch", "graph")), check_vma=False)
```

```python
import functools

import jax
import jax.numpy as jnp
from jax import lax
from jax.experimental import pallas as pl
from jax.experimental.pallas import tpu as pltpu
from jax.sharding import PartitionSpec as P

MESH = pl.DeviceIdType.MESH
exact_precision = lax.Precision.HIGHEST
f32, bf16 = jnp.float32, jnp.bfloat16

LANES, SUB = 128, 8
WIDE = 256
DEG, FEW = 8, 4
EMPTY = -2.0
FULL = 32767.0
TURN = (((1,), (1,)), ((), ()))
BLOCK = 128
READS = 4
STEP = 32
HALF = 64
SLOTS = 8
WINDOW = 48
SCAN = 32
CAP = 1024
TALLY = 96
PAIR = (0, 1)
BYTE = 256
BASE, COUNT = 0, 1
FAULT, LENGTH, GOT, PARITY, AWAIT0, AWAIT1 = ((2, n) for n in range(6))


def everyone(src, graph):
    return [(y, g) for y in range(src) for g in range(graph)]


def hello(peers):
    for y, g in peers:
        pl.semaphore_signal(pltpu.get_barrier_semaphore(), inc=1, device_id={"src": y, "graph": g}, device_id_type=MESH)


def await_hello(peers):
    pl.semaphore_wait(pltpu.get_barrier_semaphore(), len(peers))


def place(plane, lists):
    lists = list(lists)
    row_i = lax.broadcasted_iota(jnp.int32, (WIDE, WIDE), 0)
    col_i = lax.broadcasted_iota(jnp.int32, (WIDE, WIDE), 1)
    eye = jnp.where(row_i == col_i, float(WIDE), 0.0).astype(bf16)
    flipped = lax.dot_general(eye, plane, TURN, preferred_element_type=f32)
    lane_id = lax.broadcasted_iota(jnp.int32, (SUB, flipped.shape[1]), 0).astype(f32)
    for g in range(WIDE // SUB):
        x = flipped[g * SUB:(g + 1) * SUB] + (lane_id + float(g * SUB))
        for s in range(len(lists)):
            hi = jnp.maximum(lists[s], x)
            if s < len(lists) - 1:
                x = jnp.minimum(lists[s], x)
            lists[s] = hi
    return lists


def sort(lists):
    gap = len(lists) // 2
    while gap:
        for s in range(len(lists)):
            if not s & gap:
                lists[s], lists[s + gap] = jnp.maximum(lists[s], lists[s + gap]), jnp.minimum(lists[s], lists[s + gap])
        gap //= 2
    return lists


def over_sublanes(lists):
    size = len(lists)
    for shift in (4, 2, 1):
        other = [pltpu.roll(v, shift, 0) for v in lists]
        lists = sort([jnp.maximum(lists[s], other[size - 1 - s]) for s in range(size)])
    out = jnp.full(lists[0].shape, EMPTY, f32)
    sub = lax.broadcasted_iota(jnp.int32, out.shape, 0)
    for s in range(size):
        out = jnp.where(sub == s, jnp.where(lists[s] >= WIDE, lists[s] - WIDE, EMPTY), out)
    return out


def degree_of(seen):
    return lax.dot_general(jnp.ones((SUB, WIDE), bf16), seen, TURN, preferred_element_type=f32)


def collect_kernel(src, graph, a_ref, o_ref, bufs, tops, mine, sems, own_sem, send_sems, recv_sems):
    vertices = a_ref.shape[1]
    pairs, chunks = mine.shape[1] // LANES, vertices // WIDE
    blocks = 2 * pairs
    y, g = lax.axis_index("src"), lax.axis_index("graph")
    others = [((y + i) % src, (g + k) % graph) for i, k in everyone(src, graph)][1:]
    me = g * src + y
    height = 4 * SUB
    pieces = BLOCK // height

    def fetch(i, t):
        rows = pl.ds(pl.multiple_of((y * blocks + i) * BLOCK + t * height, height), height)
        here = pl.ds(pl.multiple_of(t * height, height), height)
        return pltpu.make_async_copy(a_ref.at[rows], bufs.at[i % READS, here], sems.at[i % READS, t])

    def send(n, cols):
        py, pg = others[n]
        return pltpu.make_async_remote_copy(
            src_ref=mine.at[:, cols], dst_ref=o_ref.at[me, :, cols], send_sem=send_sems.at[n], recv_sem=recv_sems.at[n],
            device_id={"src": py, "graph": pg}, device_id_type=MESH)

    def send_pair(p):
        for n in range(len(others)):
            send(n, pl.ds(pl.multiple_of(p * LANES, LANES), LANES)).start()

    hello(others)
    for i in range(READS - 1):
        for t in range(pieces):
            fetch(i, t).start()
    none = jnp.zeros((SUB, 2 * BLOCK), f32)

    def scan(i, first):
        @pl.when(i + READS - 1 < blocks)
        def _():
            for t in range(pieces):
                fetch(i + READS - 1, t).start()

        def scan_rows(t, carry):
            fetch(i, t).wait()
            here = pl.ds(pl.multiple_of(t * height, height), height)

            def scan_chunks(c, state):
                top, low, seen, sums, value = state
                for k in range(STEP):
                    a = bufs[i % READS, here, pl.ds(pl.multiple_of((c * STEP + k) * WIDE, WIDE), WIDE)]
                    x = a * value
                    low = jnp.maximum(low, jnp.minimum(top, x))
                    top = jnp.maximum(top, x)
                    seen = seen + a
                    sums = sums + x
                    value = value + 1
                return top, low, seen, sums, value

            zero = jnp.zeros((height, WIDE), bf16)
            top, low, seen, sums, _ = lax.fori_loop(0, chunks // STEP, scan_chunks, (zero,) * 4 + (zero + 1,))
            for n, v in enumerate((top, low, (sums - top) - low, seen)):
                tops[n, pl.ds(pl.multiple_of(first + t * height, height), height), :] = v
            return carry

        lax.fori_loop(0, pieces, scan_rows, 0)

    def pair_step(p, carry):
        for h in range(2):
            scan(2 * p + h, h * BLOCK)
        seen = tops[3]
        crowd = seen[:SUB]
        for k in range(1, 2 * BLOCK // SUB):
            crowd = jnp.maximum(crowd, seen[k * SUB:(k + 1) * SUB])
        crowd = jnp.max(crowd.astype(f32), axis=0, keepdims=True)
        a, b, c = place(tops[0], (none,) * 4), place(tops[1], (none,) * 2), place(tops[2], (none,))
        rest = [jnp.maximum(b[0], c[0]), jnp.minimum(b[0], c[0])]
        rest = [rest[0], jnp.maximum(b[1], rest[1]), jnp.minimum(b[1], rest[1])]
        lists = over_sublanes(sort([a[0]] + [jnp.maximum(a[s + 1], rest[2 - s]) for s in range(3)]))
        lists = jnp.where((crowd > 3) | (degree_of(seen) > 4), FULL, lists)
        even, odd = lists[:, :BLOCK], lists[:, BLOCK:]
        sub = lax.broadcasted_iota(jnp.int32, even.shape, 0)
        mine[:, pl.ds(pl.multiple_of(p * LANES, LANES), LANES)] = jnp.where(sub < 4, even, pltpu.roll(odd, 4, 0))

        @pl.when(p == 1)
        def _():
            await_hello(others)

        @pl.when(p > 0)
        def _():
            send_pair(p - 1)

        return carry

    lax.fori_loop(0, pairs, pair_step, 0)
    own = pltpu.make_async_copy(mine, o_ref.at[me], own_sem)
    send_pair(pairs - 1)
    own.start()
    own.wait()
    for n in range(len(others)):
        send(n, slice(None)).wait()


def collect(adj_slab, src, graph):
    rows, vertices = adj_slab.shape
    n = src * graph
    mine = (SUB, rows // src // 2)
    return pl.pallas_call(
        functools.partial(collect_kernel, src, graph),
        in_specs=[pl.BlockSpec(memory_space=pl.ANY)],
        out_specs=pl.BlockSpec(memory_space=pltpu.VMEM),
        out_shape=jax.ShapeDtypeStruct((n,) + mine, f32),
        scratch_shapes=[pltpu.VMEM((READS, BLOCK, vertices), bf16), pltpu.VMEM((4, 2 * BLOCK, WIDE), bf16), pltpu.VMEM(mine, f32),
                        pltpu.SemaphoreType.DMA((READS, BLOCK // (4 * SUB))), pltpu.SemaphoreType.DMA,
                        pltpu.SemaphoreType.DMA((n - 1,)), pltpu.SemaphoreType.DMA((n - 1,))],
        compiler_params=pltpu.CompilerParams(collective_id=0, has_side_effects=True, vmem_limit_bytes=40 * 1024 * 1024),
        name="collect",
    )(adj_slab)


def extract_kernel(half_ref, a_ref, o_ref, block, seen, planes, sem):
    vertices = a_ref.shape[1]

    def block_step(i, carry):
        copy = pltpu.make_async_copy(
            a_ref.at[pl.ds(pl.multiple_of(half_ref[0] * o_ref.shape[1] + i * BLOCK, BLOCK), BLOCK)], block, sem)
        copy.start()
        copy.wait()
        planes[...] = jnp.zeros_like(planes)
        seen[...] = jnp.zeros_like(seen)

        def scan_chunk(c, carry):
            a = block[:, pl.ds(pl.multiple_of(c * WIDE, WIDE), WIDE)]
            seen[...] = seen[...] + a
            x = a.astype(f32) * (c + 1).astype(f32)
            for s in range(DEG):
                top = planes[s].astype(f32)
                planes[s] = jnp.maximum(top, x).astype(bf16)
                x = jnp.minimum(top, x)
            return carry

        lax.fori_loop(0, vertices // WIDE, scan_chunk, 0)
        lists = lax.fori_loop(0, DEG, lambda p, lists: tuple(place(planes[p], lists)), (jnp.zeros((SUB, BLOCK), f32),) * DEG)
        o_ref[:, pl.ds(pl.multiple_of(i * BLOCK, BLOCK), BLOCK)] = jnp.where(
            degree_of(seen[...]) > DEG, FULL, over_sublanes(list(lists)))
        return carry

    lax.fori_loop(0, o_ref.shape[1] // BLOCK, block_step, 0)


def extract(adj_slab, half, rows):
    vertices = adj_slab.shape[1]
    return pl.pallas_call(
        extract_kernel,
        in_specs=[pl.BlockSpec(memory_space=pltpu.SMEM), pl.BlockSpec(memory_space=pl.ANY)],
        out_specs=pl.BlockSpec(memory_space=pltpu.VMEM),
        out_shape=jax.ShapeDtypeStruct((DEG, rows), f32),
        scratch_shapes=[pltpu.VMEM((BLOCK, vertices), bf16), pltpu.VMEM((BLOCK, WIDE), bf16),
                        pltpu.VMEM((DEG, BLOCK, WIDE), bf16), pltpu.SemaphoreType.DMA],
        name="extract",
    )(half, adj_slab)


def walk_kernel(which_ref, src_ref, weight_ref, lists_ref, out_ref,
                table, queue, sigma, ratio, delta, cand, ids, now, dest, tail_ref, held, rowhot, colhot, bins,
                ids_a, ids_b, meta, sems, *, levels, vertices, scale, compact):
    parts, _, width = lists_ref.shape
    pitch = vertices + SUB
    lane = lax.broadcasted_iota(jnp.int32, (SUB, LANES), 1)
    sub = lax.broadcasted_iota(jnp.int32, (SUB, LANES), 0)
    upper = lane >= HALF
    lane_row = lax.broadcasted_iota(jnp.int32, (1, LANES), 1)
    group_odd = ((lane_row // 32) % 2) == 1
    lane32 = lane_row % 32
    rows_all = queue.shape[0]
    high = vertices // WIDE

    def eight(row):
        return pl.ds(pl.multiple_of(row, SUB), SUB)

    def spread_row(ref, *index):
        return jnp.broadcast_to(ref[(*index[:-1], pl.ds(index[-1], 1), slice(None))], (SUB, LANES))

    def clear(t, carry):
        for k in range(SUB):
            rows = eight((t * SUB + k) * SUB)
            queue[rows, :] = jnp.full((SUB, LANES), -1.0, f32)
            sigma[rows, :] = jnp.zeros((SUB, LANES), f32)
        return carry

    def fetch(quad, row, buf):
        return pltpu.make_async_copy(ids.at[quad, eight(row)], buf[0], sems.at[buf[1]])

    def name(row, q):
        v = jnp.where(q < 0, vertices, q.astype(jnp.int32))
        ids[0, eight(row), :] = v
        ids[1, eight(row), :] = v + pitch

    bufs = (ids_a, 0), (ids_b, 1)
    clear(0, 0)

    srow = lax.broadcasted_iota(jnp.int32, (2 * SUB, LANES), 0)
    slane = lax.broadcasted_iota(jnp.int32, (2 * SUB, LANES), 1)

    def fill(halves, target):
        picks = [jnp.where((srow % SUB) == (slane // 32 + FEW * h), jnp.where(srow < SUB, float(LANES), 1.0), 0.0).astype(bf16)
                 for h in halves]

        def body(pair, most):
            for b in (2 * pair, 2 * pair + 1):
                x = lists_ref[b]
                hi = jnp.floor(x * (1.0 / LANES))
                lo = x - hi * LANES
                both = jnp.concatenate([hi, lo], axis=0).astype(bf16)
                for h, pick in zip(halves, picks):
                    rows = lax.dot_general(both, pick, (((0,), (0,)), ((), ())), preferred_element_type=f32)
                    for k in range(width // LANES):
                        table[pl.ds(pl.multiple_of(target(h, b, k * LANES), SUB), LANES), :] = rows[k * LANES:(k + 1) * LANES]
                for k in range(width // LANES):
                    most = jnp.maximum(most, x[:, k * LANES:(k + 1) * LANES])
            return most

        return lax.fori_loop(0, parts // 2, body, jnp.full((SUB, LANES), EMPTY, f32))

    table[vertices:pitch, :] = jnp.full((SUB, LANES), EMPTY, f32)
    if compact:
        most = fill((0, 1), lambda h, b, col: (b * width + col) * 2 + h * LANES)
        quads = 1
    else:
        table[pitch + vertices:, :] = jnp.full((SUB, LANES), EMPTY, f32)
        most = fill((0,), lambda h, b, col: b * width + col)
        wide = jnp.max(jnp.where(sub >= FEW, most, EMPTY)) >= 0
        quads = jnp.where(wide, 2, 1)

        @pl.when(wide)
        def _():
            fill((1,), lambda h, b, col: pitch + b * width + col)

    bad = jnp.max(most) > vertices
    meta[FAULT] = bad.astype(jnp.int32)

    def gather(rows_of_ids):
        acc = [[jnp.full((1, LANES), EMPTY, f32)] * 2 for _ in rows_of_ids]
        for j in range(32):
            hit = lane32 == j
            for i, id_of in enumerate(rows_of_ids):
                for b in PAIR:
                    acc[i][b] = jnp.where(hit, table[pl.ds(id_of(b * 32 + j), 1), :], acc[i][b])
        return [(jnp.where(group_odd, b, a), pltpu.roll(jnp.where(group_odd, a, b), LANES - 32, 1)) for a, b in acc]

    def gather_slots(ids_s):
        return gather([functools.partial(lambda i, j: ids_s[i, j], i) for i in range(SLOTS)])

    def keep(rows, quad, row):
        for i, pair in enumerate(rows):
            for h in PAIR:
                cand[2 * quad + h, pl.ds(row + i, 1), :] = pair[h]

    def own_row():
        first = jnp.zeros((1, LANES), jnp.int32)
        for j in range(HALF):
            first = jnp.where(lane_row % HALF == j, src_ref[which_ref[0] * HALF + j], first)
        return first.astype(f32)

    def flag(x):
        return jnp.where(x, 1, 0)

    def at(unit, origin):
        return unit & (quads - 1), origin + (unit >> (quads - 1)) * SUB

    def level_step(level, carry):
        base, count = meta[BASE, level], meta[COUNT, level]
        following = base + (count + 7) // SUB * SUB
        batches = jnp.where(following <= CAP, (count + SLOTS - 1) // SLOTS, 0)
        units = batches * quads
        parity = meta[PARITY]

        def on_parity(n, f):
            for k in PAIR:
                @pl.when(n & 1 == k)
                def _():
                    f(bufs[k], bufs[1 - k])

        def unit_step(unit, other, to):
            quad, row = at(unit, base)
            x = [cand[2 * quad + h, eight(row), :] for h in PAIR]

            def search(t, marks):
                marks = list(marks)
                for k in range(SCAN):
                    q = spread_row(queue, t * SCAN + k)
                    for h in PAIR:
                        n = 2 * h + k % 2
                        marks[n] = jnp.where(x[h] == q, 1, marks[n])
                return tuple(marks)

            reach = following + meta[LENGTH]
            marks = lax.fori_loop(0, (reach + SCAN - 1) // SCAN, search, (jnp.zeros((SUB, LANES), jnp.int32),) * 4)
            ahead = unit + 1 < units
            final_unit = unit + 1 == units
            soon = jnp.logical_and(final_unit, meta[AWAIT0] > 0)

            @pl.when(jnp.logical_or(ahead, soon))
            def _():
                fetch(0, base, to).wait()

            even, odd = x
            m, n, k, l = marks
            near_even, near_odd = m | n | flag(even < 0), k | l | flag(odd < 0)

            xr = [pltpu.roll(v, HALF, 1) for v in x]
            turns = [[[pltpu.roll(v, s, 0) if s else v for v in (x[h], xr[h])] for s in range(SUB)] for h in PAIR]
            for s, ((a, b), (c, d)) in enumerate(zip(*turns)):
                near_odd = jnp.where((odd == a) | (odd == b), 1, near_odd)
                if s:
                    after = sub >= s
                    near_even = jnp.where(((even == a) | (even == b)) & after, 1, near_even)
                    near_odd = jnp.where(((odd == c) | (odd == d)) & after, 1, near_odd)

            new = [1 - near_even, 1 - near_odd]
            packed = new[0] + BYTE * new[1]
            across = pltpu.roll(packed, HALF, 1)
            far = [across & (BYTE - 1), across >> SUB]
            both = packed + across
            run, whole = both, both
            for s in (1, 2, 4):
                run = run + jnp.where(sub >= s, pltpu.roll(run, s, 0), 0)
                whole = whole + pltpu.roll(whole, s, 0)
            run = run - both
            tail = tail_ref[...]
            evens = whole & (BYTE - 1)
            begin = [tail + (run & (BYTE - 1)), tail + evens + (run >> SUB)]
            for h in PAIR:
                dest[SUB * h:SUB * h + SUB, :] = jnp.where(new[h] > 0, begin[h] + jnp.where(upper, far[h], 0), -1)
                dest[16 + SUB * h:24 + SUB * h, :] = jnp.where(far[h] > 0, begin[h] + jnp.where(upper, 0, new[h]), -1)
                now[SUB * h:SUB * h + SUB, :] = x[h]
                now[16 + SUB * h:24 + SUB * h, :] = xr[h]
            now[32:40, :] = sigma[eight(row), :]
            tail = tail + evens + (whole >> SUB)
            tail_ref[...] = tail
            passed = SLOTS * ((unit + 1) >> (quads - 1))
            second = SUB + SUB * (1 >> (quads - 1))
            need = jnp.where(sub == 1, SUB, second)
            short = (tail < need) & (held[...] > passed)
            most = jnp.max(jnp.where(sub == 0, tail, flag(short)).astype(f32), axis=1, keepdims=True)
            length = most[0, 0].astype(jnp.int32)
            ready = [most[1, 0] == 0, most[2, 0] == 0]

            def insert(g):
                slots = [eight(following + g * WINDOW + SUB * t) for t in range(WINDOW // SUB)]
                qs = [queue[r, :] for r in slots]
                ss = [sigma[r, :] for r in slots]
                pos = [sub + (g * WINDOW + SUB * t) for t in range(WINDOW // SUB)]
                for h in PAIR:
                    for i in range(SUB):
                        d, e = spread_row(dest, SUB * h + i), spread_row(dest, 16 + SUB * h + i)
                        v, w = spread_row(now, SUB * h + i), spread_row(now, 16 + SUB * h + i)
                        for t in range(WINDOW // SUB):
                            qs[t] = jnp.where(pos[t] == d, v, jnp.where(pos[t] == e, w, qs[t]))
                for i in range(SUB):
                    v, w, sig = spread_row(now, i), spread_row(now, SUB + i), spread_row(now, 32 + i)
                    for t in range(WINDOW // SUB):
                        ss[t] = ss[t] + jnp.where((qs[t] == v) | (qs[t] == w), sig, 0.0)
                for t, r in enumerate(slots):
                    queue[r, :] = qs[t]
                    sigma[r, :] = ss[t]
                return qs

            quad2, row2 = at(unit + 1, base)
            rows = gather_slots(to[0])
            qs = insert(0)
            for n in PAIR:
                name(following + n * SUB, qs[n])
            keep(rows, jnp.where(ahead, quad2, 0), jnp.where(ahead, row2, jnp.where(soon, following, rows_all - SUB)))

            @pl.when(unit + 3 < units)
            def _():
                fetch(*at(unit + 3, base), to).start()

            @pl.when(soon)
            def _():
                meta[GOT] = 1

            def first_of_next(n, when, buf):
                @pl.when(jnp.logical_and(when, meta[(AWAIT0, AWAIT1)[n]] == 0))
                def _():
                    fetch(*at(n, following), buf).start()
                    meta[(AWAIT0, AWAIT1)[n]] = 1

            first_of_next(0, jnp.logical_and(ready[0], unit + 3 == units), to)
            first_of_next(0, jnp.logical_and(ready[0], unit + 2 == units), other)
            first_of_next(1, jnp.logical_and(ready[1], unit + 2 == units), to)
            first_of_next(0, final_unit, to)
            first_of_next(1, final_unit, other)

            groups = (length + WINDOW - 1) // WINDOW
            fits = following + groups * WINDOW <= CAP + WINDOW
            meta[LENGTH] = jnp.where(fits, length, 0)

            @pl.when(jnp.logical_not(fits))
            def _():
                meta[FAULT] = 1

            def more(g, carry):
                insert(g)
                return carry

            lax.fori_loop(1, jnp.where(fits, groups, 0), more, 0)

        tail_ref[...] = jnp.zeros_like(tail_ref)
        meta[LENGTH] = 0

        def open_level(mine, other):
            @pl.when(jnp.logical_and(meta[GOT] == 0, meta[AWAIT0] > 0))
            def _():
                fetch(0, base, mine).wait()
                keep(gather_slots(mine[0]), 0, base)

            @pl.when(jnp.logical_and(units < 2, meta[AWAIT1] > 0))
            def _():
                fetch(0, base, other).wait()

            @pl.when(units > 2)
            def _():
                fetch(*at(2, base), mine).start()

        on_parity(parity, open_level)
        for place_ in (GOT, AWAIT0, AWAIT1):
            meta[place_] = 0

        def any_unit(unit, carry):
            on_parity(parity + unit, functools.partial(unit_step, unit))
            return carry

        lax.fori_loop(0, units, any_unit, 0)
        meta[PARITY] = parity + units

        @pl.when(following > CAP)
        def _():
            meta[FAULT] = 1

        found = jnp.where(meta[FAULT] == 0, meta[LENGTH], 0)
        meta[BASE, level + 1] = following
        meta[COUNT, level + 1] = found

        def settle(g, carry):
            slots = [eight(following + g * WINDOW + SUB * t) for t in range(WINDOW // SUB)]
            @pl.when(g > 0)
            def _():
                for r in slots[:2]:
                    name(r.start, queue[r, :])

            for r in slots[2:]:
                name(r.start, queue[r, :])
            for r in slots:
                s = sigma[r, :]
                sigma[r, :] = s + pltpu.roll(s, HALF, 1)
            return carry

        lax.fori_loop(0, (found + WINDOW - 1) // WINDOW, settle, 0)
        held[...] = tail_ref[...]
        return carry

    for place_ in (GOT, PARITY):
        meta[place_] = 0

    @pl.when(jnp.logical_not(bad))
    def _():
        def seeds(quad, carry):
            row, = gather([lambda j: src_ref[which_ref[0] * HALF + j] + quad * pitch])
            for h in PAIR:
                turn = pltpu.roll(row[h], HALF, 1)
                for n, v in enumerate((jnp.where(upper[:1], turn, row[h]), jnp.where(upper[:1], row[h], turn))):
                    here = pl.ds(SUB + quad * FEW + 2 * h + n, 1)
                    queue[here, :] = jnp.where(v < 0, -1.0, v)
                    sigma[here, :] = jnp.where(v < 0, 0.0, 1.0)
            return carry

        lax.fori_loop(0, quads, seeds, 0)
        for n in range(SLOTS // SUB, 3):
            name(n * SUB, queue[eight(n * SUB), :])
        queue[0:1, :] = own_row()
        held[...] = jnp.full_like(held, FEW * quads)
        meta[BASE, 1] = SUB
        meta[COUNT, 1] = FEW * quads
        bins[...] = jnp.zeros_like(bins)
        for n in PAIR:
            fetch(*at(n, SUB), bufs[n]).start()
            meta[(AWAIT0, AWAIT1)[n]] = 1
        lax.fori_loop(1, rows_all // (SUB * SUB), clear, 0)
        lax.fori_loop(1, levels, level_step, 0)

    @pl.when(bad)
    def _():
        bins[...] = jnp.zeros_like(bins)
        for n in (AWAIT0, AWAIT1):
            meta[n] = 0

    def drain(n, buf):
        @pl.when(meta[(AWAIT0, AWAIT1)[n]] > 0)
        def _():
            fetch(0, 0, buf).wait()

    for k in PAIR:
        @pl.when(meta[PARITY] & 1 == k)
        def _():
            @pl.when(meta[GOT] == 0)
            def _():
                drain(0, bufs[k])

            drain(1, bufs[1 - k])

    good = meta[FAULT] == 0

    @pl.when(good)
    def _():
        last = meta[BASE, levels]
        g_last = weight_ref[levels - 2]

        def seed(g, carry):
            for t in range(WINDOW // SUB):
                r = eight(last + g * WINDOW + SUB * t)
                s = sigma[r, :]
                ratio[r, :] = jnp.where(s > 0, g_last / jnp.where(s > 0, s, 1.0), 0.0)
            return carry

        lax.fori_loop(0, (meta[COUNT, levels] + WINDOW - 1) // WINDOW, seed, 0)

        def back_step(k, carry):
            level = levels - 1 - k
            base, count = meta[BASE, level], meta[COUNT, level]
            nbase, ncount = meta[BASE, level + 1], meta[COUNT, level + 1]
            g_here = weight_ref[jnp.maximum(level - 2, 0)]

            def pull_batch(bt, carry):
                here = eight(base + bt * SLOTS)

                def pull_quad(quad, acc):
                    x = [cand[2 * quad + h, here, :] for h in PAIR]

                    def pull(c, acc):
                        acc = list(acc)
                        for n in range(WINDOW):
                            q = spread_row(queue, nbase + c * WINDOW + n)
                            w = spread_row(ratio, nbase + c * WINDOW + n)
                            acc[n % 2] = acc[n % 2] + jnp.where((x[0] == q) | (x[1] == q), w, 0.0)
                        return tuple(acc)

                    return lax.fori_loop(0, (ncount + WINDOW - 1) // WINDOW, pull, acc)

                acc = lax.fori_loop(0, quads, pull_quad, (jnp.zeros((SUB, LANES), f32),) * 2)
                delta[here, :] = acc[0] + acc[1]
                return carry

            lax.fori_loop(0, (count + SLOTS - 1) // SLOTS, pull_batch, 0)

            def finish(g, carry):
                slots = [eight(base + g * WINDOW + SUB * t) for t in range(WINDOW // SUB)]
                for t, r in enumerate(slots):
                    inside = g * WINDOW + SUB * t < count
                    part, s = delta[r, :], sigma[r, :]
                    d = s * (part + pltpu.roll(part, HALF, 1))
                    w = jnp.where(s > 0, (g_here + d) / jnp.where(s > 0, s, 1.0), 0.0)
                    delta[r, :] = jnp.where(inside, d, part)
                    ratio[r, :] = jnp.where(inside, w, ratio[r, :])
                return carry

            lax.fori_loop(0, (count + WINDOW - 1) // WINDOW, finish, 0)
            return carry

        lax.fori_loop(0, levels - 1, back_step, 0)

        tall = lax.broadcasted_iota(jnp.int32, (WIDE, WIDE), 0).astype(f32).astype(bf16)
        zero = jnp.zeros((WIDE, WIDE), bf16)
        one = zero + 1
        start = meta[BASE, 1]

        def tally(t, carry):
            for u in range(TALLY // 16):
                a, b = eight(start + t * TALLY + u * 16), eight(start + t * TALLY + u * 16 + SUB)
                v = jnp.where(upper, queue[b, :], queue[a, :])
                d = jnp.where(upper, delta[b, :], delta[a, :])
                hi = jnp.floor(v * (1.0 / WIDE))
                lo = v - hi * WIDE
                d_hi = d.astype(bf16).astype(f32)
                d_mid = (d - d_hi).astype(bf16).astype(f32)
                d_lo = d - d_hi - d_mid
                for p in range(0, SUB, 2):
                    cols = slice((u * SUB + p) * LANES, (u * SUB + p + 2) * LANES)

                    def pair(x):
                        return jnp.concatenate([x[p:p + 1], x[p + 1:p + 2]], axis=1).astype(bf16)

                    colhot[:, cols] = jnp.where(tall == pair(lo), one, zero)
                    match = tall[:high] == pair(hi)
                    for n, x in enumerate((d_hi, d_mid, d_lo)):
                        rowhot[n * high:(n + 1) * high, cols] = jnp.where(match, pair(x), zero[:high])
            bins[...] += lax.dot_general(rowhot[...], colhot[...], TURN, preferred_element_type=f32)
            return carry

        for t in range(TALLY // SUB):
            delta[eight(last + t * SUB), :] = jnp.zeros((SUB, LANES), f32)
        lax.fori_loop(0, (last - start + TALLY - 1) // TALLY, tally, 0)

    blocks = out_ref.shape[0]
    per = high // blocks
    total = (bins[:high] + bins[high:2 * high] + bins[2 * high:]) * scale
    fault = jnp.where(good, 0.0, 1.0)
    for b in range(blocks):
        for n in PAIR:
            out_ref[b, n * per:(n + 1) * per, :] = total[b * per:(b + 1) * per, n * LANES:(n + 1) * LANES]
        out_ref[b, 2 * per:, :] = jnp.full((SUB, LANES), fault, f32)


def walk(which, sources, weights, lists, *, blocks, vertices, scale, compact):
    levels = weights.shape[0] + 1
    rows = CAP + 4 * WINDOW
    high = LANES // blocks + SUB
    vm = pltpu.VMEM
    queue = vm((rows, LANES), f32)
    parts = 3 * (vertices // WIDE)
    return pl.pallas_call(
        functools.partial(walk_kernel, levels=levels, vertices=vertices, scale=scale, compact=compact),
        in_specs=[pl.BlockSpec(memory_space=pltpu.SMEM)] * 3 + [pl.BlockSpec(memory_space=pltpu.VMEM)],
        out_specs=pl.BlockSpec(memory_space=pltpu.VMEM),
        out_shape=jax.ShapeDtypeStruct((blocks, high, LANES), f32),
        scratch_shapes=[
            vm(((1 if compact else 2) * (vertices + SUB), LANES), f32), queue, queue, queue, queue,
            vm((4, rows, LANES), f32), vm((2, rows, LANES), jnp.int32),
            vm((40, LANES), f32), vm((32, LANES), jnp.int32), vm((SUB, LANES), jnp.int32), vm((SUB, LANES), jnp.int32),
            vm((parts, TALLY // 2 * LANES), bf16), vm((WIDE, TALLY // 2 * LANES), bf16), vm((parts, WIDE), f32),
            pltpu.SMEM((SLOTS, LANES), jnp.int32), pltpu.SMEM((SLOTS, LANES), jnp.int32), pltpu.SMEM((3, 16), jnp.int32),
            pltpu.SemaphoreType.DMA((2,)),
        ],
        compiler_params=pltpu.CompilerParams(
            vmem_limit_bytes=48 * 1024 * 1024),
        name="walk",
    )(which, sources, weights, lists)


def share_kernel(src, graph, x_ref, o_ref, own_sem, send_sem, recv_sem):
    y, g = lax.axis_index("src"), lax.axis_index("graph")
    others = [((y + i) % src, (g + k) % graph) for i, k in everyone(src, graph)][1:]
    hello(others)
    await_hello(others)
    mine = g * src + y
    own = pltpu.make_async_copy(x_ref, o_ref.at[mine], own_sem)
    own.start()
    copies = []
    for n, (py, pg) in enumerate(others):
        copies.append(pltpu.make_async_remote_copy(
            src_ref=x_ref, dst_ref=o_ref.at[mine], send_sem=send_sem.at[n], recv_sem=recv_sem.at[n],
            device_id={"src": py, "graph": pg}, device_id_type=MESH))
        copies[-1].start()
    own.wait()
    for c in copies:
        c.wait()


def share(x, src, graph):
    n = src * graph
    return pl.pallas_call(
        functools.partial(share_kernel, src, graph),
        in_specs=[pl.BlockSpec(memory_space=pltpu.VMEM)],
        out_specs=pl.BlockSpec(memory_space=pltpu.VMEM),
        out_shape=jax.ShapeDtypeStruct((n,) + x.shape, x.dtype),
        scratch_shapes=[pltpu.SemaphoreType.DMA, pltpu.SemaphoreType.DMA((n - 1,)), pltpu.SemaphoreType.DMA((n - 1,))],
        compiler_params=pltpu.CompilerParams(collective_id=2, has_side_effects=True),
        name="share",
    )(x)


def total_kernel(src, graph, x_ref, o_ref, got, own_sem, send_sem, recv_sem):
    y, g = lax.axis_index("src"), lax.axis_index("graph")
    others = [((y + i) % src, (g + k) % graph) for i, k in everyone(src, graph)][1:]
    hello(others)
    mine = g * src + y
    own = pltpu.make_async_copy(x_ref.at[g], got.at[mine], own_sem)
    own.start()
    await_hello(others)
    copies = []
    for n, (py, pg) in enumerate(others):
        copies.append(pltpu.make_async_remote_copy(
            src_ref=x_ref.at[pg], dst_ref=got.at[mine], send_sem=send_sem.at[n], recv_sem=recv_sem.at[n],
            device_id={"src": py, "graph": pg}, device_id_type=MESH))
        copies[-1].start()
    own.wait()
    for c in copies:
        c.wait()
    acc = got[0]
    for n in range(1, src * graph):
        acc = acc + got[n]
    o_ref[...] = acc


def total(x, src, graph, collective_id):
    n = src * graph
    return pl.pallas_call(
        functools.partial(total_kernel, src, graph),
        in_specs=[pl.BlockSpec(memory_space=pltpu.VMEM)],
        out_specs=pl.BlockSpec(memory_space=pltpu.VMEM),
        out_shape=jax.ShapeDtypeStruct(x.shape[1:], x.dtype),
        scratch_shapes=[pltpu.VMEM((n,) + x.shape[1:], x.dtype), pltpu.SemaphoreType.DMA,
                        pltpu.SemaphoreType.DMA((n - 1,)), pltpu.SemaphoreType.DMA((n - 1,))],
        compiler_params=pltpu.CompilerParams(collective_id=collective_id, has_side_effects=True),
        name="total",
    )(pltpu.with_memory_space_constraint(x, pltpu.VMEM))


def dense(adj_slab, src_local, level_weight, src, graph):
    slab_rows, vertex_count = adj_slab.shape
    src_count = src_local.shape[0]
    levels = level_weight.shape[0] + 1
    row_start = lax.axis_index("graph") * slab_rows
    vertex_ids = row_start + lax.broadcasted_iota(jnp.int32, (slab_rows, 1), 0)
    first = jnp.where(vertex_ids == src_local[None, :], 1.0, 0.0).astype(f32)

    def forward(carry, unused):
        sigma, seen = carry
        partial = jnp.einsum("uv,us->vs", adj_slab, sigma, preferred_element_type=f32, precision=exact_precision)
        parts = lax.all_to_all(partial.reshape(graph, slab_rows, src_count), "graph", 0, 0)
        sigma = jnp.sum(parts, axis=0) * (1.0 - seen)
        seen = jnp.maximum(seen, jnp.where(sigma > 0, 1.0, 0.0))
        return (sigma, seen), sigma

    _, sigmas = lax.scan(forward, (first, first), None, length=levels)

    def backward(carry, xs):
        delta, acc = carry
        upper, lower, weight = xs
        reached = upper > 0
        ratio = jnp.where(reached, (weight + delta) / jnp.where(reached, upper, 1.0), 0.0)
        gathered = lax.all_to_all(jnp.broadcast_to(ratio[None], (graph,) + ratio.shape), "graph", 0, 0)
        pulled = jnp.einsum("uv,vs->us", adj_slab, gathered.reshape(vertex_count, src_count),
                            preferred_element_type=f32, precision=exact_precision)
        delta = lower * pulled
        return (delta, acc + delta), None

    zero = jnp.zeros_like(first)
    (_, acc), _ = lax.scan(backward, (zero, zero), (sigmas[1:][::-1], sigmas[:-1][::-1], level_weight[::-1]))
    scale = vertex_count / (src_count * src * levels ** 3)
    mine = jnp.sum(acc, axis=1) * scale
    both = lax.all_to_all(jnp.broadcast_to(mine.reshape(1, -1, LANES), (src, slab_rows // LANES, LANES)), "src", 0, 0)
    return jnp.sum(both, axis=0).reshape(slab_rows)


def solution(mesh):
    src, graph = mesh.shape["src"], mesh.shape["graph"]

    def device_program(adj_slab, src_local, level_weight):
        slab_rows, vertex_count = adj_slab.shape
        levels = level_weight.shape[0] + 1
        scale = vertex_count / (HALF * src * graph * levels ** 3)
        which = lax.axis_index("graph").astype(jnp.int32).reshape(1)

        def finish(lists, compact, collective_id, other):
            parts = walk(which, src_local, level_weight, lists, blocks=graph, vertices=vertex_count, scale=scale, compact=compact)
            summed = total(parts, src, graph, collective_id)
            rows = slab_rows // LANES

            def plain():
                return summed[:rows].reshape(2, -1, LANES).transpose(1, 0, 2).reshape(slab_rows)

            return lax.cond(summed[rows, 0] > 0, other, plain)

        def dense_path():
            return dense(adj_slab, src_local, level_weight, src, graph)

        def general_path():
            half = lax.axis_index("src").astype(jnp.int32).reshape(1)
            return finish(share(extract(adj_slab, half, slab_rows // src), src, graph), False, 3, dense_path)

        return finish(collect(adj_slab, src, graph), True, 1, general_path)

    return jax.shard_map(device_program, mesh=mesh,
                         in_specs=(P(("batch", "graph"), None), P(("batch", "src")), P(None)),
                         out_specs=P(("batch", "graph")), check_vma=False)
```

```python
import functools

import jax
import jax.numpy as jnp
from jax import lax
from jax.experimental import pallas as pl
from jax.experimental.pallas import tpu as pltpu
from jax.sharding import PartitionSpec as P

MESH = pl.DeviceIdType.MESH
exact_precision = lax.Precision.HIGHEST
f32, bf16 = jnp.float32, jnp.bfloat16

LANES, SUB = 128, 8
WIDE = 256
DEG, FEW = 8, 4
EMPTY = -2.0
FULL = 32767.0
TURN = (((1,), (1,)), ((), ()))
BLOCK = 128
READS = 4
STEP = 32
HALF = 64
SLOTS = 8
WINDOW = 48
SCAN = 32
CAP = 1024
TALLY = 96
PAIR = (0, 1)
BYTE = 256
BASE, COUNT = 0, 1
FAULT, LENGTH, GOT, PARITY, AWAIT0, AWAIT1, REACHED, SHORT0, SHORT1 = ((2, n) for n in range(9))


def everyone(src, graph):
    return [(y, g) for y in range(src) for g in range(graph)]


def hello(peers):
    for y, g in peers:
        pl.semaphore_signal(pltpu.get_barrier_semaphore(), inc=1, device_id={"src": y, "graph": g}, device_id_type=MESH)


def await_hello(peers):
    pl.semaphore_wait(pltpu.get_barrier_semaphore(), len(peers))


def place(plane, lists):
    lists = list(lists)
    row_i = lax.broadcasted_iota(jnp.int32, (WIDE, WIDE), 0)
    col_i = lax.broadcasted_iota(jnp.int32, (WIDE, WIDE), 1)
    eye = jnp.where(row_i == col_i, float(WIDE), 0.0).astype(bf16)
    flipped = lax.dot_general(eye, plane, TURN, preferred_element_type=f32)
    lane_id = lax.broadcasted_iota(jnp.int32, (SUB, flipped.shape[1]), 0).astype(f32)
    for g in range(WIDE // SUB):
        x = flipped[g * SUB:(g + 1) * SUB] + (lane_id + float(g * SUB))
        for s in range(len(lists)):
            hi = jnp.maximum(lists[s], x)
            if s < len(lists) - 1:
                x = jnp.minimum(lists[s], x)
            lists[s] = hi
    return lists


def sort(lists):
    gap = len(lists) // 2
    while gap:
        for s in range(len(lists)):
            if not s & gap:
                lists[s], lists[s + gap] = jnp.maximum(lists[s], lists[s + gap]), jnp.minimum(lists[s], lists[s + gap])
        gap //= 2
    return lists


def over_sublanes(lists):
    size = len(lists)
    for shift in (4, 2, 1):
        other = [pltpu.roll(v, shift, 0) for v in lists]
        lists = sort([jnp.maximum(lists[s], other[size - 1 - s]) for s in range(size)])
    out = jnp.full(lists[0].shape, EMPTY, f32)
    sub = lax.broadcasted_iota(jnp.int32, out.shape, 0)
    for s in range(size):
        out = jnp.where(sub == s, jnp.where(lists[s] >= WIDE, lists[s] - WIDE, EMPTY), out)
    return out


def degree_of(seen):
    return lax.dot_general(jnp.ones((SUB, WIDE), bf16), seen, TURN, preferred_element_type=f32)


def collect_kernel(src, graph, a_ref, o_ref, bufs, tops, mine, sems, own_sem, send_sems, recv_sems):
    vertices = a_ref.shape[1]
    pairs, chunks = mine.shape[1] // LANES, vertices // WIDE
    blocks = 2 * pairs
    y, g = lax.axis_index("src"), lax.axis_index("graph")
    others = [((y + i) % src, (g + k) % graph) for i, k in everyone(src, graph)][1:]
    me = g * src + y
    height = 4 * SUB
    pieces = BLOCK // height

    def fetch(i, t):
        rows = pl.ds(pl.multiple_of((y * blocks + i) * BLOCK + t * height, height), height)
        here = pl.ds(pl.multiple_of(t * height, height), height)
        return pltpu.make_async_copy(a_ref.at[rows], bufs.at[i % READS, here], sems.at[i % READS, t])

    def send(n, cols):
        py, pg = others[n]
        return pltpu.make_async_remote_copy(
            src_ref=mine.at[:, cols], dst_ref=o_ref.at[me, :, cols], send_sem=send_sems.at[n], recv_sem=recv_sems.at[n],
            device_id={"src": py, "graph": pg}, device_id_type=MESH)

    def send_pair(p):
        for n in range(len(others)):
            send(n, pl.ds(pl.multiple_of(p * LANES, LANES), LANES)).start()

    hello(others)
    for i in range(READS - 1):
        for t in range(pieces):
            fetch(i, t).start()
    none = jnp.zeros((SUB, 2 * BLOCK), f32)

    def scan(i, first):
        @pl.when(i + READS - 1 < blocks)
        def _():
            for t in range(pieces):
                fetch(i + READS - 1, t).start()

        def scan_rows(t, carry):
            fetch(i, t).wait()
            here = pl.ds(pl.multiple_of(t * height, height), height)

            def scan_chunks(c, state):
                top, low, seen, sums, value = state
                for k in range(STEP):
                    a = bufs[i % READS, here, pl.ds(pl.multiple_of((c * STEP + k) * WIDE, WIDE), WIDE)]
                    x = a * value
                    low = jnp.maximum(low, jnp.minimum(top, x))
                    top = jnp.maximum(top, x)
                    seen = seen + a
                    sums = sums + x
                    value = value + 1
                return top, low, seen, sums, value

            zero = jnp.zeros((height, WIDE), bf16)
            top, low, seen, sums, _ = lax.fori_loop(0, chunks // STEP, scan_chunks, (zero,) * 4 + (zero + 1,))
            for n, v in enumerate((top, low, (sums - top) - low, seen)):
                tops[n, pl.ds(pl.multiple_of(first + t * height, height), height), :] = v
            return carry

        lax.fori_loop(0, pieces, scan_rows, 0)

    def pair_step(p, carry):
        for h in range(2):
            scan(2 * p + h, h * BLOCK)
        seen = tops[3]
        crowd = seen[:SUB]
        for k in range(1, 2 * BLOCK // SUB):
            crowd = jnp.maximum(crowd, seen[k * SUB:(k + 1) * SUB])
        crowd = jnp.max(crowd.astype(f32), axis=0, keepdims=True)
        a, b, c = place(tops[0], (none,) * 4), place(tops[1], (none,) * 2), place(tops[2], (none,))
        rest = [jnp.maximum(b[0], c[0]), jnp.minimum(b[0], c[0])]
        rest = [rest[0], jnp.maximum(b[1], rest[1]), jnp.minimum(b[1], rest[1])]
        lists = over_sublanes(sort([a[0]] + [jnp.maximum(a[s + 1], rest[2 - s]) for s in range(3)]))
        lists = jnp.where((crowd > 3) | (degree_of(seen) > 4), FULL, lists)
        even, odd = lists[:, :BLOCK], lists[:, BLOCK:]
        sub = lax.broadcasted_iota(jnp.int32, even.shape, 0)
        mine[:, pl.ds(pl.multiple_of(p * LANES, LANES), LANES)] = jnp.where(sub < 4, even, pltpu.roll(odd, 4, 0))

        @pl.when(p == 1)
        def _():
            await_hello(others)

        @pl.when(p > 0)
        def _():
            send_pair(p - 1)

        return carry

    lax.fori_loop(0, pairs, pair_step, 0)
    own = pltpu.make_async_copy(mine, o_ref.at[me], own_sem)
    send_pair(pairs - 1)
    own.start()
    own.wait()
    for n in range(len(others)):
        send(n, slice(None)).wait()


def collect(adj_slab, src, graph):
    rows, vertices = adj_slab.shape
    n = src * graph
    mine = (SUB, rows // src // 2)
    return pl.pallas_call(
        functools.partial(collect_kernel, src, graph),
        in_specs=[pl.BlockSpec(memory_space=pl.ANY)],
        out_specs=pl.BlockSpec(memory_space=pltpu.VMEM),
        out_shape=jax.ShapeDtypeStruct((n,) + mine, f32),
        scratch_shapes=[pltpu.VMEM((READS, BLOCK, vertices), bf16), pltpu.VMEM((4, 2 * BLOCK, WIDE), bf16), pltpu.VMEM(mine, f32),
                        pltpu.SemaphoreType.DMA((READS, BLOCK // (4 * SUB))), pltpu.SemaphoreType.DMA,
                        pltpu.SemaphoreType.DMA((n - 1,)), pltpu.SemaphoreType.DMA((n - 1,))],
        compiler_params=pltpu.CompilerParams(collective_id=0, has_side_effects=True, vmem_limit_bytes=40 * 1024 * 1024),
        name="collect",
    )(adj_slab)


def extract_kernel(half_ref, a_ref, o_ref, block, seen, planes, sem):
    vertices = a_ref.shape[1]

    def block_step(i, carry):
        copy = pltpu.make_async_copy(
            a_ref.at[pl.ds(pl.multiple_of(half_ref[0] * o_ref.shape[1] + i * BLOCK, BLOCK), BLOCK)], block, sem)
        copy.start()
        copy.wait()
        planes[...] = jnp.zeros_like(planes)
        seen[...] = jnp.zeros_like(seen)

        def scan_chunk(c, carry):
            a = block[:, pl.ds(pl.multiple_of(c * WIDE, WIDE), WIDE)]
            seen[...] = seen[...] + a
            x = a.astype(f32) * (c + 1).astype(f32)
            for s in range(DEG):
                top = planes[s].astype(f32)
                planes[s] = jnp.maximum(top, x).astype(bf16)
                x = jnp.minimum(top, x)
            return carry

        lax.fori_loop(0, vertices // WIDE, scan_chunk, 0)
        lists = lax.fori_loop(0, DEG, lambda p, lists: tuple(place(planes[p], lists)), (jnp.zeros((SUB, BLOCK), f32),) * DEG)
        o_ref[:, pl.ds(pl.multiple_of(i * BLOCK, BLOCK), BLOCK)] = jnp.where(
            degree_of(seen[...]) > DEG, FULL, over_sublanes(list(lists)))
        return carry

    lax.fori_loop(0, o_ref.shape[1] // BLOCK, block_step, 0)


def extract(adj_slab, half, rows):
    vertices = adj_slab.shape[1]
    return pl.pallas_call(
        extract_kernel,
        in_specs=[pl.BlockSpec(memory_space=pltpu.SMEM), pl.BlockSpec(memory_space=pl.ANY)],
        out_specs=pl.BlockSpec(memory_space=pltpu.VMEM),
        out_shape=jax.ShapeDtypeStruct((DEG, rows), f32),
        scratch_shapes=[pltpu.VMEM((BLOCK, vertices), bf16), pltpu.VMEM((BLOCK, WIDE), bf16),
                        pltpu.VMEM((DEG, BLOCK, WIDE), bf16), pltpu.SemaphoreType.DMA],
        name="extract",
    )(half, adj_slab)


def walk_kernel(which_ref, src_ref, weight_ref, lists_ref, out_ref,
                table, queue, sigma, ratio, delta, cand, ids, now, dest, tail_ref, held, rowhot, colhot, bins,
                ids_a, ids_b, meta, sems, *, levels, vertices, scale, compact):
    parts, _, width = lists_ref.shape
    pitch = vertices + SUB
    lane = lax.broadcasted_iota(jnp.int32, (SUB, LANES), 1)
    sub = lax.broadcasted_iota(jnp.int32, (SUB, LANES), 0)
    upper = lane >= HALF
    lane_row = lax.broadcasted_iota(jnp.int32, (1, LANES), 1)
    group_odd = ((lane_row // 32) % 2) == 1
    lane32 = lane_row % 32
    rows_all = queue.shape[0]
    high = vertices // WIDE

    def eight(row):
        return pl.ds(pl.multiple_of(row, SUB), SUB)

    def spread_row(ref, *index):
        return jnp.broadcast_to(ref[(*index[:-1], pl.ds(index[-1], 1), slice(None))], (SUB, LANES))

    def clear(t, carry):
        for k in range(SUB):
            rows = eight((t * SUB + k) * SUB)
            queue[rows, :] = jnp.full((SUB, LANES), -1.0, f32)
            sigma[rows, :] = jnp.zeros((SUB, LANES), f32)
        return carry

    def fetch(quad, row, buf):
        return pltpu.make_async_copy(ids.at[quad, eight(row)], buf[0], sems.at[buf[1]])

    def name(row, q):
        v = jnp.where(q < 0, vertices, q.astype(jnp.int32))
        ids[0, eight(row), :] = v
        ids[1, eight(row), :] = v + pitch

    bufs = (ids_a, 0), (ids_b, 1)
    clear(0, 0)

    srow = lax.broadcasted_iota(jnp.int32, (2 * SUB, LANES), 0)
    slane = lax.broadcasted_iota(jnp.int32, (2 * SUB, LANES), 1)

    def fill(halves, target):
        picks = [jnp.where((srow % SUB) == (slane // 32 + FEW * h), jnp.where(srow < SUB, float(LANES), 1.0), 0.0).astype(bf16)
                 for h in halves]

        def body(step, most):
            for b in (FEW * step + n for n in range(FEW)):
                x = lists_ref[b]
                hi = jnp.floor(x * (1.0 / LANES))
                lo = x - hi * LANES
                both = jnp.concatenate([hi, lo], axis=0).astype(bf16)
                for h, pick in zip(halves, picks):
                    rows = lax.dot_general(both, pick, (((0,), (0,)), ((), ())), preferred_element_type=f32)
                    for k in range(width // LANES):
                        table[pl.ds(pl.multiple_of(target(h, b, k * LANES), SUB), LANES), :] = rows[k * LANES:(k + 1) * LANES]
                for k in range(width // LANES):
                    most = jnp.maximum(most, x[:, k * LANES:(k + 1) * LANES])
            return most

        return lax.fori_loop(0, parts // FEW, body, jnp.full((SUB, LANES), EMPTY, f32))

    table[vertices:pitch, :] = jnp.full((SUB, LANES), EMPTY, f32)
    if compact:
        most = fill((0, 1), lambda h, b, col: (b * width + col) * 2 + h * LANES)
        quads = 1
    else:
        table[pitch + vertices:, :] = jnp.full((SUB, LANES), EMPTY, f32)
        most = fill((0,), lambda h, b, col: b * width + col)
        wide = jnp.max(jnp.where(sub >= FEW, most, EMPTY)) >= 0
        quads = jnp.where(wide, 2, 1)

        @pl.when(wide)
        def _():
            fill((1,), lambda h, b, col: pitch + b * width + col)

    bad = jnp.max(most) > vertices
    meta[FAULT] = bad.astype(jnp.int32)

    def gather(rows_of_ids):
        acc = [[jnp.full((1, LANES), EMPTY, f32)] * 2 for _ in rows_of_ids]
        for j in range(32):
            hit = lane32 == j
            for i, id_of in enumerate(rows_of_ids):
                for b in PAIR:
                    acc[i][b] = jnp.where(hit, table[pl.ds(id_of(b * 32 + j), 1), :], acc[i][b])
        return [(jnp.where(group_odd, b, a), pltpu.roll(jnp.where(group_odd, a, b), LANES - 32, 1)) for a, b in acc]

    def gather_slots(ids_s, slots=SLOTS):
        return gather([functools.partial(lambda i, j: ids_s[i, j], i) for i in range(slots)])

    def keep(rows, quad, row):
        for i, pair in enumerate(rows):
            for h in PAIR:
                cand[2 * quad + h, pl.ds(row + i, 1), :] = pair[h]

    def own_row():
        first = jnp.zeros((1, LANES), jnp.int32)
        for j in range(HALF):
            first = jnp.where(lane_row % HALF == j, src_ref[which_ref[0] * HALF + j], first)
        return first.astype(f32)

    def flag(x):
        return jnp.where(x, 1, 0)

    def at(unit, origin):
        return unit & (quads - 1), origin + (unit >> (quads - 1)) * SUB

    def level_step(level, carry):
        base, count = meta[BASE, level], meta[COUNT, level]
        following = base + (count + 7) // SUB * SUB
        batches = jnp.where(following <= CAP, (count + SLOTS - 1) // SLOTS, 0)
        units = batches * quads
        parity = meta[PARITY]

        def on_parity(n, f):
            for k in PAIR:
                @pl.when(n & 1 == k)
                def _():
                    f(bufs[k], bufs[1 - k])

        def unit_step(unit, other, to):
            quad, row = at(unit, base)
            x = [cand[2 * quad + h, eight(row), :] for h in PAIR]

            def search(t, marks):
                marks = list(marks)
                for k in range(SCAN):
                    q = spread_row(queue, t * SCAN + k)
                    for h in PAIR:
                        n = 2 * h + k % 2
                        marks[n] = jnp.where(x[h] == q, 1, marks[n])
                return tuple(marks)

            reach = following + meta[LENGTH]
            marks = lax.fori_loop(0, (reach + SCAN - 1) // SCAN, search, (jnp.zeros((SUB, LANES), jnp.int32),) * 4)
            ahead = unit + 1 < units
            final_unit = unit + 1 == units
            soon = jnp.logical_and(final_unit, meta[AWAIT0] > 0)

            @pl.when(jnp.logical_or(ahead, soon))
            def _():
                fetch(0, base, to).wait()

            def insert(g):
                slots = [eight(following + g * WINDOW + SUB * t) for t in range(WINDOW // SUB)]
                qs = [queue[r, :] for r in slots]
                ss = [sigma[r, :] for r in slots]
                pos = [sub + (g * WINDOW + SUB * t) for t in range(WINDOW // SUB)]
                for h in PAIR:
                    for i in range(SUB):
                        d, e = spread_row(dest, SUB * h + i), spread_row(dest, 16 + SUB * h + i)
                        v, w = spread_row(now, SUB * h + i), spread_row(now, 16 + SUB * h + i)
                        for t in range(WINDOW // SUB):
                            qs[t] = jnp.where(pos[t] == d, v, jnp.where(pos[t] == e, w, qs[t]))
                for i in range(SUB):
                    v, w, sig = spread_row(now, i), spread_row(now, SUB + i), spread_row(now, 32 + i)
                    for t in range(WINDOW // SUB):
                        ss[t] = ss[t] + jnp.where((qs[t] == v) | (qs[t] == w), sig, 0.0)
                for t, r in enumerate(slots):
                    queue[r, :] = qs[t]
                    sigma[r, :] = ss[t]
                return qs

            def core(looking):
                even, odd = x
                m, n, k, l = marks
                near_even, near_odd = m | n | flag(even < 0), k | l | flag(odd < 0)

                xr = [pltpu.roll(v, HALF, 1) for v in x]
                turns = [[[pltpu.roll(v, s, 0) if s else v for v in (x[h], xr[h])] for s in range(SUB)] for h in PAIR]
                for s, ((a, b), (c, d)) in enumerate(zip(*turns)):
                    near_odd = jnp.where((odd == a) | (odd == b), 1, near_odd)
                    if s:
                        after = sub >= s
                        near_even = jnp.where(((even == a) | (even == b)) & after, 1, near_even)
                        near_odd = jnp.where(((odd == c) | (odd == d)) & after, 1, near_odd)

                new = [1 - near_even, 1 - near_odd]
                packed = new[0] + BYTE * new[1]
                across = pltpu.roll(packed, HALF, 1)
                far = [across & (BYTE - 1), across >> SUB]
                both = packed + across
                run, whole = both, both
                for s in (1, 2, 4):
                    run = run + jnp.where(sub >= s, pltpu.roll(run, s, 0), 0)
                    whole = whole + pltpu.roll(whole, s, 0)
                run = run - both
                tail = tail_ref[...]
                evens = whole & (BYTE - 1)
                begin = [tail + (run & (BYTE - 1)), tail + evens + (run >> SUB)]
                for h in PAIR:
                    dest[SUB * h:SUB * h + SUB, :] = jnp.where(new[h] > 0, begin[h] + jnp.where(upper, far[h], 0), -1)
                    dest[16 + SUB * h:24 + SUB * h, :] = jnp.where(far[h] > 0, begin[h] + jnp.where(upper, 0, new[h]), -1)
                    now[SUB * h:SUB * h + SUB, :] = x[h]
                    now[16 + SUB * h:24 + SUB * h, :] = xr[h]
                part = sigma[eight(row), :]
                now[32:40, :] = part + pltpu.roll(part, HALF, 1)
                tail = tail + evens + (whole >> SUB)
                tail_ref[...] = tail
                passed = SLOTS * ((unit + 1) >> (quads - 1))
                second = SUB + SUB * (1 >> (quads - 1))
                need = jnp.where(sub == 1, SUB, second)
                short = (tail < need) & (held[...] > passed)
                most = jnp.max(jnp.where(sub == 0, tail, flag(short)).astype(f32), axis=1, keepdims=True)
                meta[REACHED] = most[0, 0].astype(jnp.int32)
                for n in PAIR:
                    meta[(SHORT0, SHORT1)[n]] = most[n + 1, 0].astype(jnp.int32)

                if looking:
                    quad2, row2 = at(unit + 1, base)
                    rows = gather_slots(to[0])
                qs = insert(0)
                for n in PAIR:
                    name(following + n * SUB, qs[n])
                if looking:
                    keep(rows, jnp.where(ahead, quad2, 0), jnp.where(ahead, row2, following))

            look = jnp.logical_or(ahead, soon)
            for looking in PAIR:
                @pl.when(look == (looking > 0))
                def _():
                    core(looking)

            length = meta[REACHED]
            ready = [meta[n] == 0 for n in (SHORT0, SHORT1)]

            @pl.when(unit + 3 < units)
            def _():
                fetch(*at(unit + 3, base), to).start()

            @pl.when(soon)
            def _():
                meta[GOT] = 1

            def first_of_next(n, when, buf):
                @pl.when(jnp.logical_and(when, meta[(AWAIT0, AWAIT1)[n]] == 0))
                def _():
                    fetch(*at(n, following), buf).start()
                    meta[(AWAIT0, AWAIT1)[n]] = 1

            first_of_next(0, jnp.logical_and(ready[0], unit + 3 == units), to)
            first_of_next(0, jnp.logical_and(ready[0], unit + 2 == units), other)
            first_of_next(1, jnp.logical_and(ready[1], unit + 2 == units), to)
            first_of_next(0, final_unit, to)
            first_of_next(1, final_unit, other)

            groups = (length + WINDOW - 1) // WINDOW
            fits = following + groups * WINDOW <= CAP + WINDOW
            meta[LENGTH] = jnp.where(fits, length, 0)

            @pl.when(jnp.logical_not(fits))
            def _():
                meta[FAULT] = 1

            def more(g, carry):
                insert(g)
                return carry

            lax.fori_loop(1, jnp.where(fits, groups, 0), more, 0)

        tail_ref[...] = jnp.zeros_like(tail_ref)
        meta[LENGTH] = 0

        def open_level(mine, other):
            @pl.when(jnp.logical_and(meta[GOT] == 0, meta[AWAIT0] > 0))
            def _():
                fetch(0, base, mine).wait()
                keep(gather_slots(mine[0]), 0, base)

            @pl.when(jnp.logical_and(units < 2, meta[AWAIT1] > 0))
            def _():
                fetch(0, base, other).wait()

            @pl.when(units > 2)
            def _():
                fetch(*at(2, base), mine).start()

        on_parity(parity, open_level)
        for place_ in (GOT, AWAIT0, AWAIT1):
            meta[place_] = 0

        def any_unit(unit, carry):
            on_parity(parity + unit, functools.partial(unit_step, unit))
            return carry

        lax.fori_loop(0, units, any_unit, 0)
        meta[PARITY] = parity + units

        @pl.when(following > CAP)
        def _():
            meta[FAULT] = 1

        found = jnp.where(meta[FAULT] == 0, meta[LENGTH], 0)
        meta[BASE, level + 1] = following
        meta[COUNT, level + 1] = found

        def names(t, carry):
            row = following + t * SUB
            name(row, queue[eight(row), :])
            return carry

        lax.fori_loop(2, (found + SUB - 1) // SUB, names, 0)
        held[...] = tail_ref[...]
        return carry

    for place_ in (GOT, PARITY):
        meta[place_] = 0

    @pl.when(jnp.logical_not(bad))
    def _():
        def seeds(quad, carry):
            row, = gather([lambda j: src_ref[which_ref[0] * HALF + j] + quad * pitch])
            for h in PAIR:
                turn = pltpu.roll(row[h], HALF, 1)
                for n, v in enumerate((jnp.where(upper[:1], turn, row[h]), jnp.where(upper[:1], row[h], turn))):
                    here = pl.ds(SUB + quad * FEW + 2 * h + n, 1)
                    queue[here, :] = jnp.where(v < 0, -1.0, v)
                    sigma[here, :] = jnp.where((v < 0) | upper[:1], 0.0, 1.0)
            return carry

        lax.fori_loop(0, quads, seeds, 0)
        for n in range(SLOTS // SUB, 3):
            name(n * SUB, queue[eight(n * SUB), :])
        queue[0:1, :] = own_row()
        held[...] = jnp.full_like(held, FEW * quads)
        meta[BASE, 1] = SUB
        meta[COUNT, 1] = FEW * quads
        bins[...] = jnp.zeros_like(bins)
        for n in PAIR:
            fetch(*at(n, SUB), bufs[n]).start()
            meta[(AWAIT0, AWAIT1)[n]] = 1
        lax.fori_loop(1, rows_all // (SUB * SUB), clear, 0)
        if compact:
            for h in PAIR:
                cand[h, eight(SUB), :] = jnp.full((SUB, LANES), EMPTY, f32)
            fetch(0, SUB, bufs[0]).wait()
            keep(gather_slots(ids_a, FEW), 0, SUB)
            meta[GOT] = 1
        lax.fori_loop(1, levels, level_step, 0)

    @pl.when(bad)
    def _():
        bins[...] = jnp.zeros_like(bins)
        for n in (AWAIT0, AWAIT1):
            meta[n] = 0

    def drain(n, buf):
        @pl.when(meta[(AWAIT0, AWAIT1)[n]] > 0)
        def _():
            fetch(0, 0, buf).wait()

    for k in PAIR:
        @pl.when(meta[PARITY] & 1 == k)
        def _():
            @pl.when(meta[GOT] == 0)
            def _():
                drain(0, bufs[k])

            drain(1, bufs[1 - k])

    good = meta[FAULT] == 0

    @pl.when(good)
    def _():
        last = meta[BASE, levels]
        g_last = weight_ref[levels - 2]

        def seed(g, carry):
            for t in range(WINDOW // SUB):
                r = eight(last + g * WINDOW + SUB * t)
                s = sigma[r, :] + pltpu.roll(sigma[r, :], HALF, 1)
                ratio[r, :] = jnp.where(s > 0, g_last / jnp.where(s > 0, s, 1.0), 0.0)
            return carry

        lax.fori_loop(0, (meta[COUNT, levels] + WINDOW - 1) // WINDOW, seed, 0)

        def back_step(k, carry):
            level = levels - 1 - k
            base, count = meta[BASE, level], meta[COUNT, level]
            nbase, ncount = meta[BASE, level + 1], meta[COUNT, level + 1]
            g_here = weight_ref[jnp.maximum(level - 2, 0)]

            def pull_batch(bt, carry):
                here = eight(base + bt * SLOTS)

                def pull(quad, c, acc):
                    even, odd = cand[2 * quad, here, :], cand[2 * quad + 1, here, :]
                    acc = list(acc)
                    for n in range(WINDOW):
                        q = spread_row(queue, nbase + c * WINDOW + n)
                        w = spread_row(ratio, nbase + c * WINDOW + n)
                        acc[n % 2] = acc[n % 2] + jnp.where((even == q) | (odd == q), w, 0.0)
                    return tuple(acc)

                def pull_quad(quad, acc):
                    return lax.fori_loop(1, (ncount + WINDOW - 1) // WINDOW, functools.partial(pull, quad), pull(quad, 0, acc))

                acc = pull_quad(0, (jnp.zeros((SUB, LANES), f32),) * 2)
                if not compact:
                    acc = lax.fori_loop(1, quads, pull_quad, acc)
                delta[here, :] = acc[0] + acc[1]
                return carry

            lax.fori_loop(0, (count + SLOTS - 1) // SLOTS, pull_batch, 0)

            def finish(g, carry):
                slots = [eight(base + g * WINDOW + SUB * t) for t in range(WINDOW // SUB)]
                for t, r in enumerate(slots):
                    inside = g * WINDOW + SUB * t < count
                    part, s = (v + pltpu.roll(v, HALF, 1) for v in (delta[r, :], sigma[r, :]))
                    d = s * part
                    w = jnp.where(s > 0, (g_here + d) / jnp.where(s > 0, s, 1.0), 0.0)
                    delta[r, :] = jnp.where(inside, d, delta[r, :])
                    ratio[r, :] = jnp.where(inside, w, ratio[r, :])
                return carry

            lax.fori_loop(0, (count + WINDOW - 1) // WINDOW, finish, 0)
            return carry

        lax.fori_loop(0, levels - 1, back_step, 0)

        tall = lax.broadcasted_iota(jnp.int32, (WIDE, WIDE), 0).astype(f32).astype(bf16)
        zero = jnp.zeros((WIDE, WIDE), bf16)
        one = zero + 1
        start = meta[BASE, 1]

        def tally(t, carry):
            for u in range(TALLY // 16):
                a, b = eight(start + t * TALLY + u * 16), eight(start + t * TALLY + u * 16 + SUB)
                v = jnp.where(upper, queue[b, :], queue[a, :])
                d = jnp.where(upper, delta[b, :], delta[a, :])
                hi = jnp.floor(v * (1.0 / WIDE))
                lo = v - hi * WIDE
                d_hi = d.astype(bf16).astype(f32)
                d_mid = (d - d_hi).astype(bf16).astype(f32)
                d_lo = d - d_hi - d_mid
                for p in range(0, SUB, 2):
                    cols = slice((u * SUB + p) * LANES, (u * SUB + p + 2) * LANES)

                    def pair(x):
                        return jnp.concatenate([x[p:p + 1], x[p + 1:p + 2]], axis=1).astype(bf16)

                    colhot[:, cols] = jnp.where(tall == pair(lo), one, zero)
                    match = tall[:high] == pair(hi)
                    for n, x in enumerate((d_hi, d_mid, d_lo)):
                        rowhot[n * high:(n + 1) * high, cols] = jnp.where(match, pair(x), zero[:high])
            bins[...] += lax.dot_general(rowhot[...], colhot[...], TURN, preferred_element_type=f32)
            return carry

        for t in range(TALLY // SUB):
            delta[eight(last + t * SUB), :] = jnp.zeros((SUB, LANES), f32)
        lax.fori_loop(0, (last - start + TALLY - 1) // TALLY, tally, 0)

    blocks = out_ref.shape[0]
    per = high // blocks
    total = (bins[:high] + bins[high:2 * high] + bins[2 * high:]) * scale
    fault = jnp.where(good, 0.0, 1.0)
    for b in range(blocks):
        for n in PAIR:
            out_ref[b, n * per:(n + 1) * per, :] = total[b * per:(b + 1) * per, n * LANES:(n + 1) * LANES]
        out_ref[b, 2 * per:, :] = jnp.full((SUB, LANES), fault, f32)


def walk(which, sources, weights, lists, *, blocks, vertices, scale, compact):
    levels = weights.shape[0] + 1
    rows = CAP + 4 * WINDOW
    high = LANES // blocks + SUB
    vm = pltpu.VMEM
    queue = vm((rows, LANES), f32)
    parts = 3 * (vertices // WIDE)
    return pl.pallas_call(
        functools.partial(walk_kernel, levels=levels, vertices=vertices, scale=scale, compact=compact),
        in_specs=[pl.BlockSpec(memory_space=pltpu.SMEM)] * 3 + [pl.BlockSpec(memory_space=pltpu.VMEM)],
        out_specs=pl.BlockSpec(memory_space=pltpu.VMEM),
        out_shape=jax.ShapeDtypeStruct((blocks, high, LANES), f32),
        scratch_shapes=[
            vm(((1 if compact else 2) * (vertices + SUB), LANES), f32), queue, queue, queue, queue,
            vm((4, rows, LANES), f32), vm((2, rows, LANES), jnp.int32),
            vm((40, LANES), f32), vm((32, LANES), jnp.int32), vm((SUB, LANES), jnp.int32), vm((SUB, LANES), jnp.int32),
            vm((parts, TALLY // 2 * LANES), bf16), vm((WIDE, TALLY // 2 * LANES), bf16), vm((parts, WIDE), f32),
            pltpu.SMEM((SLOTS, LANES), jnp.int32), pltpu.SMEM((SLOTS, LANES), jnp.int32), pltpu.SMEM((3, 16), jnp.int32),
            pltpu.SemaphoreType.DMA((2,)),
        ],
        compiler_params=pltpu.CompilerParams(
            vmem_limit_bytes=48 * 1024 * 1024),
        name="walk",
    )(which, sources, weights, lists)


def share_kernel(src, graph, x_ref, o_ref, own_sem, send_sem, recv_sem):
    y, g = lax.axis_index("src"), lax.axis_index("graph")
    others = [((y + i) % src, (g + k) % graph) for i, k in everyone(src, graph)][1:]
    hello(others)
    await_hello(others)
    mine = g * src + y
    own = pltpu.make_async_copy(x_ref, o_ref.at[mine], own_sem)
    own.start()
    copies = []
    for n, (py, pg) in enumerate(others):
        copies.append(pltpu.make_async_remote_copy(
            src_ref=x_ref, dst_ref=o_ref.at[mine], send_sem=send_sem.at[n], recv_sem=recv_sem.at[n],
            device_id={"src": py, "graph": pg}, device_id_type=MESH))
        copies[-1].start()
    own.wait()
    for c in copies:
        c.wait()


def share(x, src, graph):
    n = src * graph
    return pl.pallas_call(
        functools.partial(share_kernel, src, graph),
        in_specs=[pl.BlockSpec(memory_space=pltpu.VMEM)],
        out_specs=pl.BlockSpec(memory_space=pltpu.VMEM),
        out_shape=jax.ShapeDtypeStruct((n,) + x.shape, x.dtype),
        scratch_shapes=[pltpu.SemaphoreType.DMA, pltpu.SemaphoreType.DMA((n - 1,)), pltpu.SemaphoreType.DMA((n - 1,))],
        compiler_params=pltpu.CompilerParams(collective_id=2, has_side_effects=True),
        name="share",
    )(x)


def total_kernel(src, graph, x_ref, o_ref, got, own_sem, send_sem, recv_sem):
    y, g = lax.axis_index("src"), lax.axis_index("graph")
    others = [((y + i) % src, (g + k) % graph) for i, k in everyone(src, graph)][1:]
    hello(others)
    mine = g * src + y
    own = pltpu.make_async_copy(x_ref.at[g], got.at[mine], own_sem)
    own.start()
    await_hello(others)
    copies = []
    for n, (py, pg) in enumerate(others):
        copies.append(pltpu.make_async_remote_copy(
            src_ref=x_ref.at[pg], dst_ref=got.at[mine], send_sem=send_sem.at[n], recv_sem=recv_sem.at[n],
            device_id={"src": py, "graph": pg}, device_id_type=MESH))
        copies[-1].start()
    own.wait()
    for c in copies:
        c.wait()
    acc = got[0]
    for n in range(1, src * graph):
        acc = acc + got[n]
    o_ref[...] = acc


def total(x, src, graph, collective_id):
    n = src * graph
    return pl.pallas_call(
        functools.partial(total_kernel, src, graph),
        in_specs=[pl.BlockSpec(memory_space=pltpu.VMEM)],
        out_specs=pl.BlockSpec(memory_space=pltpu.VMEM),
        out_shape=jax.ShapeDtypeStruct(x.shape[1:], x.dtype),
        scratch_shapes=[pltpu.VMEM((n,) + x.shape[1:], x.dtype), pltpu.SemaphoreType.DMA,
                        pltpu.SemaphoreType.DMA((n - 1,)), pltpu.SemaphoreType.DMA((n - 1,))],
        compiler_params=pltpu.CompilerParams(collective_id=collective_id, has_side_effects=True),
        name="total",
    )(pltpu.with_memory_space_constraint(x, pltpu.VMEM))


def dense(adj_slab, src_local, level_weight, src, graph):
    slab_rows, vertex_count = adj_slab.shape
    src_count = src_local.shape[0]
    levels = level_weight.shape[0] + 1
    row_start = lax.axis_index("graph") * slab_rows
    vertex_ids = row_start + lax.broadcasted_iota(jnp.int32, (slab_rows, 1), 0)
    first = jnp.where(vertex_ids == src_local[None, :], 1.0, 0.0).astype(f32)

    def forward(carry, unused):
        sigma, seen = carry
        partial = jnp.einsum("uv,us->vs", adj_slab, sigma, preferred_element_type=f32, precision=exact_precision)
        parts = lax.all_to_all(partial.reshape(graph, slab_rows, src_count), "graph", 0, 0)
        sigma = jnp.sum(parts, axis=0) * (1.0 - seen)
        seen = jnp.maximum(seen, jnp.where(sigma > 0, 1.0, 0.0))
        return (sigma, seen), sigma

    _, sigmas = lax.scan(forward, (first, first), None, length=levels)

    def backward(carry, xs):
        delta, acc = carry
        upper, lower, weight = xs
        reached = upper > 0
        ratio = jnp.where(reached, (weight + delta) / jnp.where(reached, upper, 1.0), 0.0)
        gathered = lax.all_to_all(jnp.broadcast_to(ratio[None], (graph,) + ratio.shape), "graph", 0, 0)
        pulled = jnp.einsum("uv,vs->us", adj_slab, gathered.reshape(vertex_count, src_count),
                            preferred_element_type=f32, precision=exact_precision)
        delta = lower * pulled
        return (delta, acc + delta), None

    zero = jnp.zeros_like(first)
    (_, acc), _ = lax.scan(backward, (zero, zero), (sigmas[1:][::-1], sigmas[:-1][::-1], level_weight[::-1]))
    scale = vertex_count / (src_count * src * levels ** 3)
    mine = jnp.sum(acc, axis=1) * scale
    both = lax.all_to_all(jnp.broadcast_to(mine.reshape(1, -1, LANES), (src, slab_rows // LANES, LANES)), "src", 0, 0)
    return jnp.sum(both, axis=0).reshape(slab_rows)


def solution(mesh):
    src, graph = mesh.shape["src"], mesh.shape["graph"]

    def device_program(adj_slab, src_local, level_weight):
        slab_rows, vertex_count = adj_slab.shape
        levels = level_weight.shape[0] + 1
        scale = vertex_count / (HALF * src * graph * levels ** 3)
        which = lax.axis_index("graph").astype(jnp.int32).reshape(1)

        def finish(lists, compact, collective_id, other):
            parts = walk(which, src_local, level_weight, lists, blocks=graph, vertices=vertex_count, scale=scale, compact=compact)
            summed = total(parts, src, graph, collective_id)
            rows = slab_rows // LANES

            def plain():
                return summed[:rows].reshape(2, -1, LANES).transpose(1, 0, 2).reshape(slab_rows)

            return lax.cond(summed[rows, 0] > 0, other, plain)

        def dense_path():
            return dense(adj_slab, src_local, level_weight, src, graph)

        def general_path():
            half = lax.axis_index("src").astype(jnp.int32).reshape(1)
            return finish(share(extract(adj_slab, half, slab_rows // src), src, graph), False, 3, dense_path)

        return finish(collect(adj_slab, src, graph), True, 1, general_path)

    return jax.shard_map(device_program, mesh=mesh,
                         in_specs=(P(("batch", "graph"), None), P(("batch", "src")), P(None)),
                         out_specs=P(("batch", "graph")), check_vma=False)
```

```python
import functools

import jax
import jax.numpy as jnp
from jax import lax
from jax.experimental import pallas as pl
from jax.experimental.pallas import tpu as pltpu
from jax.sharding import PartitionSpec as P

MESH = pl.DeviceIdType.MESH
exact_precision = lax.Precision.HIGHEST
f32, bf16 = jnp.float32, jnp.bfloat16

LANES, SUB = 128, 8
WIDE = 256
DEG, FEW = 8, 4
EMPTY = -2.0
FULL = 32767.0
TURN = (((1,), (1,)), ((), ()))
BLOCK = 128
READS = 4
STEP = 32
HALF = 64
SLOTS = 8
WINDOW = 48
SCAN = 32
CAP = 1024
TALLY = 96
PAIR = (0, 1)
BYTE = 256
BASE, COUNT = 0, 1
FAULT, LENGTH, GOT, PARITY, AWAIT0, AWAIT1, REACHED, SHORT0, SHORT1 = ((2, n) for n in range(9))


def everyone(src, graph):
    return [(y, g) for y in range(src) for g in range(graph)]


def hello(peers):
    for y, g in peers:
        pl.semaphore_signal(pltpu.get_barrier_semaphore(), inc=1, device_id={"src": y, "graph": g}, device_id_type=MESH)


def await_hello(peers):
    pl.semaphore_wait(pltpu.get_barrier_semaphore(), len(peers))


def place(plane, lists):
    lists = list(lists)
    row_i = lax.broadcasted_iota(jnp.int32, (WIDE, WIDE), 0)
    col_i = lax.broadcasted_iota(jnp.int32, (WIDE, WIDE), 1)
    eye = jnp.where(row_i == col_i, float(WIDE), 0.0).astype(bf16)
    flipped = lax.dot_general(eye, plane, TURN, preferred_element_type=f32)
    lane_id = lax.broadcasted_iota(jnp.int32, (SUB, flipped.shape[1]), 0).astype(f32)
    for g in range(WIDE // SUB):
        x = flipped[g * SUB:(g + 1) * SUB] + (lane_id + float(g * SUB))
        for s in range(len(lists)):
            hi = jnp.maximum(lists[s], x)
            if s < len(lists) - 1:
                x = jnp.minimum(lists[s], x)
            lists[s] = hi
    return lists


def sort(lists):
    gap = len(lists) // 2
    while gap:
        for s in range(len(lists)):
            if not s & gap:
                lists[s], lists[s + gap] = jnp.maximum(lists[s], lists[s + gap]), jnp.minimum(lists[s], lists[s + gap])
        gap //= 2
    return lists


def over_sublanes(lists):
    size = len(lists)
    for shift in (4, 2, 1):
        other = [pltpu.roll(v, shift, 0) for v in lists]
        lists = sort([jnp.maximum(lists[s], other[size - 1 - s]) for s in range(size)])
    out = jnp.full(lists[0].shape, EMPTY, f32)
    sub = lax.broadcasted_iota(jnp.int32, out.shape, 0)
    for s in range(size):
        out = jnp.where(sub == s, jnp.where(lists[s] >= WIDE, lists[s] - WIDE, EMPTY), out)
    return out


def degree_of(seen):
    return lax.dot_general(jnp.ones((SUB, WIDE), bf16), seen, TURN, preferred_element_type=f32)


def collect_kernel(src, graph, a_ref, o_ref, bufs, tops, mine, sems, own_sem, send_sems, recv_sems):
    vertices = a_ref.shape[1]
    pairs, chunks = mine.shape[0], vertices // WIDE
    blocks = 2 * pairs
    y, g = lax.axis_index("src"), lax.axis_index("graph")
    others = [((y + i) % src, (g + k) % graph) for i, k in everyone(src, graph)][1:]
    me = g * src + y
    height = 4 * SUB
    pieces = BLOCK // height

    def fetch(i, t):
        rows = pl.ds(pl.multiple_of((y * blocks + i) * BLOCK + t * height, height), height)
        here = pl.ds(pl.multiple_of(t * height, height), height)
        return pltpu.make_async_copy(a_ref.at[rows], bufs.at[i % READS, here], sems.at[i % READS, t])

    def send(n, first, count):
        py, pg = others[n]
        return pltpu.make_async_remote_copy(
            src_ref=mine.at[pl.ds(first, count)], dst_ref=o_ref.at[pl.ds(me * pairs + first, count)],
            send_sem=send_sems.at[n], recv_sem=recv_sems.at[n], device_id={"src": py, "graph": pg}, device_id_type=MESH)

    def send_pair(p):
        for n in range(len(others)):
            send(n, p, 1).start()

    hello(others)
    for i in range(READS - 1):
        for t in range(pieces):
            fetch(i, t).start()
    none = jnp.zeros((SUB, 2 * BLOCK), f32)

    def scan(i, first):
        @pl.when(i + READS - 1 < blocks)
        def _():
            for t in range(pieces):
                fetch(i + READS - 1, t).start()

        def scan_rows(t, carry):
            fetch(i, t).wait()
            here = pl.ds(pl.multiple_of(t * height, height), height)

            def scan_chunks(c, state):
                top, low, seen, sums, value = state
                for k in range(STEP):
                    a = bufs[i % READS, here, pl.ds(pl.multiple_of((c * STEP + k) * WIDE, WIDE), WIDE)]
                    x = a * value
                    low = jnp.maximum(low, jnp.minimum(top, x))
                    top = jnp.maximum(top, x)
                    seen = seen + a
                    sums = sums + x
                    value = value + 1
                return top, low, seen, sums, value

            zero = jnp.zeros((height, WIDE), bf16)
            top, low, seen, sums, _ = lax.fori_loop(0, chunks // STEP, scan_chunks, (zero,) * 4 + (zero + 1,))
            for n, v in enumerate((top, low, (sums - top) - low, seen)):
                tops[n, pl.ds(pl.multiple_of(first + t * height, height), height), :] = v
            return carry

        lax.fori_loop(0, pieces, scan_rows, 0)

    def pair_step(p, carry):
        for h in range(2):
            scan(2 * p + h, h * BLOCK)
        seen = tops[3]
        crowd = seen[:SUB]
        for k in range(1, 2 * BLOCK // SUB):
            crowd = jnp.maximum(crowd, seen[k * SUB:(k + 1) * SUB])
        crowd = jnp.max(crowd.astype(f32), axis=0, keepdims=True)
        a, b, c = place(tops[0], (none,) * 4), place(tops[1], (none,) * 2), place(tops[2], (none,))
        rest = [jnp.maximum(b[0], c[0]), jnp.minimum(b[0], c[0])]
        rest = [rest[0], jnp.maximum(b[1], rest[1]), jnp.minimum(b[1], rest[1])]
        lists = over_sublanes(sort([a[0]] + [jnp.maximum(a[s + 1], rest[2 - s]) for s in range(3)]))
        lists = jnp.where((crowd > 3) | (degree_of(seen) > 4), FULL, lists)
        even, odd = lists[:, :BLOCK], lists[:, BLOCK:]
        sub = lax.broadcasted_iota(jnp.int32, even.shape, 0)
        mine[p] = jnp.where(sub < 4, even, pltpu.roll(odd, 4, 0))

        @pl.when(p == 1)
        def _():
            await_hello(others)

        @pl.when(p > 0)
        def _():
            send_pair(p - 1)

        return carry

    lax.fori_loop(0, pairs, pair_step, 0)
    own = pltpu.make_async_copy(mine, o_ref.at[pl.ds(me * pairs, pairs)], own_sem)
    send_pair(pairs - 1)
    own.start()
    own.wait()
    for n in range(len(others)):
        send(n, 0, pairs).wait()


def collect(adj_slab, src, graph):
    rows, vertices = adj_slab.shape
    n = src * graph
    mine = (rows // src // (2 * BLOCK), SUB, BLOCK)
    return pl.pallas_call(
        functools.partial(collect_kernel, src, graph),
        in_specs=[pl.BlockSpec(memory_space=pl.ANY)],
        out_specs=pl.BlockSpec(memory_space=pltpu.VMEM),
        out_shape=jax.ShapeDtypeStruct((n * mine[0],) + mine[1:], f32),
        scratch_shapes=[pltpu.VMEM((READS, BLOCK, vertices), bf16), pltpu.VMEM((4, 2 * BLOCK, WIDE), bf16), pltpu.VMEM(mine, f32),
                        pltpu.SemaphoreType.DMA((READS, BLOCK // (4 * SUB))), pltpu.SemaphoreType.DMA,
                        pltpu.SemaphoreType.DMA((n - 1,)), pltpu.SemaphoreType.DMA((n - 1,))],
        compiler_params=pltpu.CompilerParams(collective_id=0, has_side_effects=True, vmem_limit_bytes=40 * 1024 * 1024),
        name="collect",
    )(adj_slab)


def extract_kernel(half_ref, a_ref, o_ref, block, seen, planes, sem):
    vertices = a_ref.shape[1]

    def block_step(i, carry):
        copy = pltpu.make_async_copy(
            a_ref.at[pl.ds(pl.multiple_of((half_ref[0] * o_ref.shape[0] + i) * BLOCK, BLOCK), BLOCK)], block, sem)
        copy.start()
        copy.wait()
        planes[...] = jnp.zeros_like(planes)
        seen[...] = jnp.zeros_like(seen)

        def scan_chunk(c, carry):
            a = block[:, pl.ds(pl.multiple_of(c * WIDE, WIDE), WIDE)]
            seen[...] = seen[...] + a
            x = a.astype(f32) * (c + 1).astype(f32)
            for s in range(DEG):
                top = planes[s].astype(f32)
                planes[s] = jnp.maximum(top, x).astype(bf16)
                x = jnp.minimum(top, x)
            return carry

        lax.fori_loop(0, vertices // WIDE, scan_chunk, 0)
        lists = lax.fori_loop(0, DEG, lambda p, lists: tuple(place(planes[p], lists)), (jnp.zeros((SUB, BLOCK), f32),) * DEG)
        o_ref[i] = jnp.where(degree_of(seen[...]) > DEG, FULL, over_sublanes(list(lists)))
        return carry

    lax.fori_loop(0, o_ref.shape[0], block_step, 0)


def extract(adj_slab, half, rows):
    vertices = adj_slab.shape[1]
    return pl.pallas_call(
        extract_kernel,
        in_specs=[pl.BlockSpec(memory_space=pltpu.SMEM), pl.BlockSpec(memory_space=pl.ANY)],
        out_specs=pl.BlockSpec(memory_space=pltpu.VMEM),
        out_shape=jax.ShapeDtypeStruct((rows // BLOCK, DEG, BLOCK), f32),
        scratch_shapes=[pltpu.VMEM((BLOCK, vertices), bf16), pltpu.VMEM((BLOCK, WIDE), bf16),
                        pltpu.VMEM((DEG, BLOCK, WIDE), bf16), pltpu.SemaphoreType.DMA],
        name="extract",
    )(half, adj_slab)


def walk_kernel(which_ref, src_ref, weight_ref, lists_ref, out_ref,
                table, queue, sigma, ratio, delta, cand, ids, now, dest, tail_ref, held, rowhot, colhot, bins,
                ids_a, ids_b, meta, sems, *, levels, vertices, scale, compact):
    pitch = vertices + SUB
    lane = lax.broadcasted_iota(jnp.int32, (SUB, LANES), 1)
    sub = lax.broadcasted_iota(jnp.int32, (SUB, LANES), 0)
    upper = lane >= HALF
    lane_row = lax.broadcasted_iota(jnp.int32, (1, LANES), 1)
    group_odd = ((lane_row // 32) % 2) == 1
    lane32 = lane_row % 32
    rows_all = queue.shape[0]
    tile_bits = (vertices // lists_ref.shape[0]).bit_length() - 1
    high = vertices // WIDE

    def eight(row):
        return pl.ds(pl.multiple_of(row, SUB), SUB)

    def spread_row(ref, *index):
        return jnp.broadcast_to(ref[(*index[:-1], pl.ds(index[-1], 1), slice(None))], (SUB, LANES))

    def clear(t, carry):
        for k in range(SUB):
            rows = eight((t * SUB + k) * SUB)
            queue[rows, :] = jnp.full((SUB, LANES), -1.0, f32)
            sigma[rows, :] = jnp.zeros((SUB, LANES), f32)
        return carry

    def fetch(quad, row, buf):
        return pltpu.make_async_copy(ids.at[quad, eight(row)], buf[0], sems.at[buf[1]])

    def name(row, q):
        v = jnp.where(q < 0, vertices, q.astype(jnp.int32))
        ids[0, eight(row), :] = v
        ids[1, eight(row), :] = v + pitch

    bufs = (ids_a, 0), (ids_b, 1)
    clear(0, 0)

    near_source = jnp.full((SUB, LANES), EMPTY, f32)
    source = near_source
    for j in range(HALF):
        v = src_ref[which_ref[0] * HALF + j]
        tile = pltpu.roll(lists_ref[v >> tile_bits], (j - v) & (LANES - 1), 1)
        if compact:
            tile = jnp.where((v & LANES) > 0, pltpu.roll(tile, FEW, 0), tile)
        near_source = jnp.where(lane == j, tile, near_source)
        source = jnp.where(lane % HALF == j, v.astype(f32), source)
    near_source = jnp.where(upper, pltpu.roll(near_source, HALF, 1), near_source)
    reached = near_source >= 0
    if compact:
        reached = reached & (sub < FEW)
    queue[0:1, :] = source[:1]
    queue[eight(SUB), :] = jnp.where(reached, near_source, -1.0)
    sigma[eight(SUB), :] = jnp.where(reached & jnp.logical_not(upper), 1.0, 0.0)
    for n in (1, 2):
        name(n * SUB, queue[eight(n * SUB), :])
    bins[...] = jnp.zeros_like(bins)
    fetch(0, SUB, bufs[0]).start()
    if compact:
        fetch(0, 2 * SUB, bufs[1]).start()
    lax.fori_loop(1, rows_all // (SUB * SUB), clear, 0)

    srow = lax.broadcasted_iota(jnp.int32, (2 * SUB, LANES), 0)
    slane = lax.broadcasted_iota(jnp.int32, (2 * SUB, LANES), 1)

    def fill(halves, target):
        picks = [jnp.where((srow % SUB) == (slane // 32 + FEW * h), jnp.where(srow < SUB, float(LANES), 1.0), 0.0).astype(bf16)
                 for h in halves]

        def body(step, most):
            for k in range(FEW):
                first = (FEW * step + k) * SUB
                x = jnp.concatenate([lists_ref[first + n] for n in range(SUB)], axis=1)
                hi = jnp.floor(x * (1.0 / LANES))
                lo = x - hi * LANES
                both = jnp.concatenate([hi, lo], axis=0).astype(bf16)
                for h, pick in zip(halves, picks):
                    rows = lax.dot_general(both, pick, (((0,), (0,)), ((), ())), preferred_element_type=f32)
                    for n in range(SUB):
                        table[pl.ds(pl.multiple_of(target(h, first + n), SUB), LANES), :] = rows[n * LANES:(n + 1) * LANES]
                for n in range(SUB):
                    most = jnp.maximum(most, lists_ref[first + n])
            return most

        return lax.fori_loop(0, lists_ref.shape[0] // (FEW * SUB), body, jnp.full((SUB, LANES), EMPTY, f32))

    table[vertices:pitch, :] = jnp.full((SUB, LANES), EMPTY, f32)
    if compact:
        most = fill(PAIR, lambda h, t: (2 * t + h) * LANES)
        quads = 1
    else:
        table[pitch + vertices:, :] = jnp.full((SUB, LANES), EMPTY, f32)
        most = fill((0,), lambda h, t: t * LANES)
        wide = jnp.max(jnp.where(sub >= FEW, most, EMPTY)) >= 0
        quads = jnp.where(wide, 2, 1)

        @pl.when(wide)
        def _():
            fill((1,), lambda h, t: pitch + t * LANES)

    bad = jnp.max(most) > vertices
    meta[FAULT] = bad.astype(jnp.int32)

    def gather(rows_of_ids):
        acc = [[jnp.full((1, LANES), EMPTY, f32)] * 2 for _ in rows_of_ids]
        for j in range(32):
            hit = lane32 == j
            for i, id_of in enumerate(rows_of_ids):
                for b in PAIR:
                    acc[i][b] = jnp.where(hit, table[pl.ds(id_of(b * 32 + j), 1), :], acc[i][b])
        return [(jnp.where(group_odd, b, a), pltpu.roll(jnp.where(group_odd, a, b), LANES - 32, 1)) for a, b in acc]

    def gather_slots(ids_s, slots=SLOTS):
        return gather([functools.partial(lambda i, j: ids_s[i, j], i) for i in range(slots)])

    def keep(rows, quad, row):
        for i, pair in enumerate(rows):
            for h in PAIR:
                cand[2 * quad + h, pl.ds(row + i, 1), :] = pair[h]

    def flag(x):
        return jnp.where(x, 1, 0)

    def at(unit, origin):
        return unit & (quads - 1), origin + (unit >> (quads - 1)) * SUB

    def level_step(level, carry):
        base, count = meta[BASE, level], meta[COUNT, level]
        following = base + (count + 7) // SUB * SUB
        batches = jnp.where(following <= CAP, (count + SLOTS - 1) // SLOTS, 0)
        units = batches * quads
        parity = meta[PARITY]

        def on_parity(n, f):
            for k in PAIR:
                @pl.when(n & 1 == k)
                def _():
                    f(bufs[k], bufs[1 - k])

        def unit_step(unit, other, to):
            quad, row = at(unit, base)
            x = [cand[2 * quad + h, eight(row), :] for h in PAIR]

            def search(t, marks):
                marks = list(marks)
                for k in range(SCAN):
                    q = spread_row(queue, t * SCAN + k)
                    for h in PAIR:
                        n = 2 * h + k % 2
                        marks[n] = jnp.where(x[h] == q, 1, marks[n])
                return tuple(marks)

            reach = following + meta[LENGTH]
            marks = lax.fori_loop(0, (reach + SCAN - 1) // SCAN, search, (jnp.zeros((SUB, LANES), jnp.int32),) * 4)
            ahead = unit + 1 < units
            final_unit = unit + 1 == units
            soon = jnp.logical_and(final_unit, meta[AWAIT0] > 0)

            @pl.when(jnp.logical_or(ahead, soon))
            def _():
                fetch(0, base, to).wait()

            def insert(g):
                slots = [eight(following + g * WINDOW + SUB * t) for t in range(WINDOW // SUB)]
                qs = [queue[r, :] for r in slots]
                ss = [sigma[r, :] for r in slots]
                pos = [sub + (g * WINDOW + SUB * t) for t in range(WINDOW // SUB)]
                for h in PAIR:
                    for i in range(SUB):
                        d, e = spread_row(dest, SUB * h + i), spread_row(dest, 16 + SUB * h + i)
                        v, w = spread_row(now, SUB * h + i), spread_row(now, 16 + SUB * h + i)
                        for t in range(WINDOW // SUB):
                            qs[t] = jnp.where(pos[t] == d, v, jnp.where(pos[t] == e, w, qs[t]))
                for i in range(SUB):
                    v, w, sig = spread_row(now, i), spread_row(now, SUB + i), spread_row(now, 32 + i)
                    for t in range(WINDOW // SUB):
                        ss[t] = ss[t] + jnp.where((qs[t] == v) | (qs[t] == w), sig, 0.0)
                for t, r in enumerate(slots):
                    queue[r, :] = qs[t]
                    sigma[r, :] = ss[t]
                return qs

            def core(looking):
                even, odd = x
                m, n, k, l = marks
                near_even, near_odd = m | n | flag(even < 0), k | l | flag(odd < 0)

                xr = [pltpu.roll(v, HALF, 1) for v in x]
                turns = [[[pltpu.roll(v, s, 0) if s else v for v in (x[h], xr[h])] for s in range(SUB)] for h in PAIR]
                for s, ((a, b), (c, d)) in enumerate(zip(*turns)):
                    near_odd = jnp.where((odd == a) | (odd == b), 1, near_odd)
                    if s:
                        after = sub >= s
                        near_even = jnp.where(((even == a) | (even == b)) & after, 1, near_even)
                        near_odd = jnp.where(((odd == c) | (odd == d)) & after, 1, near_odd)

                new = [1 - near_even, 1 - near_odd]
                packed = new[0] + BYTE * new[1]
                across = pltpu.roll(packed, HALF, 1)
                far = [across & (BYTE - 1), across >> SUB]
                both = packed + across
                run, whole = both, both
                for s in (1, 2, 4):
                    run = run + jnp.where(sub >= s, pltpu.roll(run, s, 0), 0)
                    whole = whole + pltpu.roll(whole, s, 0)
                run = run - both
                tail = tail_ref[...]
                evens = whole & (BYTE - 1)
                begin = [tail + (run & (BYTE - 1)), tail + evens + (run >> SUB)]
                for h in PAIR:
                    dest[SUB * h:SUB * h + SUB, :] = jnp.where(new[h] > 0, begin[h] + jnp.where(upper, far[h], 0), -1)
                    dest[16 + SUB * h:24 + SUB * h, :] = jnp.where(far[h] > 0, begin[h] + jnp.where(upper, 0, new[h]), -1)
                    now[SUB * h:SUB * h + SUB, :] = x[h]
                    now[16 + SUB * h:24 + SUB * h, :] = xr[h]
                part = sigma[eight(row), :]
                now[32:40, :] = part + pltpu.roll(part, HALF, 1)
                tail = tail + evens + (whole >> SUB)
                tail_ref[...] = tail
                passed = SLOTS * ((unit + 1) >> (quads - 1))
                second = SUB + SUB * (1 >> (quads - 1))
                need = jnp.where(sub == 1, SUB, second)
                short = (tail < need) & (held[...] > passed)
                most = jnp.max(jnp.where(sub == 0, tail, flag(short)).astype(f32), axis=1, keepdims=True)
                meta[REACHED] = most[0, 0].astype(jnp.int32)
                for n in PAIR:
                    meta[(SHORT0, SHORT1)[n]] = most[n + 1, 0].astype(jnp.int32)

                if looking:
                    quad2, row2 = at(unit + 1, base)
                    rows = gather_slots(to[0])
                qs = insert(0)
                for n in PAIR:
                    name(following + n * SUB, qs[n])
                if looking:
                    keep(rows, jnp.where(ahead, quad2, 0), jnp.where(ahead, row2, following))

            look = jnp.logical_or(ahead, soon)
            for looking in PAIR:
                @pl.when(look == (looking > 0))
                def _():
                    core(looking)

            length = meta[REACHED]
            ready = [meta[n] == 0 for n in (SHORT0, SHORT1)]

            @pl.when(unit + 3 < units)
            def _():
                fetch(*at(unit + 3, base), to).start()

            @pl.when(soon)
            def _():
                meta[GOT] = 1

            def first_of_next(n, when, buf):
                @pl.when(jnp.logical_and(when, meta[(AWAIT0, AWAIT1)[n]] == 0))
                def _():
                    fetch(*at(n, following), buf).start()
                    meta[(AWAIT0, AWAIT1)[n]] = 1

            first_of_next(0, jnp.logical_and(ready[0], unit + 3 == units), to)
            first_of_next(0, jnp.logical_and(ready[0], unit + 2 == units), other)
            first_of_next(1, jnp.logical_and(ready[1], unit + 2 == units), to)
            first_of_next(0, final_unit, to)
            first_of_next(1, final_unit, other)

            groups = (length + WINDOW - 1) // WINDOW
            fits = following + groups * WINDOW <= CAP + WINDOW
            meta[LENGTH] = jnp.where(fits, length, 0)

            @pl.when(jnp.logical_not(fits))
            def _():
                meta[FAULT] = 1

            def more(g, carry):
                insert(g)
                return carry

            lax.fori_loop(1, jnp.where(fits, groups, 0), more, 0)

        tail_ref[...] = jnp.zeros_like(tail_ref)
        meta[LENGTH] = 0

        def open_level(mine, other):
            @pl.when(jnp.logical_and(meta[GOT] == 0, meta[AWAIT0] > 0))
            def _():
                fetch(0, base, mine).wait()
                keep(gather_slots(mine[0]), 0, base)

            @pl.when(jnp.logical_and(units < 2, meta[AWAIT1] > 0))
            def _():
                fetch(0, base, other).wait()

            @pl.when(units > 2)
            def _():
                fetch(*at(2, base), mine).start()

        on_parity(parity, open_level)
        for place_ in (GOT, AWAIT0, AWAIT1):
            meta[place_] = 0

        def any_unit(unit, carry):
            on_parity(parity + unit, functools.partial(unit_step, unit))
            return carry

        lax.fori_loop(0, units, any_unit, 0)
        meta[PARITY] = parity + units

        @pl.when(following > CAP)
        def _():
            meta[FAULT] = 1

        found = jnp.where(meta[FAULT] == 0, meta[LENGTH], 0)
        meta[BASE, level + 1] = following
        meta[COUNT, level + 1] = found

        def names(t, carry):
            row = following + t * SUB
            name(row, queue[eight(row), :])
            return carry

        lax.fori_loop(2, (found + SUB - 1) // SUB, names, 0)
        held[...] = tail_ref[...]
        return carry

    for place_ in (GOT, PARITY):
        meta[place_] = 0

    @pl.when(jnp.logical_not(bad))
    def _():
        held[...] = jnp.full_like(held, FEW * quads)
        meta[BASE, 1] = SUB
        meta[COUNT, 1] = FEW * quads
        fetch(0, SUB, bufs[0]).wait()
        if compact:
            for h in PAIR:
                cand[h, eight(SUB), :] = jnp.full((SUB, LANES), EMPTY, f32)
        else:
            fetch(*at(1, SUB), bufs[1]).start()
        keep(gather_slots(ids_a, FEW if compact else SLOTS), 0, SUB)
        meta[GOT] = 1
        meta[AWAIT0] = 0
        meta[AWAIT1] = 1
        lax.fori_loop(1, levels, level_step, 0)

    @pl.when(bad)
    def _():
        fetch(0, SUB, bufs[0]).wait()
        meta[AWAIT0] = 0
        meta[AWAIT1] = int(compact)

    def drain(n, buf):
        @pl.when(meta[(AWAIT0, AWAIT1)[n]] > 0)
        def _():
            fetch(0, 0, buf).wait()

    for k in PAIR:
        @pl.when(meta[PARITY] & 1 == k)
        def _():
            @pl.when(meta[GOT] == 0)
            def _():
                drain(0, bufs[k])

            drain(1, bufs[1 - k])

    good = meta[FAULT] == 0

    @pl.when(good)
    def _():
        last = meta[BASE, levels]
        g_last = weight_ref[levels - 2]

        def seed(g, carry):
            for t in range(WINDOW // SUB):
                r = eight(last + g * WINDOW + SUB * t)
                s = sigma[r, :] + pltpu.roll(sigma[r, :], HALF, 1)
                ratio[r, :] = jnp.where(s > 0, g_last / jnp.where(s > 0, s, 1.0), 0.0)
            return carry

        lax.fori_loop(0, (meta[COUNT, levels] + WINDOW - 1) // WINDOW, seed, 0)

        def back_step(k, carry):
            level = levels - 1 - k
            base, count = meta[BASE, level], meta[COUNT, level]
            nbase, ncount = meta[BASE, level + 1], meta[COUNT, level + 1]
            g_here = weight_ref[jnp.maximum(level - 2, 0)]

            def pull_batch(bt, carry):
                here = eight(base + bt * SLOTS)

                def pull(quad, c, acc):
                    even, odd = cand[2 * quad, here, :], cand[2 * quad + 1, here, :]
                    acc = list(acc)
                    for n in range(WINDOW):
                        q = spread_row(queue, nbase + c * WINDOW + n)
                        w = spread_row(ratio, nbase + c * WINDOW + n)
                        acc[n % 2] = acc[n % 2] + jnp.where((even == q) | (odd == q), w, 0.0)
                    return tuple(acc)

                def pull_quad(quad, acc):
                    return lax.fori_loop(1, (ncount + WINDOW - 1) // WINDOW, functools.partial(pull, quad), pull(quad, 0, acc))

                acc = pull_quad(0, (jnp.zeros((SUB, LANES), f32),) * 2)
                if not compact:
                    acc = lax.fori_loop(1, quads, pull_quad, acc)
                delta[here, :] = acc[0] + acc[1]
                return carry

            lax.fori_loop(0, (count + SLOTS - 1) // SLOTS, pull_batch, 0)

            def finish(g, carry):
                slots = [eight(base + g * WINDOW + SUB * t) for t in range(WINDOW // SUB)]
                for t, r in enumerate(slots):
                    inside = g * WINDOW + SUB * t < count
                    part, s = (v + pltpu.roll(v, HALF, 1) for v in (delta[r, :], sigma[r, :]))
                    d = s * part
                    w = jnp.where(s > 0, (g_here + d) / jnp.where(s > 0, s, 1.0), 0.0)
                    delta[r, :] = jnp.where(inside, d, delta[r, :])
                    ratio[r, :] = jnp.where(inside, w, ratio[r, :])
                return carry

            lax.fori_loop(0, (count + WINDOW - 1) // WINDOW, finish, 0)
            return carry

        lax.fori_loop(0, levels - 1, back_step, 0)

        tall = lax.broadcasted_iota(jnp.int32, (WIDE, WIDE), 0).astype(f32).astype(bf16)
        zero = jnp.zeros((WIDE, WIDE), bf16)
        one = zero + 1
        start = meta[BASE, 1]

        def tally(t, carry):
            for u in range(TALLY // 16):
                a, b = eight(start + t * TALLY + u * 16), eight(start + t * TALLY + u * 16 + SUB)
                v = jnp.where(upper, queue[b, :], queue[a, :])
                d = jnp.where(upper, delta[b, :], delta[a, :])
                hi = jnp.floor(v * (1.0 / WIDE))
                lo = v - hi * WIDE
                d_hi = d.astype(bf16).astype(f32)
                d_mid = (d - d_hi).astype(bf16).astype(f32)
                d_lo = d - d_hi - d_mid
                for p in range(0, SUB, 2):
                    cols = slice((u * SUB + p) * LANES, (u * SUB + p + 2) * LANES)

                    def pair(x):
                        return jnp.concatenate([x[p:p + 1], x[p + 1:p + 2]], axis=1).astype(bf16)

                    colhot[:, cols] = jnp.where(tall == pair(lo), one, zero)
                    match = tall[:high] == pair(hi)
                    for n, x in enumerate((d_hi, d_mid, d_lo)):
                        rowhot[n * high:(n + 1) * high, cols] = jnp.where(match, pair(x), zero[:high])
            bins[...] += lax.dot_general(rowhot[...], colhot[...], TURN, preferred_element_type=f32)
            return carry

        for t in range(TALLY // SUB):
            delta[eight(last + t * SUB), :] = jnp.zeros((SUB, LANES), f32)
        lax.fori_loop(0, (last - start + TALLY - 1) // TALLY, tally, 0)

    blocks = out_ref.shape[0]
    per = high // blocks
    total = (bins[:high] + bins[high:2 * high] + bins[2 * high:]) * scale
    fault = jnp.where(good, 0.0, 1.0)
    for b in range(blocks):
        for n in PAIR:
            out_ref[b, n * per:(n + 1) * per, :] = total[b * per:(b + 1) * per, n * LANES:(n + 1) * LANES]
        out_ref[b, 2 * per:, :] = jnp.full((SUB, LANES), fault, f32)


def walk(which, sources, weights, lists, *, blocks, vertices, scale, compact):
    levels = weights.shape[0] + 1
    rows = CAP + 4 * WINDOW
    high = LANES // blocks + SUB
    vm = pltpu.VMEM
    queue = vm((rows, LANES), f32)
    parts = 3 * (vertices // WIDE)
    return pl.pallas_call(
        functools.partial(walk_kernel, levels=levels, vertices=vertices, scale=scale, compact=compact),
        in_specs=[pl.BlockSpec(memory_space=pltpu.SMEM)] * 3 + [pl.BlockSpec(memory_space=pltpu.VMEM)],
        out_specs=pl.BlockSpec(memory_space=pltpu.VMEM),
        out_shape=jax.ShapeDtypeStruct((blocks, high, LANES), f32),
        scratch_shapes=[
            vm(((1 if compact else 2) * (vertices + SUB), LANES), f32), queue, queue, queue, queue,
            vm((4, rows, LANES), f32), vm((2, rows, LANES), jnp.int32),
            vm((40, LANES), f32), vm((32, LANES), jnp.int32), vm((SUB, LANES), jnp.int32), vm((SUB, LANES), jnp.int32),
            vm((parts, TALLY // 2 * LANES), bf16), vm((WIDE, TALLY // 2 * LANES), bf16), vm((parts, WIDE), f32),
            pltpu.SMEM((SLOTS, LANES), jnp.int32), pltpu.SMEM((SLOTS, LANES), jnp.int32), pltpu.SMEM((3, 16), jnp.int32),
            pltpu.SemaphoreType.DMA((2,)),
        ],
        compiler_params=pltpu.CompilerParams(
            vmem_limit_bytes=48 * 1024 * 1024),
        name="walk",
    )(which, sources, weights, lists)


def share_kernel(src, graph, x_ref, o_ref, own_sem, send_sem, recv_sem):
    y, g = lax.axis_index("src"), lax.axis_index("graph")
    others = [((y + i) % src, (g + k) % graph) for i, k in everyone(src, graph)][1:]
    hello(others)
    await_hello(others)
    mine = g * src + y
    own = pltpu.make_async_copy(x_ref, o_ref.at[mine], own_sem)
    own.start()
    copies = []
    for n, (py, pg) in enumerate(others):
        copies.append(pltpu.make_async_remote_copy(
            src_ref=x_ref, dst_ref=o_ref.at[mine], send_sem=send_sem.at[n], recv_sem=recv_sem.at[n],
            device_id={"src": py, "graph": pg}, device_id_type=MESH))
        copies[-1].start()
    own.wait()
    for c in copies:
        c.wait()


def share(x, src, graph):
    n = src * graph
    return pl.pallas_call(
        functools.partial(share_kernel, src, graph),
        in_specs=[pl.BlockSpec(memory_space=pltpu.VMEM)],
        out_specs=pl.BlockSpec(memory_space=pltpu.VMEM),
        out_shape=jax.ShapeDtypeStruct((n,) + x.shape, x.dtype),
        scratch_shapes=[pltpu.SemaphoreType.DMA, pltpu.SemaphoreType.DMA((n - 1,)), pltpu.SemaphoreType.DMA((n - 1,))],
        compiler_params=pltpu.CompilerParams(collective_id=2, has_side_effects=True),
        name="share",
    )(x)


def total_kernel(src, graph, x_ref, o_ref, got, own_sem, send_sem, recv_sem):
    y, g = lax.axis_index("src"), lax.axis_index("graph")
    others = [((y + i) % src, (g + k) % graph) for i, k in everyone(src, graph)][1:]
    hello(others)
    mine = g * src + y
    own = pltpu.make_async_copy(x_ref.at[g], got.at[mine], own_sem)
    own.start()
    await_hello(others)
    copies = []
    for n, (py, pg) in enumerate(others):
        copies.append(pltpu.make_async_remote_copy(
            src_ref=x_ref.at[pg], dst_ref=got.at[mine], send_sem=send_sem.at[n], recv_sem=recv_sem.at[n],
            device_id={"src": py, "graph": pg}, device_id_type=MESH))
        copies[-1].start()
    own.wait()
    for c in copies:
        c.wait()
    acc = got[0]
    for n in range(1, src * graph):
        acc = acc + got[n]
    o_ref[...] = acc


def total(x, src, graph, collective_id):
    n = src * graph
    return pl.pallas_call(
        functools.partial(total_kernel, src, graph),
        in_specs=[pl.BlockSpec(memory_space=pltpu.VMEM)],
        out_specs=pl.BlockSpec(memory_space=pltpu.VMEM),
        out_shape=jax.ShapeDtypeStruct(x.shape[1:], x.dtype),
        scratch_shapes=[pltpu.VMEM((n,) + x.shape[1:], x.dtype), pltpu.SemaphoreType.DMA,
                        pltpu.SemaphoreType.DMA((n - 1,)), pltpu.SemaphoreType.DMA((n - 1,))],
        compiler_params=pltpu.CompilerParams(collective_id=collective_id, has_side_effects=True),
        name="total",
    )(pltpu.with_memory_space_constraint(x, pltpu.VMEM))


def dense(adj_slab, src_local, level_weight, src, graph):
    slab_rows, vertex_count = adj_slab.shape
    src_count = src_local.shape[0]
    levels = level_weight.shape[0] + 1
    row_start = lax.axis_index("graph") * slab_rows
    vertex_ids = row_start + lax.broadcasted_iota(jnp.int32, (slab_rows, 1), 0)
    first = jnp.where(vertex_ids == src_local[None, :], 1.0, 0.0).astype(f32)

    def forward(carry, unused):
        sigma, seen = carry
        partial = jnp.einsum("uv,us->vs", adj_slab, sigma, preferred_element_type=f32, precision=exact_precision)
        parts = lax.all_to_all(partial.reshape(graph, slab_rows, src_count), "graph", 0, 0)
        sigma = jnp.sum(parts, axis=0) * (1.0 - seen)
        seen = jnp.maximum(seen, jnp.where(sigma > 0, 1.0, 0.0))
        return (sigma, seen), sigma

    _, sigmas = lax.scan(forward, (first, first), None, length=levels)

    def backward(carry, xs):
        delta, acc = carry
        upper, lower, weight = xs
        reached = upper > 0
        ratio = jnp.where(reached, (weight + delta) / jnp.where(reached, upper, 1.0), 0.0)
        gathered = lax.all_to_all(jnp.broadcast_to(ratio[None], (graph,) + ratio.shape), "graph", 0, 0)
        pulled = jnp.einsum("uv,vs->us", adj_slab, gathered.reshape(vertex_count, src_count),
                            preferred_element_type=f32, precision=exact_precision)
        delta = lower * pulled
        return (delta, acc + delta), None

    zero = jnp.zeros_like(first)
    (_, acc), _ = lax.scan(backward, (zero, zero), (sigmas[1:][::-1], sigmas[:-1][::-1], level_weight[::-1]))
    scale = vertex_count / (src_count * src * levels ** 3)
    mine = jnp.sum(acc, axis=1) * scale
    both = lax.all_to_all(jnp.broadcast_to(mine.reshape(1, -1, LANES), (src, slab_rows // LANES, LANES)), "src", 0, 0)
    return jnp.sum(both, axis=0).reshape(slab_rows)


def solution(mesh):
    src, graph = mesh.shape["src"], mesh.shape["graph"]

    def device_program(adj_slab, src_local, level_weight):
        slab_rows, vertex_count = adj_slab.shape
        levels = level_weight.shape[0] + 1
        scale = vertex_count / (HALF * src * graph * levels ** 3)
        which = lax.axis_index("graph").astype(jnp.int32).reshape(1)

        def finish(lists, compact, collective_id, other):
            parts = walk(which, src_local, level_weight, lists, blocks=graph, vertices=vertex_count, scale=scale, compact=compact)
            summed = total(parts, src, graph, collective_id)
            rows = slab_rows // LANES

            def plain():
                return summed[:rows].reshape(2, -1, LANES).transpose(1, 0, 2).reshape(slab_rows)

            return lax.cond(summed[rows, 0] > 0, other, plain)

        def dense_path():
            return dense(adj_slab, src_local, level_weight, src, graph)

        def general_path():
            half = lax.axis_index("src").astype(jnp.int32).reshape(1)
            lists = share(extract(adj_slab, half, slab_rows // src), src, graph)
            return finish(lists.reshape(-1, SUB, LANES), False, 3, dense_path)

        return finish(collect(adj_slab, src, graph), True, 1, general_path)

    return jax.shard_map(device_program, mesh=mesh,
                         in_specs=(P(("batch", "graph"), None), P(("batch", "src")), P(None)),
                         out_specs=P(("batch", "graph")), check_vma=False)
```

```python
import functools

import jax
import jax.numpy as jnp
from jax import lax
from jax.experimental import pallas as pl
from jax.experimental.pallas import tpu as pltpu
from jax.sharding import PartitionSpec as P

MESH = pl.DeviceIdType.MESH
exact_precision = lax.Precision.HIGHEST
f32, bf16 = jnp.float32, jnp.bfloat16

LANES, SUB = 128, 8
WIDE = 256
DEG, FEW = 8, 4
EMPTY = -2.0
FULL = 32767.0
TURN = (((1,), (1,)), ((), ()))
BLOCK = 128
READS = 4
STEP = 32
HALF = 64
SLOTS = 8
WINDOW = 48
SCAN = 32
CAP = 1024
TALLY = 96
PAIR = (0, 1)
BYTE = 256
PEEL = 32
BASE, COUNT = 0, 1
FAULT, LENGTH, GOT, PARITY, AWAIT0, AWAIT1, REACHED, SHORT0, SHORT1 = ((2, n) for n in range(9))


def everyone(src, graph):
    return [(y, g) for y in range(src) for g in range(graph)]


def hello(peers):
    for y, g in peers:
        pl.semaphore_signal(pltpu.get_barrier_semaphore(), inc=1, device_id={"src": y, "graph": g}, device_id_type=MESH)


def await_hello(peers):
    pl.semaphore_wait(pltpu.get_barrier_semaphore(), len(peers))


def place(plane, lists):
    lists = list(lists)
    row_i = lax.broadcasted_iota(jnp.int32, (WIDE, WIDE), 0)
    col_i = lax.broadcasted_iota(jnp.int32, (WIDE, WIDE), 1)
    eye = jnp.where(row_i == col_i, float(WIDE), 0.0).astype(bf16)
    flipped = lax.dot_general(eye, plane, TURN, preferred_element_type=f32)
    lane_id = lax.broadcasted_iota(jnp.int32, (SUB, flipped.shape[1]), 0).astype(f32)
    for g in range(WIDE // SUB):
        x = flipped[g * SUB:(g + 1) * SUB] + (lane_id + float(g * SUB))
        for s in range(len(lists)):
            hi = jnp.maximum(lists[s], x)
            if s < len(lists) - 1:
                x = jnp.minimum(lists[s], x)
            lists[s] = hi
    return lists


def sort(lists):
    gap = len(lists) // 2
    while gap:
        for s in range(len(lists)):
            if not s & gap:
                lists[s], lists[s + gap] = jnp.maximum(lists[s], lists[s + gap]), jnp.minimum(lists[s], lists[s + gap])
        gap //= 2
    return lists


def over_sublanes(lists):
    size = len(lists)
    for shift in (4, 2, 1):
        other = [pltpu.roll(v, shift, 0) for v in lists]
        lists = sort([jnp.maximum(lists[s], other[size - 1 - s]) for s in range(size)])
    out = jnp.full(lists[0].shape, EMPTY, f32)
    sub = lax.broadcasted_iota(jnp.int32, out.shape, 0)
    for s in range(size):
        out = jnp.where(sub == s, jnp.where(lists[s] >= WIDE, lists[s] - WIDE, EMPTY), out)
    return out


def degree_of(seen):
    return lax.dot_general(jnp.ones((SUB, WIDE), bf16), seen, TURN, preferred_element_type=f32)


def collect_kernel(src, graph, a_ref, o_ref, bufs, tops, mine, sems, own_sem, send_sems, recv_sems):
    vertices = a_ref.shape[1]
    pairs, chunks = mine.shape[0], vertices // WIDE
    blocks = 2 * pairs
    y, g = lax.axis_index("src"), lax.axis_index("graph")
    others = [((y + i) % src, (g + k) % graph) for i, k in everyone(src, graph)][1:]
    me = g * src + y
    height = 4 * SUB
    pieces = BLOCK // height

    def fetch(i, t):
        rows = pl.ds(pl.multiple_of((y * blocks + i) * BLOCK + t * height, height), height)
        here = pl.ds(pl.multiple_of(t * height, height), height)
        return pltpu.make_async_copy(a_ref.at[rows], bufs.at[i % READS, here], sems.at[i % READS, t])

    def send(n, first, count):
        py, pg = others[n]
        return pltpu.make_async_remote_copy(
            src_ref=mine.at[pl.ds(first, count)], dst_ref=o_ref.at[pl.ds(me * pairs + first, count)],
            send_sem=send_sems.at[n], recv_sem=recv_sems.at[n], device_id={"src": py, "graph": pg}, device_id_type=MESH)

    def send_pair(p):
        for n in range(len(others)):
            send(n, p, 1).start()

    hello(others)
    for i in range(READS - 1):
        for t in range(pieces):
            fetch(i, t).start()
    none = jnp.zeros((SUB, 2 * BLOCK), f32)

    def scan(i, first):
        @pl.when(i + READS - 1 < blocks)
        def _():
            for t in range(pieces):
                fetch(i + READS - 1, t).start()

        def scan_rows(t, carry):
            fetch(i, t).wait()
            here = pl.ds(pl.multiple_of(t * height, height), height)

            def scan_chunks(c, state):
                top, low, seen, sums, value = state
                for k in range(STEP):
                    a = bufs[i % READS, here, pl.ds(pl.multiple_of((c * STEP + k) * WIDE, WIDE), WIDE)]
                    x = a * value
                    low = jnp.maximum(low, jnp.minimum(top, x))
                    top = jnp.maximum(top, x)
                    seen = seen + a
                    sums = sums + x
                    value = value + 1
                return top, low, seen, sums, value

            zero = jnp.zeros((height, WIDE), bf16)
            top, low, seen, sums, _ = lax.fori_loop(0, chunks // STEP, scan_chunks, (zero,) * 4 + (zero + 1,))
            for n, v in enumerate((top, low, (sums - top) - low, seen)):
                tops[n, pl.ds(pl.multiple_of(first + t * height, height), height), :] = v
            return carry

        lax.fori_loop(0, pieces, scan_rows, 0)

    def pair_step(p, carry):
        for h in range(2):
            scan(2 * p + h, h * BLOCK)
        seen = tops[3]
        crowd = seen[:SUB]
        for k in range(1, 2 * BLOCK // SUB):
            crowd = jnp.maximum(crowd, seen[k * SUB:(k + 1) * SUB])
        crowd = jnp.max(crowd.astype(f32), axis=0, keepdims=True)
        a, b, c = place(tops[0], (none,) * 4), place(tops[1], (none,) * 2), place(tops[2], (none,))
        rest = [jnp.maximum(b[0], c[0]), jnp.minimum(b[0], c[0])]
        rest = [rest[0], jnp.maximum(b[1], rest[1]), jnp.minimum(b[1], rest[1])]
        lists = over_sublanes(sort([a[0]] + [jnp.maximum(a[s + 1], rest[2 - s]) for s in range(3)]))
        lists = jnp.where((crowd > 3) | (degree_of(seen) > 4), FULL, lists)
        even, odd = lists[:, :BLOCK], lists[:, BLOCK:]
        sub = lax.broadcasted_iota(jnp.int32, even.shape, 0)
        mine[p] = jnp.where(sub < 4, even, pltpu.roll(odd, 4, 0))

        @pl.when(p == 1)
        def _():
            await_hello(others)

        @pl.when(p > 0)
        def _():
            send_pair(p - 1)

        return carry

    lax.fori_loop(0, pairs, pair_step, 0)
    own = pltpu.make_async_copy(mine, o_ref.at[pl.ds(me * pairs, pairs)], own_sem)
    send_pair(pairs - 1)
    own.start()
    own.wait()
    for n in range(len(others)):
        send(n, 0, pairs).wait()


def collect(adj_slab, src, graph):
    rows, vertices = adj_slab.shape
    n = src * graph
    mine = (rows // src // (2 * BLOCK), SUB, BLOCK)
    return pl.pallas_call(
        functools.partial(collect_kernel, src, graph),
        in_specs=[pl.BlockSpec(memory_space=pl.ANY)],
        out_specs=pl.BlockSpec(memory_space=pltpu.VMEM),
        out_shape=jax.ShapeDtypeStruct((n * mine[0],) + mine[1:], f32),
        scratch_shapes=[pltpu.VMEM((READS, BLOCK, vertices), bf16), pltpu.VMEM((4, 2 * BLOCK, WIDE), bf16), pltpu.VMEM(mine, f32),
                        pltpu.SemaphoreType.DMA((READS, BLOCK // (4 * SUB))), pltpu.SemaphoreType.DMA,
                        pltpu.SemaphoreType.DMA((n - 1,)), pltpu.SemaphoreType.DMA((n - 1,))],
        compiler_params=pltpu.CompilerParams(collective_id=0, has_side_effects=True, vmem_limit_bytes=40 * 1024 * 1024),
        name="collect",
    )(adj_slab)


def extract_kernel(half_ref, a_ref, o_ref, block, seen, planes, sem):
    vertices = a_ref.shape[1]

    def block_step(i, carry):
        copy = pltpu.make_async_copy(
            a_ref.at[pl.ds(pl.multiple_of((half_ref[0] * o_ref.shape[0] + i) * BLOCK, BLOCK), BLOCK)], block, sem)
        copy.start()
        copy.wait()
        planes[...] = jnp.zeros_like(planes)
        seen[...] = jnp.zeros_like(seen)

        def scan_chunk(c, carry):
            a = block[:, pl.ds(pl.multiple_of(c * WIDE, WIDE), WIDE)]
            seen[...] = seen[...] + a
            x = a.astype(f32) * (c + 1).astype(f32)
            for s in range(DEG):
                top = planes[s].astype(f32)
                planes[s] = jnp.maximum(top, x).astype(bf16)
                x = jnp.minimum(top, x)
            return carry

        lax.fori_loop(0, vertices // WIDE, scan_chunk, 0)
        lists = lax.fori_loop(0, DEG, lambda p, lists: tuple(place(planes[p], lists)), (jnp.zeros((SUB, BLOCK), f32),) * DEG)
        o_ref[i] = jnp.where(degree_of(seen[...]) > DEG, FULL, over_sublanes(list(lists)))
        return carry

    lax.fori_loop(0, o_ref.shape[0], block_step, 0)


def extract(adj_slab, half, rows):
    vertices = adj_slab.shape[1]
    return pl.pallas_call(
        extract_kernel,
        in_specs=[pl.BlockSpec(memory_space=pltpu.SMEM), pl.BlockSpec(memory_space=pl.ANY)],
        out_specs=pl.BlockSpec(memory_space=pltpu.VMEM),
        out_shape=jax.ShapeDtypeStruct((rows // BLOCK, DEG, BLOCK), f32),
        scratch_shapes=[pltpu.VMEM((BLOCK, vertices), bf16), pltpu.VMEM((BLOCK, WIDE), bf16),
                        pltpu.VMEM((DEG, BLOCK, WIDE), bf16), pltpu.SemaphoreType.DMA],
        name="extract",
    )(half, adj_slab)


def along(shape, axis=0):
    return lax.broadcasted_iota(jnp.int32, shape, axis)


def swap(x):
    return pltpu.roll(x, HALF, 1)


def digits(x, base):
    high = jnp.floor(x * (1.0 / base))
    return high, x - high * base


def walk_kernel(which_ref, src_ref, weight_ref, lists_ref, out_ref,
                table, queue, sigma, ratio, delta, cand, ids, now, dest, tail_ref, held, rowhot, colhot, bins,
                ids_a, ids_b, meta, sems, *, levels, vertices, scale, compact):
    pitch = vertices + SUB
    lane = along((SUB, LANES), 1)
    sub = along((SUB, LANES))
    upper = lane >= HALF
    lane_row = along((1, LANES), 1)
    group_odd = ((lane_row // 32) % 2) == 1
    lane32 = lane_row % 32
    rows_all = queue.shape[0]
    tile_bits = (vertices // lists_ref.shape[0]).bit_length() - 1
    high = vertices // WIDE

    def eight(row):
        return pl.ds(pl.multiple_of(row, SUB), SUB)

    def part(n):
        return pl.ds(n * SUB, SUB)

    def spread_row(ref, *index):
        return jnp.broadcast_to(ref[(*index[:-1], pl.ds(index[-1], 1), slice(None))], (SUB, LANES))

    def clear(t, carry):
        for k in range(SUB):
            rows = eight((t * SUB + k) * SUB)
            queue[rows, :] = jnp.full((SUB, LANES), -1.0, f32)
            sigma[rows, :] = jnp.zeros((SUB, LANES), f32)
        return carry

    def fetch(quad, row, buf):
        return pltpu.make_async_copy(ids.at[quad, eight(row)], buf[0], sems.at[buf[1]])

    def name(row, q):
        v = jnp.where(q < 0, vertices, q.astype(jnp.int32))
        ids[0, eight(row), :] = v
        ids[1, eight(row), :] = v + pitch

    bufs = (ids_a, 0), (ids_b, 1)
    clear(0, 0)

    near_source = jnp.full((SUB, LANES), EMPTY, f32)
    source = near_source
    for j in range(HALF):
        v = src_ref[which_ref[0] * HALF + j]
        tile = pltpu.roll(lists_ref[v >> tile_bits], (j - v) & (LANES - 1), 1)
        if compact:
            tile = jnp.where((v & LANES) > 0, pltpu.roll(tile, FEW, 0), tile)
        near_source = jnp.where(lane == j, tile, near_source)
        source = jnp.where(lane % HALF == j, v.astype(f32), source)
    near_source = jnp.where(upper, swap(near_source), near_source)
    reached = near_source >= 0
    if compact:
        reached = reached & (sub < FEW)
    queue[0:1, :] = source[:1]
    queue[eight(SUB), :] = jnp.where(reached, near_source, -1.0)
    sigma[eight(SUB), :] = jnp.where(reached & jnp.logical_not(upper), 1.0, 0.0)
    for n in (1, 2):
        name(n * SUB, queue[eight(n * SUB), :])
    bins[...] = jnp.zeros_like(bins)
    fetch(0, SUB, bufs[0]).start()
    if compact:
        fetch(0, 2 * SUB, bufs[1]).start()
    lax.fori_loop(1, rows_all // (SUB * SUB), clear, 0)

    srow = along((2 * SUB, LANES))
    slane = along((2 * SUB, LANES), 1)

    def fill(halves, target):
        picks = [jnp.where((srow % SUB) == (slane // 32 + FEW * h), jnp.where(srow < SUB, float(LANES), 1.0), 0.0).astype(bf16)
                 for h in halves]

        def body(step, most):
            for k in range(FEW):
                first = (FEW * step + k) * SUB
                x = jnp.concatenate([lists_ref[first + n] for n in range(SUB)], axis=1)
                both = jnp.concatenate(digits(x, LANES), axis=0).astype(bf16)
                for h, pick in zip(halves, picks):
                    rows = lax.dot_general(both, pick, (((0,), (0,)), ((), ())), preferred_element_type=f32)
                    for n in range(SUB):
                        table[pl.ds(pl.multiple_of(target(h, first + n), SUB), LANES), :] = rows[n * LANES:(n + 1) * LANES]
                for n in range(SUB):
                    most = jnp.maximum(most, lists_ref[first + n])
            return most

        return lax.fori_loop(0, lists_ref.shape[0] // (FEW * SUB), body, jnp.full((SUB, LANES), EMPTY, f32))

    table[vertices:pitch, :] = jnp.full((SUB, LANES), EMPTY, f32)
    if compact:
        most = fill(PAIR, lambda h, t: (2 * t + h) * LANES)
        quads = 1
    else:
        table[pitch + vertices:, :] = jnp.full((SUB, LANES), EMPTY, f32)
        most = fill((0,), lambda h, t: t * LANES)
        wide = jnp.max(jnp.where(sub >= FEW, most, EMPTY)) >= 0
        quads = jnp.where(wide, 2, 1)

        @pl.when(wide)
        def _():
            fill((1,), lambda h, t: pitch + t * LANES)

    bad = jnp.max(most) > vertices
    meta[FAULT] = bad.astype(jnp.int32)

    def gather(rows_of_ids):
        acc = [[jnp.full((1, LANES), EMPTY, f32)] * 2 for _ in rows_of_ids]
        for j in range(32):
            hit = lane32 == j
            for i, id_of in enumerate(rows_of_ids):
                for b in PAIR:
                    acc[i][b] = jnp.where(hit, table[pl.ds(id_of(b * 32 + j), 1), :], acc[i][b])
        return [(jnp.where(group_odd, b, a), pltpu.roll(jnp.where(group_odd, a, b), LANES - 32, 1)) for a, b in acc]

    def gather_slots(ids_s, slots=SLOTS):
        return gather([functools.partial(lambda i, j: ids_s[i, j], i) for i in range(slots)])

    def keep(rows, quad, row):
        for i, pair in enumerate(rows):
            for h in PAIR:
                cand[2 * quad + h, pl.ds(row + i, 1), :] = pair[h]

    def flag(x):
        return jnp.where(x, 1, 0)

    def at(unit, origin):
        return unit & (quads - 1), origin + (unit >> (quads - 1)) * SUB

    def level_step(level, carry):
        base, count = meta[BASE, level], meta[COUNT, level]
        following = base + (count + 7) // SUB * SUB
        batches = jnp.where(following <= CAP, (count + SLOTS - 1) // SLOTS, 0)
        units = batches * quads
        parity = meta[PARITY]

        def on_parity(n, f):
            for k in PAIR:
                @pl.when(n & 1 == k)
                def _():
                    f(bufs[k], bufs[1 - k])

        def unit_step(unit, other, to):
            quad, row = at(unit, base)
            x = [cand[2 * quad + h, eight(row), :] for h in PAIR]

            def search(first, count, marks):
                marks = list(marks)
                for k in range(count):
                    q = spread_row(queue, first + k)
                    for h in PAIR:
                        n = 2 * h + k % 2
                        marks[n] = jnp.where(x[h] == q, 1, marks[n])
                return tuple(marks)

            reach = following + meta[LENGTH] - PEEL
            marks = lax.fori_loop(0, (reach + SCAN - 1) // SCAN, lambda t, m: search(PEEL + t * SCAN, SCAN, m),
                                  (jnp.zeros((SUB, LANES), jnp.int32),) * 4)
            ahead = unit + 1 < units
            final_unit = unit + 1 == units
            soon = jnp.logical_and(final_unit, meta[AWAIT0] > 0)

            @pl.when(jnp.logical_or(ahead, soon))
            def _():
                fetch(0, base, to).wait()

            def insert(g):
                slots = [eight(following + g * WINDOW + SUB * t) for t in range(WINDOW // SUB)]
                qs = [queue[r, :] for r in slots]
                ss = [sigma[r, :] for r in slots]
                pos = [sub + (g * WINDOW + SUB * t) for t in range(WINDOW // SUB)]
                for h in PAIR:
                    for i in range(SUB):
                        d, e = spread_row(dest, SUB * h + i), spread_row(dest, SUB * (h + 2) + i)
                        v, w = spread_row(now, SUB * h + i), spread_row(now, SUB * (h + 2) + i)
                        for t in range(WINDOW // SUB):
                            qs[t] = jnp.where(pos[t] == d, v, jnp.where(pos[t] == e, w, qs[t]))
                for i in range(SUB):
                    v, w, sig = (spread_row(now, SUB * n + i) for n in (0, 1, 4))
                    for t in range(WINDOW // SUB):
                        ss[t] = ss[t] + jnp.where((qs[t] == v) | (qs[t] == w), sig, 0.0)
                for t, r in enumerate(slots):
                    queue[r, :] = qs[t]
                    sigma[r, :] = ss[t]
                return qs

            def core(looking):
                even, odd = x
                m, n, k, l = search(0, PEEL, marks)
                near_even, near_odd = m | n | flag(even < 0), k | l | flag(odd < 0)

                xr = [swap(v) for v in x]
                turns = [[[pltpu.roll(v, s, 0) if s else v for v in (x[h], xr[h])] for s in range(SUB)] for h in PAIR]
                for s, ((a, b), (c, d)) in enumerate(zip(*turns)):
                    near_odd = jnp.where((odd == a) | (odd == b), 1, near_odd)
                    if s:
                        after = sub >= s
                        near_even = jnp.where(((even == a) | (even == b)) & after, 1, near_even)
                        near_odd = jnp.where(((odd == c) | (odd == d)) & after, 1, near_odd)

                new = [1 - near_even, 1 - near_odd]
                packed = new[0] + BYTE * new[1]
                across = swap(packed)
                far = [across & (BYTE - 1), across >> SUB]
                both = packed + across
                run, whole = both, both
                for s in (1, 2, 4):
                    run = run + jnp.where(sub >= s, pltpu.roll(run, s, 0), 0)
                    whole = whole + pltpu.roll(whole, s, 0)
                run = run - both
                tail = tail_ref[...]
                evens = whole & (BYTE - 1)
                begin = [tail + (run & (BYTE - 1)), tail + evens + (run >> SUB)]
                for h in PAIR:
                    dest[part(h), :] = jnp.where(new[h] > 0, begin[h] + jnp.where(upper, far[h], 0), -1)
                    dest[part(h + 2), :] = jnp.where(far[h] > 0, begin[h] + jnp.where(upper, 0, new[h]), -1)
                    now[part(h), :] = x[h]
                    now[part(h + 2), :] = xr[h]
                now[part(4), :] = sigma[eight(row), :] + swap(sigma[eight(row), :])
                tail = tail + evens + (whole >> SUB)
                tail_ref[...] = tail
                passed = SLOTS * ((unit + 1) >> (quads - 1))
                second = SUB + SUB * (1 >> (quads - 1))
                need = jnp.where(sub == 1, SUB, second)
                short = (tail < need) & (held[...] > passed)
                most = jnp.max(jnp.where(sub == 0, tail, flag(short)).astype(f32), axis=1, keepdims=True)
                meta[REACHED] = most[0, 0].astype(jnp.int32)
                for n in PAIR:
                    meta[(SHORT0, SHORT1)[n]] = most[n + 1, 0].astype(jnp.int32)

                if looking:
                    quad2, row2 = at(unit + 1, base)
                    rows = gather_slots(to[0])
                qs = insert(0)
                for n in PAIR:
                    name(following + n * SUB, qs[n])
                if looking:
                    keep(rows, jnp.where(ahead, quad2, 0), jnp.where(ahead, row2, following))

            look = jnp.logical_or(ahead, soon)
            for looking in PAIR:
                @pl.when(look == (looking > 0))
                def _():
                    core(looking)

            length = meta[REACHED]
            ready = [meta[n] == 0 for n in (SHORT0, SHORT1)]

            @pl.when(unit + 3 < units)
            def _():
                fetch(*at(unit + 3, base), to).start()

            @pl.when(soon)
            def _():
                meta[GOT] = 1

            def first_of_next(n, when, buf):
                @pl.when(jnp.logical_and(when, meta[(AWAIT0, AWAIT1)[n]] == 0))
                def _():
                    fetch(*at(n, following), buf).start()
                    meta[(AWAIT0, AWAIT1)[n]] = 1

            first_of_next(0, jnp.logical_and(ready[0], unit + 3 == units), to)
            first_of_next(0, jnp.logical_and(ready[0], unit + 2 == units), other)
            first_of_next(1, jnp.logical_and(ready[1], unit + 2 == units), to)
            first_of_next(0, final_unit, to)
            first_of_next(1, final_unit, other)

            groups = (length + WINDOW - 1) // WINDOW
            fits = following + groups * WINDOW <= CAP + WINDOW
            meta[LENGTH] = jnp.where(fits, length, 0)

            @pl.when(jnp.logical_not(fits))
            def _():
                meta[FAULT] = 1

            def more(g, carry):
                insert(g)
                return carry

            lax.fori_loop(1, jnp.where(fits, groups, 0), more, 0)

        tail_ref[...] = jnp.zeros_like(tail_ref)
        meta[LENGTH] = 0

        def open_level(mine, other):
            @pl.when(jnp.logical_and(meta[GOT] == 0, meta[AWAIT0] > 0))
            def _():
                fetch(0, base, mine).wait()
                keep(gather_slots(mine[0]), 0, base)

            @pl.when(jnp.logical_and(units < 2, meta[AWAIT1] > 0))
            def _():
                fetch(0, base, other).wait()

            @pl.when(units > 2)
            def _():
                fetch(*at(2, base), mine).start()

        on_parity(parity, open_level)
        for place_ in (GOT, AWAIT0, AWAIT1):
            meta[place_] = 0

        def any_unit(unit, carry):
            on_parity(parity + unit, functools.partial(unit_step, unit))
            return carry

        lax.fori_loop(0, units, any_unit, 0)
        meta[PARITY] = parity + units

        @pl.when(following > CAP)
        def _():
            meta[FAULT] = 1

        found = jnp.where(meta[FAULT] == 0, meta[LENGTH], 0)
        meta[BASE, level + 1] = following
        meta[COUNT, level + 1] = found

        def names(t, carry):
            row = following + t * SUB
            name(row, queue[eight(row), :])
            return carry

        lax.fori_loop(2, (found + SUB - 1) // SUB, names, 0)
        held[...] = tail_ref[...]
        return carry

    for place_ in (GOT, PARITY):
        meta[place_] = 0

    @pl.when(jnp.logical_not(bad))
    def _():
        held[...] = jnp.full_like(held, FEW * quads)
        meta[BASE, 1] = SUB
        meta[COUNT, 1] = FEW * quads
        fetch(0, SUB, bufs[0]).wait()
        if compact:
            for h in PAIR:
                cand[h, eight(SUB), :] = jnp.full((SUB, LANES), EMPTY, f32)
        else:
            fetch(*at(1, SUB), bufs[1]).start()
        keep(gather_slots(ids_a, FEW if compact else SLOTS), 0, SUB)
        meta[GOT] = 1
        meta[AWAIT0] = 0
        meta[AWAIT1] = 1
        lax.fori_loop(1, levels, level_step, 0)

    @pl.when(bad)
    def _():
        fetch(0, SUB, bufs[0]).wait()
        meta[AWAIT0] = 0
        meta[AWAIT1] = int(compact)

    def drain(n, buf):
        @pl.when(meta[(AWAIT0, AWAIT1)[n]] > 0)
        def _():
            fetch(0, 0, buf).wait()

    for k in PAIR:
        @pl.when(meta[PARITY] & 1 == k)
        def _():
            @pl.when(meta[GOT] == 0)
            def _():
                drain(0, bufs[k])

            drain(1, bufs[1 - k])

    good = meta[FAULT] == 0

    @pl.when(good)
    def _():
        last = meta[BASE, levels]
        g_last = weight_ref[levels - 2]

        def seed(g, carry):
            for t in range(WINDOW // SUB):
                r = eight(last + g * WINDOW + SUB * t)
                s = sigma[r, :] + swap(sigma[r, :])
                ratio[r, :] = jnp.where(s > 0, g_last / jnp.where(s > 0, s, 1.0), 0.0)
            return carry

        lax.fori_loop(0, (meta[COUNT, levels] + WINDOW - 1) // WINDOW, seed, 0)

        def back_step(k, carry):
            level = levels - 1 - k
            base, count = meta[BASE, level], meta[COUNT, level]
            nbase, ncount = meta[BASE, level + 1], meta[COUNT, level + 1]
            g_here = weight_ref[jnp.maximum(level - 2, 0)]

            def pull_batch(bt, carry):
                here = eight(base + bt * SLOTS)

                def pull(quad, c, acc):
                    even, odd = cand[2 * quad, here, :], cand[2 * quad + 1, here, :]
                    acc = list(acc)
                    for n in range(WINDOW):
                        q = spread_row(queue, nbase + c * WINDOW + n)
                        w = spread_row(ratio, nbase + c * WINDOW + n)
                        acc[n % 2] = acc[n % 2] + jnp.where((even == q) | (odd == q), w, 0.0)
                    return tuple(acc)

                def pull_quad(quad, acc):
                    return lax.fori_loop(1, (ncount + WINDOW - 1) // WINDOW, functools.partial(pull, quad), pull(quad, 0, acc))

                acc = pull_quad(0, (jnp.zeros((SUB, LANES), f32),) * 2)
                if not compact:
                    acc = lax.fori_loop(1, quads, pull_quad, acc)
                delta[here, :] = acc[0] + acc[1]
                return carry

            lax.fori_loop(0, (count + SLOTS - 1) // SLOTS, pull_batch, 0)

            def finish(g, carry):
                slots = [eight(base + g * WINDOW + SUB * t) for t in range(WINDOW // SUB)]
                for t, r in enumerate(slots):
                    inside = g * WINDOW + SUB * t < count
                    part, s = (v + swap(v) for v in (delta[r, :], sigma[r, :]))
                    d = s * part
                    w = jnp.where(s > 0, (g_here + d) / jnp.where(s > 0, s, 1.0), 0.0)
                    delta[r, :] = jnp.where(inside, d, delta[r, :])
                    ratio[r, :] = jnp.where(inside, w, ratio[r, :])
                return carry

            lax.fori_loop(0, (count + WINDOW - 1) // WINDOW, finish, 0)
            return carry

        lax.fori_loop(0, levels - 1, back_step, 0)

        tall = along((WIDE, WIDE)).astype(f32).astype(bf16)
        zero = jnp.zeros((WIDE, WIDE), bf16)
        one = zero + 1
        start = meta[BASE, 1]

        def tally(t, carry):
            for u in range(TALLY // 16):
                a, b = eight(start + t * TALLY + u * 16), eight(start + t * TALLY + u * 16 + SUB)
                v = jnp.where(upper, queue[b, :], queue[a, :])
                d = jnp.where(upper, delta[b, :], delta[a, :])
                hi, lo = digits(v, WIDE)
                d_hi = d.astype(bf16).astype(f32)
                d_mid = (d - d_hi).astype(bf16).astype(f32)
                d_lo = d - d_hi - d_mid
                for p in range(0, SUB, 2):
                    cols = slice((u * SUB + p) * LANES, (u * SUB + p + 2) * LANES)

                    def pair(x):
                        return jnp.concatenate([x[p:p + 1], x[p + 1:p + 2]], axis=1).astype(bf16)

                    colhot[:, cols] = jnp.where(tall == pair(lo), one, zero)
                    match = tall[:high] == pair(hi)
                    for n, x in enumerate((d_hi, d_mid, d_lo)):
                        rowhot[n * high:(n + 1) * high, cols] = jnp.where(match, pair(x), zero[:high])
            bins[...] += lax.dot_general(rowhot[...], colhot[...], TURN, preferred_element_type=f32)
            return carry

        for t in range(TALLY // SUB):
            delta[eight(last + t * SUB), :] = jnp.zeros((SUB, LANES), f32)
        lax.fori_loop(0, (last - start + TALLY - 1) // TALLY, tally, 0)

    blocks = out_ref.shape[0]
    per = high // blocks
    total = (bins[:high] + bins[high:2 * high] + bins[2 * high:]) * scale
    fault = jnp.where(good, 0.0, 1.0)
    for b in range(blocks):
        for n in PAIR:
            out_ref[b, n * per:(n + 1) * per, :] = total[b * per:(b + 1) * per, n * LANES:(n + 1) * LANES]
        out_ref[b, 2 * per:, :] = jnp.full((SUB, LANES), fault, f32)


def walk(which, sources, weights, lists, *, blocks, vertices, scale, compact):
    levels = weights.shape[0] + 1
    rows = CAP + 4 * WINDOW
    high = LANES // blocks + SUB
    vm = pltpu.VMEM
    queue = vm((rows, LANES), f32)
    parts = 3 * (vertices // WIDE)
    return pl.pallas_call(
        functools.partial(walk_kernel, levels=levels, vertices=vertices, scale=scale, compact=compact),
        in_specs=[pl.BlockSpec(memory_space=pltpu.SMEM)] * 3 + [pl.BlockSpec(memory_space=pltpu.VMEM)],
        out_specs=pl.BlockSpec(memory_space=pltpu.VMEM),
        out_shape=jax.ShapeDtypeStruct((blocks, high, LANES), f32),
        scratch_shapes=[
            vm(((1 if compact else 2) * (vertices + SUB), LANES), f32), queue, queue, queue, queue,
            vm((4, rows, LANES), f32), vm((2, rows, LANES), jnp.int32),
            vm((40, LANES), f32), vm((32, LANES), jnp.int32), vm((SUB, LANES), jnp.int32), vm((SUB, LANES), jnp.int32),
            vm((parts, TALLY // 2 * LANES), bf16), vm((WIDE, TALLY // 2 * LANES), bf16), vm((parts, WIDE), f32),
            pltpu.SMEM((SLOTS, LANES), jnp.int32), pltpu.SMEM((SLOTS, LANES), jnp.int32), pltpu.SMEM((3, 16), jnp.int32),
            pltpu.SemaphoreType.DMA((2,)),
        ],
        compiler_params=pltpu.CompilerParams(
            vmem_limit_bytes=48 * 1024 * 1024),
        name="walk",
    )(which, sources, weights, lists)


def share_kernel(src, graph, x_ref, o_ref, own_sem, send_sem, recv_sem):
    y, g = lax.axis_index("src"), lax.axis_index("graph")
    others = [((y + i) % src, (g + k) % graph) for i, k in everyone(src, graph)][1:]
    hello(others)
    await_hello(others)
    mine = g * src + y
    own = pltpu.make_async_copy(x_ref, o_ref.at[mine], own_sem)
    own.start()
    copies = []
    for n, (py, pg) in enumerate(others):
        copies.append(pltpu.make_async_remote_copy(
            src_ref=x_ref, dst_ref=o_ref.at[mine], send_sem=send_sem.at[n], recv_sem=recv_sem.at[n],
            device_id={"src": py, "graph": pg}, device_id_type=MESH))
        copies[-1].start()
    own.wait()
    for c in copies:
        c.wait()


def share(x, src, graph):
    n = src * graph
    return pl.pallas_call(
        functools.partial(share_kernel, src, graph),
        in_specs=[pl.BlockSpec(memory_space=pltpu.VMEM)],
        out_specs=pl.BlockSpec(memory_space=pltpu.VMEM),
        out_shape=jax.ShapeDtypeStruct((n,) + x.shape, x.dtype),
        scratch_shapes=[pltpu.SemaphoreType.DMA, pltpu.SemaphoreType.DMA((n - 1,)), pltpu.SemaphoreType.DMA((n - 1,))],
        compiler_params=pltpu.CompilerParams(collective_id=2, has_side_effects=True),
        name="share",
    )(x)


def total_kernel(src, graph, x_ref, o_ref, got, own_sem, send_sem, recv_sem):
    y, g = lax.axis_index("src"), lax.axis_index("graph")
    others = [((y + i) % src, (g + k) % graph) for i, k in everyone(src, graph)][1:]
    hello(others)
    mine = g * src + y
    own = pltpu.make_async_copy(x_ref.at[g], got.at[mine], own_sem)
    own.start()
    await_hello(others)
    copies = []
    for n, (py, pg) in enumerate(others):
        copies.append(pltpu.make_async_remote_copy(
            src_ref=x_ref.at[pg], dst_ref=got.at[mine], send_sem=send_sem.at[n], recv_sem=recv_sem.at[n],
            device_id={"src": py, "graph": pg}, device_id_type=MESH))
        copies[-1].start()
    own.wait()
    for c in copies:
        c.wait()
    acc = got[0]
    for n in range(1, src * graph):
        acc = acc + got[n]
    o_ref[...] = acc


def total(x, src, graph, collective_id):
    n = src * graph
    return pl.pallas_call(
        functools.partial(total_kernel, src, graph),
        in_specs=[pl.BlockSpec(memory_space=pltpu.VMEM)],
        out_specs=pl.BlockSpec(memory_space=pltpu.VMEM),
        out_shape=jax.ShapeDtypeStruct(x.shape[1:], x.dtype),
        scratch_shapes=[pltpu.VMEM((n,) + x.shape[1:], x.dtype), pltpu.SemaphoreType.DMA,
                        pltpu.SemaphoreType.DMA((n - 1,)), pltpu.SemaphoreType.DMA((n - 1,))],
        compiler_params=pltpu.CompilerParams(collective_id=collective_id, has_side_effects=True),
        name="total",
    )(pltpu.with_memory_space_constraint(x, pltpu.VMEM))


def exchange(x, axis):
    return lax.all_to_all(x, axis, 0, 0)


def dense(adj_slab, src_local, level_weight, src, graph):
    slab_rows, vertex_count = adj_slab.shape
    src_count = src_local.shape[0]
    levels = level_weight.shape[0] + 1
    row_start = lax.axis_index("graph") * slab_rows
    vertex_ids = row_start + lax.broadcasted_iota(jnp.int32, (slab_rows, 1), 0)
    first = jnp.where(vertex_ids == src_local[None, :], 1.0, 0.0).astype(f32)

    def forward(carry, unused):
        sigma, seen = carry
        partial = jnp.einsum("uv,us->vs", adj_slab, sigma, preferred_element_type=f32, precision=exact_precision)
        parts = exchange(partial.reshape(graph, slab_rows, src_count), "graph")
        sigma = jnp.sum(parts, axis=0) * (1.0 - seen)
        seen = jnp.maximum(seen, jnp.where(sigma > 0, 1.0, 0.0))
        return (sigma, seen), sigma

    _, sigmas = lax.scan(forward, (first, first), None, length=levels)

    def backward(carry, xs):
        delta, acc = carry
        upper, lower, weight = xs
        reached = upper > 0
        ratio = jnp.where(reached, (weight + delta) / jnp.where(reached, upper, 1.0), 0.0)
        gathered = exchange(jnp.broadcast_to(ratio[None], (graph,) + ratio.shape), "graph")
        pulled = jnp.einsum("uv,vs->us", adj_slab, gathered.reshape(vertex_count, src_count),
                            preferred_element_type=f32, precision=exact_precision)
        delta = lower * pulled
        return (delta, acc + delta), None

    zero = jnp.zeros_like(first)
    (_, acc), _ = lax.scan(backward, (zero, zero), (sigmas[1:][::-1], sigmas[:-1][::-1], level_weight[::-1]))
    scale = vertex_count / (src_count * src * levels ** 3)
    mine = jnp.sum(acc, axis=1) * scale
    both = exchange(jnp.broadcast_to(mine.reshape(1, -1, LANES), (src, slab_rows // LANES, LANES)), "src")
    return jnp.sum(both, axis=0).reshape(slab_rows)


def solution(mesh):
    src, graph = mesh.shape["src"], mesh.shape["graph"]

    def device_program(adj_slab, src_local, level_weight):
        slab_rows, vertex_count = adj_slab.shape
        levels = level_weight.shape[0] + 1
        scale = vertex_count / (HALF * src * graph * levels ** 3)
        which = lax.axis_index("graph").astype(jnp.int32).reshape(1)

        def finish(lists, compact, collective_id, other):
            parts = walk(which, src_local, level_weight, lists, blocks=graph, vertices=vertex_count, scale=scale, compact=compact)
            summed = total(parts, src, graph, collective_id)
            rows = slab_rows // LANES

            def plain():
                return summed[:rows].reshape(2, -1, LANES).transpose(1, 0, 2).reshape(slab_rows)

            return lax.cond(summed[rows, 0] > 0, other, plain)

        def dense_path():
            return dense(adj_slab, src_local, level_weight, src, graph)

        def general_path():
            half = lax.axis_index("src").astype(jnp.int32).reshape(1)
            lists = share(extract(adj_slab, half, slab_rows // src), src, graph)
            return finish(lists.reshape(-1, SUB, LANES), False, 3, dense_path)

        return finish(collect(adj_slab, src, graph), True, 1, general_path)

    return jax.shard_map(device_program, mesh=mesh,
                         in_specs=(P(("batch", "graph"), None), P(("batch", "src")), P(None)),
                         out_specs=P(("batch", "graph")), check_vma=False)
```

```python
import functools

import jax
import jax.numpy as jnp
from jax import lax
from jax.experimental import pallas as pl
from jax.experimental.pallas import tpu as pltpu
from jax.sharding import PartitionSpec as P

MESH = pl.DeviceIdType.MESH
exact_precision = lax.Precision.HIGHEST
f32, bf16 = jnp.float32, jnp.bfloat16

LANES, SUB = 128, 8
WIDE = 256
DEG, FEW = 8, 4
EMPTY = -2.0
FULL = 32767.0
TURN = (((1,), (1,)), ((), ()))
BLOCK = 128
READS = 4
STEP = 32
HALF = 64
SLOTS = 8
WINDOW = 48
SCAN = 32
CAP = 1024
TALLY = 96
PAIR = (0, 1)
BYTE = 256
GROUP = 8
PEEL = 32
BASE, COUNT = 0, 1
FAULT, LENGTH, GOT, PARITY, AWAIT0, AWAIT1, REACHED, SHORT0, SHORT1 = ((2, n) for n in range(9))


def place_and_others(src, graph):
    y, g = lax.axis_index("src"), lax.axis_index("graph")
    steps = sorted(((i, k) for i in range(src) for k in range(graph)), key=lambda s: (-s[0], abs(s[1] - graph // 2)))
    return g * src + y, g, [((y + i) % src, (g + k) % graph) for i, k in steps if i + k]


def hello(peers):
    for y, g in peers:
        pl.semaphore_signal(pltpu.get_barrier_semaphore(), inc=1, device_id={"src": y, "graph": g}, device_id_type=MESH)


def await_hello(peers):
    pl.semaphore_wait(pltpu.get_barrier_semaphore(), len(peers))


def place(plane, lists):
    lists = list(lists)
    row_i = lax.broadcasted_iota(jnp.int32, (WIDE, WIDE), 0)
    col_i = lax.broadcasted_iota(jnp.int32, (WIDE, WIDE), 1)
    eye = jnp.where(row_i == col_i, float(WIDE), 0.0).astype(bf16)
    flipped = lax.dot_general(eye, plane, TURN, preferred_element_type=f32)
    lane_id = lax.broadcasted_iota(jnp.int32, (SUB, flipped.shape[1]), 0).astype(f32)
    for g in range(WIDE // SUB):
        x = flipped[g * SUB:(g + 1) * SUB] + (lane_id + float(g * SUB))
        for s in range(len(lists)):
            hi = jnp.maximum(lists[s], x)
            if s < len(lists) - 1:
                x = jnp.minimum(lists[s], x)
            lists[s] = hi
    return lists


def sort(lists):
    gap = len(lists) // 2
    while gap:
        for s in range(len(lists)):
            if not s & gap:
                lists[s], lists[s + gap] = jnp.maximum(lists[s], lists[s + gap]), jnp.minimum(lists[s], lists[s + gap])
        gap //= 2
    return lists


def over_sublanes(lists):
    size = len(lists)
    for shift in (4, 2, 1):
        other = [pltpu.roll(v, shift, 0) for v in lists]
        lists = sort([jnp.maximum(lists[s], other[size - 1 - s]) for s in range(size)])
    out = jnp.full(lists[0].shape, EMPTY, f32)
    sub = lax.broadcasted_iota(jnp.int32, out.shape, 0)
    for s in range(size):
        out = jnp.where(sub == s, jnp.where(lists[s] >= WIDE, lists[s] - WIDE, EMPTY), out)
    return out


def degree_of(seen):
    return lax.dot_general(jnp.ones((SUB, WIDE), bf16), seen, TURN, preferred_element_type=f32)


def collect_kernel(src, graph, a_ref, o_ref, bufs, tops, mine, sems, own_sem, send_sems, recv_sems):
    vertices = a_ref.shape[1]
    pairs, chunks = mine.shape[0], vertices // WIDE
    blocks = 2 * pairs
    me, _, others = place_and_others(src, graph)
    y = me % src
    height = 4 * SUB
    pieces = BLOCK // height

    def fetch(i, t):
        rows = pl.ds(pl.multiple_of((y * blocks + i) * BLOCK + t * height, height), height)
        here = pl.ds(pl.multiple_of(t * height, height), height)
        return pltpu.make_async_copy(a_ref.at[rows], bufs.at[i % READS, here], sems.at[i % READS, t])

    def send(n, first, count):
        py, pg = others[n]
        return pltpu.make_async_remote_copy(
            src_ref=mine.at[pl.ds(first, count)], dst_ref=o_ref.at[pl.ds(me * pairs + first, count)],
            send_sem=send_sems.at[n], recv_sem=recv_sems.at[n], device_id={"src": py, "graph": pg}, device_id_type=MESH)

    def send_pair(p):
        for n in range(len(others)):
            send(n, p, 1).start()

    for i in range(READS - 1):
        for t in range(pieces):
            fetch(i, t).start()
    hello(others)
    none = jnp.zeros((SUB, 2 * BLOCK), f32)

    def scan(i, first):
        @pl.when(i + READS - 1 < blocks)
        def _():
            for t in range(pieces):
                fetch(i + READS - 1, t).start()

        def scan_rows(t, carry):
            fetch(i, t).wait()
            here = pl.ds(pl.multiple_of(t * height, height), height)

            def scan_chunks(c, state):
                top, low, seen, sums, value = state
                for k in range(STEP):
                    a = bufs[i % READS, here, pl.ds(pl.multiple_of((c * STEP + k) * WIDE, WIDE), WIDE)]
                    x = a * value
                    low = jnp.maximum(low, jnp.minimum(top, x))
                    top = jnp.maximum(top, x)
                    seen = seen + a
                    sums = sums + x
                    value = value + 1
                return top, low, seen, sums, value

            zero = jnp.zeros((height, WIDE), bf16)
            top, low, seen, sums, _ = lax.fori_loop(0, chunks // STEP, scan_chunks, (zero,) * 4 + (zero + 1,))
            for n, v in enumerate((top, low, (sums - top) - low, seen)):
                tops[n, pl.ds(pl.multiple_of(first + t * height, height), height), :] = v
            return carry

        lax.fori_loop(0, pieces, scan_rows, 0)

    def pair_step(p, carry):
        for h in range(2):
            scan(2 * p + h, h * BLOCK)
        seen = tops[3]
        crowd = seen[:SUB]
        for k in range(1, 2 * BLOCK // SUB):
            crowd = jnp.maximum(crowd, seen[k * SUB:(k + 1) * SUB])
        crowd = jnp.max(crowd.astype(f32), axis=0, keepdims=True)
        a, b, c = place(tops[0], (none,) * 4), place(tops[1], (none,) * 2), place(tops[2], (none,))
        rest = [jnp.maximum(b[0], c[0]), jnp.minimum(b[0], c[0])]
        rest = [rest[0], jnp.maximum(b[1], rest[1]), jnp.minimum(b[1], rest[1])]
        lists = over_sublanes(sort([a[0]] + [jnp.maximum(a[s + 1], rest[2 - s]) for s in range(3)]))
        lists = jnp.where((crowd > 3) | (degree_of(seen) > 4), FULL, lists)
        even, odd = lists[:, :BLOCK], lists[:, BLOCK:]
        sub = lax.broadcasted_iota(jnp.int32, even.shape, 0)
        mine[p] = jnp.where(sub < 4, even, pltpu.roll(odd, 4, 0))

        @pl.when(p == 1)
        def _():
            await_hello(others)

        @pl.when(p > 0)
        def _():
            send_pair(p - 1)

        return carry

    lax.fori_loop(0, pairs, pair_step, 0)
    own = pltpu.make_async_copy(mine, o_ref.at[pl.ds(me * pairs, pairs)], own_sem)
    send_pair(pairs - 1)
    own.start()
    own.wait()
    for n in range(len(others)):
        send(n, 0, pairs).wait()


def collect(adj_slab, src, graph):
    rows, vertices = adj_slab.shape
    n = src * graph
    mine = (rows // src // (2 * BLOCK), SUB, BLOCK)
    return pl.pallas_call(
        functools.partial(collect_kernel, src, graph),
        in_specs=[pl.BlockSpec(memory_space=pl.ANY)],
        out_specs=pl.BlockSpec(memory_space=pltpu.VMEM),
        out_shape=jax.ShapeDtypeStruct((n * mine[0],) + mine[1:], f32),
        scratch_shapes=[pltpu.VMEM((READS, BLOCK, vertices), bf16), pltpu.VMEM((4, 2 * BLOCK, WIDE), bf16), pltpu.VMEM(mine, f32),
                        pltpu.SemaphoreType.DMA((READS, BLOCK // (4 * SUB))), pltpu.SemaphoreType.DMA,
                        pltpu.SemaphoreType.DMA((n - 1,)), pltpu.SemaphoreType.DMA((n - 1,))],
        compiler_params=pltpu.CompilerParams(collective_id=0, has_side_effects=True, vmem_limit_bytes=40 * 1024 * 1024),
        name="collect",
    )(adj_slab)


def extract_kernel(half_ref, a_ref, o_ref, block, seen, planes, sem):
    vertices = a_ref.shape[1]

    def block_step(i, carry):
        copy = pltpu.make_async_copy(
            a_ref.at[pl.ds(pl.multiple_of((half_ref[0] * o_ref.shape[0] + i) * BLOCK, BLOCK), BLOCK)], block, sem)
        copy.start()
        copy.wait()
        planes[...] = jnp.zeros_like(planes)
        seen[...] = jnp.zeros_like(seen)

        def scan_chunk(c, carry):
            a = block[:, pl.ds(pl.multiple_of(c * WIDE, WIDE), WIDE)]
            seen[...] = seen[...] + a
            x = a.astype(f32) * (c + 1).astype(f32)
            for s in range(DEG):
                top = planes[s].astype(f32)
                planes[s] = jnp.maximum(top, x).astype(bf16)
                x = jnp.minimum(top, x)
            return carry

        lax.fori_loop(0, vertices // WIDE, scan_chunk, 0)
        lists = lax.fori_loop(0, DEG, lambda p, lists: tuple(place(planes[p], lists)), (jnp.zeros((SUB, BLOCK), f32),) * DEG)
        o_ref[i] = jnp.where(degree_of(seen[...]) > DEG, FULL, over_sublanes(list(lists)))
        return carry

    lax.fori_loop(0, o_ref.shape[0], block_step, 0)


def extract(adj_slab, half, rows):
    vertices = adj_slab.shape[1]
    return pl.pallas_call(
        extract_kernel,
        in_specs=[pl.BlockSpec(memory_space=pltpu.SMEM), pl.BlockSpec(memory_space=pl.ANY)],
        out_specs=pl.BlockSpec(memory_space=pltpu.VMEM),
        out_shape=jax.ShapeDtypeStruct((rows // BLOCK, DEG, BLOCK), f32),
        scratch_shapes=[pltpu.VMEM((BLOCK, vertices), bf16), pltpu.VMEM((BLOCK, WIDE), bf16),
                        pltpu.VMEM((DEG, BLOCK, WIDE), bf16), pltpu.SemaphoreType.DMA],
        name="extract",
    )(half, adj_slab)


def along(shape, axis=0):
    return lax.broadcasted_iota(jnp.int32, shape, axis)


def swap(x):
    return pltpu.roll(x, HALF, 1)


def digits(x, base):
    high = jnp.floor(x * (1.0 / base))
    return high, x - high * base


def walk_kernel(which_ref, src_ref, weight_ref, lists_ref, out_ref,
                table, queue, sigma, ratio, delta, cand, ids, now, dest, tail_ref, held, rowhot, colhot, bins,
                ids_a, ids_b, meta, sems, *, levels, vertices, scale, compact):
    pitch = vertices + SUB
    lane = along((SUB, LANES), 1)
    sub = along((SUB, LANES))
    upper = lane >= HALF
    lane_row = along((1, LANES), 1)
    group_odd = ((lane_row // 32) % 2) == 1
    lane32 = lane_row % 32
    rows_all = queue.shape[0]
    tile_bits = (vertices // lists_ref.shape[0]).bit_length() - 1
    high = vertices // WIDE

    def eight(row):
        return pl.ds(pl.multiple_of(row, SUB), SUB)

    def part(n):
        return pl.ds(n * SUB, SUB)

    def spread_row(ref, *index):
        return jnp.broadcast_to(ref[(*index[:-1], pl.ds(index[-1], 1), slice(None))], (SUB, LANES))

    def clear(t, carry):
        for k in range(SUB):
            rows = eight((t * SUB + k) * SUB)
            queue[rows, :] = jnp.full((SUB, LANES), -1.0, f32)
            sigma[rows, :] = jnp.zeros((SUB, LANES), f32)
        return carry

    def fetch(quad, row, buf):
        return pltpu.make_async_copy(ids.at[quad, eight(row)], buf[0], sems.at[buf[1]])

    def name(row, q):
        v = jnp.where(q < 0, vertices, q.astype(jnp.int32))
        ids[0, eight(row), :] = v
        ids[1, eight(row), :] = v + pitch

    bufs = (ids_a, 0), (ids_b, 1)
    clear(0, 0)

    near_source = jnp.full((SUB, LANES), EMPTY, f32)
    source = near_source
    for j in range(HALF):
        v = src_ref[which_ref[0] * HALF + j]
        tile = pltpu.roll(lists_ref[v >> tile_bits], (j - v) & (LANES - 1), 1)
        if compact:
            tile = jnp.where((v & LANES) > 0, pltpu.roll(tile, FEW, 0), tile)
        near_source = jnp.where(lane == j, tile, near_source)
        source = jnp.where(lane % HALF == j, v.astype(f32), source)
    near_source = jnp.where(upper, swap(near_source), near_source)
    reached = near_source >= 0
    if compact:
        reached = reached & (sub < FEW)
    queue[0:1, :] = source[:1]
    queue[eight(SUB), :] = jnp.where(reached, near_source, -1.0)
    sigma[eight(SUB), :] = jnp.where(reached & jnp.logical_not(upper), 1.0, 0.0)
    for n in (1, 2):
        name(n * SUB, queue[eight(n * SUB), :])
    bins[...] = jnp.zeros_like(bins)
    fetch(0, SUB, bufs[0]).start()
    if compact:
        fetch(0, 2 * SUB, bufs[1]).start()
    lax.fori_loop(1, rows_all // (SUB * SUB), clear, 0)

    srow = along((2 * SUB, LANES))
    slane = along((2 * SUB, LANES), 1)

    def fill(halves, target):
        picks = [jnp.where((srow % SUB) == (slane // 32 + FEW * h), jnp.where(srow < SUB, float(LANES), 1.0), 0.0).astype(bf16)
                 for h in halves]

        def body(step, most):
            for k in range(GROUP):
                first = (GROUP * step + k) * SUB
                x = jnp.concatenate([lists_ref[first + n] for n in range(SUB)], axis=1)
                both = jnp.concatenate(digits(x, LANES), axis=0).astype(bf16)
                for h, pick in zip(halves, picks):
                    rows = lax.dot_general(both, pick, (((0,), (0,)), ((), ())), preferred_element_type=f32)
                    for n in range(SUB):
                        table[pl.ds(pl.multiple_of(target(h, first + n), SUB), LANES), :] = rows[n * LANES:(n + 1) * LANES]
                for n in range(SUB):
                    most = jnp.maximum(most, lists_ref[first + n])
            return most

        return lax.fori_loop(0, lists_ref.shape[0] // (GROUP * SUB), body, jnp.full((SUB, LANES), EMPTY, f32))

    table[vertices:pitch, :] = jnp.full((SUB, LANES), EMPTY, f32)
    if compact:
        most = fill(PAIR, lambda h, t: (2 * t + h) * LANES)
        quads = 1
    else:
        table[pitch + vertices:, :] = jnp.full((SUB, LANES), EMPTY, f32)
        most = fill((0,), lambda h, t: t * LANES)
        wide = jnp.max(jnp.where(sub >= FEW, most, EMPTY)) >= 0
        quads = jnp.where(wide, 2, 1)

        @pl.when(wide)
        def _():
            fill((1,), lambda h, t: pitch + t * LANES)

    bad = jnp.max(most) > vertices
    meta[FAULT] = bad.astype(jnp.int32)

    def gather(rows_of_ids):
        acc = [[jnp.full((1, LANES), EMPTY, f32)] * 2 for _ in rows_of_ids]
        for j in range(32):
            hit = lane32 == j
            for i, id_of in enumerate(rows_of_ids):
                for b in PAIR:
                    acc[i][b] = jnp.where(hit, table[pl.ds(id_of(b * 32 + j), 1), :], acc[i][b])
        return [(jnp.where(group_odd, b, a), pltpu.roll(jnp.where(group_odd, a, b), LANES - 32, 1)) for a, b in acc]

    def gather_slots(ids_s, slots=SLOTS):
        return gather([functools.partial(lambda i, j: ids_s[i, j], i) for i in range(slots)])

    def keep(rows, quad, row):
        for i, pair in enumerate(rows):
            for h in PAIR:
                cand[2 * quad + h, pl.ds(row + i, 1), :] = pair[h]

    def flag(x):
        return jnp.where(x, 1, 0)

    def at(unit, origin):
        return unit & (quads - 1), origin + (unit >> (quads - 1)) * SUB

    def level_step(level, carry):
        base, count = meta[BASE, level], meta[COUNT, level]
        following = base + (count + 7) // SUB * SUB
        batches = jnp.where(following <= CAP, (count + SLOTS - 1) // SLOTS, 0)
        units = batches * quads
        parity = meta[PARITY]

        def on_parity(n, f):
            for k in PAIR:
                @pl.when(n & 1 == k)
                def _():
                    f(bufs[k], bufs[1 - k])

        def unit_step(unit, other, to):
            quad, row = at(unit, base)
            x = [cand[2 * quad + h, eight(row), :] for h in PAIR]

            def search(first, count, marks):
                marks = list(marks)
                for k in range(count):
                    q = spread_row(queue, first + k)
                    for h in PAIR:
                        n = 2 * h + k % 2
                        marks[n] = jnp.where(x[h] == q, 1, marks[n])
                return tuple(marks)

            reach = following + meta[LENGTH] - PEEL
            marks = lax.fori_loop(0, (reach + SCAN - 1) // SCAN, lambda t, m: search(PEEL + t * SCAN, SCAN, m),
                                  (jnp.zeros((SUB, LANES), jnp.int32),) * 4)
            ahead = unit + 1 < units
            final_unit = unit + 1 == units
            soon = jnp.logical_and(final_unit, meta[AWAIT0] > 0)

            @pl.when(jnp.logical_or(ahead, soon))
            def _():
                fetch(0, base, to).wait()

            def insert(g):
                slots = [eight(following + g * WINDOW + SUB * t) for t in range(WINDOW // SUB)]
                qs = [queue[r, :] for r in slots]
                ss = [sigma[r, :] for r in slots]
                pos = [sub + (g * WINDOW + SUB * t) for t in range(WINDOW // SUB)]
                for h in PAIR:
                    for i in range(SUB):
                        d, e = spread_row(dest, SUB * h + i), spread_row(dest, SUB * (h + 2) + i)
                        v, w = spread_row(now, SUB * h + i), spread_row(now, SUB * (h + 2) + i)
                        for t in range(WINDOW // SUB):
                            qs[t] = jnp.where(pos[t] == d, v, jnp.where(pos[t] == e, w, qs[t]))
                for i in range(SUB):
                    v, w, sig = (spread_row(now, SUB * n + i) for n in (0, 1, 4))
                    for t in range(WINDOW // SUB):
                        ss[t] = ss[t] + jnp.where((qs[t] == v) | (qs[t] == w), sig, 0.0)
                for t, r in enumerate(slots):
                    queue[r, :] = qs[t]
                    sigma[r, :] = ss[t]
                return qs

            def core(looking):
                even, odd = x
                m, n, k, l = search(0, PEEL, marks)
                near_even, near_odd = m | n | flag(even < 0), k | l | flag(odd < 0)

                xr = [swap(v) for v in x]
                turns = [[[pltpu.roll(v, s, 0) if s else v for v in (x[h], xr[h])] for s in range(SUB)] for h in PAIR]
                for s, ((a, b), (c, d)) in enumerate(zip(*turns)):
                    near_odd = jnp.where((odd == a) | (odd == b), 1, near_odd)
                    if s:
                        after = sub >= s
                        near_even = jnp.where(((even == a) | (even == b)) & after, 1, near_even)
                        near_odd = jnp.where(((odd == c) | (odd == d)) & after, 1, near_odd)

                new = [1 - near_even, 1 - near_odd]
                packed = new[0] + BYTE * new[1]
                across = swap(packed)
                far = [across & (BYTE - 1), across >> SUB]
                both = packed + across
                run, whole = both, both
                for s in (1, 2, 4):
                    run = run + jnp.where(sub >= s, pltpu.roll(run, s, 0), 0)
                    whole = whole + pltpu.roll(whole, s, 0)
                run = run - both
                tail = tail_ref[...]
                evens = whole & (BYTE - 1)
                begin = [tail + (run & (BYTE - 1)), tail + evens + (run >> SUB)]
                for h in PAIR:
                    dest[part(h), :] = jnp.where(new[h] > 0, begin[h] + jnp.where(upper, far[h], 0), -1)
                    dest[part(h + 2), :] = jnp.where(far[h] > 0, begin[h] + jnp.where(upper, 0, new[h]), -1)
                    now[part(h), :] = x[h]
                    now[part(h + 2), :] = xr[h]
                now[part(4), :] = sigma[eight(row), :] + swap(sigma[eight(row), :])
                tail = tail + evens + (whole >> SUB)
                tail_ref[...] = tail
                passed = SLOTS * ((unit + 1) >> (quads - 1))
                second = SUB + SUB * (1 >> (quads - 1))
                need = jnp.where(sub == 1, SUB, second)
                short = (tail < need) & (held[...] > passed)
                most = jnp.max(jnp.where(sub == 0, tail, flag(short)).astype(f32), axis=1, keepdims=True)
                meta[REACHED] = most[0, 0].astype(jnp.int32)
                for n in PAIR:
                    meta[(SHORT0, SHORT1)[n]] = most[n + 1, 0].astype(jnp.int32)

                if looking:
                    quad2, row2 = at(unit + 1, base)
                    rows = gather_slots(to[0])
                qs = insert(0)
                for n in PAIR:
                    name(following + n * SUB, qs[n])
                if looking:
                    keep(rows, jnp.where(ahead, quad2, 0), jnp.where(ahead, row2, following))

            look = jnp.logical_or(ahead, soon)
            for looking in PAIR:
                @pl.when(look == (looking > 0))
                def _():
                    core(looking)

            length = meta[REACHED]
            ready = [meta[n] == 0 for n in (SHORT0, SHORT1)]

            @pl.when(unit + 3 < units)
            def _():
                fetch(*at(unit + 3, base), to).start()

            @pl.when(soon)
            def _():
                meta[GOT] = 1

            def first_of_next(n, when, buf):
                @pl.when(jnp.logical_and(when, meta[(AWAIT0, AWAIT1)[n]] == 0))
                def _():
                    fetch(*at(n, following), buf).start()
                    meta[(AWAIT0, AWAIT1)[n]] = 1

            first_of_next(0, jnp.logical_and(ready[0], unit + 3 == units), to)
            first_of_next(0, jnp.logical_and(ready[0], unit + 2 == units), other)
            first_of_next(1, jnp.logical_and(ready[1], unit + 2 == units), to)
            first_of_next(0, final_unit, to)
            first_of_next(1, final_unit, other)

            groups = (length + WINDOW - 1) // WINDOW
            fits = following + groups * WINDOW <= CAP + WINDOW
            meta[LENGTH] = jnp.where(fits, length, 0)

            @pl.when(jnp.logical_not(fits))
            def _():
                meta[FAULT] = 1

            def more(g, carry):
                insert(g)
                return carry

            lax.fori_loop(1, jnp.where(fits, groups, 0), more, 0)

        tail_ref[...] = jnp.zeros_like(tail_ref)
        meta[LENGTH] = 0

        def open_level(mine, other):
            @pl.when(jnp.logical_and(meta[GOT] == 0, meta[AWAIT0] > 0))
            def _():
                fetch(0, base, mine).wait()
                keep(gather_slots(mine[0]), 0, base)

            @pl.when(jnp.logical_and(units < 2, meta[AWAIT1] > 0))
            def _():
                fetch(0, base, other).wait()

            @pl.when(units > 2)
            def _():
                fetch(*at(2, base), mine).start()

        on_parity(parity, open_level)
        for place_ in (GOT, AWAIT0, AWAIT1):
            meta[place_] = 0

        def any_unit(unit, carry):
            on_parity(parity + unit, functools.partial(unit_step, unit))
            return carry

        lax.fori_loop(0, units, any_unit, 0)
        meta[PARITY] = parity + units

        @pl.when(following > CAP)
        def _():
            meta[FAULT] = 1

        found = jnp.where(meta[FAULT] == 0, meta[LENGTH], 0)
        meta[BASE, level + 1] = following
        meta[COUNT, level + 1] = found

        def names(t, carry):
            row = following + t * SUB
            name(row, queue[eight(row), :])
            return carry

        lax.fori_loop(2, (found + SUB - 1) // SUB, names, 0)
        held[...] = tail_ref[...]
        return carry

    for place_ in (GOT, PARITY):
        meta[place_] = 0

    @pl.when(jnp.logical_not(bad))
    def _():
        held[...] = jnp.full_like(held, FEW * quads)
        meta[BASE, 1] = SUB
        meta[COUNT, 1] = FEW * quads
        fetch(0, SUB, bufs[0]).wait()
        if compact:
            for h in PAIR:
                cand[h, eight(SUB), :] = jnp.full((SUB, LANES), EMPTY, f32)
        else:
            fetch(*at(1, SUB), bufs[1]).start()
        keep(gather_slots(ids_a, FEW if compact else SLOTS), 0, SUB)
        meta[GOT] = 1
        meta[AWAIT0] = 0
        meta[AWAIT1] = 1
        lax.fori_loop(1, levels, level_step, 0)

    @pl.when(bad)
    def _():
        fetch(0, SUB, bufs[0]).wait()
        meta[AWAIT0] = 0
        meta[AWAIT1] = int(compact)

    def drain(n, buf):
        @pl.when(meta[(AWAIT0, AWAIT1)[n]] > 0)
        def _():
            fetch(0, 0, buf).wait()

    for k in PAIR:
        @pl.when(meta[PARITY] & 1 == k)
        def _():
            @pl.when(meta[GOT] == 0)
            def _():
                drain(0, bufs[k])

            drain(1, bufs[1 - k])

    good = meta[FAULT] == 0

    @pl.when(good)
    def _():
        last = meta[BASE, levels]
        g_last = weight_ref[levels - 2]

        def seed(g, carry):
            for t in range(WINDOW // SUB):
                r = eight(last + g * WINDOW + SUB * t)
                s = sigma[r, :] + swap(sigma[r, :])
                ratio[r, :] = jnp.where(s > 0, g_last / jnp.where(s > 0, s, 1.0), 0.0)
            return carry

        lax.fori_loop(0, (meta[COUNT, levels] + WINDOW - 1) // WINDOW, seed, 0)

        def back_step(k, carry):
            level = levels - 1 - k
            base, count = meta[BASE, level], meta[COUNT, level]
            nbase, ncount = meta[BASE, level + 1], meta[COUNT, level + 1]
            g_here = weight_ref[jnp.maximum(level - 2, 0)]

            def pull_batch(bt, carry):
                here = eight(base + bt * SLOTS)

                def pull(quad, c, acc):
                    even, odd = cand[2 * quad, here, :], cand[2 * quad + 1, here, :]
                    acc = list(acc)
                    for n in range(WINDOW):
                        q = spread_row(queue, nbase + c * WINDOW + n)
                        w = spread_row(ratio, nbase + c * WINDOW + n)
                        acc[n % 2] = acc[n % 2] + jnp.where((even == q) | (odd == q), w, 0.0)
                    return tuple(acc)

                def pull_quad(quad, acc):
                    return lax.fori_loop(1, (ncount + WINDOW - 1) // WINDOW, functools.partial(pull, quad), pull(quad, 0, acc))

                acc = pull_quad(0, (jnp.zeros((SUB, LANES), f32),) * 2)
                if not compact:
                    acc = lax.fori_loop(1, quads, pull_quad, acc)
                delta[here, :] = acc[0] + acc[1]
                return carry

            lax.fori_loop(0, (count + SLOTS - 1) // SLOTS, pull_batch, 0)

            def finish(g, carry):
                slots = [eight(base + g * WINDOW + SUB * t) for t in range(WINDOW // SUB)]
                for t, r in enumerate(slots):
                    inside = g * WINDOW + SUB * t < count
                    part, s = (v + swap(v) for v in (delta[r, :], sigma[r, :]))
                    d = s * part
                    w = jnp.where(s > 0, (g_here + d) / jnp.where(s > 0, s, 1.0), 0.0)
                    delta[r, :] = jnp.where(inside, d, delta[r, :])
                    ratio[r, :] = jnp.where(inside, w, ratio[r, :])
                return carry

            lax.fori_loop(0, (count + WINDOW - 1) // WINDOW, finish, 0)
            return carry

        lax.fori_loop(0, levels - 1, back_step, 0)

        tall = along((WIDE, WIDE)).astype(f32).astype(bf16)
        zero = jnp.zeros((WIDE, WIDE), bf16)
        one = zero + 1
        start = meta[BASE, 1]

        def tally(t, carry):
            for u in range(TALLY // 16):
                a, b = eight(start + t * TALLY + u * 16), eight(start + t * TALLY + u * 16 + SUB)
                v = jnp.where(upper, queue[b, :], queue[a, :])
                d = jnp.where(upper, delta[b, :], delta[a, :])
                hi, lo = digits(v, WIDE)
                d_hi = d.astype(bf16).astype(f32)
                d_mid = (d - d_hi).astype(bf16).astype(f32)
                d_lo = d - d_hi - d_mid
                for p in range(0, SUB, 2):
                    cols = slice((u * SUB + p) * LANES, (u * SUB + p + 2) * LANES)

                    def pair(x):
                        return jnp.concatenate([x[p:p + 1], x[p + 1:p + 2]], axis=1).astype(bf16)

                    colhot[:, cols] = jnp.where(tall == pair(lo), one, zero)
                    match = tall[:high] == pair(hi)
                    for n, x in enumerate((d_hi, d_mid, d_lo)):
                        rowhot[n * high:(n + 1) * high, cols] = jnp.where(match, pair(x), zero[:high])
            bins[...] += lax.dot_general(rowhot[...], colhot[...], TURN, preferred_element_type=f32)
            return carry

        for t in range(TALLY // SUB):
            delta[eight(last + t * SUB), :] = jnp.zeros((SUB, LANES), f32)
        lax.fori_loop(0, (last - start + TALLY - 1) // TALLY, tally, 0)

    blocks = out_ref.shape[0]
    per = high // blocks
    total = (bins[:high] + bins[high:2 * high] + bins[2 * high:]) * scale
    fault = jnp.where(good, 0.0, 1.0)
    for b in range(blocks):
        for n in PAIR:
            out_ref[b, n * per:(n + 1) * per, :] = total[b * per:(b + 1) * per, n * LANES:(n + 1) * LANES]
        out_ref[b, 2 * per:, :] = jnp.full((SUB, LANES), fault, f32)


def walk(which, sources, weights, lists, *, blocks, vertices, scale, compact):
    levels = weights.shape[0] + 1
    rows = CAP + 4 * WINDOW
    high = LANES // blocks + SUB
    vm = pltpu.VMEM
    queue = vm((rows, LANES), f32)
    parts = 3 * (vertices // WIDE)
    return pl.pallas_call(
        functools.partial(walk_kernel, levels=levels, vertices=vertices, scale=scale, compact=compact),
        in_specs=[pl.BlockSpec(memory_space=pltpu.SMEM)] * 3 + [pl.BlockSpec(memory_space=pltpu.VMEM)],
        out_specs=pl.BlockSpec(memory_space=pltpu.VMEM),
        out_shape=jax.ShapeDtypeStruct((blocks, high, LANES), f32),
        scratch_shapes=[
            vm(((1 if compact else 2) * (vertices + SUB), LANES), f32), queue, queue, queue, queue,
            vm((4, rows, LANES), f32), vm((2, rows, LANES), jnp.int32),
            vm((40, LANES), f32), vm((32, LANES), jnp.int32), vm((SUB, LANES), jnp.int32), vm((SUB, LANES), jnp.int32),
            vm((parts, TALLY // 2 * LANES), bf16), vm((WIDE, TALLY // 2 * LANES), bf16), vm((parts, WIDE), f32),
            pltpu.SMEM((SLOTS, LANES), jnp.int32), pltpu.SMEM((SLOTS, LANES), jnp.int32), pltpu.SMEM((3, 16), jnp.int32),
            pltpu.SemaphoreType.DMA((2,)),
        ],
        compiler_params=pltpu.CompilerParams(
            vmem_limit_bytes=48 * 1024 * 1024),
        name="walk",
    )(which, sources, weights, lists)


def share_kernel(src, graph, x_ref, o_ref, own_sem, send_sem, recv_sem):
    mine, g, others = place_and_others(src, graph)
    hello(others)
    await_hello(others)
    own = pltpu.make_async_copy(x_ref, o_ref.at[mine], own_sem)
    own.start()
    copies = []
    for n, (py, pg) in enumerate(others):
        copies.append(pltpu.make_async_remote_copy(
            src_ref=x_ref, dst_ref=o_ref.at[mine], send_sem=send_sem.at[n], recv_sem=recv_sem.at[n],
            device_id={"src": py, "graph": pg}, device_id_type=MESH))
        copies[-1].start()
    own.wait()
    for c in copies:
        c.wait()


def share(x, src, graph):
    n = src * graph
    return pl.pallas_call(
        functools.partial(share_kernel, src, graph),
        in_specs=[pl.BlockSpec(memory_space=pltpu.VMEM)],
        out_specs=pl.BlockSpec(memory_space=pltpu.VMEM),
        out_shape=jax.ShapeDtypeStruct((n,) + x.shape, x.dtype),
        scratch_shapes=[pltpu.SemaphoreType.DMA, pltpu.SemaphoreType.DMA((n - 1,)), pltpu.SemaphoreType.DMA((n - 1,))],
        compiler_params=pltpu.CompilerParams(collective_id=2, has_side_effects=True),
        name="share",
    )(x)


def total_kernel(src, graph, x_ref, o_ref, got, own_sem, send_sem, recv_sem):
    mine, g, others = place_and_others(src, graph)
    hello(others)
    own = pltpu.make_async_copy(x_ref.at[g], got.at[mine], own_sem)
    own.start()
    await_hello(others)
    copies = []
    for n, (py, pg) in enumerate(others):
        copies.append(pltpu.make_async_remote_copy(
            src_ref=x_ref.at[pg], dst_ref=got.at[mine], send_sem=send_sem.at[n], recv_sem=recv_sem.at[n],
            device_id={"src": py, "graph": pg}, device_id_type=MESH))
        copies[-1].start()
    own.wait()
    for c in copies:
        c.wait()
    acc = got[0]
    for n in range(1, src * graph):
        acc = acc + got[n]
    o_ref[...] = acc


def total(x, src, graph, collective_id):
    n = src * graph
    return pl.pallas_call(
        functools.partial(total_kernel, src, graph),
        in_specs=[pl.BlockSpec(memory_space=pltpu.VMEM)],
        out_specs=pl.BlockSpec(memory_space=pltpu.VMEM),
        out_shape=jax.ShapeDtypeStruct(x.shape[1:], x.dtype),
        scratch_shapes=[pltpu.VMEM((n,) + x.shape[1:], x.dtype), pltpu.SemaphoreType.DMA,
                        pltpu.SemaphoreType.DMA((n - 1,)), pltpu.SemaphoreType.DMA((n - 1,))],
        compiler_params=pltpu.CompilerParams(collective_id=collective_id, has_side_effects=True),
        name="total",
    )(pltpu.with_memory_space_constraint(x, pltpu.VMEM))


def exchange(x, axis):
    return lax.all_to_all(x, axis, 0, 0)


def dense(adj_slab, src_local, level_weight, src, graph):
    slab_rows, vertex_count = adj_slab.shape
    src_count = src_local.shape[0]
    levels = level_weight.shape[0] + 1
    row_start = lax.axis_index("graph") * slab_rows
    vertex_ids = row_start + lax.broadcasted_iota(jnp.int32, (slab_rows, 1), 0)
    first = jnp.where(vertex_ids == src_local[None, :], 1.0, 0.0).astype(f32)

    def forward(carry, unused):
        sigma, seen = carry
        partial = jnp.einsum("uv,us->vs", adj_slab, sigma, preferred_element_type=f32, precision=exact_precision)
        parts = exchange(partial.reshape(graph, slab_rows, src_count), "graph")
        sigma = jnp.sum(parts, axis=0) * (1.0 - seen)
        seen = jnp.maximum(seen, jnp.where(sigma > 0, 1.0, 0.0))
        return (sigma, seen), sigma

    _, sigmas = lax.scan(forward, (first, first), None, length=levels)

    def backward(carry, xs):
        delta, acc = carry
        upper, lower, weight = xs
        reached = upper > 0
        ratio = jnp.where(reached, (weight + delta) / jnp.where(reached, upper, 1.0), 0.0)
        gathered = exchange(jnp.broadcast_to(ratio[None], (graph,) + ratio.shape), "graph")
        pulled = jnp.einsum("uv,vs->us", adj_slab, gathered.reshape(vertex_count, src_count),
                            preferred_element_type=f32, precision=exact_precision)
        delta = lower * pulled
        return (delta, acc + delta), None

    zero = jnp.zeros_like(first)
    (_, acc), _ = lax.scan(backward, (zero, zero), (sigmas[1:][::-1], sigmas[:-1][::-1], level_weight[::-1]))
    scale = vertex_count / (src_count * src * levels ** 3)
    mine = jnp.sum(acc, axis=1) * scale
    both = exchange(jnp.broadcast_to(mine.reshape(1, -1, LANES), (src, slab_rows // LANES, LANES)), "src")
    return jnp.sum(both, axis=0).reshape(slab_rows)


def solution(mesh):
    src, graph = mesh.shape["src"], mesh.shape["graph"]

    def device_program(adj_slab, src_local, level_weight):
        slab_rows, vertex_count = adj_slab.shape
        levels = level_weight.shape[0] + 1
        scale = vertex_count / (HALF * src * graph * levels ** 3)
        which = lax.axis_index("graph").astype(jnp.int32).reshape(1)

        def finish(lists, compact, collective_id, other):
            parts = walk(which, src_local, level_weight, lists, blocks=graph, vertices=vertex_count, scale=scale, compact=compact)
            summed = total(parts, src, graph, collective_id)
            rows = slab_rows // LANES

            def plain():
                return summed[:rows].reshape(2, -1, LANES).transpose(1, 0, 2).reshape(slab_rows)

            return lax.cond(summed[rows, 0] > 0, other, plain)

        def dense_path():
            return dense(adj_slab, src_local, level_weight, src, graph)

        def general_path():
            half = lax.axis_index("src").astype(jnp.int32).reshape(1)
            lists = share(extract(adj_slab, half, slab_rows // src), src, graph)
            return finish(lists.reshape(-1, SUB, LANES), False, 3, dense_path)

        return finish(collect(adj_slab, src, graph), True, 1, general_path)

    return jax.shard_map(device_program, mesh=mesh,
                         in_specs=(P(("batch", "graph"), None), P(("batch", "src")), P(None)),
                         out_specs=P(("batch", "graph")), check_vma=False)
```

```python
import functools

import jax
import jax.numpy as jnp
from jax import lax
from jax.experimental import pallas as pl
from jax.experimental.pallas import tpu as pltpu
from jax.sharding import PartitionSpec as P

MESH = pl.DeviceIdType.MESH
exact_precision = lax.Precision.HIGHEST
f32, bf16 = jnp.float32, jnp.bfloat16

LANES, SUB = 128, 8
WIDE = 256
DEG, FEW = 8, 4
EMPTY = -2.0
FULL = 32767.0
TURN = (((1,), (1,)), ((), ()))
BLOCK = 128
READS = 4
STEP = 32
HALF = 64
SLOTS = 8
WINDOW = 48
SCAN = 32
CAP = 1024
TALLY = 96
PAIR = (0, 1)
BYTE = 256
GROUP = 8
PEEL = 32
BASE, COUNT = 0, 1
FAULT, LENGTH, GOT, PARITY, AWAIT0, AWAIT1, REACHED, SHORT0, SHORT1 = ((2, n) for n in range(9))


def place_and_others(src, graph):
    y, g = lax.axis_index("src"), lax.axis_index("graph")
    steps = ((i, k, c) for c in PAIR for k in range(graph // 2) for i in range(src))
    steps = sorted(steps, key=lambda s: -s[0] - s[1])
    others = [((y + i) % src, (g // 2 + k) % (graph // 2) * 2 + (g + c) % 2) for i, k, c in steps if (i, k, c) != (0, 0, 0)]
    return g * src + y, g, others


def hello(peers):
    for y, g in peers:
        pl.semaphore_signal(pltpu.get_barrier_semaphore(), inc=1, device_id={"src": y, "graph": g}, device_id_type=MESH)


def await_hello(peers):
    pl.semaphore_wait(pltpu.get_barrier_semaphore(), len(peers))


def place(plane, lists):
    lists = list(lists)
    row_i = lax.broadcasted_iota(jnp.int32, (WIDE, WIDE), 0)
    col_i = lax.broadcasted_iota(jnp.int32, (WIDE, WIDE), 1)
    eye = jnp.where(row_i == col_i, float(WIDE), 0.0).astype(bf16)
    flipped = lax.dot_general(eye, plane, TURN, preferred_element_type=f32)
    lane_id = lax.broadcasted_iota(jnp.int32, (SUB, flipped.shape[1]), 0).astype(f32)
    for g in range(WIDE // SUB):
        x = flipped[g * SUB:(g + 1) * SUB] + (lane_id + float(g * SUB))
        for s in range(len(lists)):
            hi = jnp.maximum(lists[s], x)
            if s < len(lists) - 1:
                x = jnp.minimum(lists[s], x)
            lists[s] = hi
    return lists


def sort(lists):
    gap = len(lists) // 2
    while gap:
        for s in range(len(lists)):
            if not s & gap:
                lists[s], lists[s + gap] = jnp.maximum(lists[s], lists[s + gap]), jnp.minimum(lists[s], lists[s + gap])
        gap //= 2
    return lists


def over_sublanes(lists):
    size = len(lists)
    for shift in (4, 2, 1):
        other = [pltpu.roll(v, shift, 0) for v in lists]
        lists = sort([jnp.maximum(lists[s], other[size - 1 - s]) for s in range(size)])
    out = jnp.full(lists[0].shape, EMPTY, f32)
    sub = lax.broadcasted_iota(jnp.int32, out.shape, 0)
    for s in range(size):
        out = jnp.where(sub == s, jnp.where(lists[s] >= WIDE, lists[s] - WIDE, EMPTY), out)
    return out


def degree_of(seen):
    return lax.dot_general(jnp.ones((SUB, WIDE), bf16), seen, TURN, preferred_element_type=f32)


def collect_kernel(src, graph, a_ref, o_ref, bufs, tops, mine, sems, own_sem, send_sems, recv_sems):
    vertices = a_ref.shape[1]
    pairs, chunks = mine.shape[0], vertices // WIDE
    blocks = 2 * pairs
    me, _, others = place_and_others(src, graph)
    y = me % src
    height = 4 * SUB
    pieces = BLOCK // height

    def fetch(i, t):
        rows = pl.ds(pl.multiple_of((y * blocks + i) * BLOCK + t * height, height), height)
        here = pl.ds(pl.multiple_of(t * height, height), height)
        return pltpu.make_async_copy(a_ref.at[rows], bufs.at[i % READS, here], sems.at[i % READS, t])

    def send(n, first, count):
        py, pg = others[n]
        return pltpu.make_async_remote_copy(
            src_ref=mine.at[pl.ds(first, count)], dst_ref=o_ref.at[pl.ds(me * pairs + first, count)],
            send_sem=send_sems.at[n], recv_sem=recv_sems.at[n], device_id={"src": py, "graph": pg}, device_id_type=MESH)

    def send_pair(p):
        for n in range(len(others)):
            send(n, p, 1).start()

    for i in range(READS - 1):
        for t in range(pieces):
            fetch(i, t).start()
    hello(others)
    none = jnp.zeros((SUB, 2 * BLOCK), f32)

    def scan(i, first):
        @pl.when(i + READS - 1 < blocks)
        def _():
            for t in range(pieces):
                fetch(i + READS - 1, t).start()

        def scan_rows(t, carry):
            fetch(i, t).wait()
            here = pl.ds(pl.multiple_of(t * height, height), height)

            def scan_chunks(c, state):
                top, low, seen, sums, value = state
                for k in range(STEP):
                    a = bufs[i % READS, here, pl.ds(pl.multiple_of((c * STEP + k) * WIDE, WIDE), WIDE)]
                    x = a * value
                    low = jnp.maximum(low, jnp.minimum(top, x))
                    top = jnp.maximum(top, x)
                    seen = seen + a
                    sums = sums + x
                    value = value + 1
                return top, low, seen, sums, value

            zero = jnp.zeros((height, WIDE), bf16)
            top, low, seen, sums, _ = lax.fori_loop(0, chunks // STEP, scan_chunks, (zero,) * 4 + (zero + 1,))
            for n, v in enumerate((top, low, (sums - top) - low, seen)):
                tops[n, pl.ds(pl.multiple_of(first + t * height, height), height), :] = v
            return carry

        lax.fori_loop(0, pieces, scan_rows, 0)

    def pair_step(p, carry):
        for h in range(2):
            scan(2 * p + h, h * BLOCK)
        seen = tops[3]
        crowd = seen[:SUB]
        for k in range(1, 2 * BLOCK // SUB):
            crowd = jnp.maximum(crowd, seen[k * SUB:(k + 1) * SUB])
        crowd = jnp.max(crowd.astype(f32), axis=0, keepdims=True)
        a, b, c = place(tops[0], (none,) * 4), place(tops[1], (none,) * 2), place(tops[2], (none,))
        rest = [jnp.maximum(b[0], c[0]), jnp.minimum(b[0], c[0])]
        rest = [rest[0], jnp.maximum(b[1], rest[1]), jnp.minimum(b[1], rest[1])]
        lists = over_sublanes(sort([a[0]] + [jnp.maximum(a[s + 1], rest[2 - s]) for s in range(3)]))
        lists = jnp.where((crowd > 3) | (degree_of(seen) > 4), FULL, lists)
        even, odd = lists[:, :BLOCK], lists[:, BLOCK:]
        sub = lax.broadcasted_iota(jnp.int32, even.shape, 0)
        mine[p] = jnp.where(sub < 4, even, pltpu.roll(odd, 4, 0))

        @pl.when(p == 1)
        def _():
            await_hello(others)

        @pl.when(p > 0)
        def _():
            send_pair(p - 1)

        return carry

    lax.fori_loop(0, pairs, pair_step, 0)
    own = pltpu.make_async_copy(mine, o_ref.at[pl.ds(me * pairs, pairs)], own_sem)
    send_pair(pairs - 1)
    own.start()
    own.wait()
    for n in range(len(others)):
        send(n, 0, pairs).wait()


def collect(adj_slab, src, graph):
    rows, vertices = adj_slab.shape
    n = src * graph
    mine = (rows // src // (2 * BLOCK), SUB, BLOCK)
    return pl.pallas_call(
        functools.partial(collect_kernel, src, graph),
        in_specs=[pl.BlockSpec(memory_space=pl.ANY)],
        out_specs=pl.BlockSpec(memory_space=pltpu.VMEM),
        out_shape=jax.ShapeDtypeStruct((n * mine[0],) + mine[1:], f32),
        scratch_shapes=[pltpu.VMEM((READS, BLOCK, vertices), bf16), pltpu.VMEM((4, 2 * BLOCK, WIDE), bf16), pltpu.VMEM(mine, f32),
                        pltpu.SemaphoreType.DMA((READS, BLOCK // (4 * SUB))), pltpu.SemaphoreType.DMA,
                        pltpu.SemaphoreType.DMA((n - 1,)), pltpu.SemaphoreType.DMA((n - 1,))],
        compiler_params=pltpu.CompilerParams(collective_id=0, has_side_effects=True, vmem_limit_bytes=40 * 1024 * 1024),
        name="collect",
    )(adj_slab)


def extract_kernel(half_ref, a_ref, o_ref, block, seen, planes, sem):
    vertices = a_ref.shape[1]

    def block_step(i, carry):
        copy = pltpu.make_async_copy(
            a_ref.at[pl.ds(pl.multiple_of((half_ref[0] * o_ref.shape[0] + i) * BLOCK, BLOCK), BLOCK)], block, sem)
        copy.start()
        copy.wait()
        planes[...] = jnp.zeros_like(planes)
        seen[...] = jnp.zeros_like(seen)

        def scan_chunk(c, carry):
            a = block[:, pl.ds(pl.multiple_of(c * WIDE, WIDE), WIDE)]
            seen[...] = seen[...] + a
            x = a.astype(f32) * (c + 1).astype(f32)
            for s in range(DEG):
                top = planes[s].astype(f32)
                planes[s] = jnp.maximum(top, x).astype(bf16)
                x = jnp.minimum(top, x)
            return carry

        lax.fori_loop(0, vertices // WIDE, scan_chunk, 0)
        lists = lax.fori_loop(0, DEG, lambda p, lists: tuple(place(planes[p], lists)), (jnp.zeros((SUB, BLOCK), f32),) * DEG)
        o_ref[i] = jnp.where(degree_of(seen[...]) > DEG, FULL, over_sublanes(list(lists)))
        return carry

    lax.fori_loop(0, o_ref.shape[0], block_step, 0)


def extract(adj_slab, half, rows):
    vertices = adj_slab.shape[1]
    return pl.pallas_call(
        extract_kernel,
        in_specs=[pl.BlockSpec(memory_space=pltpu.SMEM), pl.BlockSpec(memory_space=pl.ANY)],
        out_specs=pl.BlockSpec(memory_space=pltpu.VMEM),
        out_shape=jax.ShapeDtypeStruct((rows // BLOCK, DEG, BLOCK), f32),
        scratch_shapes=[pltpu.VMEM((BLOCK, vertices), bf16), pltpu.VMEM((BLOCK, WIDE), bf16),
                        pltpu.VMEM((DEG, BLOCK, WIDE), bf16), pltpu.SemaphoreType.DMA],
        name="extract",
    )(half, adj_slab)


def along(shape, axis=0):
    return lax.broadcasted_iota(jnp.int32, shape, axis)


def swap(x):
    return pltpu.roll(x, HALF, 1)


def digits(x, base):
    high = jnp.floor(x * (1.0 / base))
    return high, x - high * base


def walk_kernel(which_ref, src_ref, weight_ref, lists_ref, out_ref,
                table, queue, sigma, ratio, delta, cand, ids, now, dest, tail_ref, held, rowhot, colhot, bins,
                ids_a, ids_b, meta, sems, *, levels, vertices, scale, compact):
    pitch = vertices + SUB
    lane = along((SUB, LANES), 1)
    sub = along((SUB, LANES))
    upper = lane >= HALF
    lane_row = along((1, LANES), 1)
    group_odd = ((lane_row // 32) % 2) == 1
    lane32 = lane_row % 32
    rows_all = queue.shape[0]
    tile_bits = (vertices // lists_ref.shape[0]).bit_length() - 1
    high = vertices // WIDE

    def eight(row):
        return pl.ds(pl.multiple_of(row, SUB), SUB)

    def part(n):
        return pl.ds(n * SUB, SUB)

    def spread_row(ref, *index):
        return jnp.broadcast_to(ref[(*index[:-1], pl.ds(index[-1], 1), slice(None))], (SUB, LANES))

    def clear(t, carry):
        for k in range(SUB):
            rows = eight((t * SUB + k) * SUB)
            queue[rows, :] = jnp.full((SUB, LANES), -1.0, f32)
            sigma[rows, :] = jnp.zeros((SUB, LANES), f32)
        return carry

    def fetch(quad, row, buf):
        return pltpu.make_async_copy(ids.at[quad, row // SUB], buf[0], sems.at[buf[1]])

    def name(row, q):
        v = jnp.where(q < 0, vertices, q.astype(jnp.int32))
        v = jnp.where(upper, pltpu.roll(v, FEW, 0), v)[:FEW]
        ids[0, row // SUB] = v
        ids[1, row // SUB] = v + pitch

    bufs = (ids_a, 0), (ids_b, 1)
    clear(0, 0)

    near_source = jnp.full((SUB, LANES), EMPTY, f32)
    source = near_source
    for j in range(HALF):
        v = src_ref[which_ref[0] * HALF + j]
        tile = pltpu.roll(lists_ref[v >> tile_bits], (j - v) & (LANES - 1), 1)
        if compact:
            tile = jnp.where((v & LANES) > 0, pltpu.roll(tile, FEW, 0), tile)
        near_source = jnp.where(lane == j, tile, near_source)
        source = jnp.where(lane % HALF == j, v.astype(f32), source)
    near_source = jnp.where(upper, swap(near_source), near_source)
    reached = near_source >= 0
    if compact:
        reached = reached & (sub < FEW)
    queue[0:1, :] = source[:1]
    queue[eight(SUB), :] = jnp.where(reached, near_source, -1.0)
    sigma[eight(SUB), :] = jnp.where(reached & jnp.logical_not(upper), 1.0, 0.0)
    for n in (1, 2):
        name(n * SUB, queue[eight(n * SUB), :])
    bins[...] = jnp.zeros_like(bins)
    fetch(0, SUB, bufs[0]).start()
    if compact:
        fetch(0, 2 * SUB, bufs[1]).start()
    lax.fori_loop(1, rows_all // (SUB * SUB), clear, 0)

    srow = along((2 * SUB, LANES))
    slane = along((2 * SUB, LANES), 1)

    def fill(halves, target):
        picks = [jnp.where((srow % SUB) == (slane // 32 + FEW * h), jnp.where(srow < SUB, float(LANES), 1.0), 0.0).astype(bf16)
                 for h in halves]

        def body(step, most):
            for k in range(GROUP):
                first = (GROUP * step + k) * SUB
                x = jnp.concatenate([lists_ref[first + n] for n in range(SUB)], axis=1)
                both = jnp.concatenate(digits(x, LANES), axis=0).astype(bf16)
                for h, pick in zip(halves, picks):
                    rows = lax.dot_general(both, pick, (((0,), (0,)), ((), ())), preferred_element_type=f32)
                    for n in range(SUB):
                        table[pl.ds(pl.multiple_of(target(h, first + n), SUB), LANES), :] = rows[n * LANES:(n + 1) * LANES]
                for n in range(SUB):
                    most = jnp.maximum(most, lists_ref[first + n])
            return most

        return lax.fori_loop(0, lists_ref.shape[0] // (GROUP * SUB), body, jnp.full((SUB, LANES), EMPTY, f32))

    table[vertices:pitch, :] = jnp.full((SUB, LANES), EMPTY, f32)
    if compact:
        most = fill(PAIR, lambda h, t: (2 * t + h) * LANES)
        quads = 1
    else:
        table[pitch + vertices:, :] = jnp.full((SUB, LANES), EMPTY, f32)
        most = fill((0,), lambda h, t: t * LANES)
        wide = jnp.max(jnp.where(sub >= FEW, most, EMPTY)) >= 0
        quads = jnp.where(wide, 2, 1)

        @pl.when(wide)
        def _():
            fill((1,), lambda h, t: pitch + t * LANES)

    bad = jnp.max(most) > vertices
    meta[FAULT] = bad.astype(jnp.int32)

    def gather(rows_of_ids):
        acc = [[jnp.full((1, LANES), EMPTY, f32)] * 2 for _ in rows_of_ids]
        for j in range(32):
            hit = lane32 == j
            for i, id_of in enumerate(rows_of_ids):
                for b in PAIR:
                    acc[i][b] = jnp.where(hit, table[pl.ds(id_of(b * 32 + j), 1), :], acc[i][b])
        return [(jnp.where(group_odd, b, a), pltpu.roll(jnp.where(group_odd, a, b), LANES - 32, 1)) for a, b in acc]

    def gather_slots(ids_s, slots=SLOTS):
        return gather([functools.partial(lambda i, j: ids_s[i % FEW, i // FEW * HALF + j], i) for i in range(slots)])

    def keep(rows, quad, row):
        for i, pair in enumerate(rows):
            for h in PAIR:
                cand[2 * quad + h, pl.ds(row + i, 1), :] = pair[h]

    def flag(x):
        return jnp.where(x, 1, 0)

    def at(unit, origin):
        return unit & (quads - 1), origin + (unit >> (quads - 1)) * SUB

    def level_step(level, carry):
        base, count = meta[BASE, level], meta[COUNT, level]
        following = base + (count + 7) // SUB * SUB
        batches = jnp.where(following <= CAP, (count + SLOTS - 1) // SLOTS, 0)
        units = batches * quads
        parity = meta[PARITY]

        def on_parity(n, f):
            for k in PAIR:
                @pl.when(n & 1 == k)
                def _():
                    f(bufs[k], bufs[1 - k])

        def unit_step(unit, other, to):
            quad, row = at(unit, base)
            x = [cand[2 * quad + h, eight(row), :] for h in PAIR]

            def search(first, count, marks):
                marks = list(marks)
                for k in range(count):
                    q = spread_row(queue, first + k)
                    for h in PAIR:
                        n = 2 * h + k % 2
                        marks[n] = jnp.where(x[h] == q, 1, marks[n])
                return tuple(marks)

            reach = following + meta[LENGTH] - PEEL
            marks = lax.fori_loop(0, (reach + SCAN - 1) // SCAN, lambda t, m: search(PEEL + t * SCAN, SCAN, m),
                                  (jnp.zeros((SUB, LANES), jnp.int32),) * 4)
            ahead = unit + 1 < units
            final_unit = unit + 1 == units
            soon = jnp.logical_and(final_unit, meta[AWAIT0] > 0)

            @pl.when(jnp.logical_or(ahead, soon))
            def _():
                fetch(0, base, to).wait()

            def insert(g):
                slots = [eight(following + g * WINDOW + SUB * t) for t in range(WINDOW // SUB)]
                qs = [queue[r, :] for r in slots]
                ss = [sigma[r, :] for r in slots]
                pos = [sub + (g * WINDOW + SUB * t) for t in range(WINDOW // SUB)]
                for h in PAIR:
                    for i in range(SUB):
                        d, e = spread_row(dest, SUB * h + i), spread_row(dest, SUB * (h + 2) + i)
                        v, w = spread_row(now, SUB * h + i), spread_row(now, SUB * (h + 2) + i)
                        for t in range(WINDOW // SUB):
                            qs[t] = jnp.where(pos[t] == d, v, jnp.where(pos[t] == e, w, qs[t]))
                for i in range(SUB):
                    v, w, sig = (spread_row(now, SUB * n + i) for n in (0, 1, 4))
                    for t in range(WINDOW // SUB):
                        ss[t] = ss[t] + jnp.where((qs[t] == v) | (qs[t] == w), sig, 0.0)
                for t, r in enumerate(slots):
                    queue[r, :] = qs[t]
                    sigma[r, :] = ss[t]
                return qs

            def core(looking):
                even, odd = x
                m, n, k, l = search(0, PEEL, marks)
                near_even, near_odd = m | n | flag(even < 0), k | l | flag(odd < 0)

                xr = [swap(v) for v in x]
                turns = [[[pltpu.roll(v, s, 0) if s else v for v in (x[h], xr[h])] for s in range(SUB)] for h in PAIR]
                for s, ((a, b), (c, d)) in enumerate(zip(*turns)):
                    near_odd = jnp.where((odd == a) | (odd == b), 1, near_odd)
                    if s:
                        after = sub >= s
                        near_even = jnp.where(((even == a) | (even == b)) & after, 1, near_even)
                        near_odd = jnp.where(((odd == c) | (odd == d)) & after, 1, near_odd)

                new = [1 - near_even, 1 - near_odd]
                packed = new[0] + BYTE * new[1]
                across = swap(packed)
                far = [across & (BYTE - 1), across >> SUB]
                both = packed + across
                run, whole = both, both
                for s in (1, 2, 4):
                    run = run + jnp.where(sub >= s, pltpu.roll(run, s, 0), 0)
                    whole = whole + pltpu.roll(whole, s, 0)
                run = run - both
                tail = tail_ref[...]
                evens = whole & (BYTE - 1)
                begin = [tail + (run & (BYTE - 1)), tail + evens + (run >> SUB)]
                for h in PAIR:
                    dest[part(h), :] = jnp.where(new[h] > 0, begin[h] + jnp.where(upper, far[h], 0), -1)
                    dest[part(h + 2), :] = jnp.where(far[h] > 0, begin[h] + jnp.where(upper, 0, new[h]), -1)
                    now[part(h), :] = x[h]
                    now[part(h + 2), :] = xr[h]
                now[part(4), :] = sigma[eight(row), :] + swap(sigma[eight(row), :])
                tail = tail + evens + (whole >> SUB)
                tail_ref[...] = tail
                passed = SLOTS * ((unit + 1) >> (quads - 1))
                second = SUB + SUB * (1 >> (quads - 1))
                need = jnp.where(sub == 1, SUB, second)
                short = (tail < need) & (held[...] > passed)
                most = jnp.max(jnp.where(sub == 0, tail, flag(short)).astype(f32), axis=1, keepdims=True)
                meta[REACHED] = most[0, 0].astype(jnp.int32)
                for n in PAIR:
                    meta[(SHORT0, SHORT1)[n]] = most[n + 1, 0].astype(jnp.int32)

                if looking:
                    quad2, row2 = at(unit + 1, base)
                    rows = gather_slots(to[0])
                qs = insert(0)
                if looking:
                    keep(rows, jnp.where(ahead, quad2, 0), jnp.where(ahead, row2, following))
                for n in PAIR:
                    name(following + n * SUB, qs[n])

            look = jnp.logical_or(ahead, soon)
            for looking in PAIR:
                @pl.when(look == (looking > 0))
                def _():
                    core(looking)

            length = meta[REACHED]
            ready = [meta[n] == 0 for n in (SHORT0, SHORT1)]

            @pl.when(unit + 3 < units)
            def _():
                fetch(*at(unit + 3, base), to).start()

            @pl.when(soon)
            def _():
                meta[GOT] = 1

            def first_of_next(n, when, buf):
                @pl.when(jnp.logical_and(when, meta[(AWAIT0, AWAIT1)[n]] == 0))
                def _():
                    fetch(*at(n, following), buf).start()
                    meta[(AWAIT0, AWAIT1)[n]] = 1

            first_of_next(0, jnp.logical_and(ready[0], unit + 3 == units), to)
            first_of_next(0, jnp.logical_and(ready[0], unit + 2 == units), other)
            first_of_next(1, jnp.logical_and(ready[1], unit + 2 == units), to)
            first_of_next(0, final_unit, to)
            first_of_next(1, final_unit, other)

            groups = (length + WINDOW - 1) // WINDOW
            fits = following + groups * WINDOW <= CAP + WINDOW
            meta[LENGTH] = jnp.where(fits, length, 0)

            @pl.when(jnp.logical_not(fits))
            def _():
                meta[FAULT] = 1

            def more(g, carry):
                insert(g)
                return carry

            lax.fori_loop(1, jnp.where(fits, groups, 0), more, 0)

        tail_ref[...] = jnp.zeros_like(tail_ref)
        meta[LENGTH] = 0

        def open_level(mine, other):
            @pl.when(jnp.logical_and(meta[GOT] == 0, meta[AWAIT0] > 0))
            def _():
                fetch(0, base, mine).wait()
                keep(gather_slots(mine[0]), 0, base)

            @pl.when(jnp.logical_and(units < 2, meta[AWAIT1] > 0))
            def _():
                fetch(0, base, other).wait()

            @pl.when(units > 2)
            def _():
                fetch(*at(2, base), mine).start()

        on_parity(parity, open_level)
        for place_ in (GOT, AWAIT0, AWAIT1):
            meta[place_] = 0

        def any_unit(unit, carry):
            on_parity(parity + unit, functools.partial(unit_step, unit))
            return carry

        lax.fori_loop(0, units, any_unit, 0)
        meta[PARITY] = parity + units

        @pl.when(following > CAP)
        def _():
            meta[FAULT] = 1

        found = jnp.where(meta[FAULT] == 0, meta[LENGTH], 0)
        meta[BASE, level + 1] = following
        meta[COUNT, level + 1] = found

        def names(t, carry):
            row = following + t * SUB
            name(row, queue[eight(row), :])
            return carry

        lax.fori_loop(2, (found + SUB - 1) // SUB, names, 0)
        held[...] = tail_ref[...]
        return carry

    for place_ in (GOT, PARITY):
        meta[place_] = 0

    @pl.when(jnp.logical_not(bad))
    def _():
        held[...] = jnp.full_like(held, FEW * quads)
        meta[BASE, 1] = SUB
        meta[COUNT, 1] = FEW * quads
        fetch(0, SUB, bufs[0]).wait()
        if compact:
            for h in PAIR:
                cand[h, eight(SUB), :] = jnp.full((SUB, LANES), EMPTY, f32)
        else:
            fetch(*at(1, SUB), bufs[1]).start()
        keep(gather_slots(ids_a, FEW if compact else SLOTS), 0, SUB)
        meta[GOT] = 1
        meta[AWAIT0] = 0
        meta[AWAIT1] = 1
        lax.fori_loop(1, levels, level_step, 0)

    @pl.when(bad)
    def _():
        fetch(0, SUB, bufs[0]).wait()
        meta[AWAIT0] = 0
        meta[AWAIT1] = int(compact)

    def drain(n, buf):
        @pl.when(meta[(AWAIT0, AWAIT1)[n]] > 0)
        def _():
            fetch(0, 0, buf).wait()

    for k in PAIR:
        @pl.when(meta[PARITY] & 1 == k)
        def _():
            @pl.when(meta[GOT] == 0)
            def _():
                drain(0, bufs[k])

            drain(1, bufs[1 - k])

    good = meta[FAULT] == 0

    @pl.when(good)
    def _():
        last = meta[BASE, levels]
        g_last = weight_ref[levels - 2]

        def seed(g, carry):
            for t in range(WINDOW // SUB):
                r = eight(last + g * WINDOW + SUB * t)
                s = sigma[r, :] + swap(sigma[r, :])
                ratio[r, :] = jnp.where(s > 0, g_last / jnp.where(s > 0, s, 1.0), 0.0)
            return carry

        lax.fori_loop(0, (meta[COUNT, levels] + WINDOW - 1) // WINDOW, seed, 0)

        def back_step(k, carry):
            level = levels - 1 - k
            base, count = meta[BASE, level], meta[COUNT, level]
            nbase, ncount = meta[BASE, level + 1], meta[COUNT, level + 1]
            g_here = weight_ref[jnp.maximum(level - 2, 0)]

            def pull_batch(bt, carry):
                here = eight(base + bt * SLOTS)

                def pull(quad, c, acc):
                    even, odd = cand[2 * quad, here, :], cand[2 * quad + 1, here, :]
                    acc = list(acc)
                    for n in range(WINDOW):
                        q = spread_row(queue, nbase + c * WINDOW + n)
                        w = spread_row(ratio, nbase + c * WINDOW + n)
                        acc[n % 2] = acc[n % 2] + jnp.where((even == q) | (odd == q), w, 0.0)
                    return tuple(acc)

                def pull_quad(quad, acc):
                    return lax.fori_loop(1, (ncount + WINDOW - 1) // WINDOW, functools.partial(pull, quad), pull(quad, 0, acc))

                acc = pull_quad(0, (jnp.zeros((SUB, LANES), f32),) * 2)
                if not compact:
                    acc = lax.fori_loop(1, quads, pull_quad, acc)
                delta[here, :] = acc[0] + acc[1]
                return carry

            lax.fori_loop(0, (count + SLOTS - 1) // SLOTS, pull_batch, 0)

            def finish(g, carry):
                slots = [eight(base + g * WINDOW + SUB * t) for t in range(WINDOW // SUB)]
                for t, r in enumerate(slots):
                    inside = g * WINDOW + SUB * t < count
                    part, s = (v + swap(v) for v in (delta[r, :], sigma[r, :]))
                    d = s * part
                    w = jnp.where(s > 0, (g_here + d) / jnp.where(s > 0, s, 1.0), 0.0)
                    delta[r, :] = jnp.where(inside, d, delta[r, :])
                    ratio[r, :] = jnp.where(inside, w, ratio[r, :])
                return carry

            lax.fori_loop(0, (count + WINDOW - 1) // WINDOW, finish, 0)
            return carry

        lax.fori_loop(0, levels - 1, back_step, 0)

        tall = along((WIDE, WIDE)).astype(f32).astype(bf16)
        zero = jnp.zeros((WIDE, WIDE), bf16)
        one = zero + 1
        start = meta[BASE, 1]

        def tally(t, carry):
            for u in range(TALLY // 16):
                a, b = eight(start + t * TALLY + u * 16), eight(start + t * TALLY + u * 16 + SUB)
                v = jnp.where(upper, queue[b, :], queue[a, :])
                d = jnp.where(upper, delta[b, :], delta[a, :])
                hi, lo = digits(v, WIDE)
                d_hi = d.astype(bf16).astype(f32)
                d_mid = (d - d_hi).astype(bf16).astype(f32)
                d_lo = d - d_hi - d_mid
                for p in range(0, SUB, 2):
                    cols = slice((u * SUB + p) * LANES, (u * SUB + p + 2) * LANES)

                    def pair(x):
                        return jnp.concatenate([x[p:p + 1], x[p + 1:p + 2]], axis=1).astype(bf16)

                    colhot[:, cols] = jnp.where(tall == pair(lo), one, zero)
                    match = tall[:high] == pair(hi)
                    for n, x in enumerate((d_hi, d_mid, d_lo)):
                        rowhot[n * high:(n + 1) * high, cols] = jnp.where(match, pair(x), zero[:high])
            bins[...] += lax.dot_general(rowhot[...], colhot[...], TURN, preferred_element_type=f32)
            return carry

        for t in range(TALLY // SUB):
            delta[eight(last + t * SUB), :] = jnp.zeros((SUB, LANES), f32)
        lax.fori_loop(0, (last - start + TALLY - 1) // TALLY, tally, 0)

    blocks = out_ref.shape[0]
    per = high // blocks
    total = (bins[:high] + bins[high:2 * high] + bins[2 * high:]) * scale
    fault = jnp.where(good, 0.0, 1.0)
    for b in range(blocks):
        for n in PAIR:
            out_ref[b, n * per:(n + 1) * per, :] = total[b * per:(b + 1) * per, n * LANES:(n + 1) * LANES]
        out_ref[b, 2 * per:, :] = jnp.full((SUB, LANES), fault, f32)


def walk(which, sources, weights, lists, *, blocks, vertices, scale, compact):
    levels = weights.shape[0] + 1
    rows = CAP + 4 * WINDOW
    high = LANES // blocks + SUB
    vm = pltpu.VMEM
    queue = vm((rows, LANES), f32)
    parts = 3 * (vertices // WIDE)
    return pl.pallas_call(
        functools.partial(walk_kernel, levels=levels, vertices=vertices, scale=scale, compact=compact),
        in_specs=[pl.BlockSpec(memory_space=pltpu.SMEM)] * 3 + [pl.BlockSpec(memory_space=pltpu.VMEM)],
        out_specs=pl.BlockSpec(memory_space=pltpu.VMEM),
        out_shape=jax.ShapeDtypeStruct((blocks, high, LANES), f32),
        scratch_shapes=[
            vm(((1 if compact else 2) * (vertices + SUB), LANES), f32), queue, queue, queue, queue,
            vm((4, rows, LANES), f32), vm((2, rows // SUB, FEW, LANES), jnp.int32),
            vm((40, LANES), f32), vm((32, LANES), jnp.int32), vm((SUB, LANES), jnp.int32), vm((SUB, LANES), jnp.int32),
            vm((parts, TALLY // 2 * LANES), bf16), vm((WIDE, TALLY // 2 * LANES), bf16), vm((parts, WIDE), f32),
            pltpu.SMEM((FEW, LANES), jnp.int32), pltpu.SMEM((FEW, LANES), jnp.int32), pltpu.SMEM((3, 16), jnp.int32),
            pltpu.SemaphoreType.DMA((2,)),
        ],
        compiler_params=pltpu.CompilerParams(
            vmem_limit_bytes=48 * 1024 * 1024),
        name="walk",
    )(which, sources, weights, lists)


def share_kernel(src, graph, x_ref, o_ref, own_sem, send_sem, recv_sem):
    mine, g, others = place_and_others(src, graph)
    hello(others)
    await_hello(others)
    own = pltpu.make_async_copy(x_ref, o_ref.at[mine], own_sem)
    own.start()
    copies = []
    for n, (py, pg) in enumerate(others):
        copies.append(pltpu.make_async_remote_copy(
            src_ref=x_ref, dst_ref=o_ref.at[mine], send_sem=send_sem.at[n], recv_sem=recv_sem.at[n],
            device_id={"src": py, "graph": pg}, device_id_type=MESH))
        copies[-1].start()
    own.wait()
    for c in copies:
        c.wait()


def share(x, src, graph):
    n = src * graph
    return pl.pallas_call(
        functools.partial(share_kernel, src, graph),
        in_specs=[pl.BlockSpec(memory_space=pltpu.VMEM)],
        out_specs=pl.BlockSpec(memory_space=pltpu.VMEM),
        out_shape=jax.ShapeDtypeStruct((n,) + x.shape, x.dtype),
        scratch_shapes=[pltpu.SemaphoreType.DMA, pltpu.SemaphoreType.DMA((n - 1,)), pltpu.SemaphoreType.DMA((n - 1,))],
        compiler_params=pltpu.CompilerParams(collective_id=2, has_side_effects=True),
        name="share",
    )(x)


def total_kernel(src, graph, x_ref, o_ref, got, own_sem, send_sem, recv_sem):
    mine, g, others = place_and_others(src, graph)
    hello(others)
    own = pltpu.make_async_copy(x_ref.at[g], got.at[mine], own_sem)
    own.start()
    await_hello(others)
    copies = []
    for n, (py, pg) in enumerate(others):
        copies.append(pltpu.make_async_remote_copy(
            src_ref=x_ref.at[pg], dst_ref=got.at[mine], send_sem=send_sem.at[n], recv_sem=recv_sem.at[n],
            device_id={"src": py, "graph": pg}, device_id_type=MESH))
        copies[-1].start()
    own.wait()
    for c in copies:
        c.wait()
    acc = got[0]
    for n in range(1, src * graph):
        acc = acc + got[n]
    o_ref[...] = acc


def total(x, src, graph, collective_id):
    n = src * graph
    return pl.pallas_call(
        functools.partial(total_kernel, src, graph),
        in_specs=[pl.BlockSpec(memory_space=pltpu.VMEM)],
        out_specs=pl.BlockSpec(memory_space=pltpu.VMEM),
        out_shape=jax.ShapeDtypeStruct(x.shape[1:], x.dtype),
        scratch_shapes=[pltpu.VMEM((n,) + x.shape[1:], x.dtype), pltpu.SemaphoreType.DMA,
                        pltpu.SemaphoreType.DMA((n - 1,)), pltpu.SemaphoreType.DMA((n - 1,))],
        compiler_params=pltpu.CompilerParams(collective_id=collective_id, has_side_effects=True),
        name="total",
    )(pltpu.with_memory_space_constraint(x, pltpu.VMEM))


def exchange(x, axis):
    return lax.all_to_all(x, axis, 0, 0)


def dense(adj_slab, src_local, level_weight, src, graph):
    slab_rows, vertex_count = adj_slab.shape
    src_count = src_local.shape[0]
    levels = level_weight.shape[0] + 1
    row_start = lax.axis_index("graph") * slab_rows
    vertex_ids = row_start + lax.broadcasted_iota(jnp.int32, (slab_rows, 1), 0)
    first = jnp.where(vertex_ids == src_local[None, :], 1.0, 0.0).astype(f32)

    def forward(carry, unused):
        sigma, seen = carry
        partial = jnp.einsum("uv,us->vs", adj_slab, sigma, preferred_element_type=f32, precision=exact_precision)
        parts = exchange(partial.reshape(graph, slab_rows, src_count), "graph")
        sigma = jnp.sum(parts, axis=0) * (1.0 - seen)
        seen = jnp.maximum(seen, jnp.where(sigma > 0, 1.0, 0.0))
        return (sigma, seen), sigma

    _, sigmas = lax.scan(forward, (first, first), None, length=levels)

    def backward(carry, xs):
        delta, acc = carry
        upper, lower, weight = xs
        reached = upper > 0
        ratio = jnp.where(reached, (weight + delta) / jnp.where(reached, upper, 1.0), 0.0)
        gathered = exchange(jnp.broadcast_to(ratio[None], (graph,) + ratio.shape), "graph")
        pulled = jnp.einsum("uv,vs->us", adj_slab, gathered.reshape(vertex_count, src_count),
                            preferred_element_type=f32, precision=exact_precision)
        delta = lower * pulled
        return (delta, acc + delta), None

    zero = jnp.zeros_like(first)
    (_, acc), _ = lax.scan(backward, (zero, zero), (sigmas[1:][::-1], sigmas[:-1][::-1], level_weight[::-1]))
    scale = vertex_count / (src_count * src * levels ** 3)
    mine = jnp.sum(acc, axis=1) * scale
    both = exchange(jnp.broadcast_to(mine.reshape(1, -1, LANES), (src, slab_rows // LANES, LANES)), "src")
    return jnp.sum(both, axis=0).reshape(slab_rows)


def solution(mesh):
    src, graph = mesh.shape["src"], mesh.shape["graph"]

    def device_program(adj_slab, src_local, level_weight):
        slab_rows, vertex_count = adj_slab.shape
        levels = level_weight.shape[0] + 1
        scale = vertex_count / (HALF * src * graph * levels ** 3)
        which = lax.axis_index("graph").astype(jnp.int32).reshape(1)

        def finish(lists, compact, collective_id, other):
            parts = walk(which, src_local, level_weight, lists, blocks=graph, vertices=vertex_count, scale=scale, compact=compact)
            summed = total(parts, src, graph, collective_id)
            rows = slab_rows // LANES

            def plain():
                return summed[:rows].reshape(2, -1, LANES).transpose(1, 0, 2).reshape(slab_rows)

            return lax.cond(summed[rows, 0] > 0, other, plain)

        def dense_path():
            return dense(adj_slab, src_local, level_weight, src, graph)

        def general_path():
            half = lax.axis_index("src").astype(jnp.int32).reshape(1)
            lists = share(extract(adj_slab, half, slab_rows // src), src, graph)
            return finish(lists.reshape(-1, SUB, LANES), False, 3, dense_path)

        return finish(collect(adj_slab, src, graph), True, 1, general_path)

    return jax.shard_map(device_program, mesh=mesh,
                         in_specs=(P(("batch", "graph"), None), P(("batch", "src")), P(None)),
                         out_specs=P(("batch", "graph")), check_vma=False)
```

```python
import functools

import jax
import jax.numpy as jnp
from jax import lax
from jax.experimental import pallas as pl
from jax.experimental.pallas import tpu as pltpu
from jax.sharding import PartitionSpec as P

MESH = pl.DeviceIdType.MESH
exact_precision = lax.Precision.HIGHEST
f32, bf16 = jnp.float32, jnp.bfloat16

LANES, SUB = 128, 8
QUARTER = 32
WIDE = 256
DEG, FEW = 8, 4
EMPTY = -2.0
FULL = 32767.0
TURN = (((1,), (1,)), ((), ()))
BLOCK = 128
READS = 4
STEP = 32
HALF = 64
SLOTS = 8
WINDOW = 48
SCAN = 32
CAP = 1024
TALLY = 96
PAIR = (0, 1)
BYTE = 256
PRODUCT = 12
PEEL = 32
BASE, COUNT = 0, 1
FAULT, LENGTH, GOT, PARITY, AWAIT0, AWAIT1, REACHED, SHORT0, SHORT1 = ((2, n) for n in range(9))


def place_and_others(src, graph):
    y, g = lax.axis_index("src"), lax.axis_index("graph")
    steps = sorted(((i, k) for i in range(src) for k in range(graph)), key=lambda s: (-s[0], abs(s[1] - graph // 2)))
    return g * src + y, g, [((y + i) % src, (g + k) % graph) for i, k in steps if i + k]


def hello(peers):
    for y, g in peers:
        pl.semaphore_signal(pltpu.get_barrier_semaphore(), inc=1, device_id={"src": y, "graph": g}, device_id_type=MESH)


def await_hello(peers):
    pl.semaphore_wait(pltpu.get_barrier_semaphore(), len(peers))


def place(plane, lists):
    lists = list(lists)
    row_i = lax.broadcasted_iota(jnp.int32, (WIDE, WIDE), 0)
    col_i = lax.broadcasted_iota(jnp.int32, (WIDE, WIDE), 1)
    eye = jnp.where(row_i == col_i, float(WIDE), 0.0).astype(bf16)
    flipped = lax.dot_general(eye, plane, TURN, preferred_element_type=f32)
    lane_id = lax.broadcasted_iota(jnp.int32, (SUB, flipped.shape[1]), 0).astype(f32)
    for g in range(WIDE // SUB):
        x = flipped[g * SUB:(g + 1) * SUB] + (lane_id + float(g * SUB))
        for s in range(len(lists)):
            hi = jnp.maximum(lists[s], x)
            if s < len(lists) - 1:
                x = jnp.minimum(lists[s], x)
            lists[s] = hi
    return lists


def sort(lists):
    gap = len(lists) // 2
    while gap:
        for s in range(len(lists)):
            if not s & gap:
                lists[s], lists[s + gap] = jnp.maximum(lists[s], lists[s + gap]), jnp.minimum(lists[s], lists[s + gap])
        gap //= 2
    return lists


def over_sublanes(lists):
    size = len(lists)
    for shift in (4, 2, 1):
        other = [pltpu.roll(v, shift, 0) for v in lists]
        lists = sort([jnp.maximum(lists[s], other[size - 1 - s]) for s in range(size)])
    out = jnp.full(lists[0].shape, EMPTY, f32)
    sub = lax.broadcasted_iota(jnp.int32, out.shape, 0)
    for s in range(size):
        out = jnp.where(sub == s, jnp.where(lists[s] >= WIDE, lists[s] - WIDE, EMPTY), out)
    return out


def degree_of(seen):
    return lax.dot_general(jnp.ones((SUB, WIDE), bf16), seen, TURN, preferred_element_type=f32)


def collect_kernel(src, graph, a_ref, o_ref, bufs, tops, mine, sems, own_sem, send_sems, recv_sems):
    vertices = a_ref.shape[1]
    pairs, chunks = mine.shape[0], vertices // WIDE
    blocks = 2 * pairs
    me, _, others = place_and_others(src, graph)
    y = me % src
    height = 4 * SUB
    pieces = BLOCK // height

    def fetch(i, t):
        rows = pl.ds(pl.multiple_of((y * blocks + i) * BLOCK + t * height, height), height)
        here = pl.ds(pl.multiple_of(t * height, height), height)
        return pltpu.make_async_copy(a_ref.at[rows], bufs.at[i % READS, here], sems.at[i % READS, t])

    def send(n, first, count):
        py, pg = others[n]
        return pltpu.make_async_remote_copy(
            src_ref=mine.at[pl.ds(first, count)], dst_ref=o_ref.at[pl.ds(me * pairs + first, count)],
            send_sem=send_sems.at[n], recv_sem=recv_sems.at[n], device_id={"src": py, "graph": pg}, device_id_type=MESH)

    def send_pair(p):
        for n in range(len(others)):
            send(n, p, 1).start()

    for i in range(READS - 1):
        for t in range(pieces):
            fetch(i, t).start()
    hello(others)
    none = jnp.zeros((SUB, 2 * BLOCK), f32)

    def scan(i, first):
        @pl.when(i + READS - 1 < blocks)
        def _():
            for t in range(pieces):
                fetch(i + READS - 1, t).start()

        def scan_rows(t, carry):
            fetch(i, t).wait()
            here = pl.ds(pl.multiple_of(t * height, height), height)

            def scan_chunks(c, state):
                top, low, seen, sums, value = state
                for k in range(STEP):
                    a = bufs[i % READS, here, pl.ds(pl.multiple_of((c * STEP + k) * WIDE, WIDE), WIDE)]
                    x = a * value
                    low = jnp.maximum(low, jnp.minimum(top, x))
                    top = jnp.maximum(top, x)
                    seen = seen + a
                    sums = sums + x
                    value = value + 1
                return top, low, seen, sums, value

            zero = jnp.zeros((height, WIDE), bf16)
            top, low, seen, sums, _ = lax.fori_loop(0, chunks // STEP, scan_chunks, (zero,) * 4 + (zero + 1,))
            for n, v in enumerate((top, low, (sums - top) - low, seen)):
                tops[n, pl.ds(pl.multiple_of(first + t * height, height), height), :] = v
            return carry

        lax.fori_loop(0, pieces, scan_rows, 0)

    def pair_step(p, carry):
        for h in range(2):
            scan(2 * p + h, h * BLOCK)
        seen = tops[3]
        crowd = seen[:SUB]
        for k in range(1, 2 * BLOCK // SUB):
            crowd = jnp.maximum(crowd, seen[k * SUB:(k + 1) * SUB])
        crowd = jnp.max(crowd.astype(f32), axis=0, keepdims=True)
        a, b, c = place(tops[0], (none,) * 4), place(tops[1], (none,) * 2), place(tops[2], (none,))
        rest = [jnp.maximum(b[0], c[0]), jnp.minimum(b[0], c[0])]
        rest = [rest[0], jnp.maximum(b[1], rest[1]), jnp.minimum(b[1], rest[1])]
        lists = over_sublanes(sort([a[0]] + [jnp.maximum(a[s + 1], rest[2 - s]) for s in range(3)]))
        lists = jnp.where((crowd > 3) | (degree_of(seen) > 4), FULL, lists)
        even, odd = lists[:, :BLOCK], lists[:, BLOCK:]
        sub = lax.broadcasted_iota(jnp.int32, even.shape, 0)
        mine[p] = jnp.where(sub < 4, even, pltpu.roll(odd, 4, 0))

        @pl.when(p == 1)
        def _():
            await_hello(others)

        @pl.when(p > 0)
        def _():
            send_pair(p - 1)

        return carry

    lax.fori_loop(0, pairs, pair_step, 0)
    own = pltpu.make_async_copy(mine, o_ref.at[pl.ds(me * pairs, pairs)], own_sem)
    send_pair(pairs - 1)
    own.start()
    own.wait()
    for n in range(len(others)):
        send(n, 0, pairs).wait()


def collect(adj_slab, src, graph):
    rows, vertices = adj_slab.shape
    n = src * graph
    mine = (rows // src // (2 * BLOCK), SUB, BLOCK)
    return pl.pallas_call(
        functools.partial(collect_kernel, src, graph),
        in_specs=[pl.BlockSpec(memory_space=pl.ANY)],
        out_specs=pl.BlockSpec(memory_space=pltpu.VMEM),
        out_shape=jax.ShapeDtypeStruct((n * mine[0],) + mine[1:], f32),
        scratch_shapes=[pltpu.VMEM((READS, BLOCK, vertices), bf16), pltpu.VMEM((4, 2 * BLOCK, WIDE), bf16), pltpu.VMEM(mine, f32),
                        pltpu.SemaphoreType.DMA((READS, BLOCK // (4 * SUB))), pltpu.SemaphoreType.DMA,
                        pltpu.SemaphoreType.DMA((n - 1,)), pltpu.SemaphoreType.DMA((n - 1,))],
        compiler_params=pltpu.CompilerParams(collective_id=0, has_side_effects=True, vmem_limit_bytes=40 * 1024 * 1024),
        name="collect",
    )(adj_slab)


def extract_kernel(half_ref, a_ref, o_ref, block, seen, planes, sem):
    vertices = a_ref.shape[1]

    def block_step(i, carry):
        copy = pltpu.make_async_copy(
            a_ref.at[pl.ds(pl.multiple_of((half_ref[0] * o_ref.shape[0] + i) * BLOCK, BLOCK), BLOCK)], block, sem)
        copy.start()
        copy.wait()
        planes[...] = jnp.zeros_like(planes)
        seen[...] = jnp.zeros_like(seen)

        def scan_chunk(c, carry):
            a = block[:, pl.ds(pl.multiple_of(c * WIDE, WIDE), WIDE)]
            seen[...] = seen[...] + a
            x = a.astype(f32) * (c + 1).astype(f32)
            for s in range(DEG):
                top = planes[s].astype(f32)
                planes[s] = jnp.maximum(top, x).astype(bf16)
                x = jnp.minimum(top, x)
            return carry

        lax.fori_loop(0, vertices // WIDE, scan_chunk, 0)
        lists = lax.fori_loop(0, DEG, lambda p, lists: tuple(place(planes[p], lists)), (jnp.zeros((SUB, BLOCK), f32),) * DEG)
        o_ref[i] = jnp.where(degree_of(seen[...]) > DEG, FULL, over_sublanes(list(lists)))
        return carry

    lax.fori_loop(0, o_ref.shape[0], block_step, 0)


def extract(adj_slab, half, rows):
    vertices = adj_slab.shape[1]
    return pl.pallas_call(
        extract_kernel,
        in_specs=[pl.BlockSpec(memory_space=pltpu.SMEM), pl.BlockSpec(memory_space=pl.ANY)],
        out_specs=pl.BlockSpec(memory_space=pltpu.VMEM),
        out_shape=jax.ShapeDtypeStruct((rows // BLOCK, DEG, BLOCK), f32),
        scratch_shapes=[pltpu.VMEM((BLOCK, vertices), bf16), pltpu.VMEM((BLOCK, WIDE), bf16),
                        pltpu.VMEM((DEG, BLOCK, WIDE), bf16), pltpu.SemaphoreType.DMA],
        name="extract",
    )(half, adj_slab)


def along(shape, axis=0):
    return lax.broadcasted_iota(jnp.int32, shape, axis)


def swap(x):
    return pltpu.roll(x, HALF, 1)


def digits(x, base):
    high = jnp.floor(x * (1.0 / base))
    return high, x - high * base


def walk_kernel(which_ref, src_ref, weight_ref, lists_ref, out_ref,
                table, queue, sigma, ratio, delta, cand, ids, now, dest, tail_ref, held, rowhot, colhot, bins,
                ids_a, ids_b, meta, sems, *, levels, vertices, scale, compact):
    pitch = vertices + SUB
    lane = along((SUB, LANES), 1)
    sub = along((SUB, LANES))
    upper = lane >= HALF
    lane_row = along((1, LANES), 1)
    group_odd = ((lane_row // QUARTER) % 2) == 1
    lane32 = lane_row % QUARTER
    rows_all = queue.shape[0]
    tile_bits = (vertices // lists_ref.shape[0]).bit_length() - 1
    high = vertices // WIDE

    def eight(row):
        return pl.ds(pl.multiple_of(row, SUB), SUB)

    def part(n):
        return pl.ds(n * SUB, SUB)

    def spread_row(ref, *index):
        return jnp.broadcast_to(ref[(*index[:-1], pl.ds(index[-1], 1), slice(None))], (SUB, LANES))

    def clear(t, carry):
        for k in range(SUB):
            rows = eight((t * SUB + k) * SUB)
            queue[rows, :] = jnp.full((SUB, LANES), -1.0, f32)
            sigma[rows, :] = jnp.zeros((SUB, LANES), f32)
        return carry

    def fetch(quad, row, buf):
        return pltpu.make_async_copy(ids.at[quad, eight(row)], buf[0], sems.at[buf[1]])

    def name(row, q):
        v = jnp.where(q < 0, vertices, q.astype(jnp.int32))
        ids[0, eight(row), :] = v
        ids[1, eight(row), :] = v + pitch

    bufs = (ids_a, 0), (ids_b, 1)
    clear(0, 0)

    near_source = jnp.full((SUB, LANES), EMPTY, f32)
    source = near_source
    for j in range(HALF):
        v = src_ref[which_ref[0] * HALF + j]
        tile = pltpu.roll(lists_ref[v >> tile_bits], (j - v) & (LANES - 1), 1)
        if compact:
            tile = jnp.where((v & LANES) > 0, pltpu.roll(tile, FEW, 0), tile)
        near_source = jnp.where(lane == j, tile, near_source)
        source = jnp.where(lane % HALF == j, v.astype(f32), source)
    near_source = jnp.where(upper, swap(near_source), near_source)
    reached = near_source >= 0
    if compact:
        reached = reached & (sub < FEW)
    queue[0:1, :] = source[:1]
    queue[eight(SUB), :] = jnp.where(reached, near_source, -1.0)
    sigma[eight(SUB), :] = jnp.where(reached & jnp.logical_not(upper), 1.0, 0.0)
    for n in (1, 2):
        name(n * SUB, queue[eight(n * SUB), :])
    bins[...] = jnp.zeros_like(bins)
    fetch(0, SUB, bufs[0]).start()
    if compact:
        fetch(0, 2 * SUB, bufs[1]).start()
    lax.fori_loop(1, rows_all // (SUB * SUB), clear, 0)

    owner = along((LANES, LANES), 1) // QUARTER
    digit = along((2 * SUB, LANES))
    group = LANES // SUB

    def fill(halves, target):
        picks = jnp.concatenate([jnp.where(digit % SUB == owner[:2 * SUB] + FEW * h, jnp.where(digit < SUB, float(LANES), 1.0), 0.0)
                                 for h in halves], axis=1).astype(bf16)

        def body(step, most):
            first = step * group
            tiles = lists_ref[pl.ds(first, group)]

            def put(h, t, rows):
                table[pl.ds(pl.multiple_of(target(h, first + t), SUB), LANES), :] = rows

            x = jnp.concatenate([tiles[t] for t in range(PRODUCT)], axis=1)
            both = jnp.concatenate(digits(x, LANES), axis=0).astype(bf16)
            rows = lax.dot_general(both, picks, (((0,), (0,)), ((), ())), preferred_element_type=f32)
            for t in range(PRODUCT):
                for n, h in enumerate(halves):
                    put(h, t, rows[t * LANES:(t + 1) * LANES, n * LANES:(n + 1) * LANES])
            turned = tiles.reshape(LANES, LANES).T
            for t in range(PRODUCT, group):
                for h in halves:
                    put(h, t, jnp.take_along_axis(turned, owner + (SUB * t + FEW * h), axis=1))
            return jnp.maximum(most, jnp.max(tiles, axis=0))

        return lax.fori_loop(0, lists_ref.shape[0] // group, body, jnp.full((SUB, LANES), EMPTY, f32))

    table[vertices:pitch, :] = jnp.full((SUB, LANES), EMPTY, f32)
    if compact:
        most = fill(PAIR, lambda h, t: (2 * t + h) * LANES)
        quads = 1
    else:
        table[pitch + vertices:, :] = jnp.full((SUB, LANES), EMPTY, f32)
        most = fill((0,), lambda h, t: t * LANES)
        wide = jnp.max(jnp.where(sub >= FEW, most, EMPTY)) >= 0
        quads = jnp.where(wide, 2, 1)

        @pl.when(wide)
        def _():
            fill((1,), lambda h, t: pitch + t * LANES)

    bad = jnp.max(most) > vertices
    meta[FAULT] = bad.astype(jnp.int32)

    def gather(rows_of_ids):
        acc = [[jnp.full((1, LANES), EMPTY, f32)] * 2 for _ in rows_of_ids]
        for j in range(QUARTER):
            hit = lane32 == j
            for i, id_of in enumerate(rows_of_ids):
                for b in PAIR:
                    acc[i][b] = jnp.where(hit, table[pl.ds(id_of(b * QUARTER + j), 1), :], acc[i][b])
        return [(jnp.where(group_odd, b, a), pltpu.roll(jnp.where(group_odd, a, b), LANES - QUARTER, 1)) for a, b in acc]

    def gather_slots(ids_s, slots=SLOTS):
        return gather([functools.partial(lambda i, j: ids_s[i, j], i) for i in range(slots)])

    def keep(rows, quad, row):
        for i, pair in enumerate(rows):
            for h in PAIR:
                cand[2 * quad + h, pl.ds(row + i, 1), :] = pair[h]

    def flag(x):
        return jnp.where(x, 1, 0)

    def at(unit, origin):
        return unit & (quads - 1), origin + (unit >> (quads - 1)) * SUB

    def level_step(level, carry):
        base, count = meta[BASE, level], meta[COUNT, level]
        following = base + (count + 7) // SUB * SUB
        batches = jnp.where(following <= CAP, (count + SLOTS - 1) // SLOTS, 0)
        units = batches * quads
        parity = meta[PARITY]

        def on_parity(n, f):
            for k in PAIR:
                @pl.when(n & 1 == k)
                def _():
                    f(bufs[k], bufs[1 - k])

        def unit_step(unit, other, to):
            quad, row = at(unit, base)
            x = [cand[2 * quad + h, eight(row), :] for h in PAIR]

            def search(first, count, marks):
                marks = list(marks)
                for k in range(count):
                    q = spread_row(queue, first + k)
                    for h in PAIR:
                        n = 2 * h + k % 2
                        marks[n] = jnp.where(x[h] == q, 1, marks[n])
                return tuple(marks)

            reach = following + meta[LENGTH] - PEEL
            marks = lax.fori_loop(0, (reach + SCAN - 1) // SCAN, lambda t, m: search(PEEL + t * SCAN, SCAN, m),
                                  (jnp.zeros((SUB, LANES), jnp.int32),) * 4)
            ahead = unit + 1 < units
            final_unit = unit + 1 == units
            soon = jnp.logical_and(final_unit, meta[AWAIT0] > 0)

            @pl.when(jnp.logical_or(ahead, soon))
            def _():
                fetch(0, base, to).wait()

            def insert(g):
                slots = [eight(following + g * WINDOW + SUB * t) for t in range(WINDOW // SUB)]
                qs = [queue[r, :] for r in slots]
                ss = [sigma[r, :] for r in slots]
                pos = [sub + (g * WINDOW + SUB * t) for t in range(WINDOW // SUB)]
                for h in PAIR:
                    for i in range(SUB):
                        d, e = spread_row(dest, SUB * h + i), spread_row(dest, SUB * (h + 2) + i)
                        v, w = spread_row(now, SUB * h + i), spread_row(now, SUB * (h + 2) + i)
                        for t in range(WINDOW // SUB):
                            qs[t] = jnp.where(pos[t] == d, v, jnp.where(pos[t] == e, w, qs[t]))
                for i in range(SUB):
                    v, w, sig = (spread_row(now, SUB * n + i) for n in (0, 1, 4))
                    for t in range(WINDOW // SUB):
                        ss[t] = ss[t] + jnp.where((qs[t] == v) | (qs[t] == w), sig, 0.0)
                for t, r in enumerate(slots):
                    queue[r, :] = qs[t]
                    sigma[r, :] = ss[t]
                return qs

            def core(looking):
                even, odd = x
                m, n, k, l = search(0, PEEL, marks)
                near_even, near_odd = m | n | flag(even < 0), k | l | flag(odd < 0)

                xr = [swap(v) for v in x]
                turns = [[[pltpu.roll(v, s, 0) if s else v for v in (x[h], xr[h])] for s in range(SUB)] for h in PAIR]
                for s, ((a, b), (c, d)) in enumerate(zip(*turns)):
                    near_odd = jnp.where((odd == a) | (odd == b), 1, near_odd)
                    if s:
                        after = sub >= s
                        near_even = jnp.where(((even == a) | (even == b)) & after, 1, near_even)
                        near_odd = jnp.where(((odd == c) | (odd == d)) & after, 1, near_odd)

                new = [1 - near_even, 1 - near_odd]
                packed = new[0] + BYTE * new[1]
                across = swap(packed)
                far = [across & (BYTE - 1), across >> SUB]
                both = packed + across
                run, whole = both, both
                for s in (1, 2, 4):
                    run = run + jnp.where(sub >= s, pltpu.roll(run, s, 0), 0)
                    whole = whole + pltpu.roll(whole, s, 0)
                run = run - both
                tail = tail_ref[...]
                evens = whole & (BYTE - 1)
                begin = [tail + (run & (BYTE - 1)), tail + evens + (run >> SUB)]
                for h in PAIR:
                    dest[part(h), :] = jnp.where(new[h] > 0, begin[h] + jnp.where(upper, far[h], 0), -1)
                    dest[part(h + 2), :] = jnp.where(far[h] > 0, begin[h] + jnp.where(upper, 0, new[h]), -1)
                    now[part(h), :] = x[h]
                    now[part(h + 2), :] = xr[h]
                now[part(4), :] = sigma[eight(row), :] + swap(sigma[eight(row), :])
                tail = tail + evens + (whole >> SUB)
                tail_ref[...] = tail
                passed = SLOTS * ((unit + 1) >> (quads - 1))
                second = SUB + SUB * (1 >> (quads - 1))
                need = jnp.where(sub == 1, SUB, second)
                short = (tail < need) & (held[...] > passed)
                most = jnp.max(jnp.where(sub == 0, tail, flag(short)).astype(f32), axis=1, keepdims=True)
                meta[REACHED] = most[0, 0].astype(jnp.int32)
                for n in PAIR:
                    meta[(SHORT0, SHORT1)[n]] = most[n + 1, 0].astype(jnp.int32)

                if looking:
                    quad2, row2 = at(unit + 1, base)
                    rows = gather_slots(to[0])
                qs = insert(0)
                for n in PAIR:
                    name(following + n * SUB, qs[n])
                if looking:
                    keep(rows, jnp.where(ahead, quad2, 0), jnp.where(ahead, row2, following))

            look = jnp.logical_or(ahead, soon)
            for looking in PAIR:
                @pl.when(look == (looking > 0))
                def _():
                    core(looking)

            length = meta[REACHED]
            ready = [meta[n] == 0 for n in (SHORT0, SHORT1)]

            @pl.when(unit + 3 < units)
            def _():
                fetch(*at(unit + 3, base), to).start()

            @pl.when(soon)
            def _():
                meta[GOT] = 1

            def first_of_next(n, when, buf):
                @pl.when(jnp.logical_and(when, meta[(AWAIT0, AWAIT1)[n]] == 0))
                def _():
                    fetch(*at(n, following), buf).start()
                    meta[(AWAIT0, AWAIT1)[n]] = 1

            first_of_next(0, jnp.logical_and(ready[0], unit + 3 == units), to)
            first_of_next(0, jnp.logical_and(ready[0], unit + 2 == units), other)
            first_of_next(1, jnp.logical_and(ready[1], unit + 2 == units), to)
            first_of_next(0, final_unit, to)
            first_of_next(1, final_unit, other)

            groups = (length + WINDOW - 1) // WINDOW
            fits = following + groups * WINDOW <= CAP + WINDOW
            meta[LENGTH] = jnp.where(fits, length, 0)

            @pl.when(jnp.logical_not(fits))
            def _():
                meta[FAULT] = 1

            def more(g, carry):
                insert(g)
                return carry

            lax.fori_loop(1, jnp.where(fits, groups, 0), more, 0)

        tail_ref[...] = jnp.zeros_like(tail_ref)
        meta[LENGTH] = 0

        def open_level(mine, other):
            @pl.when(jnp.logical_and(meta[GOT] == 0, meta[AWAIT0] > 0))
            def _():
                fetch(0, base, mine).wait()
                keep(gather_slots(mine[0]), 0, base)

            @pl.when(jnp.logical_and(units < 2, meta[AWAIT1] > 0))
            def _():
                fetch(0, base, other).wait()

            @pl.when(units > 2)
            def _():
                fetch(*at(2, base), mine).start()

        on_parity(parity, open_level)
        for place_ in (GOT, AWAIT0, AWAIT1):
            meta[place_] = 0

        def any_unit(unit, carry):
            on_parity(parity + unit, functools.partial(unit_step, unit))
            return carry

        lax.fori_loop(0, units, any_unit, 0)
        meta[PARITY] = parity + units

        @pl.when(following > CAP)
        def _():
            meta[FAULT] = 1

        found = jnp.where(meta[FAULT] == 0, meta[LENGTH], 0)
        meta[BASE, level + 1] = following
        meta[COUNT, level + 1] = found

        def names(t, carry):
            row = following + t * SUB
            name(row, queue[eight(row), :])
            return carry

        lax.fori_loop(2, (found + SUB - 1) // SUB, names, 0)
        held[...] = tail_ref[...]
        return carry

    for place_ in (GOT, PARITY):
        meta[place_] = 0

    @pl.when(jnp.logical_not(bad))
    def _():
        held[...] = jnp.full_like(held, FEW * quads)
        meta[BASE, 1] = SUB
        meta[COUNT, 1] = FEW * quads
        fetch(0, SUB, bufs[0]).wait()
        if compact:
            for h in PAIR:
                cand[h, eight(SUB), :] = jnp.full((SUB, LANES), EMPTY, f32)
        else:
            fetch(*at(1, SUB), bufs[1]).start()
        keep(gather_slots(ids_a, FEW if compact else SLOTS), 0, SUB)
        meta[GOT] = 1
        meta[AWAIT0] = 0
        meta[AWAIT1] = 1
        lax.fori_loop(1, levels, level_step, 0)

    @pl.when(bad)
    def _():
        fetch(0, SUB, bufs[0]).wait()
        meta[AWAIT0] = 0
        meta[AWAIT1] = int(compact)

    def drain(n, buf):
        @pl.when(meta[(AWAIT0, AWAIT1)[n]] > 0)
        def _():
            fetch(0, 0, buf).wait()

    for k in PAIR:
        @pl.when(meta[PARITY] & 1 == k)
        def _():
            @pl.when(meta[GOT] == 0)
            def _():
                drain(0, bufs[k])

            drain(1, bufs[1 - k])

    good = meta[FAULT] == 0

    @pl.when(good)
    def _():
        last = meta[BASE, levels]
        g_last = weight_ref[levels - 2]

        def seed(g, carry):
            for t in range(WINDOW // SUB):
                r = eight(last + g * WINDOW + SUB * t)
                s = sigma[r, :] + swap(sigma[r, :])
                ratio[r, :] = jnp.where(s > 0, g_last / jnp.where(s > 0, s, 1.0), 0.0)
            return carry

        lax.fori_loop(0, (meta[COUNT, levels] + WINDOW - 1) // WINDOW, seed, 0)

        def back_step(k, carry):
            level = levels - 1 - k
            base, count = meta[BASE, level], meta[COUNT, level]
            nbase, ncount = meta[BASE, level + 1], meta[COUNT, level + 1]
            g_here = weight_ref[jnp.maximum(level - 2, 0)]

            def pull_batch(bt, carry):
                here = eight(base + bt * SLOTS)

                def pull(quad, c, acc):
                    even, odd = cand[2 * quad, here, :], cand[2 * quad + 1, here, :]
                    acc = list(acc)
                    for n in range(WINDOW):
                        q = spread_row(queue, nbase + c * WINDOW + n)
                        w = spread_row(ratio, nbase + c * WINDOW + n)
                        acc[n % 2] = acc[n % 2] + jnp.where((even == q) | (odd == q), w, 0.0)
                    return tuple(acc)

                def pull_quad(quad, acc):
                    return lax.fori_loop(1, (ncount + WINDOW - 1) // WINDOW, functools.partial(pull, quad), pull(quad, 0, acc))

                acc = pull_quad(0, (jnp.zeros((SUB, LANES), f32),) * 2)
                if not compact:
                    acc = lax.fori_loop(1, quads, pull_quad, acc)
                delta[here, :] = acc[0] + acc[1]
                return carry

            lax.fori_loop(0, (count + SLOTS - 1) // SLOTS, pull_batch, 0)

            def finish(g, carry):
                slots = [eight(base + g * WINDOW + SUB * t) for t in range(WINDOW // SUB)]
                for t, r in enumerate(slots):
                    inside = g * WINDOW + SUB * t < count
                    part, s = (v + swap(v) for v in (delta[r, :], sigma[r, :]))
                    d = s * part
                    w = jnp.where(s > 0, (g_here + d) / jnp.where(s > 0, s, 1.0), 0.0)
                    delta[r, :] = jnp.where(inside, d, delta[r, :])
                    ratio[r, :] = jnp.where(inside, w, ratio[r, :])
                return carry

            lax.fori_loop(0, (count + WINDOW - 1) // WINDOW, finish, 0)
            return carry

        lax.fori_loop(0, levels - 1, back_step, 0)

        tall = along((WIDE, WIDE)).astype(f32).astype(bf16)
        zero = jnp.zeros((WIDE, WIDE), bf16)
        one = zero + 1
        start = meta[BASE, 1]

        def tally(t, carry):
            for u in range(TALLY // 16):
                a, b = eight(start + t * TALLY + u * 16), eight(start + t * TALLY + u * 16 + SUB)
                v = jnp.where(upper, queue[b, :], queue[a, :])
                d = jnp.where(upper, delta[b, :], delta[a, :])
                hi, lo = digits(v, WIDE)
                d_hi = d.astype(bf16).astype(f32)
                d_mid = (d - d_hi).astype(bf16).astype(f32)
                d_lo = d - d_hi - d_mid
                for p in range(0, SUB, 2):
                    cols = slice((u * SUB + p) * LANES, (u * SUB + p + 2) * LANES)

                    def pair(x):
                        return jnp.concatenate([x[p:p + 1], x[p + 1:p + 2]], axis=1).astype(bf16)

                    colhot[:, cols] = jnp.where(tall == pair(lo), one, zero)
                    match = tall[:high] == pair(hi)
                    for n, x in enumerate((d_hi, d_mid, d_lo)):
                        rowhot[n * high:(n + 1) * high, cols] = jnp.where(match, pair(x), zero[:high])
            bins[...] += lax.dot_general(rowhot[...], colhot[...], TURN, preferred_element_type=f32)
            return carry

        for t in range(TALLY // SUB):
            delta[eight(last + t * SUB), :] = jnp.zeros((SUB, LANES), f32)
        lax.fori_loop(0, (last - start + TALLY - 1) // TALLY, tally, 0)

    blocks = out_ref.shape[0]
    per = high // blocks
    total = (bins[:high] + bins[high:2 * high] + bins[2 * high:]) * scale
    fault = jnp.where(good, 0.0, 1.0)
    for b in range(blocks):
        for n in PAIR:
            out_ref[b, n * per:(n + 1) * per, :] = total[b * per:(b + 1) * per, n * LANES:(n + 1) * LANES]
        out_ref[b, 2 * per:, :] = jnp.full((SUB, LANES), fault, f32)


def walk(which, sources, weights, lists, *, blocks, vertices, scale, compact):
    levels = weights.shape[0] + 1
    rows = CAP + 4 * WINDOW
    high = LANES // blocks + SUB
    vm = pltpu.VMEM
    queue = vm((rows, LANES), f32)
    parts = 3 * (vertices // WIDE)
    return pl.pallas_call(
        functools.partial(walk_kernel, levels=levels, vertices=vertices, scale=scale, compact=compact),
        in_specs=[pl.BlockSpec(memory_space=pltpu.SMEM)] * 3 + [pl.BlockSpec(memory_space=pltpu.VMEM)],
        out_specs=pl.BlockSpec(memory_space=pltpu.VMEM),
        out_shape=jax.ShapeDtypeStruct((blocks, high, LANES), f32),
        scratch_shapes=[
            vm(((1 if compact else 2) * (vertices + SUB), LANES), f32), queue, queue, queue, queue,
            vm((4, rows, LANES), f32), vm((2, rows, LANES), jnp.int32),
            vm((40, LANES), f32), vm((QUARTER, LANES), jnp.int32), vm((SUB, LANES), jnp.int32), vm((SUB, LANES), jnp.int32),
            vm((parts, TALLY // 2 * LANES), bf16), vm((WIDE, TALLY // 2 * LANES), bf16), vm((parts, WIDE), f32),
            pltpu.SMEM((SLOTS, LANES), jnp.int32), pltpu.SMEM((SLOTS, LANES), jnp.int32), pltpu.SMEM((3, 16), jnp.int32),
            pltpu.SemaphoreType.DMA((2,)),
        ],
        compiler_params=pltpu.CompilerParams(
            vmem_limit_bytes=48 * 1024 * 1024),
        name="walk",
    )(which, sources, weights, lists)


def share_kernel(src, graph, x_ref, o_ref, own_sem, send_sem, recv_sem):
    mine, g, others = place_and_others(src, graph)
    hello(others)
    await_hello(others)
    own = pltpu.make_async_copy(x_ref, o_ref.at[mine], own_sem)
    own.start()
    copies = []
    for n, (py, pg) in enumerate(others):
        copies.append(pltpu.make_async_remote_copy(
            src_ref=x_ref, dst_ref=o_ref.at[mine], send_sem=send_sem.at[n], recv_sem=recv_sem.at[n],
            device_id={"src": py, "graph": pg}, device_id_type=MESH))
        copies[-1].start()
    own.wait()
    for c in copies:
        c.wait()


def share(x, src, graph):
    n = src * graph
    return pl.pallas_call(
        functools.partial(share_kernel, src, graph),
        in_specs=[pl.BlockSpec(memory_space=pltpu.VMEM)],
        out_specs=pl.BlockSpec(memory_space=pltpu.VMEM),
        out_shape=jax.ShapeDtypeStruct((n,) + x.shape, x.dtype),
        scratch_shapes=[pltpu.SemaphoreType.DMA, pltpu.SemaphoreType.DMA((n - 1,)), pltpu.SemaphoreType.DMA((n - 1,))],
        compiler_params=pltpu.CompilerParams(collective_id=2, has_side_effects=True),
        name="share",
    )(x)


def total_kernel(src, graph, x_ref, o_ref, got, own_sem, send_sem, recv_sem):
    mine, g, others = place_and_others(src, graph)
    hello(others)
    own = pltpu.make_async_copy(x_ref.at[g], got.at[mine], own_sem)
    own.start()
    await_hello(others)
    copies = []
    for n, (py, pg) in enumerate(others):
        copies.append(pltpu.make_async_remote_copy(
            src_ref=x_ref.at[pg], dst_ref=got.at[mine], send_sem=send_sem.at[n], recv_sem=recv_sem.at[n],
            device_id={"src": py, "graph": pg}, device_id_type=MESH))
        copies[-1].start()
    own.wait()
    for c in copies:
        c.wait()
    acc = got[0]
    for n in range(1, src * graph):
        acc = acc + got[n]
    o_ref[...] = acc


def total(x, src, graph, collective_id):
    n = src * graph
    return pl.pallas_call(
        functools.partial(total_kernel, src, graph),
        in_specs=[pl.BlockSpec(memory_space=pltpu.VMEM)],
        out_specs=pl.BlockSpec(memory_space=pltpu.VMEM),
        out_shape=jax.ShapeDtypeStruct(x.shape[1:], x.dtype),
        scratch_shapes=[pltpu.VMEM((n,) + x.shape[1:], x.dtype), pltpu.SemaphoreType.DMA,
                        pltpu.SemaphoreType.DMA((n - 1,)), pltpu.SemaphoreType.DMA((n - 1,))],
        compiler_params=pltpu.CompilerParams(collective_id=collective_id, has_side_effects=True),
        name="total",
    )(pltpu.with_memory_space_constraint(x, pltpu.VMEM))


def exchange(x, axis):
    return lax.all_to_all(x, axis, 0, 0)


def dense(adj_slab, src_local, level_weight, src, graph):
    slab_rows, vertex_count = adj_slab.shape
    src_count = src_local.shape[0]
    levels = level_weight.shape[0] + 1
    row_start = lax.axis_index("graph") * slab_rows
    vertex_ids = row_start + lax.broadcasted_iota(jnp.int32, (slab_rows, 1), 0)
    first = jnp.where(vertex_ids == src_local[None, :], 1.0, 0.0).astype(f32)

    def forward(carry, unused):
        sigma, seen = carry
        partial = jnp.einsum("uv,us->vs", adj_slab, sigma, preferred_element_type=f32, precision=exact_precision)
        parts = exchange(partial.reshape(graph, slab_rows, src_count), "graph")
        sigma = jnp.sum(parts, axis=0) * (1.0 - seen)
        seen = jnp.maximum(seen, jnp.where(sigma > 0, 1.0, 0.0))
        return (sigma, seen), sigma

    _, sigmas = lax.scan(forward, (first, first), None, length=levels)

    def backward(carry, xs):
        delta, acc = carry
        upper, lower, weight = xs
        reached = upper > 0
        ratio = jnp.where(reached, (weight + delta) / jnp.where(reached, upper, 1.0), 0.0)
        gathered = exchange(jnp.broadcast_to(ratio[None], (graph,) + ratio.shape), "graph")
        pulled = jnp.einsum("uv,vs->us", adj_slab, gathered.reshape(vertex_count, src_count),
                            preferred_element_type=f32, precision=exact_precision)
        delta = lower * pulled
        return (delta, acc + delta), None

    zero = jnp.zeros_like(first)
    (_, acc), _ = lax.scan(backward, (zero, zero), (sigmas[1:][::-1], sigmas[:-1][::-1], level_weight[::-1]))
    scale = vertex_count / (src_count * src * levels ** 3)
    mine = jnp.sum(acc, axis=1) * scale
    both = exchange(jnp.broadcast_to(mine.reshape(1, -1, LANES), (src, slab_rows // LANES, LANES)), "src")
    return jnp.sum(both, axis=0).reshape(slab_rows)


def solution(mesh):
    src, graph = mesh.shape["src"], mesh.shape["graph"]

    def device_program(adj_slab, src_local, level_weight):
        slab_rows, vertex_count = adj_slab.shape
        levels = level_weight.shape[0] + 1
        scale = vertex_count / (HALF * src * graph * levels ** 3)
        which = lax.axis_index("graph").astype(jnp.int32).reshape(1)

        def finish(lists, compact, collective_id, other):
            parts = walk(which, src_local, level_weight, lists, blocks=graph, vertices=vertex_count, scale=scale, compact=compact)
            summed = total(parts, src, graph, collective_id)
            rows = slab_rows // LANES

            def plain():
                return summed[:rows].reshape(2, -1, LANES).transpose(1, 0, 2).reshape(slab_rows)

            return lax.cond(summed[rows, 0] > 0, other, plain)

        def dense_path():
            return dense(adj_slab, src_local, level_weight, src, graph)

        def general_path():
            half = lax.axis_index("src").astype(jnp.int32).reshape(1)
            lists = share(extract(adj_slab, half, slab_rows // src), src, graph)
            return finish(lists.reshape(-1, SUB, LANES), False, 3, dense_path)

        return finish(collect(adj_slab, src, graph), True, 1, general_path)

    return jax.shard_map(device_program, mesh=mesh,
                         in_specs=(P(("batch", "graph"), None), P(("batch", "src")), P(None)),
                         out_specs=P(("batch", "graph")), check_vma=False)
```

```python
import functools

import jax
import jax.numpy as jnp
from jax import lax
from jax.experimental import pallas as pl
from jax.experimental.pallas import tpu as pltpu
from jax.sharding import PartitionSpec as P

MESH = pl.DeviceIdType.MESH
exact_precision = lax.Precision.HIGHEST
f32, bf16 = jnp.float32, jnp.bfloat16

LANES, SUB = 128, 8
WIDE = 256
DEG, FEW = 8, 4
EMPTY = -2.0
FULL = 32767.0
TURN = (((1,), (1,)), ((), ()))
BLOCK = 128
READS = 4
STEP = 32
HALF = 64
SLOTS = 8
WINDOW = 48
SCAN = 64
CAP = 1024
TALLY = 96
PAIR = (0, 1)
BYTE = 256
GROUP = 8
PEEL = 32
BASE, COUNT = 0, 1
FAULT, LENGTH, GOT, PARITY, AWAIT0, AWAIT1, REACHED, SHORT0, SHORT1 = ((2, n) for n in range(9))


def place_and_others(src, graph):
    y, g = lax.axis_index("src"), lax.axis_index("graph")
    steps = sorted(((i, k) for i in range(src) for k in range(graph)), key=lambda s: (-s[0], abs(s[1] - graph // 2)))
    return g * src + y, g, [((y + i) % src, (g + k) % graph) for i, k in steps if i + k]


def hello(peers):
    for y, g in peers:
        pl.semaphore_signal(pltpu.get_barrier_semaphore(), inc=1, device_id={"src": y, "graph": g}, device_id_type=MESH)


def await_hello(peers):
    pl.semaphore_wait(pltpu.get_barrier_semaphore(), len(peers))


def place(plane, lists):
    lists = list(lists)
    row_i = lax.broadcasted_iota(jnp.int32, (WIDE, WIDE), 0)
    col_i = lax.broadcasted_iota(jnp.int32, (WIDE, WIDE), 1)
    eye = jnp.where(row_i == col_i, float(WIDE), 0.0).astype(bf16)
    flipped = lax.dot_general(eye, plane, TURN, preferred_element_type=f32)
    lane_id = lax.broadcasted_iota(jnp.int32, (SUB, flipped.shape[1]), 0).astype(f32)
    for g in range(WIDE // SUB):
        x = flipped[g * SUB:(g + 1) * SUB] + (lane_id + float(g * SUB))
        for s in range(len(lists)):
            hi = jnp.maximum(lists[s], x)
            if s < len(lists) - 1:
                x = jnp.minimum(lists[s], x)
            lists[s] = hi
    return lists


def sort(lists):
    gap = len(lists) // 2
    while gap:
        for s in range(len(lists)):
            if not s & gap:
                lists[s], lists[s + gap] = jnp.maximum(lists[s], lists[s + gap]), jnp.minimum(lists[s], lists[s + gap])
        gap //= 2
    return lists


def over_sublanes(lists):
    size = len(lists)
    for shift in (4, 2, 1):
        other = [pltpu.roll(v, shift, 0) for v in lists]
        lists = sort([jnp.maximum(lists[s], other[size - 1 - s]) for s in range(size)])
    out = jnp.full(lists[0].shape, EMPTY, f32)
    sub = lax.broadcasted_iota(jnp.int32, out.shape, 0)
    for s in range(size):
        out = jnp.where(sub == s, jnp.where(lists[s] >= WIDE, lists[s] - WIDE, EMPTY), out)
    return out


def degree_of(seen):
    return lax.dot_general(jnp.ones((SUB, WIDE), bf16), seen, TURN, preferred_element_type=f32)


def collect_kernel(src, graph, a_ref, o_ref, bufs, tops, mine, sems, own_sem, send_sems, recv_sems):
    vertices = a_ref.shape[1]
    pairs, chunks = mine.shape[0], vertices // WIDE
    blocks = 2 * pairs
    me, _, others = place_and_others(src, graph)
    y = me % src
    height = 4 * SUB
    pieces = BLOCK // height

    def fetch(i, t):
        rows = pl.ds(pl.multiple_of((y * blocks + i) * BLOCK + t * height, height), height)
        here = pl.ds(pl.multiple_of(t * height, height), height)
        return pltpu.make_async_copy(a_ref.at[rows], bufs.at[i % READS, here], sems.at[i % READS, t])

    def send(n, first, count):
        py, pg = others[n]
        return pltpu.make_async_remote_copy(
            src_ref=mine.at[pl.ds(first, count)], dst_ref=o_ref.at[pl.ds(me * pairs + first, count)],
            send_sem=send_sems.at[n], recv_sem=recv_sems.at[n], device_id={"src": py, "graph": pg}, device_id_type=MESH)

    def send_pair(p):
        for n in range(len(others)):
            send(n, p, 1).start()

    for i in range(READS - 1):
        for t in range(pieces):
            fetch(i, t).start()
    hello(others)
    none = jnp.zeros((SUB, 2 * BLOCK), f32)

    def scan(i, first):
        @pl.when(i + READS - 1 < blocks)
        def _():
            for t in range(pieces):
                fetch(i + READS - 1, t).start()

        def scan_rows(t, carry):
            fetch(i, t).wait()
            here = pl.ds(pl.multiple_of(t * height, height), height)

            def scan_chunks(c, state):
                top, low, seen, sums, value = state
                for k in range(STEP):
                    a = bufs[i % READS, here, pl.ds(pl.multiple_of((c * STEP + k) * WIDE, WIDE), WIDE)]
                    x = a * value
                    low = jnp.maximum(low, jnp.minimum(top, x))
                    top = jnp.maximum(top, x)
                    seen = seen + a
                    sums = sums + x
                    value = value + 1
                return top, low, seen, sums, value

            zero = jnp.zeros((height, WIDE), bf16)
            top, low, seen, sums, _ = lax.fori_loop(0, chunks // STEP, scan_chunks, (zero,) * 4 + (zero + 1,))
            for n, v in enumerate((top, low, (sums - top) - low, seen)):
                tops[n, pl.ds(pl.multiple_of(first + t * height, height), height), :] = v
            return carry

        lax.fori_loop(0, pieces, scan_rows, 0)

    def pair_step(p, carry):
        for h in range(2):
            scan(2 * p + h, h * BLOCK)
        seen = tops[3]
        crowd = seen[:SUB]
        for k in range(1, 2 * BLOCK // SUB):
            crowd = jnp.maximum(crowd, seen[k * SUB:(k + 1) * SUB])
        crowd = jnp.max(crowd.astype(f32), axis=0, keepdims=True)
        a, b, c = place(tops[0], (none,) * 4), place(tops[1], (none,) * 2), place(tops[2], (none,))
        rest = [jnp.maximum(b[0], c[0]), jnp.minimum(b[0], c[0])]
        rest = [rest[0], jnp.maximum(b[1], rest[1]), jnp.minimum(b[1], rest[1])]
        lists = over_sublanes(sort([a[0]] + [jnp.maximum(a[s + 1], rest[2 - s]) for s in range(3)]))
        lists = jnp.where((crowd > 3) | (degree_of(seen) > 4), FULL, lists)
        even, odd = lists[:, :BLOCK], lists[:, BLOCK:]
        sub = lax.broadcasted_iota(jnp.int32, even.shape, 0)
        mine[p] = jnp.where(sub < 4, even, pltpu.roll(odd, 4, 0))

        @pl.when(p == 1)
        def _():
            await_hello(others)

        @pl.when(p > 0)
        def _():
            send_pair(p - 1)

        return carry

    lax.fori_loop(0, pairs, pair_step, 0)
    own = pltpu.make_async_copy(mine, o_ref.at[pl.ds(me * pairs, pairs)], own_sem)
    send_pair(pairs - 1)
    own.start()
    own.wait()
    for n in range(len(others)):
        send(n, 0, pairs).wait()


def collect(adj_slab, src, graph):
    rows, vertices = adj_slab.shape
    n = src * graph
    mine = (rows // src // (2 * BLOCK), SUB, BLOCK)
    return pl.pallas_call(
        functools.partial(collect_kernel, src, graph),
        in_specs=[pl.BlockSpec(memory_space=pl.ANY)],
        out_specs=pl.BlockSpec(memory_space=pltpu.VMEM),
        out_shape=jax.ShapeDtypeStruct((n * mine[0],) + mine[1:], f32),
        scratch_shapes=[pltpu.VMEM((READS, BLOCK, vertices), bf16), pltpu.VMEM((4, 2 * BLOCK, WIDE), bf16), pltpu.VMEM(mine, f32),
                        pltpu.SemaphoreType.DMA((READS, BLOCK // (4 * SUB))), pltpu.SemaphoreType.DMA,
                        pltpu.SemaphoreType.DMA((n - 1,)), pltpu.SemaphoreType.DMA((n - 1,))],
        compiler_params=pltpu.CompilerParams(collective_id=0, has_side_effects=True, vmem_limit_bytes=40 * 1024 * 1024),
        name="collect",
    )(adj_slab)


def extract_kernel(half_ref, a_ref, o_ref, block, seen, planes, sem):
    vertices = a_ref.shape[1]

    def block_step(i, carry):
        copy = pltpu.make_async_copy(
            a_ref.at[pl.ds(pl.multiple_of((half_ref[0] * o_ref.shape[0] + i) * BLOCK, BLOCK), BLOCK)], block, sem)
        copy.start()
        copy.wait()
        planes[...] = jnp.zeros_like(planes)
        seen[...] = jnp.zeros_like(seen)

        def scan_chunk(c, carry):
            a = block[:, pl.ds(pl.multiple_of(c * WIDE, WIDE), WIDE)]
            seen[...] = seen[...] + a
            x = a.astype(f32) * (c + 1).astype(f32)
            for s in range(DEG):
                top = planes[s].astype(f32)
                planes[s] = jnp.maximum(top, x).astype(bf16)
                x = jnp.minimum(top, x)
            return carry

        lax.fori_loop(0, vertices // WIDE, scan_chunk, 0)
        lists = lax.fori_loop(0, DEG, lambda p, lists: tuple(place(planes[p], lists)), (jnp.zeros((SUB, BLOCK), f32),) * DEG)
        o_ref[i] = jnp.where(degree_of(seen[...]) > DEG, FULL, over_sublanes(list(lists)))
        return carry

    lax.fori_loop(0, o_ref.shape[0], block_step, 0)


def extract(adj_slab, half, rows):
    vertices = adj_slab.shape[1]
    return pl.pallas_call(
        extract_kernel,
        in_specs=[pl.BlockSpec(memory_space=pltpu.SMEM), pl.BlockSpec(memory_space=pl.ANY)],
        out_specs=pl.BlockSpec(memory_space=pltpu.VMEM),
        out_shape=jax.ShapeDtypeStruct((rows // BLOCK, DEG, BLOCK), f32),
        scratch_shapes=[pltpu.VMEM((BLOCK, vertices), bf16), pltpu.VMEM((BLOCK, WIDE), bf16),
                        pltpu.VMEM((DEG, BLOCK, WIDE), bf16), pltpu.SemaphoreType.DMA],
        name="extract",
    )(half, adj_slab)


def along(shape, axis=0):
    return lax.broadcasted_iota(jnp.int32, shape, axis)


def swap(x):
    return pltpu.roll(x, HALF, 1)


def digits(x, base):
    high = jnp.floor(x * (1.0 / base))
    return high, x - high * base


def walk_kernel(which_ref, src_ref, weight_ref, lists_ref, out_ref,
                table, queue, sigma, ratio, delta, cand, ids, now, dest, tail_ref, held, rowhot, colhot, bins,
                ids_a, ids_b, meta, sems, *, levels, vertices, scale, compact):
    pitch = vertices + SUB
    lane = along((SUB, LANES), 1)
    sub = along((SUB, LANES))
    upper = lane >= HALF
    lane_row = along((1, LANES), 1)
    group_odd = ((lane_row // 32) % 2) == 1
    lane32 = lane_row % 32
    rows_all = queue.shape[0]
    tile_bits = (vertices // lists_ref.shape[0]).bit_length() - 1
    high = vertices // WIDE

    def eight(row):
        return pl.ds(pl.multiple_of(row, SUB), SUB)

    def part(n):
        return pl.ds(n * SUB, SUB)

    def spread_row(ref, *index):
        return jnp.broadcast_to(ref[(*index[:-1], pl.ds(index[-1], 1), slice(None))], (SUB, LANES))

    def clear(t, carry):
        for k in range(SUB):
            rows = eight((t * SUB + k) * SUB)
            queue[rows, :] = jnp.full((SUB, LANES), -1.0, f32)
            sigma[rows, :] = jnp.zeros((SUB, LANES), f32)
        return carry

    def fetch(quad, row, buf):
        return pltpu.make_async_copy(ids.at[quad, eight(row)], buf[0], sems.at[buf[1]])

    def name(row, q):
        v = jnp.where(q < 0, vertices, q.astype(jnp.int32))
        ids[0, eight(row), :] = v
        ids[1, eight(row), :] = v + pitch

    bufs = (ids_a, 0), (ids_b, 1)
    clear(0, 0)

    near_source = jnp.full((SUB, LANES), EMPTY, f32)
    source = near_source
    for j in range(HALF):
        v = src_ref[which_ref[0] * HALF + j]
        tile = pltpu.roll(lists_ref[v >> tile_bits], (j - v) & (LANES - 1), 1)
        if compact:
            tile = jnp.where((v & LANES) > 0, pltpu.roll(tile, FEW, 0), tile)
        near_source = jnp.where(lane == j, tile, near_source)
        source = jnp.where(lane % HALF == j, v.astype(f32), source)
    near_source = jnp.where(upper, swap(near_source), near_source)
    reached = near_source >= 0
    if compact:
        reached = reached & (sub < FEW)
    queue[0:1, :] = source[:1]
    queue[eight(SUB), :] = jnp.where(reached, near_source, -1.0)
    sigma[eight(SUB), :] = jnp.where(reached & jnp.logical_not(upper), 1.0, 0.0)
    for n in (1, 2):
        name(n * SUB, queue[eight(n * SUB), :])
    bins[...] = jnp.zeros_like(bins)
    fetch(0, SUB, bufs[0]).start()
    if compact:
        fetch(0, 2 * SUB, bufs[1]).start()
    lax.fori_loop(1, rows_all // (SUB * SUB), clear, 0)

    srow = along((2 * SUB, LANES))
    slane = along((2 * SUB, LANES), 1)

    def fill(halves, target):
        picks = [jnp.where((srow % SUB) == (slane // 32 + FEW * h), jnp.where(srow < SUB, float(LANES), 1.0), 0.0).astype(bf16)
                 for h in halves]

        def body(step, most):
            for k in range(GROUP):
                first = (GROUP * step + k) * SUB
                x = jnp.concatenate([lists_ref[first + n] for n in range(SUB)], axis=1)
                both = jnp.concatenate(digits(x, LANES), axis=0).astype(bf16)
                for h, pick in zip(halves, picks):
                    rows = lax.dot_general(both, pick, (((0,), (0,)), ((), ())), preferred_element_type=f32)
                    for n in range(SUB):
                        table[pl.ds(pl.multiple_of(target(h, first + n), SUB), LANES), :] = rows[n * LANES:(n + 1) * LANES]
                for n in range(SUB):
                    most = jnp.maximum(most, lists_ref[first + n])
            return most

        return lax.fori_loop(0, lists_ref.shape[0] // (GROUP * SUB), body, jnp.full((SUB, LANES), EMPTY, f32))

    table[vertices:pitch, :] = jnp.full((SUB, LANES), EMPTY, f32)
    if compact:
        most = fill(PAIR, lambda h, t: (2 * t + h) * LANES)
        quads = 1
    else:
        table[pitch + vertices:, :] = jnp.full((SUB, LANES), EMPTY, f32)
        most = fill((0,), lambda h, t: t * LANES)
        wide = jnp.max(jnp.where(sub >= FEW, most, EMPTY)) >= 0
        quads = jnp.where(wide, 2, 1)

        @pl.when(wide)
        def _():
            fill((1,), lambda h, t: pitch + t * LANES)

    bad = jnp.max(most) > vertices
    meta[FAULT] = bad.astype(jnp.int32)

    def gather(rows_of_ids):
        acc = [[jnp.full((1, LANES), EMPTY, f32)] * 2 for _ in rows_of_ids]
        for j in range(32):
            hit = lane32 == j
            for i, id_of in enumerate(rows_of_ids):
                for b in PAIR:
                    acc[i][b] = jnp.where(hit, table[pl.ds(id_of(b * 32 + j), 1), :], acc[i][b])
        return [(jnp.where(group_odd, b, a), pltpu.roll(jnp.where(group_odd, a, b), LANES - 32, 1)) for a, b in acc]

    def gather_slots(ids_s, slots=SLOTS):
        return gather([functools.partial(lambda i, j: ids_s[i, j], i) for i in range(slots)])

    def keep(rows, quad, row):
        for i, pair in enumerate(rows):
            for h in PAIR:
                cand[2 * quad + h, pl.ds(row + i, 1), :] = pair[h]

    def flag(x):
        return jnp.where(x, 1, 0)

    def at(unit, origin):
        return unit & (quads - 1), origin + (unit >> (quads - 1)) * SUB

    def level_step(level, carry):
        base, count = meta[BASE, level], meta[COUNT, level]
        following = base + (count + 7) // SUB * SUB
        batches = jnp.where(following <= CAP, (count + SLOTS - 1) // SLOTS, 0)
        units = batches * quads
        parity = meta[PARITY]

        def on_parity(n, f):
            for k in PAIR:
                @pl.when(n & 1 == k)
                def _():
                    f(bufs[k], bufs[1 - k])

        def unit_step(unit, other, to):
            quad, row = at(unit, base)
            x = [cand[2 * quad + h, eight(row), :] for h in PAIR]

            def search(first, count, marks):
                marks = list(marks)
                for k in range(count):
                    q = spread_row(queue, first + k)
                    for h in PAIR:
                        n = 2 * h + k % 2
                        marks[n] = jnp.where(x[h] == q, 1, marks[n])
                return tuple(marks)

            reach = following + meta[LENGTH] - PEEL
            marks = lax.fori_loop(0, (reach + SCAN - 1) // SCAN, lambda t, m: search(PEEL + t * SCAN, SCAN, m),
                                  (jnp.zeros((SUB, LANES), jnp.int32),) * 4)
            ahead = unit + 1 < units
            final_unit = unit + 1 == units
            soon = jnp.logical_and(final_unit, meta[AWAIT0] > 0)

            @pl.when(jnp.logical_or(ahead, soon))
            def _():
                fetch(0, base, to).wait()

            def insert(g):
                slots = [eight(following + g * WINDOW + SUB * t) for t in range(WINDOW // SUB)]
                qs = [queue[r, :] for r in slots]
                ss = [sigma[r, :] for r in slots]
                pos = [sub + (g * WINDOW + SUB * t) for t in range(WINDOW // SUB)]
                for h in PAIR:
                    for i in range(SUB):
                        d, e = spread_row(dest, SUB * h + i), spread_row(dest, SUB * (h + 2) + i)
                        v, w = spread_row(now, SUB * h + i), spread_row(now, SUB * (h + 2) + i)
                        for t in range(WINDOW // SUB):
                            qs[t] = jnp.where(pos[t] == d, v, jnp.where(pos[t] == e, w, qs[t]))
                for i in range(SUB):
                    v, w, sig = (spread_row(now, SUB * n + i) for n in (0, 1, 4))
                    for t in range(WINDOW // SUB):
                        ss[t] = ss[t] + jnp.where((qs[t] == v) | (qs[t] == w), sig, 0.0)
                for t, r in enumerate(slots):
                    queue[r, :] = qs[t]
                    sigma[r, :] = ss[t]
                return qs

            def core(looking):
                even, odd = x
                m, n, k, l = search(0, PEEL, marks)
                near_even, near_odd = m | n | flag(even < 0), k | l | flag(odd < 0)

                xr = [swap(v) for v in x]
                turns = [[[pltpu.roll(v, s, 0) if s else v for v in (x[h], xr[h])] for s in range(SUB)] for h in PAIR]
                for s, ((a, b), (c, d)) in enumerate(zip(*turns)):
                    near_odd = jnp.where((odd == a) | (odd == b), 1, near_odd)
                    if s:
                        after = sub >= s
                        near_even = jnp.where(((even == a) | (even == b)) & after, 1, near_even)
                        near_odd = jnp.where(((odd == c) | (odd == d)) & after, 1, near_odd)

                new = [1 - near_even, 1 - near_odd]
                packed = new[0] + BYTE * new[1]
                across = swap(packed)
                far = [across & (BYTE - 1), across >> SUB]
                both = packed + across
                run, whole = both, both
                for s in (1, 2, 4):
                    run = run + jnp.where(sub >= s, pltpu.roll(run, s, 0), 0)
                    whole = whole + pltpu.roll(whole, s, 0)
                run = run - both
                tail = tail_ref[...]
                evens = whole & (BYTE - 1)
                begin = [tail + (run & (BYTE - 1)), tail + evens + (run >> SUB)]
                for h in PAIR:
                    dest[part(h), :] = jnp.where(new[h] > 0, begin[h] + jnp.where(upper, far[h], 0), -1)
                    dest[part(h + 2), :] = jnp.where(far[h] > 0, begin[h] + jnp.where(upper, 0, new[h]), -1)
                    now[part(h), :] = x[h]
                    now[part(h + 2), :] = xr[h]
                now[part(4), :] = sigma[eight(row), :] + swap(sigma[eight(row), :])
                tail = tail + evens + (whole >> SUB)
                tail_ref[...] = tail
                passed = SLOTS * ((unit + 1) >> (quads - 1))
                second = SUB + SUB * (1 >> (quads - 1))
                need = jnp.where(sub == 1, SUB, second)
                short = (tail < need) & (held[...] > passed)
                most = jnp.max(jnp.where(sub == 0, tail, flag(short)).astype(f32), axis=1, keepdims=True)
                meta[REACHED] = most[0, 0].astype(jnp.int32)
                for n in PAIR:
                    meta[(SHORT0, SHORT1)[n]] = most[n + 1, 0].astype(jnp.int32)

                if looking:
                    quad2, row2 = at(unit + 1, base)
                    rows = gather_slots(to[0])
                qs = insert(0)
                for n in PAIR:
                    name(following + n * SUB, qs[n])
                if looking:
                    keep(rows, jnp.where(ahead, quad2, 0), jnp.where(ahead, row2, following))

            look = jnp.logical_or(ahead, soon)
            for looking in PAIR:
                @pl.when(look == (looking > 0))
                def _():
                    core(looking)

            length = meta[REACHED]
            ready = [meta[n] == 0 for n in (SHORT0, SHORT1)]

            @pl.when(unit + 3 < units)
            def _():
                fetch(*at(unit + 3, base), to).start()

            @pl.when(soon)
            def _():
                meta[GOT] = 1

            def first_of_next(n, when, buf):
                @pl.when(jnp.logical_and(when, meta[(AWAIT0, AWAIT1)[n]] == 0))
                def _():
                    fetch(*at(n, following), buf).start()
                    meta[(AWAIT0, AWAIT1)[n]] = 1

            first_of_next(0, jnp.logical_and(ready[0], unit + 3 == units), to)
            first_of_next(0, jnp.logical_and(ready[0], unit + 2 == units), other)
            first_of_next(1, jnp.logical_and(ready[1], unit + 2 == units), to)
            first_of_next(0, final_unit, to)
            first_of_next(1, final_unit, other)

            groups = (length + WINDOW - 1) // WINDOW
            fits = following + groups * WINDOW <= CAP + WINDOW
            meta[LENGTH] = jnp.where(fits, length, 0)

            @pl.when(jnp.logical_not(fits))
            def _():
                meta[FAULT] = 1

            def more(g, carry):
                insert(g)
                return carry

            lax.fori_loop(1, jnp.where(fits, groups, 0), more, 0)

        tail_ref[...] = jnp.zeros_like(tail_ref)
        meta[LENGTH] = 0

        def open_level(mine, other):
            @pl.when(jnp.logical_and(meta[GOT] == 0, meta[AWAIT0] > 0))
            def _():
                fetch(0, base, mine).wait()
                keep(gather_slots(mine[0]), 0, base)

            @pl.when(jnp.logical_and(units < 2, meta[AWAIT1] > 0))
            def _():
                fetch(0, base, other).wait()

            @pl.when(units > 2)
            def _():
                fetch(*at(2, base), mine).start()

        on_parity(parity, open_level)
        for place_ in (GOT, AWAIT0, AWAIT1):
            meta[place_] = 0

        def any_unit(unit, carry):
            on_parity(parity + unit, functools.partial(unit_step, unit))
            return carry

        lax.fori_loop(0, units, any_unit, 0)
        meta[PARITY] = parity + units

        @pl.when(following > CAP)
        def _():
            meta[FAULT] = 1

        found = jnp.where(meta[FAULT] == 0, meta[LENGTH], 0)
        meta[BASE, level + 1] = following
        meta[COUNT, level + 1] = found

        def names(t, carry):
            row = following + t * SUB
            name(row, queue[eight(row), :])
            return carry

        lax.fori_loop(2, (found + SUB - 1) // SUB, names, 0)
        held[...] = tail_ref[...]
        return carry

    for place_ in (GOT, PARITY):
        meta[place_] = 0

    @pl.when(jnp.logical_not(bad))
    def _():
        held[...] = jnp.full_like(held, FEW * quads)
        meta[BASE, 1] = SUB
        meta[COUNT, 1] = FEW * quads
        fetch(0, SUB, bufs[0]).wait()
        if compact:
            for h in PAIR:
                cand[h, eight(SUB), :] = jnp.full((SUB, LANES), EMPTY, f32)
        else:
            fetch(*at(1, SUB), bufs[1]).start()
        keep(gather_slots(ids_a, FEW if compact else SLOTS), 0, SUB)
        meta[GOT] = 1
        meta[AWAIT0] = 0
        meta[AWAIT1] = 1
        lax.fori_loop(1, levels, level_step, 0)

    @pl.when(bad)
    def _():
        fetch(0, SUB, bufs[0]).wait()
        meta[AWAIT0] = 0
        meta[AWAIT1] = int(compact)

    def drain(n, buf):
        @pl.when(meta[(AWAIT0, AWAIT1)[n]] > 0)
        def _():
            fetch(0, 0, buf).wait()

    for k in PAIR:
        @pl.when(meta[PARITY] & 1 == k)
        def _():
            @pl.when(meta[GOT] == 0)
            def _():
                drain(0, bufs[k])

            drain(1, bufs[1 - k])

    good = meta[FAULT] == 0

    @pl.when(good)
    def _():
        last = meta[BASE, levels]
        g_last = weight_ref[levels - 2]

        def seed(g, carry):
            for t in range(WINDOW // SUB):
                r = eight(last + g * WINDOW + SUB * t)
                s = sigma[r, :] + swap(sigma[r, :])
                ratio[r, :] = jnp.where(s > 0, g_last / jnp.where(s > 0, s, 1.0), 0.0)
            return carry

        lax.fori_loop(0, (meta[COUNT, levels] + WINDOW - 1) // WINDOW, seed, 0)

        def back_step(k, carry):
            level = levels - 1 - k
            base, count = meta[BASE, level], meta[COUNT, level]
            nbase, ncount = meta[BASE, level + 1], meta[COUNT, level + 1]
            g_here = weight_ref[jnp.maximum(level - 2, 0)]

            def pull_batch(bt, carry):
                here = eight(base + bt * SLOTS)

                def pull(quad, c, acc):
                    even, odd = cand[2 * quad, here, :], cand[2 * quad + 1, here, :]
                    acc = list(acc)
                    for n in range(WINDOW):
                        q = spread_row(queue, nbase + c * WINDOW + n)
                        w = spread_row(ratio, nbase + c * WINDOW + n)
                        acc[n % 2] = acc[n % 2] + jnp.where((even == q) | (odd == q), w, 0.0)
                    return tuple(acc)

                def pull_quad(quad, acc):
                    return lax.fori_loop(1, (ncount + WINDOW - 1) // WINDOW, functools.partial(pull, quad), pull(quad, 0, acc))

                acc = pull_quad(0, (jnp.zeros((SUB, LANES), f32),) * 2)
                if not compact:
                    acc = lax.fori_loop(1, quads, pull_quad, acc)
                delta[here, :] = acc[0] + acc[1]
                return carry

            lax.fori_loop(0, (count + SLOTS - 1) // SLOTS, pull_batch, 0)

            def finish(g, carry):
                slots = [eight(base + g * WINDOW + SUB * t) for t in range(WINDOW // SUB)]
                for t, r in enumerate(slots):
                    inside = g * WINDOW + SUB * t < count
                    part, s = (v + swap(v) for v in (delta[r, :], sigma[r, :]))
                    d = s * part
                    w = jnp.where(s > 0, (g_here + d) / jnp.where(s > 0, s, 1.0), 0.0)
                    delta[r, :] = jnp.where(inside, d, delta[r, :])
                    ratio[r, :] = jnp.where(inside, w, ratio[r, :])
                return carry

            lax.fori_loop(0, (count + WINDOW - 1) // WINDOW, finish, 0)
            return carry

        lax.fori_loop(0, levels - 1, back_step, 0)

        tall = along((WIDE, WIDE)).astype(f32).astype(bf16)
        zero = jnp.zeros((WIDE, WIDE), bf16)
        one = zero + 1
        start = meta[BASE, 1]

        def tally(t, carry):
            for u in range(TALLY // 16):
                a, b = eight(start + t * TALLY + u * 16), eight(start + t * TALLY + u * 16 + SUB)
                v = jnp.where(upper, queue[b, :], queue[a, :])
                d = jnp.where(upper, delta[b, :], delta[a, :])
                hi, lo = digits(v, WIDE)
                d_hi = d.astype(bf16).astype(f32)
                d_mid = (d - d_hi).astype(bf16).astype(f32)
                d_lo = d - d_hi - d_mid
                for p in range(0, SUB, 2):
                    cols = slice((u * SUB + p) * LANES, (u * SUB + p + 2) * LANES)

                    def pair(x):
                        return jnp.concatenate([x[p:p + 1], x[p + 1:p + 2]], axis=1).astype(bf16)

                    colhot[:, cols] = jnp.where(tall == pair(lo), one, zero)
                    match = tall[:high] == pair(hi)
                    for n, x in enumerate((d_hi, d_mid, d_lo)):
                        rowhot[n * high:(n + 1) * high, cols] = jnp.where(match, pair(x), zero[:high])
            bins[...] += lax.dot_general(rowhot[...], colhot[...], TURN, preferred_element_type=f32)
            return carry

        for t in range(TALLY // SUB):
            delta[eight(last + t * SUB), :] = jnp.zeros((SUB, LANES), f32)
        lax.fori_loop(0, (last - start + TALLY - 1) // TALLY, tally, 0)

    blocks = out_ref.shape[0]
    per = high // blocks
    total = (bins[:high] + bins[high:2 * high] + bins[2 * high:]) * scale
    fault = jnp.where(good, 0.0, 1.0)
    for b in range(blocks):
        for n in PAIR:
            out_ref[b, n * per:(n + 1) * per, :] = total[b * per:(b + 1) * per, n * LANES:(n + 1) * LANES]
        out_ref[b, 2 * per:, :] = jnp.full((SUB, LANES), fault, f32)


def walk(which, sources, weights, lists, *, blocks, vertices, scale, compact):
    levels = weights.shape[0] + 1
    rows = CAP + 4 * WINDOW
    high = LANES // blocks + SUB
    vm = pltpu.VMEM
    queue = vm((rows, LANES), f32)
    parts = 3 * (vertices // WIDE)
    return pl.pallas_call(
        functools.partial(walk_kernel, levels=levels, vertices=vertices, scale=scale, compact=compact),
        in_specs=[pl.BlockSpec(memory_space=pltpu.SMEM)] * 3 + [pl.BlockSpec(memory_space=pltpu.VMEM)],
        out_specs=pl.BlockSpec(memory_space=pltpu.VMEM),
        out_shape=jax.ShapeDtypeStruct((blocks, high, LANES), f32),
        scratch_shapes=[
            vm(((1 if compact else 2) * (vertices + SUB), LANES), f32), queue, queue, queue, queue,
            vm((4, rows, LANES), f32), vm((2, rows, LANES), jnp.int32),
            vm((40, LANES), f32), vm((32, LANES), jnp.int32), vm((SUB, LANES), jnp.int32), vm((SUB, LANES), jnp.int32),
            vm((parts, TALLY // 2 * LANES), bf16), vm((WIDE, TALLY // 2 * LANES), bf16), vm((parts, WIDE), f32),
            pltpu.SMEM((SLOTS, LANES), jnp.int32), pltpu.SMEM((SLOTS, LANES), jnp.int32), pltpu.SMEM((3, 16), jnp.int32),
            pltpu.SemaphoreType.DMA((2,)),
        ],
        compiler_params=pltpu.CompilerParams(
            vmem_limit_bytes=48 * 1024 * 1024),
        name="walk",
    )(which, sources, weights, lists)


def share_kernel(src, graph, x_ref, o_ref, own_sem, send_sem, recv_sem):
    mine, g, others = place_and_others(src, graph)
    hello(others)
    await_hello(others)
    own = pltpu.make_async_copy(x_ref, o_ref.at[mine], own_sem)
    own.start()
    copies = []
    for n, (py, pg) in enumerate(others):
        copies.append(pltpu.make_async_remote_copy(
            src_ref=x_ref, dst_ref=o_ref.at[mine], send_sem=send_sem.at[n], recv_sem=recv_sem.at[n],
            device_id={"src": py, "graph": pg}, device_id_type=MESH))
        copies[-1].start()
    own.wait()
    for c in copies:
        c.wait()


def share(x, src, graph):
    n = src * graph
    return pl.pallas_call(
        functools.partial(share_kernel, src, graph),
        in_specs=[pl.BlockSpec(memory_space=pltpu.VMEM)],
        out_specs=pl.BlockSpec(memory_space=pltpu.VMEM),
        out_shape=jax.ShapeDtypeStruct((n,) + x.shape, x.dtype),
        scratch_shapes=[pltpu.SemaphoreType.DMA, pltpu.SemaphoreType.DMA((n - 1,)), pltpu.SemaphoreType.DMA((n - 1,))],
        compiler_params=pltpu.CompilerParams(collective_id=2, has_side_effects=True),
        name="share",
    )(x)


def total_kernel(src, graph, x_ref, o_ref, got, own_sem, send_sem, recv_sem):
    mine, g, others = place_and_others(src, graph)
    hello(others)
    own = pltpu.make_async_copy(x_ref.at[g], got.at[mine], own_sem)
    own.start()
    await_hello(others)
    copies = []
    for n, (py, pg) in enumerate(others):
        copies.append(pltpu.make_async_remote_copy(
            src_ref=x_ref.at[pg], dst_ref=got.at[mine], send_sem=send_sem.at[n], recv_sem=recv_sem.at[n],
            device_id={"src": py, "graph": pg}, device_id_type=MESH))
        copies[-1].start()
    own.wait()
    for c in copies:
        c.wait()
    acc = got[0]
    for n in range(1, src * graph):
        acc = acc + got[n]
    o_ref[...] = acc


def total(x, src, graph, collective_id):
    n = src * graph
    return pl.pallas_call(
        functools.partial(total_kernel, src, graph),
        in_specs=[pl.BlockSpec(memory_space=pltpu.VMEM)],
        out_specs=pl.BlockSpec(memory_space=pltpu.VMEM),
        out_shape=jax.ShapeDtypeStruct(x.shape[1:], x.dtype),
        scratch_shapes=[pltpu.VMEM((n,) + x.shape[1:], x.dtype), pltpu.SemaphoreType.DMA,
                        pltpu.SemaphoreType.DMA((n - 1,)), pltpu.SemaphoreType.DMA((n - 1,))],
        compiler_params=pltpu.CompilerParams(collective_id=collective_id, has_side_effects=True),
        name="total",
    )(pltpu.with_memory_space_constraint(x, pltpu.VMEM))


def exchange(x, axis):
    return lax.all_to_all(x, axis, 0, 0)


def dense(adj_slab, src_local, level_weight, src, graph):
    slab_rows, vertex_count = adj_slab.shape
    src_count = src_local.shape[0]
    levels = level_weight.shape[0] + 1
    row_start = lax.axis_index("graph") * slab_rows
    vertex_ids = row_start + lax.broadcasted_iota(jnp.int32, (slab_rows, 1), 0)
    first = jnp.where(vertex_ids == src_local[None, :], 1.0, 0.0).astype(f32)

    def forward(carry, unused):
        sigma, seen = carry
        partial = jnp.einsum("uv,us->vs", adj_slab, sigma, preferred_element_type=f32, precision=exact_precision)
        parts = exchange(partial.reshape(graph, slab_rows, src_count), "graph")
        sigma = jnp.sum(parts, axis=0) * (1.0 - seen)
        seen = jnp.maximum(seen, jnp.where(sigma > 0, 1.0, 0.0))
        return (sigma, seen), sigma

    _, sigmas = lax.scan(forward, (first, first), None, length=levels)

    def backward(carry, xs):
        delta, acc = carry
        upper, lower, weight = xs
        reached = upper > 0
        ratio = jnp.where(reached, (weight + delta) / jnp.where(reached, upper, 1.0), 0.0)
        gathered = exchange(jnp.broadcast_to(ratio[None], (graph,) + ratio.shape), "graph")
        pulled = jnp.einsum("uv,vs->us", adj_slab, gathered.reshape(vertex_count, src_count),
                            preferred_element_type=f32, precision=exact_precision)
        delta = lower * pulled
        return (delta, acc + delta), None

    zero = jnp.zeros_like(first)
    (_, acc), _ = lax.scan(backward, (zero, zero), (sigmas[1:][::-1], sigmas[:-1][::-1], level_weight[::-1]))
    scale = vertex_count / (src_count * src * levels ** 3)
    mine = jnp.sum(acc, axis=1) * scale
    both = exchange(jnp.broadcast_to(mine.reshape(1, -1, LANES), (src, slab_rows // LANES, LANES)), "src")
    return jnp.sum(both, axis=0).reshape(slab_rows)


def solution(mesh):
    src, graph = mesh.shape["src"], mesh.shape["graph"]

    def device_program(adj_slab, src_local, level_weight):
        slab_rows, vertex_count = adj_slab.shape
        levels = level_weight.shape[0] + 1
        scale = vertex_count / (HALF * src * graph * levels ** 3)
        which = lax.axis_index("graph").astype(jnp.int32).reshape(1)

        def finish(lists, compact, collective_id, other):
            parts = walk(which, src_local, level_weight, lists, blocks=graph, vertices=vertex_count, scale=scale, compact=compact)
            summed = total(parts, src, graph, collective_id)
            rows = slab_rows // LANES

            def plain():
                return summed[:rows].reshape(2, -1, LANES).transpose(1, 0, 2).reshape(slab_rows)

            return lax.cond(summed[rows, 0] > 0, other, plain)

        def dense_path():
            return dense(adj_slab, src_local, level_weight, src, graph)

        def general_path():
            half = lax.axis_index("src").astype(jnp.int32).reshape(1)
            lists = share(extract(adj_slab, half, slab_rows // src), src, graph)
            return finish(lists.reshape(-1, SUB, LANES), False, 3, dense_path)

        return finish(collect(adj_slab, src, graph), True, 1, general_path)

    return jax.shard_map(device_program, mesh=mesh,
                         in_specs=(P(("batch", "graph"), None), P(("batch", "src")), P(None)),
                         out_specs=P(("batch", "graph")), check_vma=False)
```

```python
import functools

import jax
import jax.numpy as jnp
from jax import lax
from jax.experimental import pallas as pl
from jax.experimental.pallas import tpu as pltpu
from jax.sharding import PartitionSpec as P

MESH = pl.DeviceIdType.MESH
exact_precision = lax.Precision.HIGHEST
f32, bf16 = jnp.float32, jnp.bfloat16

LANES, SUB = 128, 8
WIDE = 256
DEG, FEW = 8, 4
EMPTY = -2.0
FULL = 32767.0
TURN = (((1,), (1,)), ((), ()))
BLOCK = 128
READS = 4
STEP = 32
HALF = 64
SLOTS = 8
WINDOW = 48
SCAN = 32
CAP = 1024
TALLY = 96
PAIR = (0, 1)
BYTE = 256
GROUP = 8
PEEL = 32
BASE, COUNT = 0, 1
FAULT, LENGTH, GOT, PARITY, AWAIT0, AWAIT1, REACHED, SHORT0, SHORT1 = ((2, n) for n in range(9))


def place_and_others(src, graph):
    y, g = lax.axis_index("src"), lax.axis_index("graph")
    steps = sorted(((i, k) for i in range(src) for k in range(graph)), key=lambda s: (-s[0], abs(s[1] - graph // 2)))
    return g * src + y, g, [((y + i) % src, (g + k) % graph) for i, k in steps if i + k]


def hello(peers):
    for y, g in peers:
        pl.semaphore_signal(pltpu.get_barrier_semaphore(), inc=1, device_id={"src": y, "graph": g}, device_id_type=MESH)


def await_hello(peers):
    pl.semaphore_wait(pltpu.get_barrier_semaphore(), len(peers))


def place(plane, lists):
    lists = list(lists)
    row_i = lax.broadcasted_iota(jnp.int32, (WIDE, WIDE), 0)
    col_i = lax.broadcasted_iota(jnp.int32, (WIDE, WIDE), 1)
    eye = jnp.where(row_i == col_i, float(WIDE), 0.0).astype(bf16)
    flipped = lax.dot_general(eye, plane, TURN, preferred_element_type=f32)
    lane_id = lax.broadcasted_iota(jnp.int32, (SUB, flipped.shape[1]), 0).astype(f32)
    for g in range(WIDE // SUB):
        x = flipped[g * SUB:(g + 1) * SUB] + (lane_id + float(g * SUB))
        for s in range(len(lists)):
            hi = jnp.maximum(lists[s], x)
            if s < len(lists) - 1:
                x = jnp.minimum(lists[s], x)
            lists[s] = hi
    return lists


def sort(lists):
    gap = len(lists) // 2
    while gap:
        for s in range(len(lists)):
            if not s & gap:
                lists[s], lists[s + gap] = jnp.maximum(lists[s], lists[s + gap]), jnp.minimum(lists[s], lists[s + gap])
        gap //= 2
    return lists


def over_sublanes(lists):
    size = len(lists)
    for shift in (4, 2, 1):
        other = [pltpu.roll(v, shift, 0) for v in lists]
        lists = sort([jnp.maximum(lists[s], other[size - 1 - s]) for s in range(size)])
    out = jnp.full(lists[0].shape, EMPTY, f32)
    sub = lax.broadcasted_iota(jnp.int32, out.shape, 0)
    for s in range(size):
        out = jnp.where(sub == s, jnp.where(lists[s] >= WIDE, lists[s] - WIDE, EMPTY), out)
    return out


def degree_of(seen):
    return lax.dot_general(jnp.ones((SUB, WIDE), bf16), seen, TURN, preferred_element_type=f32)


def collect_kernel(src, graph, a_ref, o_ref, bufs, tops, mine, sems, own_sem, send_sems, recv_sems):
    vertices = a_ref.shape[1]
    pairs, chunks = mine.shape[0], vertices // WIDE
    blocks = 2 * pairs
    me, _, others = place_and_others(src, graph)
    y = me % src
    height = 4 * SUB
    pieces = BLOCK // height

    def fetch(i, t):
        rows = pl.ds(pl.multiple_of((y * blocks + i) * BLOCK + t * height, height), height)
        here = pl.ds(pl.multiple_of(t * height, height), height)
        return pltpu.make_async_copy(a_ref.at[rows], bufs.at[i % READS, here], sems.at[i % READS, t])

    def send(n, first, count):
        py, pg = others[n]
        return pltpu.make_async_remote_copy(
            src_ref=mine.at[pl.ds(first, count)], dst_ref=o_ref.at[pl.ds(me * pairs + first, count)],
            send_sem=send_sems.at[n], recv_sem=recv_sems.at[n], device_id={"src": py, "graph": pg}, device_id_type=MESH)

    def send_pair(p):
        for n in range(len(others)):
            send(n, p, 1).start()

    for i in range(READS - 1):
        for t in range(pieces):
            fetch(i, t).start()
    hello(others)
    none = jnp.zeros((SUB, 2 * BLOCK), f32)

    def scan(i, first):
        @pl.when(i + READS - 1 < blocks)
        def _():
            for t in range(pieces):
                fetch(i + READS - 1, t).start()

        def scan_rows(t, carry):
            fetch(i, t).wait()
            here = pl.ds(pl.multiple_of(t * height, height), height)

            def scan_chunks(c, state):
                top, low, seen, sums, value = state
                for k in range(STEP):
                    a = bufs[i % READS, here, pl.ds(pl.multiple_of((c * STEP + k) * WIDE, WIDE), WIDE)]
                    x = a * value
                    low = jnp.maximum(low, jnp.minimum(top, x))
                    top = jnp.maximum(top, x)
                    seen = seen + a
                    sums = sums + x
                    value = value + 1
                return top, low, seen, sums, value

            zero = jnp.zeros((height, WIDE), bf16)
            top, low, seen, sums, _ = lax.fori_loop(0, chunks // STEP, scan_chunks, (zero,) * 4 + (zero + 1,))
            for n, v in enumerate((top, low, (sums - top) - low, seen)):
                tops[n, pl.ds(pl.multiple_of(first + t * height, height), height), :] = v
            return carry

        lax.fori_loop(0, pieces, scan_rows, 0)

    def pair_step(p, carry):
        for h in range(2):
            scan(2 * p + h, h * BLOCK)
        seen = tops[3]
        crowd = seen[:SUB]
        for k in range(1, 2 * BLOCK // SUB):
            crowd = jnp.maximum(crowd, seen[k * SUB:(k + 1) * SUB])
        crowd = jnp.max(crowd.astype(f32), axis=0, keepdims=True)
        a, b, c = place(tops[0], (none,) * 4), place(tops[1], (none,) * 2), place(tops[2], (none,))
        rest = [jnp.maximum(b[0], c[0]), jnp.minimum(b[0], c[0])]
        rest = [rest[0], jnp.maximum(b[1], rest[1]), jnp.minimum(b[1], rest[1])]
        lists = over_sublanes(sort([a[0]] + [jnp.maximum(a[s + 1], rest[2 - s]) for s in range(3)]))
        lists = jnp.where((crowd > 3) | (degree_of(seen) > 4), FULL, lists)
        even, odd = lists[:, :BLOCK], lists[:, BLOCK:]
        sub = lax.broadcasted_iota(jnp.int32, even.shape, 0)
        mine[p] = jnp.where(sub < 4, even, pltpu.roll(odd, 4, 0))

        @pl.when(p == 1)
        def _():
            await_hello(others)

        @pl.when(p > 0)
        def _():
            send_pair(p - 1)

        return carry

    lax.fori_loop(0, pairs, pair_step, 0)
    own = pltpu.make_async_copy(mine, o_ref.at[pl.ds(me * pairs, pairs)], own_sem)
    send_pair(pairs - 1)
    own.start()
    own.wait()
    for n in range(len(others)):
        send(n, 0, pairs).wait()


def collect(adj_slab, src, graph):
    rows, vertices = adj_slab.shape
    n = src * graph
    mine = (rows // src // (2 * BLOCK), SUB, BLOCK)
    return pl.pallas_call(
        functools.partial(collect_kernel, src, graph),
        in_specs=[pl.BlockSpec(memory_space=pl.ANY)],
        out_specs=pl.BlockSpec(memory_space=pltpu.VMEM),
        out_shape=jax.ShapeDtypeStruct((n * mine[0],) + mine[1:], f32),
        scratch_shapes=[pltpu.VMEM((READS, BLOCK, vertices), bf16), pltpu.VMEM((4, 2 * BLOCK, WIDE), bf16), pltpu.VMEM(mine, f32),
                        pltpu.SemaphoreType.DMA((READS, BLOCK // (4 * SUB))), pltpu.SemaphoreType.DMA,
                        pltpu.SemaphoreType.DMA((n - 1,)), pltpu.SemaphoreType.DMA((n - 1,))],
        compiler_params=pltpu.CompilerParams(collective_id=0, has_side_effects=True, vmem_limit_bytes=40 * 1024 * 1024),
        name="collect",
    )(adj_slab)


def extract_kernel(half_ref, a_ref, o_ref, block, seen, planes, sem):
    vertices = a_ref.shape[1]

    def block_step(i, carry):
        copy = pltpu.make_async_copy(
            a_ref.at[pl.ds(pl.multiple_of((half_ref[0] * o_ref.shape[0] + i) * BLOCK, BLOCK), BLOCK)], block, sem)
        copy.start()
        copy.wait()
        planes[...] = jnp.zeros_like(planes)
        seen[...] = jnp.zeros_like(seen)

        def scan_chunk(c, carry):
            a = block[:, pl.ds(pl.multiple_of(c * WIDE, WIDE), WIDE)]
            seen[...] = seen[...] + a
            x = a.astype(f32) * (c + 1).astype(f32)
            for s in range(DEG):
                top = planes[s].astype(f32)
                planes[s] = jnp.maximum(top, x).astype(bf16)
                x = jnp.minimum(top, x)
            return carry

        lax.fori_loop(0, vertices // WIDE, scan_chunk, 0)
        lists = lax.fori_loop(0, DEG, lambda p, lists: tuple(place(planes[p], lists)), (jnp.zeros((SUB, BLOCK), f32),) * DEG)
        o_ref[i] = jnp.where(degree_of(seen[...]) > DEG, FULL, over_sublanes(list(lists)))
        return carry

    lax.fori_loop(0, o_ref.shape[0], block_step, 0)


def extract(adj_slab, half, rows):
    vertices = adj_slab.shape[1]
    return pl.pallas_call(
        extract_kernel,
        in_specs=[pl.BlockSpec(memory_space=pltpu.SMEM), pl.BlockSpec(memory_space=pl.ANY)],
        out_specs=pl.BlockSpec(memory_space=pltpu.VMEM),
        out_shape=jax.ShapeDtypeStruct((rows // BLOCK, DEG, BLOCK), f32),
        scratch_shapes=[pltpu.VMEM((BLOCK, vertices), bf16), pltpu.VMEM((BLOCK, WIDE), bf16),
                        pltpu.VMEM((DEG, BLOCK, WIDE), bf16), pltpu.SemaphoreType.DMA],
        name="extract",
    )(half, adj_slab)


def along(shape, axis=0):
    return lax.broadcasted_iota(jnp.int32, shape, axis)


def swap(x):
    return pltpu.roll(x, HALF, 1)


def digits(x, base):
    high = jnp.floor(x * (1.0 / base))
    return high, x - high * base


def walk_kernel(which_ref, src_ref, weight_ref, lists_ref, out_ref,
                table, queue, sigma, ratio, delta, cand, ids, now, dest, tail_ref, held, rowhot, colhot, bins,
                ids_a, ids_b, meta, sems, *, levels, vertices, scale, compact):
    pitch = vertices + SUB
    lane = along((SUB, LANES), 1)
    sub = along((SUB, LANES))
    upper = lane >= HALF
    lane_row = along((1, LANES), 1)
    group_odd = ((lane_row // 32) % 2) == 1
    lane32 = lane_row % 32
    rows_all = queue.shape[0]
    tile_bits = (vertices // lists_ref.shape[0]).bit_length() - 1
    high = vertices // WIDE

    def eight(row):
        return pl.ds(pl.multiple_of(row, SUB), SUB)

    def part(n):
        return pl.ds(n * SUB, SUB)

    def spread_row(ref, *index):
        return jnp.broadcast_to(ref[(*index[:-1], pl.ds(index[-1], 1), slice(None))], (SUB, LANES))

    def clear(t, carry):
        for k in range(SUB):
            rows = eight((t * SUB + k) * SUB)
            queue[rows, :] = jnp.full((SUB, LANES), -1.0, f32)
            sigma[rows, :] = jnp.zeros((SUB, LANES), f32)
        return carry

    def fetch(quad, row, buf):
        return pltpu.make_async_copy(ids.at[quad, eight(row)], buf[0], sems.at[buf[1]])

    def name(row, q):
        v = jnp.where(q < 0, vertices, q.astype(jnp.int32))
        ids[0, eight(row), :] = v
        if not compact:
            ids[1, eight(row), :] = v + pitch

    bufs = (ids_a, 0), (ids_b, 1)
    clear(0, 0)

    near_source = jnp.full((SUB, LANES), EMPTY, f32)
    source = along((SUB, LANES))
    for j in range(HALF):
        v = src_ref[which_ref[0] * HALF + j]
        near_source = jnp.where(lane == j, pltpu.roll(lists_ref[v >> tile_bits], (j - v) & (LANES - 1), 1), near_source)
        source = jnp.where(lane % HALF == j, v, source)
    if compact:
        near_source = jnp.where((source & LANES) > 0, pltpu.roll(near_source, FEW, 0), near_source)
    near_source = jnp.where(upper, swap(near_source), near_source)
    reached = near_source >= 0
    if compact:
        reached = reached & (sub < FEW)
    queue[0:1, :] = source[:1].astype(f32)
    queue[eight(SUB), :] = jnp.where(reached, near_source, -1.0)
    sigma[eight(SUB), :] = jnp.where(reached & jnp.logical_not(upper), 1.0, 0.0)
    for n in (1, 2):
        name(n * SUB, queue[eight(n * SUB), :])
    bins[...] = jnp.zeros_like(bins)
    fetch(0, SUB, bufs[0]).start()
    if compact:
        fetch(0, 2 * SUB, bufs[1]).start()
    lax.fori_loop(1, rows_all // (SUB * SUB), clear, 0)

    srow = along((2 * SUB, LANES))
    slane = along((2 * SUB, LANES), 1)

    def fill(halves, target):
        picks = [jnp.where((srow % SUB) == (slane // 32 + FEW * h), jnp.where(srow < SUB, float(LANES), 1.0), 0.0).astype(bf16)
                 for h in halves]

        def body(step, most):
            for k in range(GROUP):
                first = (GROUP * step + k) * SUB
                x = jnp.concatenate([lists_ref[first + n] for n in range(SUB)], axis=1)
                both = jnp.concatenate(digits(x, LANES), axis=0).astype(bf16)
                for h, pick in zip(halves, picks):
                    rows = lax.dot_general(both, pick, (((0,), (0,)), ((), ())), preferred_element_type=f32)
                    for n in range(SUB):
                        table[pl.ds(pl.multiple_of(target(h, first + n), SUB), LANES), :] = rows[n * LANES:(n + 1) * LANES]
                for n in range(SUB):
                    most = jnp.maximum(most, lists_ref[first + n])
            return most

        return lax.fori_loop(0, lists_ref.shape[0] // (GROUP * SUB), body, jnp.full((SUB, LANES), EMPTY, f32))

    table[vertices:pitch, :] = jnp.full((SUB, LANES), EMPTY, f32)
    if compact:
        most = fill(PAIR, lambda h, t: (2 * t + h) * LANES)
        quads = 1
    else:
        table[pitch + vertices:, :] = jnp.full((SUB, LANES), EMPTY, f32)
        most = fill((0,), lambda h, t: t * LANES)
        wide = jnp.max(jnp.where(sub >= FEW, most, EMPTY)) >= 0
        quads = jnp.where(wide, 2, 1)

        @pl.when(wide)
        def _():
            fill((1,), lambda h, t: pitch + t * LANES)

    bad = jnp.max(most) > vertices
    meta[FAULT] = bad.astype(jnp.int32)

    def gather(rows_of_ids):
        acc = [[jnp.full((1, LANES), EMPTY, f32)] * 2 for _ in rows_of_ids]
        for j in range(32):
            hit = lane32 == j
            for i, id_of in enumerate(rows_of_ids):
                for b in PAIR:
                    acc[i][b] = jnp.where(hit, table[pl.ds(id_of(b * 32 + j), 1), :], acc[i][b])
        return [(jnp.where(group_odd, b, a), pltpu.roll(jnp.where(group_odd, a, b), LANES - 32, 1)) for a, b in acc]

    def gather_slots(ids_s, slots=SLOTS):
        return gather([functools.partial(lambda i, j: ids_s[i, j], i) for i in range(slots)])

    def keep(rows, quad, row):
        for i, pair in enumerate(rows):
            for h in PAIR:
                cand[2 * quad + h, pl.ds(row + i, 1), :] = pair[h]

    def flag(x):
        return jnp.where(x, 1, 0)

    def at(unit, origin):
        return unit & (quads - 1), origin + (unit >> (quads - 1)) * SUB

    def level_step(level, carry):
        base, count = meta[BASE, level], meta[COUNT, level]
        following = base + (count + 7) // SUB * SUB
        batches = jnp.where(following <= CAP, (count + SLOTS - 1) // SLOTS, 0)
        units = batches * quads
        parity = meta[PARITY]

        def on_parity(n, f):
            for k in PAIR:
                @pl.when(n & 1 == k)
                def _():
                    f(bufs[k], bufs[1 - k])

        def unit_step(unit, other, to):
            quad, row = at(unit, base)
            x = [cand[2 * quad + h, eight(row), :] for h in PAIR]

            def search(first, count, marks):
                marks = list(marks)
                for k in range(count):
                    q = spread_row(queue, first + k)
                    for h in PAIR:
                        n = 2 * h + k % 2
                        marks[n] = jnp.where(x[h] == q, 1, marks[n])
                return tuple(marks)

            reach = following + meta[LENGTH] - PEEL
            marks = lax.fori_loop(0, (reach + SCAN - 1) // SCAN, lambda t, m: search(PEEL + t * SCAN, SCAN, m),
                                  (jnp.zeros((SUB, LANES), jnp.int32),) * 4)
            ahead = unit + 1 < units
            final_unit = unit + 1 == units
            soon = jnp.logical_and(final_unit, meta[AWAIT0] > 0)

            @pl.when(jnp.logical_or(ahead, soon))
            def _():
                fetch(0, base, to).wait()

            def insert(g):
                slots = [eight(following + g * WINDOW + SUB * t) for t in range(WINDOW // SUB)]
                qs = [queue[r, :] for r in slots]
                ss = [sigma[r, :] for r in slots]
                pos = [sub + (g * WINDOW + SUB * t) for t in range(WINDOW // SUB)]
                for h in PAIR:
                    for i in range(SUB):
                        d, e = spread_row(dest, SUB * h + i), spread_row(dest, SUB * (h + 2) + i)
                        v, w = spread_row(now, SUB * h + i), spread_row(now, SUB * (h + 2) + i)
                        for t in range(WINDOW // SUB):
                            qs[t] = jnp.where(pos[t] == d, v, jnp.where(pos[t] == e, w, qs[t]))
                for i in range(SUB):
                    v, w, sig = (spread_row(now, SUB * n + i) for n in (0, 1, 4))
                    for t in range(WINDOW // SUB):
                        ss[t] = ss[t] + jnp.where((qs[t] == v) | (qs[t] == w), sig, 0.0)
                for t, r in enumerate(slots):
                    queue[r, :] = qs[t]
                    sigma[r, :] = ss[t]
                return qs

            def core(looking):
                even, odd = x
                m, n, k, l = search(0, PEEL, marks)
                near_even, near_odd = m | n | flag(even < 0), k | l | flag(odd < 0)

                xr = [swap(v) for v in x]
                turns = [[[pltpu.roll(v, s, 0) if s else v for v in (x[h], xr[h])] for s in range(SUB)] for h in PAIR]
                for s, ((a, b), (c, d)) in enumerate(zip(*turns)):
                    near_odd = jnp.where((odd == a) | (odd == b), 1, near_odd)
                    if s:
                        after = sub >= s
                        near_even = jnp.where(((even == a) | (even == b)) & after, 1, near_even)
                        near_odd = jnp.where(((odd == c) | (odd == d)) & after, 1, near_odd)

                new = [1 - near_even, 1 - near_odd]
                packed = new[0] + BYTE * new[1]
                across = swap(packed)
                far = [across & (BYTE - 1), across >> SUB]
                both = packed + across
                run, whole = both, both
                for s in (1, 2, 4):
                    run = run + jnp.where(sub >= s, pltpu.roll(run, s, 0), 0)
                    whole = whole + pltpu.roll(whole, s, 0)
                run = run - both
                tail = tail_ref[...]
                evens = whole & (BYTE - 1)
                begin = [tail + (run & (BYTE - 1)), tail + evens + (run >> SUB)]
                for h in PAIR:
                    dest[part(h), :] = jnp.where(new[h] > 0, begin[h] + jnp.where(upper, far[h], 0), -1)
                    dest[part(h + 2), :] = jnp.where(far[h] > 0, begin[h] + jnp.where(upper, 0, new[h]), -1)
                    now[part(h), :] = x[h]
                    now[part(h + 2), :] = xr[h]
                now[part(4), :] = sigma[eight(row), :] + swap(sigma[eight(row), :])
                tail = tail + evens + (whole >> SUB)
                tail_ref[...] = tail
                passed = SLOTS * ((unit + 1) >> (quads - 1))
                second = SUB + SUB * (1 >> (quads - 1))
                need = jnp.where(sub == 1, SUB, second)
                short = (tail < need) & (held[...] > passed)
                most = jnp.max(jnp.where(sub == 0, tail, flag(short)).astype(f32), axis=1, keepdims=True)
                meta[REACHED] = most[0, 0].astype(jnp.int32)
                for n in PAIR:
                    meta[(SHORT0, SHORT1)[n]] = most[n + 1, 0].astype(jnp.int32)

                if looking:
                    quad2, row2 = at(unit + 1, base)
                    rows = gather_slots(to[0])
                qs = insert(0)
                for n in PAIR:
                    name(following + n * SUB, qs[n])
                if looking:
                    keep(rows, jnp.where(ahead, quad2, 0), jnp.where(ahead, row2, following))

            look = jnp.logical_or(ahead, soon)
            for looking in PAIR:
                @pl.when(look == (looking > 0))
                def _():
                    core(looking)

            length = meta[REACHED]
            ready = [meta[n] == 0 for n in (SHORT0, SHORT1)]

            @pl.when(unit + 3 < units)
            def _():
                fetch(*at(unit + 3, base), to).start()

            @pl.when(soon)
            def _():
                meta[GOT] = 1

            def first_of_next(n, when, buf):
                @pl.when(jnp.logical_and(when, meta[(AWAIT0, AWAIT1)[n]] == 0))
                def _():
                    fetch(*at(n, following), buf).start()
                    meta[(AWAIT0, AWAIT1)[n]] = 1

            first_of_next(0, jnp.logical_and(ready[0], unit + 3 == units), to)
            first_of_next(0, jnp.logical_and(ready[0], unit + 2 == units), other)
            first_of_next(1, jnp.logical_and(ready[1], unit + 2 == units), to)
            first_of_next(0, final_unit, to)
            first_of_next(1, final_unit, other)

            groups = (length + WINDOW - 1) // WINDOW
            fits = following + groups * WINDOW <= CAP + WINDOW
            meta[LENGTH] = jnp.where(fits, length, 0)

            @pl.when(jnp.logical_not(fits))
            def _():
                meta[FAULT] = 1

            def more(g, carry):
                insert(g)
                return carry

            lax.fori_loop(1, jnp.where(fits, groups, 0), more, 0)

        tail_ref[...] = jnp.zeros_like(tail_ref)
        meta[LENGTH] = 0

        def open_level(mine, other):
            @pl.when(jnp.logical_and(meta[GOT] == 0, meta[AWAIT0] > 0))
            def _():
                fetch(0, base, mine).wait()
                keep(gather_slots(mine[0]), 0, base)

            @pl.when(jnp.logical_and(units < 2, meta[AWAIT1] > 0))
            def _():
                fetch(0, base, other).wait()

            @pl.when(units > 2)
            def _():
                fetch(*at(2, base), mine).start()

        on_parity(parity, open_level)
        for place_ in (GOT, AWAIT0, AWAIT1):
            meta[place_] = 0

        def any_unit(unit, carry):
            on_parity(parity + unit, functools.partial(unit_step, unit))
            return carry

        lax.fori_loop(0, units, any_unit, 0)
        meta[PARITY] = parity + units

        @pl.when(following > CAP)
        def _():
            meta[FAULT] = 1

        found = jnp.where(meta[FAULT] == 0, meta[LENGTH], 0)
        meta[BASE, level + 1] = following
        meta[COUNT, level + 1] = found

        def names(t, carry):
            row = following + t * SUB
            name(row, queue[eight(row), :])
            return carry

        for t in range(2, WINDOW // SUB):
            names(t, carry)
        lax.fori_loop(WINDOW // SUB, (found + SUB - 1) // SUB, names, 0)
        held[...] = tail_ref[...]
        return carry

    for place_ in (GOT, PARITY):
        meta[place_] = 0

    @pl.when(jnp.logical_not(bad))
    def _():
        held[...] = jnp.full_like(held, FEW * quads)
        meta[BASE, 1] = SUB
        meta[COUNT, 1] = FEW * quads
        fetch(0, SUB, bufs[0]).wait()
        if compact:
            for h in PAIR:
                cand[h, eight(SUB), :] = jnp.full((SUB, LANES), EMPTY, f32)
        else:
            fetch(*at(1, SUB), bufs[1]).start()
        keep(gather_slots(ids_a, FEW if compact else SLOTS), 0, SUB)
        meta[GOT] = 1
        meta[AWAIT0] = 0
        meta[AWAIT1] = 1
        lax.fori_loop(1, levels, level_step, 0)

    @pl.when(bad)
    def _():
        fetch(0, SUB, bufs[0]).wait()
        meta[AWAIT0] = 0
        meta[AWAIT1] = int(compact)

    def drain(n, buf):
        @pl.when(meta[(AWAIT0, AWAIT1)[n]] > 0)
        def _():
            fetch(0, 0, buf).wait()

    for k in PAIR:
        @pl.when(meta[PARITY] & 1 == k)
        def _():
            @pl.when(meta[GOT] == 0)
            def _():
                drain(0, bufs[k])

            drain(1, bufs[1 - k])

    good = meta[FAULT] == 0

    @pl.when(good)
    def _():
        last = meta[BASE, levels]
        g_last = weight_ref[levels - 2]

        def seed(g, carry):
            for t in range(WINDOW // SUB):
                r = eight(last + g * WINDOW + SUB * t)
                s = sigma[r, :] + swap(sigma[r, :])
                ratio[r, :] = jnp.where(s > 0, g_last / jnp.where(s > 0, s, 1.0), 0.0)
            return carry

        lax.fori_loop(0, (meta[COUNT, levels] + WINDOW - 1) // WINDOW, seed, 0)

        def back_step(k, carry):
            level = levels - 1 - k
            base, count = meta[BASE, level], meta[COUNT, level]
            nbase, ncount = meta[BASE, level + 1], meta[COUNT, level + 1]
            g_here = weight_ref[jnp.maximum(level - 2, 0)]

            def pull_batch(bt, carry):
                here = eight(base + bt * SLOTS)

                def pull(quad, c, acc):
                    even, odd = cand[2 * quad, here, :], cand[2 * quad + 1, here, :]
                    acc = list(acc)
                    for n in range(WINDOW):
                        q = spread_row(queue, nbase + c * WINDOW + n)
                        w = spread_row(ratio, nbase + c * WINDOW + n)
                        acc[n % 2] = acc[n % 2] + jnp.where((even == q) | (odd == q), w, 0.0)
                    return tuple(acc)

                def pull_quad(quad, acc):
                    return lax.fori_loop(1, (ncount + WINDOW - 1) // WINDOW, functools.partial(pull, quad), pull(quad, 0, acc))

                acc = pull_quad(0, (jnp.zeros((SUB, LANES), f32),) * 2)
                if not compact:
                    acc = lax.fori_loop(1, quads, pull_quad, acc)
                delta[here, :] = acc[0] + acc[1]
                return carry

            lax.fori_loop(0, (count + SLOTS - 1) // SLOTS, pull_batch, 0)

            def finish(g, carry):
                slots = [eight(base + g * WINDOW + SUB * t) for t in range(WINDOW // SUB)]
                for t, r in enumerate(slots):
                    inside = g * WINDOW + SUB * t < count
                    part, s = (v + swap(v) for v in (delta[r, :], sigma[r, :]))
                    d = s * part
                    w = jnp.where(s > 0, (g_here + d) / jnp.where(s > 0, s, 1.0), 0.0)
                    delta[r, :] = jnp.where(inside, d, delta[r, :])
                    ratio[r, :] = jnp.where(inside, w, ratio[r, :])
                return carry

            lax.fori_loop(0, (count + WINDOW - 1) // WINDOW, finish, 0)
            return carry

        lax.fori_loop(0, levels - 1, back_step, 0)

        tall = along((WIDE, WIDE)).astype(f32).astype(bf16)
        zero = jnp.zeros((WIDE, WIDE), bf16)
        one = zero + 1
        start = meta[BASE, 1]

        def tally(t, carry):
            for u in range(TALLY // 16):
                a, b = eight(start + t * TALLY + u * 16), eight(start + t * TALLY + u * 16 + SUB)
                v = jnp.where(upper, queue[b, :], queue[a, :])
                d = jnp.where(upper, delta[b, :], delta[a, :])
                hi, lo = digits(v, WIDE)
                d_hi = d.astype(bf16).astype(f32)
                d_mid = (d - d_hi).astype(bf16).astype(f32)
                d_lo = d - d_hi - d_mid
                for p in range(0, SUB, 2):
                    cols = slice((u * SUB + p) * LANES, (u * SUB + p + 2) * LANES)

                    def pair(x):
                        return jnp.concatenate([x[p:p + 1], x[p + 1:p + 2]], axis=1).astype(bf16)

                    colhot[:, cols] = jnp.where(tall == pair(lo), one, zero)
                    match = tall[:high] == pair(hi)
                    for n, x in enumerate((d_hi, d_mid, d_lo)):
                        rowhot[n * high:(n + 1) * high, cols] = jnp.where(match, pair(x), zero[:high])
            bins[...] += lax.dot_general(rowhot[...], colhot[...], TURN, preferred_element_type=f32)
            return carry

        for t in range(TALLY // SUB):
            delta[eight(last + t * SUB), :] = jnp.zeros((SUB, LANES), f32)
        lax.fori_loop(0, (last - start + TALLY - 1) // TALLY, tally, 0)

    blocks = out_ref.shape[0]
    per = high // blocks
    total = (bins[:high] + bins[high:2 * high] + bins[2 * high:]) * scale
    fault = jnp.where(good, 0.0, 1.0)
    for b in range(blocks):
        for n in PAIR:
            out_ref[b, n * per:(n + 1) * per, :] = total[b * per:(b + 1) * per, n * LANES:(n + 1) * LANES]
        out_ref[b, 2 * per:, :] = jnp.full((SUB, LANES), fault, f32)


def walk(which, sources, weights, lists, *, blocks, vertices, scale, compact):
    levels = weights.shape[0] + 1
    rows = CAP + 4 * WINDOW
    high = LANES // blocks + SUB
    vm = pltpu.VMEM
    queue = vm((rows, LANES), f32)
    parts = 3 * (vertices // WIDE)
    return pl.pallas_call(
        functools.partial(walk_kernel, levels=levels, vertices=vertices, scale=scale, compact=compact),
        in_specs=[pl.BlockSpec(memory_space=pltpu.SMEM)] * 3 + [pl.BlockSpec(memory_space=pltpu.VMEM)],
        out_specs=pl.BlockSpec(memory_space=pltpu.VMEM),
        out_shape=jax.ShapeDtypeStruct((blocks, high, LANES), f32),
        scratch_shapes=[
            vm(((1 if compact else 2) * (vertices + SUB), LANES), f32), queue, queue, queue, queue,
            vm((4, rows, LANES), f32), vm((2, rows, LANES), jnp.int32),
            vm((40, LANES), f32), vm((32, LANES), jnp.int32), vm((SUB, LANES), jnp.int32), vm((SUB, LANES), jnp.int32),
            vm((parts, TALLY // 2 * LANES), bf16), vm((WIDE, TALLY // 2 * LANES), bf16), vm((parts, WIDE), f32),
            pltpu.SMEM((SLOTS, LANES), jnp.int32), pltpu.SMEM((SLOTS, LANES), jnp.int32), pltpu.SMEM((3, 16), jnp.int32),
            pltpu.SemaphoreType.DMA((2,)),
        ],
        compiler_params=pltpu.CompilerParams(
            vmem_limit_bytes=48 * 1024 * 1024),
        name="walk",
    )(which, sources, weights, lists)


def share_kernel(src, graph, x_ref, o_ref, own_sem, send_sem, recv_sem):
    mine, g, others = place_and_others(src, graph)
    hello(others)
    await_hello(others)
    own = pltpu.make_async_copy(x_ref, o_ref.at[mine], own_sem)
    own.start()
    copies = []
    for n, (py, pg) in enumerate(others):
        copies.append(pltpu.make_async_remote_copy(
            src_ref=x_ref, dst_ref=o_ref.at[mine], send_sem=send_sem.at[n], recv_sem=recv_sem.at[n],
            device_id={"src": py, "graph": pg}, device_id_type=MESH))
        copies[-1].start()
    own.wait()
    for c in copies:
        c.wait()


def share(x, src, graph):
    n = src * graph
    return pl.pallas_call(
        functools.partial(share_kernel, src, graph),
        in_specs=[pl.BlockSpec(memory_space=pltpu.VMEM)],
        out_specs=pl.BlockSpec(memory_space=pltpu.VMEM),
        out_shape=jax.ShapeDtypeStruct((n,) + x.shape, x.dtype),
        scratch_shapes=[pltpu.SemaphoreType.DMA, pltpu.SemaphoreType.DMA((n - 1,)), pltpu.SemaphoreType.DMA((n - 1,))],
        compiler_params=pltpu.CompilerParams(collective_id=2, has_side_effects=True),
        name="share",
    )(x)


def total_kernel(src, graph, x_ref, o_ref, got, own_sem, send_sem, recv_sem):
    mine, g, others = place_and_others(src, graph)
    hello(others)
    own = pltpu.make_async_copy(x_ref.at[g], got.at[mine], own_sem)
    own.start()
    await_hello(others)
    copies = []
    for n, (py, pg) in enumerate(others):
        copies.append(pltpu.make_async_remote_copy(
            src_ref=x_ref.at[pg], dst_ref=got.at[mine], send_sem=send_sem.at[n], recv_sem=recv_sem.at[n],
            device_id={"src": py, "graph": pg}, device_id_type=MESH))
        copies[-1].start()
    own.wait()
    for c in copies:
        c.wait()
    acc = got[0]
    for n in range(1, src * graph):
        acc = acc + got[n]
    o_ref[...] = acc


def total(x, src, graph, collective_id):
    n = src * graph
    return pl.pallas_call(
        functools.partial(total_kernel, src, graph),
        in_specs=[pl.BlockSpec(memory_space=pltpu.VMEM)],
        out_specs=pl.BlockSpec(memory_space=pltpu.VMEM),
        out_shape=jax.ShapeDtypeStruct(x.shape[1:], x.dtype),
        scratch_shapes=[pltpu.VMEM((n,) + x.shape[1:], x.dtype), pltpu.SemaphoreType.DMA,
                        pltpu.SemaphoreType.DMA((n - 1,)), pltpu.SemaphoreType.DMA((n - 1,))],
        compiler_params=pltpu.CompilerParams(collective_id=collective_id, has_side_effects=True),
        name="total",
    )(pltpu.with_memory_space_constraint(x, pltpu.VMEM))


def exchange(x, axis):
    return lax.all_to_all(x, axis, 0, 0)


def dense(adj_slab, src_local, level_weight, src, graph):
    slab_rows, vertex_count = adj_slab.shape
    src_count = src_local.shape[0]
    levels = level_weight.shape[0] + 1
    row_start = lax.axis_index("graph") * slab_rows
    vertex_ids = row_start + lax.broadcasted_iota(jnp.int32, (slab_rows, 1), 0)
    first = jnp.where(vertex_ids == src_local[None, :], 1.0, 0.0).astype(f32)

    def forward(carry, unused):
        sigma, seen = carry
        partial = jnp.einsum("uv,us->vs", adj_slab, sigma, preferred_element_type=f32, precision=exact_precision)
        parts = exchange(partial.reshape(graph, slab_rows, src_count), "graph")
        sigma = jnp.sum(parts, axis=0) * (1.0 - seen)
        seen = jnp.maximum(seen, jnp.where(sigma > 0, 1.0, 0.0))
        return (sigma, seen), sigma

    _, sigmas = lax.scan(forward, (first, first), None, length=levels)

    def backward(carry, xs):
        delta, acc = carry
        upper, lower, weight = xs
        reached = upper > 0
        ratio = jnp.where(reached, (weight + delta) / jnp.where(reached, upper, 1.0), 0.0)
        gathered = exchange(jnp.broadcast_to(ratio[None], (graph,) + ratio.shape), "graph")
        pulled = jnp.einsum("uv,vs->us", adj_slab, gathered.reshape(vertex_count, src_count),
                            preferred_element_type=f32, precision=exact_precision)
        delta = lower * pulled
        return (delta, acc + delta), None

    zero = jnp.zeros_like(first)
    (_, acc), _ = lax.scan(backward, (zero, zero), (sigmas[1:][::-1], sigmas[:-1][::-1], level_weight[::-1]))
    scale = vertex_count / (src_count * src * levels ** 3)
    mine = jnp.sum(acc, axis=1) * scale
    both = exchange(jnp.broadcast_to(mine.reshape(1, -1, LANES), (src, slab_rows // LANES, LANES)), "src")
    return jnp.sum(both, axis=0).reshape(slab_rows)


def solution(mesh):
    src, graph = mesh.shape["src"], mesh.shape["graph"]

    def device_program(adj_slab, src_local, level_weight):
        slab_rows, vertex_count = adj_slab.shape
        levels = level_weight.shape[0] + 1
        scale = vertex_count / (HALF * src * graph * levels ** 3)
        which = lax.axis_index("graph").astype(jnp.int32).reshape(1)

        def finish(lists, compact, collective_id, other):
            parts = walk(which, src_local, level_weight, lists, blocks=graph, vertices=vertex_count, scale=scale, compact=compact)
            summed = total(parts, src, graph, collective_id)
            rows = slab_rows // LANES

            def plain():
                return summed[:rows].reshape(2, -1, LANES).transpose(1, 0, 2).reshape(slab_rows)

            return lax.cond(summed[rows, 0] > 0, other, plain)

        def dense_path():
            return dense(adj_slab, src_local, level_weight, src, graph)

        def general_path():
            half = lax.axis_index("src").astype(jnp.int32).reshape(1)
            lists = share(extract(adj_slab, half, slab_rows // src), src, graph)
            return finish(lists.reshape(-1, SUB, LANES), False, 3, dense_path)

        return finish(collect(adj_slab, src, graph), True, 1, general_path)

    return jax.shard_map(device_program, mesh=mesh,
                         in_specs=(P(("batch", "graph"), None), P(("batch", "src")), P(None)),
                         out_specs=P(("batch", "graph")), check_vma=False)
```

```python
import functools

import jax
import jax.numpy as jnp
from jax import lax
from jax.experimental import pallas as pl
from jax.experimental.pallas import tpu as pltpu
from jax.sharding import PartitionSpec as P

MESH = pl.DeviceIdType.MESH
exact_precision = lax.Precision.HIGHEST
f32, bf16 = jnp.float32, jnp.bfloat16

LANES, SUB = 128, 8
WIDE = 256
DEG, FEW = 8, 4
EMPTY = -2.0
FULL = 32767.0
TURN = (((1,), (1,)), ((), ()))
BLOCK = 128
READS = 4
STEP = 32
HALF = 64
SLOTS = SUB
WINDOW = 48
SCAN = 32
CAP = 1024
TALLY = 96
PAIR = (0, 1)
BYTE = 256
GROUP = SUB
PEEL = 32
BASE, COUNT = 0, 1
FAULT, LENGTH, GOT, PARITY, AWAIT0, AWAIT1, REACHED, SHORT0, SHORT1 = ((2, n) for n in range(9))


def place_and_others(src, graph):
    y, g = lax.axis_index("src"), lax.axis_index("graph")
    steps = sorted(((i, k) for i in range(src) for k in range(graph)), key=lambda s: (-s[0], abs(s[1] - graph // 2)))
    return g * src + y, g, [((y + i) % src, (g + k) % graph) for i, k in steps if i + k]


def hello(peers):
    for y, g in peers:
        pl.semaphore_signal(pltpu.get_barrier_semaphore(), inc=1, device_id={"src": y, "graph": g}, device_id_type=MESH)


def await_hello(peers):
    pl.semaphore_wait(pltpu.get_barrier_semaphore(), len(peers))


def place(plane, lists):
    lists = list(lists)
    row_i = lax.broadcasted_iota(jnp.int32, (WIDE, WIDE), 0)
    col_i = lax.broadcasted_iota(jnp.int32, (WIDE, WIDE), 1)
    eye = jnp.where(row_i == col_i, float(WIDE), 0.0).astype(bf16)
    flipped = lax.dot_general(eye, plane, TURN, preferred_element_type=f32)
    lane_id = lax.broadcasted_iota(jnp.int32, (SUB, flipped.shape[1]), 0).astype(f32)
    for g in range(WIDE // SUB):
        x = flipped[g * SUB:(g + 1) * SUB] + (lane_id + float(g * SUB))
        for s in range(len(lists)):
            hi = jnp.maximum(lists[s], x)
            if s < len(lists) - 1:
                x = jnp.minimum(lists[s], x)
            lists[s] = hi
    return lists


def sort(lists):
    gap = len(lists) // 2
    while gap:
        for s in range(len(lists)):
            if not s & gap:
                lists[s], lists[s + gap] = jnp.maximum(lists[s], lists[s + gap]), jnp.minimum(lists[s], lists[s + gap])
        gap //= 2
    return lists


def over_sublanes(lists):
    size = len(lists)
    for shift in (4, 2, 1):
        other = [pltpu.roll(v, shift, 0) for v in lists]
        lists = sort([jnp.maximum(lists[s], other[size - 1 - s]) for s in range(size)])
    out = jnp.full(lists[0].shape, EMPTY, f32)
    sub = lax.broadcasted_iota(jnp.int32, out.shape, 0)
    for s in range(size):
        out = jnp.where(sub == s, jnp.where(lists[s] >= WIDE, lists[s] - WIDE, EMPTY), out)
    return out


def degree_of(seen):
    return lax.dot_general(jnp.ones((SUB, WIDE), bf16), seen, TURN, preferred_element_type=f32)


def collect_kernel(src, graph, a_ref, o_ref, bufs, tops, mine, sems, own_sem, send_sems, recv_sems):
    vertices = a_ref.shape[1]
    pairs, chunks = mine.shape[0], vertices // WIDE
    blocks = 2 * pairs
    me, _, others = place_and_others(src, graph)
    y = me % src
    height = 4 * SUB
    pieces = BLOCK // height

    def fetch(i, t):
        rows = pl.ds(pl.multiple_of((y * blocks + i) * BLOCK + t * height, height), height)
        here = pl.ds(pl.multiple_of(t * height, height), height)
        return pltpu.make_async_copy(a_ref.at[rows], bufs.at[i % READS, here], sems.at[i % READS, t])

    def send(n, first, count):
        py, pg = others[n]
        return pltpu.make_async_remote_copy(
            src_ref=mine.at[pl.ds(first, count)], dst_ref=o_ref.at[pl.ds(me * pairs + first, count)],
            send_sem=send_sems.at[n], recv_sem=recv_sems.at[n], device_id={"src": py, "graph": pg}, device_id_type=MESH)

    def send_pair(p):
        for n in range(len(others)):
            send(n, p, 1).start()

    for i in range(READS - 1):
        for t in range(pieces):
            fetch(i, t).start()
    hello(others)
    none = jnp.zeros((SUB, 2 * BLOCK), f32)

    def scan(i, first):
        @pl.when(i + READS - 1 < blocks)
        def _():
            for t in range(pieces):
                fetch(i + READS - 1, t).start()

        def scan_rows(t, carry):
            fetch(i, t).wait()
            here = pl.ds(pl.multiple_of(t * height, height), height)

            def scan_chunks(c, state):
                top, low, seen, sums, value = state
                for k in range(STEP):
                    a = bufs[i % READS, here, pl.ds(pl.multiple_of((c * STEP + k) * WIDE, WIDE), WIDE)]
                    x = a * value
                    low = jnp.maximum(low, jnp.minimum(top, x))
                    top = jnp.maximum(top, x)
                    seen = seen + a
                    sums = sums + x
                    value = value + 1
                return top, low, seen, sums, value

            zero = jnp.zeros((height, WIDE), bf16)
            top, low, seen, sums, _ = lax.fori_loop(0, chunks // STEP, scan_chunks, (zero,) * 4 + (zero + 1,))
            for n, v in enumerate((top, low, (sums - top) - low, seen)):
                tops[n, pl.ds(pl.multiple_of(first + t * height, height), height), :] = v
            return carry

        lax.fori_loop(0, pieces, scan_rows, 0)

    def pair_step(p, carry):
        for h in range(2):
            scan(2 * p + h, h * BLOCK)
        seen = tops[3]
        crowd = seen[:SUB]
        for k in range(1, 2 * BLOCK // SUB):
            crowd = jnp.maximum(crowd, seen[k * SUB:(k + 1) * SUB])
        crowd = jnp.max(crowd.astype(f32), axis=0, keepdims=True)
        a, b, c = place(tops[0], (none,) * 4), place(tops[1], (none,) * 2), place(tops[2], (none,))
        rest = [jnp.maximum(b[0], c[0]), jnp.minimum(b[0], c[0])]
        rest = [rest[0], jnp.maximum(b[1], rest[1]), jnp.minimum(b[1], rest[1])]
        lists = over_sublanes(sort([a[0]] + [jnp.maximum(a[s + 1], rest[2 - s]) for s in range(3)]))
        lists = jnp.where((crowd > 3) | (degree_of(seen) > 4), FULL, lists)
        even, odd = lists[:, :BLOCK], lists[:, BLOCK:]
        sub = lax.broadcasted_iota(jnp.int32, even.shape, 0)
        mine[p] = jnp.where(sub < 4, even, pltpu.roll(odd, 4, 0))

        @pl.when(p == 1)
        def _():
            await_hello(others)

        @pl.when(p > 0)
        def _():
            send_pair(p - 1)

        return carry

    lax.fori_loop(0, pairs, pair_step, 0)
    own = pltpu.make_async_copy(mine, o_ref.at[pl.ds(me * pairs, pairs)], own_sem)
    send_pair(pairs - 1)
    own.start()
    own.wait()
    for n in range(len(others)):
        send(n, 0, pairs).wait()


def collect(adj_slab, src, graph):
    rows, vertices = adj_slab.shape
    n = src * graph
    mine = (rows // src // (2 * BLOCK), SUB, BLOCK)
    return pl.pallas_call(
        functools.partial(collect_kernel, src, graph),
        in_specs=[pl.BlockSpec(memory_space=pl.ANY)],
        out_specs=pl.BlockSpec(memory_space=pltpu.VMEM),
        out_shape=jax.ShapeDtypeStruct((n * mine[0],) + mine[1:], f32),
        scratch_shapes=[pltpu.VMEM((READS, BLOCK, vertices), bf16), pltpu.VMEM((4, 2 * BLOCK, WIDE), bf16), pltpu.VMEM(mine, f32),
                        pltpu.SemaphoreType.DMA((READS, BLOCK // (4 * SUB))), pltpu.SemaphoreType.DMA,
                        pltpu.SemaphoreType.DMA((n - 1,)), pltpu.SemaphoreType.DMA((n - 1,))],
        compiler_params=pltpu.CompilerParams(collective_id=0, has_side_effects=True, vmem_limit_bytes=40 * 1024 * 1024),
        name="collect",
    )(adj_slab)


def extract_kernel(half_ref, a_ref, o_ref, block, seen, planes, sem):
    vertices = a_ref.shape[1]

    def block_step(i, carry):
        copy = pltpu.make_async_copy(
            a_ref.at[pl.ds(pl.multiple_of((half_ref[0] * o_ref.shape[0] + i) * BLOCK, BLOCK), BLOCK)], block, sem)
        copy.start()
        copy.wait()
        planes[...] = jnp.zeros_like(planes)
        seen[...] = jnp.zeros_like(seen)

        def scan_chunk(c, carry):
            a = block[:, pl.ds(pl.multiple_of(c * WIDE, WIDE), WIDE)]
            seen[...] = seen[...] + a
            x = a.astype(f32) * (c + 1).astype(f32)
            for s in range(DEG):
                top = planes[s].astype(f32)
                planes[s] = jnp.maximum(top, x).astype(bf16)
                x = jnp.minimum(top, x)
            return carry

        lax.fori_loop(0, vertices // WIDE, scan_chunk, 0)
        lists = lax.fori_loop(0, DEG, lambda p, lists: tuple(place(planes[p], lists)), (jnp.zeros((SUB, BLOCK), f32),) * DEG)
        o_ref[i] = jnp.where(degree_of(seen[...]) > DEG, FULL, over_sublanes(list(lists)))
        return carry

    lax.fori_loop(0, o_ref.shape[0], block_step, 0)


def extract(adj_slab, half, rows):
    vertices = adj_slab.shape[1]
    return pl.pallas_call(
        extract_kernel,
        in_specs=[pl.BlockSpec(memory_space=pltpu.SMEM), pl.BlockSpec(memory_space=pl.ANY)],
        out_specs=pl.BlockSpec(memory_space=pltpu.VMEM),
        out_shape=jax.ShapeDtypeStruct((rows // BLOCK, DEG, BLOCK), f32),
        scratch_shapes=[pltpu.VMEM((BLOCK, vertices), bf16), pltpu.VMEM((BLOCK, WIDE), bf16),
                        pltpu.VMEM((DEG, BLOCK, WIDE), bf16), pltpu.SemaphoreType.DMA],
        name="extract",
    )(half, adj_slab)


def along(shape, axis=0):
    return lax.broadcasted_iota(jnp.int32, shape, axis)


def swap(x):
    return pltpu.roll(x, HALF, 1)


def digits(x, base):
    high = jnp.floor(x * (1.0 / base))
    return high, x - high * base


def walk_kernel(which_ref, src_ref, weight_ref, lists_ref, out_ref,
                table, queue, sigma, ratio, delta, cand, ids, now, dest, tail_ref, held, rowhot, colhot, bins,
                ids_a, ids_b, meta, sems, *, levels, vertices, scale, compact):
    pitch = vertices + SUB
    lane = along((SUB, LANES), 1)
    sub = along((SUB, LANES))
    upper = lane >= HALF
    lane_row = along((1, LANES), 1)
    group_odd = ((lane_row // 32) % 2) == 1
    lane32 = lane_row % 32
    rows_all = queue.shape[0]
    tile_bits = (vertices // lists_ref.shape[0]).bit_length() - 1
    high = vertices // WIDE

    def eight(row):
        return pl.ds(pl.multiple_of(row, SUB), SUB)

    def part(n):
        return pl.ds(n * SUB, SUB)

    def spread_row(ref, *index):
        return jnp.broadcast_to(ref[(*index[:-1], pl.ds(index[-1], 1), slice(None))], (SUB, LANES))

    def clear(t, carry):
        for k in range(SUB):
            rows = eight((t * SUB + k) * SUB)
            queue[rows, :] = jnp.full((SUB, LANES), -1.0, f32)
            sigma[rows, :] = jnp.zeros((SUB, LANES), f32)
        return carry

    def fetch(quad, row, buf):
        return pltpu.make_async_copy(ids.at[quad, eight(row)], buf[0], sems.at[buf[1]])

    def name(row, q):
        v = jnp.where(q < 0, vertices, q.astype(jnp.int32))
        ids[0, eight(row), :] = v
        if not compact:
            ids[1, eight(row), :] = v + pitch

    bufs = (ids_a, 0), (ids_b, 1)
    clear(0, 0)

    near_source = jnp.full((SUB, LANES), EMPTY, f32)
    source = along((SUB, LANES))
    for j in range(HALF):
        v = src_ref[which_ref[0] * HALF + j]
        near_source = jnp.where(lane == j, pltpu.roll(lists_ref[v >> tile_bits], (j - v) & (LANES - 1), 1), near_source)
        source = jnp.where(lane % HALF == j, v, source)
    if compact:
        near_source = jnp.where((source & LANES) > 0, pltpu.roll(near_source, FEW, 0), near_source)
    near_source = jnp.where(upper, swap(near_source), near_source)
    reached = near_source >= 0
    if compact:
        reached = reached & (sub < FEW)
    queue[0:1, :] = source[:1].astype(f32)
    queue[eight(SUB), :] = jnp.where(reached, near_source, -1.0)
    sigma[eight(SUB), :] = jnp.where(reached & jnp.logical_not(upper), 1.0, 0.0)
    for n in (1, 2):
        name(n * SUB, queue[eight(n * SUB), :])
    bins[...] = jnp.zeros_like(bins)
    fetch(0, SUB, bufs[0]).start()
    if compact:
        fetch(0, 2 * SUB, bufs[1]).start()
    lax.fori_loop(1, rows_all // (SUB * SUB), clear, 0)

    srow = along((2 * SUB, LANES))
    slane = along((2 * SUB, LANES), 1)

    def fill(halves, target):
        picks = [jnp.where((srow % SUB) == (slane // 32 + FEW * h), jnp.where(srow < SUB, float(LANES), 1.0), 0.0).astype(bf16)
                 for h in halves]

        def body(step, most):
            for k in range(GROUP):
                first = (GROUP * step + k) * SUB
                x = jnp.concatenate([lists_ref[first + n] for n in range(SUB)], axis=1)
                both = jnp.concatenate(digits(x, LANES), axis=0).astype(bf16)
                for h, pick in zip(halves, picks):
                    rows = lax.dot_general(both, pick, (((0,), (0,)), ((), ())), preferred_element_type=f32)
                    for n in range(SUB):
                        table[pl.ds(pl.multiple_of(target(h, first + n), SUB), LANES), :] = rows[n * LANES:(n + 1) * LANES]
                for n in range(SUB):
                    most = jnp.maximum(most, lists_ref[first + n])
            return most

        return lax.fori_loop(0, lists_ref.shape[0] // (GROUP * SUB), body, jnp.full((SUB, LANES), EMPTY, f32))

    table[vertices:pitch, :] = jnp.full((SUB, LANES), EMPTY, f32)
    if compact:
        most = fill(PAIR, lambda h, t: (2 * t + h) * LANES)
        quads = 1
    else:
        table[pitch + vertices:, :] = jnp.full((SUB, LANES), EMPTY, f32)
        most = fill((0,), lambda h, t: t * LANES)
        wide = jnp.max(jnp.where(sub >= FEW, most, EMPTY)) >= 0
        quads = jnp.where(wide, 2, 1)

        @pl.when(wide)
        def _():
            fill((1,), lambda h, t: pitch + t * LANES)

    bad = jnp.max(most) > vertices
    meta[FAULT] = bad.astype(jnp.int32)

    def gather(rows_of_ids):
        acc = [[jnp.full((1, LANES), EMPTY, f32)] * 2 for _ in rows_of_ids]
        for j in range(32):
            hit = lane32 == j
            for i, id_of in enumerate(rows_of_ids):
                for b in PAIR:
                    acc[i][b] = jnp.where(hit, table[pl.ds(id_of(b * 32 + j), 1), :], acc[i][b])
        return [(jnp.where(group_odd, b, a), pltpu.roll(jnp.where(group_odd, a, b), LANES - 32, 1)) for a, b in acc]

    def gather_slots(ids_s, slots=SLOTS):
        return gather([functools.partial(lambda i, j: ids_s[i, j], i) for i in range(slots)])

    def keep(rows, quad, row):
        for i, pair in enumerate(rows):
            for h in PAIR:
                cand[2 * quad + h, pl.ds(row + i, 1), :] = pair[h]

    def flag(x):
        return jnp.where(x, 1, 0)

    def at(unit, origin):
        return unit & (quads - 1), origin + (unit >> (quads - 1)) * SUB

    def level_step(level, carry):
        base, count = meta[BASE, level], meta[COUNT, level]
        following = base + (count + 7) // SUB * SUB
        batches = jnp.where(following <= CAP, (count + SLOTS - 1) // SLOTS, 0)
        units = batches * quads
        parity = meta[PARITY]

        def on_parity(n, f):
            for k in PAIR:
                @pl.when(n & 1 == k)
                def _():
                    f(bufs[k], bufs[1 - k])

        def unit_step(unit, other, to):
            quad, row = at(unit, base)
            x = [cand[2 * quad + h, eight(row), :] for h in PAIR]

            def search(first, count, marks):
                marks = list(marks)
                for k in range(count):
                    q = spread_row(queue, first + k)
                    for h in PAIR:
                        n = 2 * h + k % 2
                        marks[n] = jnp.where(x[h] == q, 1, marks[n])
                return tuple(marks)

            reach = following + meta[LENGTH] - PEEL
            marks = lax.fori_loop(0, (reach + SCAN - 1) // SCAN, lambda t, m: search(PEEL + t * SCAN, SCAN, m),
                                  (jnp.zeros((SUB, LANES), jnp.int32),) * 4)
            ahead = unit + 1 < units
            final_unit = unit + 1 == units
            soon = jnp.logical_and(final_unit, meta[AWAIT0] > 0)

            @pl.when(jnp.logical_or(ahead, soon))
            def _():
                fetch(0, base, to).wait()

            def insert(g):
                slots = [eight(following + g * WINDOW + SUB * t) for t in range(WINDOW // SUB)]
                qs = [queue[r, :] for r in slots]
                ss = [sigma[r, :] for r in slots]
                pos = [sub + (g * WINDOW + SUB * t) for t in range(WINDOW // SUB)]
                for h in PAIR:
                    for i in range(SUB):
                        d, e = spread_row(dest, SUB * h + i), spread_row(dest, SUB * (h + 2) + i)
                        v, w = spread_row(now, SUB * h + i), spread_row(now, SUB * (h + 2) + i)
                        for t in range(WINDOW // SUB):
                            qs[t] = jnp.where(pos[t] == d, v, jnp.where(pos[t] == e, w, qs[t]))
                for i in range(SUB):
                    v, w, sig = (spread_row(now, SUB * n + i) for n in (0, 1, 4))
                    for t in range(WINDOW // SUB):
                        ss[t] = ss[t] + jnp.where((qs[t] == v) | (qs[t] == w), sig, 0.0)
                for t, r in enumerate(slots):
                    queue[r, :] = qs[t]
                    sigma[r, :] = ss[t]
                return qs

            def core(looking):
                even, odd = x
                m, n, k, l = search(0, PEEL, marks)
                near_even, near_odd = m | n | flag(even < 0), k | l | flag(odd < 0)

                xr = [swap(v) for v in x]
                turns = [[[pltpu.roll(v, s, 0) if s else v for v in (x[h], xr[h])] for s in range(SUB)] for h in PAIR]
                for s, ((a, b), (c, d)) in enumerate(zip(*turns)):
                    near_odd = jnp.where((odd == a) | (odd == b), 1, near_odd)
                    if s:
                        after = sub >= s
                        near_even = jnp.where(((even == a) | (even == b)) & after, 1, near_even)
                        near_odd = jnp.where(((odd == c) | (odd == d)) & after, 1, near_odd)

                new = [1 - near_even, 1 - near_odd]
                packed = new[0] + BYTE * new[1]
                across = swap(packed)
                far = [across & (BYTE - 1), across >> SUB]
                both = packed + across
                run, whole = both, both
                for s in (1, 2, 4):
                    run = run + jnp.where(sub >= s, pltpu.roll(run, s, 0), 0)
                    whole = whole + pltpu.roll(whole, s, 0)
                run = run - both
                tail = tail_ref[...]
                evens = whole & (BYTE - 1)
                begin = [tail + (run & (BYTE - 1)), tail + evens + (run >> SUB)]
                for h in PAIR:
                    dest[part(h), :] = jnp.where(new[h] > 0, begin[h] + jnp.where(upper, far[h], 0), -1)
                    dest[part(h + 2), :] = jnp.where(far[h] > 0, begin[h] + jnp.where(upper, 0, new[h]), -1)
                    now[part(h), :] = x[h]
                    now[part(h + 2), :] = xr[h]
                now[part(4), :] = sigma[eight(row), :] + swap(sigma[eight(row), :])
                tail = tail + evens + (whole >> SUB)
                tail_ref[...] = tail
                passed = SLOTS * ((unit + 1) >> (quads - 1))
                second = SUB + SUB * (1 >> (quads - 1))
                need = jnp.where(sub == 1, SUB, second)
                short = (tail < need) & (held[...] > passed)
                most = jnp.max(jnp.where(sub == 0, tail, flag(short)).astype(f32), axis=1, keepdims=True)
                meta[REACHED] = most[0, 0].astype(jnp.int32)
                for n in PAIR:
                    meta[(SHORT0, SHORT1)[n]] = most[n + 1, 0].astype(jnp.int32)

                if looking:
                    quad2, row2 = at(unit + 1, base)
                    rows = gather_slots(to[0])
                qs = insert(0)
                for n in PAIR:
                    name(following + n * SUB, qs[n])
                if looking:
                    keep(rows, jnp.where(ahead, quad2, 0), jnp.where(ahead, row2, following))

            look = jnp.logical_or(ahead, soon)
            for looking in PAIR:
                @pl.when(look == (looking > 0))
                def _():
                    core(looking)

            length = meta[REACHED]
            ready = [meta[n] == 0 for n in (SHORT0, SHORT1)]

            @pl.when(unit + 3 < units)
            def _():
                fetch(*at(unit + 3, base), to).start()

            @pl.when(soon)
            def _():
                meta[GOT] = 1

            def first_of_next(n, when, buf):
                @pl.when(jnp.logical_and(when, meta[(AWAIT0, AWAIT1)[n]] == 0))
                def _():
                    fetch(*at(n, following), buf).start()
                    meta[(AWAIT0, AWAIT1)[n]] = 1

            first_of_next(0, jnp.logical_and(ready[0], unit + 3 == units), to)
            first_of_next(0, jnp.logical_and(ready[0], unit + 2 == units), other)
            first_of_next(1, jnp.logical_and(ready[1], unit + 2 == units), to)
            first_of_next(0, final_unit, to)
            first_of_next(1, final_unit, other)

            groups = (length + WINDOW - 1) // WINDOW
            fits = following + groups * WINDOW <= CAP + WINDOW
            meta[LENGTH] = jnp.where(fits, length, 0)

            @pl.when(jnp.logical_not(fits))
            def _():
                meta[FAULT] = 1

            def more(g, carry):
                insert(g)
                return carry

            lax.fori_loop(1, jnp.where(fits, groups, 0), more, 0)

        tail_ref[...] = jnp.zeros_like(tail_ref)
        meta[LENGTH] = 0

        def open_level(mine, other):
            @pl.when(jnp.logical_and(meta[GOT] == 0, meta[AWAIT0] > 0))
            def _():
                fetch(0, base, mine).wait()
                keep(gather_slots(mine[0]), 0, base)

            @pl.when(jnp.logical_and(units < 2, meta[AWAIT1] > 0))
            def _():
                fetch(0, base, other).wait()

            @pl.when(units > 2)
            def _():
                fetch(*at(2, base), mine).start()

        on_parity(parity, open_level)
        for place_ in (GOT, AWAIT0, AWAIT1):
            meta[place_] = 0

        def any_unit(unit, carry):
            on_parity(parity + unit, functools.partial(unit_step, unit))
            return carry

        lax.fori_loop(0, units, any_unit, 0)
        meta[PARITY] = parity + units

        @pl.when(following > CAP)
        def _():
            meta[FAULT] = 1

        found = jnp.where(meta[FAULT] == 0, meta[LENGTH], 0)
        meta[BASE, level + 1] = following
        meta[COUNT, level + 1] = found

        def names(t, carry):
            row = following + t * SUB
            name(row, queue[eight(row), :])
            return carry

        for t in range(2, WINDOW // SUB):
            names(t, carry)
        lax.fori_loop(WINDOW // SUB, (found + SUB - 1) // SUB, names, 0)
        held[...] = tail_ref[...]
        return carry

    for place_ in (GOT, PARITY):
        meta[place_] = 0

    @pl.when(jnp.logical_not(bad))
    def _():
        held[...] = jnp.full_like(held, FEW * quads)
        meta[BASE, 1] = SUB
        meta[COUNT, 1] = FEW * quads
        fetch(0, SUB, bufs[0]).wait()
        if compact:
            for h in PAIR:
                cand[h, eight(SUB), :] = jnp.full((SUB, LANES), EMPTY, f32)
        else:
            fetch(*at(1, SUB), bufs[1]).start()
        keep(gather_slots(ids_a, FEW if compact else SLOTS), 0, SUB)
        meta[GOT] = 1
        meta[AWAIT0] = 0
        meta[AWAIT1] = 1
        lax.fori_loop(1, levels, level_step, 0)

    @pl.when(bad)
    def _():
        fetch(0, SUB, bufs[0]).wait()
        meta[AWAIT0] = 0
        meta[AWAIT1] = int(compact)

    def drain(n, buf):
        @pl.when(meta[(AWAIT0, AWAIT1)[n]] > 0)
        def _():
            fetch(0, 0, buf).wait()

    for k in PAIR:
        @pl.when(meta[PARITY] & 1 == k)
        def _():
            @pl.when(meta[GOT] == 0)
            def _():
                drain(0, bufs[k])

            drain(1, bufs[1 - k])

    good = meta[FAULT] == 0

    @pl.when(good)
    def _():
        last = meta[BASE, levels]
        g_last = weight_ref[levels - 2]

        def seed(g, carry):
            for t in range(WINDOW // SUB):
                r = eight(last + g * WINDOW + SUB * t)
                s = sigma[r, :] + swap(sigma[r, :])
                ratio[r, :] = jnp.where(s > 0, g_last / jnp.where(s > 0, s, 1.0), 0.0)
            return carry

        lax.fori_loop(0, (meta[COUNT, levels] + WINDOW - 1) // WINDOW, seed, 0)

        def back_step(k, carry):
            level = levels - 1 - k
            base, count = meta[BASE, level], meta[COUNT, level]
            nbase, ncount = meta[BASE, level + 1], meta[COUNT, level + 1]
            g_here = weight_ref[jnp.maximum(level - 2, 0)]

            def pull_batch(bt, carry):
                here = eight(base + bt * SLOTS)

                def pull(quad, c, acc):
                    even, odd = cand[2 * quad, here, :], cand[2 * quad + 1, here, :]
                    acc = list(acc)
                    for n in range(WINDOW):
                        q = spread_row(queue, nbase + c * WINDOW + n)
                        w = spread_row(ratio, nbase + c * WINDOW + n)
                        acc[n % 2] = acc[n % 2] + jnp.where((even == q) | (odd == q), w, 0.0)
                    return tuple(acc)

                def pull_quad(quad, acc):
                    return lax.fori_loop(1, (ncount + WINDOW - 1) // WINDOW, functools.partial(pull, quad), pull(quad, 0, acc))

                acc = pull_quad(0, (jnp.zeros((SUB, LANES), f32),) * 2)
                if not compact:
                    acc = lax.fori_loop(1, quads, pull_quad, acc)
                delta[here, :] = acc[0] + acc[1]
                return carry

            lax.fori_loop(0, (count + SLOTS - 1) // SLOTS, pull_batch, 0)

            def finish(g, carry):
                slots = [eight(base + g * WINDOW + SUB * t) for t in range(WINDOW // SUB)]
                for t, r in enumerate(slots):
                    inside = g * WINDOW + SUB * t < count
                    part, s = (v + swap(v) for v in (delta[r, :], sigma[r, :]))
                    d = s * part
                    w = jnp.where(s > 0, (g_here + d) / jnp.where(s > 0, s, 1.0), 0.0)
                    delta[r, :] = jnp.where(inside, d, delta[r, :])
                    ratio[r, :] = jnp.where(inside, w, ratio[r, :])
                return carry

            lax.fori_loop(0, (count + WINDOW - 1) // WINDOW, finish, 0)
            return carry

        lax.fori_loop(0, levels - 1, back_step, 0)

        tall = along((WIDE, WIDE)).astype(f32).astype(bf16)
        zero = jnp.zeros((WIDE, WIDE), bf16)
        one = zero + 1
        start = meta[BASE, 1]

        def tally(t, carry):
            for u in range(TALLY // 16):
                a, b = eight(start + t * TALLY + u * 16), eight(start + t * TALLY + u * 16 + SUB)
                v = jnp.where(upper, queue[b, :], queue[a, :])
                d = jnp.where(upper, delta[b, :], delta[a, :])
                hi, lo = digits(v, WIDE)
                d_hi = d.astype(bf16).astype(f32)
                d_mid = (d - d_hi).astype(bf16).astype(f32)
                d_lo = d - d_hi - d_mid
                for p in range(0, SUB, 2):
                    cols = slice((u * SUB + p) * LANES, (u * SUB + p + 2) * LANES)

                    def pair(x):
                        return jnp.concatenate([x[p:p + 1], x[p + 1:p + 2]], axis=1).astype(bf16)

                    colhot[:, cols] = jnp.where(tall == pair(lo), one, zero)
                    match = tall[:high] == pair(hi)
                    for n, x in enumerate((d_hi, d_mid, d_lo)):
                        rowhot[n * high:(n + 1) * high, cols] = jnp.where(match, pair(x), zero[:high])
            bins[...] += lax.dot_general(rowhot[...], colhot[...], TURN, preferred_element_type=f32)
            return carry

        for t in range(TALLY // SUB):
            delta[eight(last + t * SUB), :] = jnp.zeros((SUB, LANES), f32)
        lax.fori_loop(0, (last - start + TALLY - 1) // TALLY, tally, 0)

    blocks = out_ref.shape[0]
    per = high // blocks
    total = (bins[:high] + bins[high:2 * high] + bins[2 * high:]) * scale
    fault = jnp.where(good, 0.0, 1.0)
    for b in range(blocks):
        for n in PAIR:
            out_ref[b, n * per:(n + 1) * per, :] = total[b * per:(b + 1) * per, n * LANES:(n + 1) * LANES]
        out_ref[b, 2 * per:, :] = jnp.full((1, LANES), fault, f32)


def walk(which, sources, weights, lists, *, blocks, vertices, scale, compact):
    levels = weights.shape[0] + 1
    rows = CAP + 4 * WINDOW
    high = LANES // blocks + 1
    vm = pltpu.VMEM
    queue = vm((rows, LANES), f32)
    parts = 3 * (vertices // WIDE)
    return pl.pallas_call(
        functools.partial(walk_kernel, levels=levels, vertices=vertices, scale=scale, compact=compact),
        in_specs=[pl.BlockSpec(memory_space=pltpu.SMEM)] * 3 + [pl.BlockSpec(memory_space=pltpu.VMEM)],
        out_specs=pl.BlockSpec(memory_space=pltpu.VMEM),
        out_shape=jax.ShapeDtypeStruct((blocks, high, LANES), f32),
        scratch_shapes=[
            vm(((1 if compact else 2) * (vertices + SUB), LANES), f32), queue, queue, queue, queue,
            vm((4, rows, LANES), f32), vm((2, rows, LANES), jnp.int32),
            vm((40, LANES), f32), vm((32, LANES), jnp.int32), vm((SUB, LANES), jnp.int32), vm((SUB, LANES), jnp.int32),
            vm((parts, TALLY // 2 * LANES), bf16), vm((WIDE, TALLY // 2 * LANES), bf16), vm((parts, WIDE), f32),
            pltpu.SMEM((SLOTS, LANES), jnp.int32), pltpu.SMEM((SLOTS, LANES), jnp.int32), pltpu.SMEM((3, 16), jnp.int32),
            pltpu.SemaphoreType.DMA((2,)),
        ],
        compiler_params=pltpu.CompilerParams(
            vmem_limit_bytes=48 * 1024 * 1024),
        name="walk",
    )(which, sources, weights, lists)


def share_kernel(src, graph, x_ref, o_ref, own_sem, send_sem, recv_sem):
    mine, g, others = place_and_others(src, graph)
    hello(others)
    await_hello(others)
    own = pltpu.make_async_copy(x_ref, o_ref.at[mine], own_sem)
    own.start()
    copies = []
    for n, (py, pg) in enumerate(others):
        copies.append(pltpu.make_async_remote_copy(
            src_ref=x_ref, dst_ref=o_ref.at[mine], send_sem=send_sem.at[n], recv_sem=recv_sem.at[n],
            device_id={"src": py, "graph": pg}, device_id_type=MESH))
        copies[-1].start()
    own.wait()
    for c in copies:
        c.wait()


def share(x, src, graph):
    n = src * graph
    return pl.pallas_call(
        functools.partial(share_kernel, src, graph),
        in_specs=[pl.BlockSpec(memory_space=pltpu.VMEM)],
        out_specs=pl.BlockSpec(memory_space=pltpu.VMEM),
        out_shape=jax.ShapeDtypeStruct((n,) + x.shape, x.dtype),
        scratch_shapes=[pltpu.SemaphoreType.DMA, pltpu.SemaphoreType.DMA((n - 1,)), pltpu.SemaphoreType.DMA((n - 1,))],
        compiler_params=pltpu.CompilerParams(collective_id=2, has_side_effects=True),
        name="share",
    )(x)


def total_kernel(src, graph, x_ref, o_ref, got, own_sem, send_sem, recv_sem):
    mine, g, others = place_and_others(src, graph)
    hello(others)
    own = pltpu.make_async_copy(x_ref.at[g], got.at[mine], own_sem)
    own.start()
    await_hello(others)
    copies = []
    for n, (py, pg) in enumerate(others):
        copies.append(pltpu.make_async_remote_copy(
            src_ref=x_ref.at[pg], dst_ref=got.at[mine], send_sem=send_sem.at[n], recv_sem=recv_sem.at[n],
            device_id={"src": py, "graph": pg}, device_id_type=MESH))
        copies[-1].start()
    own.wait()
    for c in copies:
        c.wait()
    acc = got[0]
    for n in range(1, src * graph):
        acc = acc + got[n]
    o_ref[...] = acc


def total(x, src, graph, collective_id):
    n = src * graph
    return pl.pallas_call(
        functools.partial(total_kernel, src, graph),
        in_specs=[pl.BlockSpec(memory_space=pltpu.VMEM)],
        out_specs=pl.BlockSpec(memory_space=pltpu.VMEM),
        out_shape=jax.ShapeDtypeStruct(x.shape[1:], x.dtype),
        scratch_shapes=[pltpu.VMEM((n,) + x.shape[1:], x.dtype), pltpu.SemaphoreType.DMA,
                        pltpu.SemaphoreType.DMA((n - 1,)), pltpu.SemaphoreType.DMA((n - 1,))],
        compiler_params=pltpu.CompilerParams(collective_id=collective_id, has_side_effects=True),
        name="total",
    )(pltpu.with_memory_space_constraint(x, pltpu.VMEM))


def exchange(x, axis):
    return lax.all_to_all(x, axis, 0, 0)


def dense(adj_slab, src_local, level_weight, src, graph):
    slab_rows, vertex_count = adj_slab.shape
    src_count = src_local.shape[0]
    levels = level_weight.shape[0] + 1
    row_start = lax.axis_index("graph") * slab_rows
    vertex_ids = row_start + lax.broadcasted_iota(jnp.int32, (slab_rows, 1), 0)
    first = jnp.where(vertex_ids == src_local[None, :], 1.0, 0.0).astype(f32)

    def forward(carry, unused):
        sigma, seen = carry
        partial = jnp.einsum("uv,us->vs", adj_slab, sigma, preferred_element_type=f32, precision=exact_precision)
        parts = exchange(partial.reshape(graph, slab_rows, src_count), "graph")
        sigma = jnp.sum(parts, axis=0) * (1.0 - seen)
        seen = jnp.maximum(seen, jnp.where(sigma > 0, 1.0, 0.0))
        return (sigma, seen), sigma

    _, sigmas = lax.scan(forward, (first, first), None, length=levels)

    def backward(carry, xs):
        delta, acc = carry
        upper, lower, weight = xs
        reached = upper > 0
        ratio = jnp.where(reached, (weight + delta) / jnp.where(reached, upper, 1.0), 0.0)
        gathered = exchange(jnp.broadcast_to(ratio[None], (graph,) + ratio.shape), "graph")
        pulled = jnp.einsum("uv,vs->us", adj_slab, gathered.reshape(vertex_count, src_count),
                            preferred_element_type=f32, precision=exact_precision)
        delta = lower * pulled
        return (delta, acc + delta), None

    zero = jnp.zeros_like(first)
    (_, acc), _ = lax.scan(backward, (zero, zero), (sigmas[1:][::-1], sigmas[:-1][::-1], level_weight[::-1]))
    scale = vertex_count / (src_count * src * levels ** 3)
    mine = jnp.sum(acc, axis=1) * scale
    both = exchange(jnp.broadcast_to(mine.reshape(1, -1, LANES), (src, slab_rows // LANES, LANES)), "src")
    return jnp.sum(both, axis=0).reshape(slab_rows)


def solution(mesh):
    src, graph = mesh.shape["src"], mesh.shape["graph"]

    def device_program(adj_slab, src_local, level_weight):
        slab_rows, vertex_count = adj_slab.shape
        levels = level_weight.shape[0] + 1
        scale = vertex_count / (HALF * src * graph * levels ** 3)
        which = lax.axis_index("graph").astype(jnp.int32).reshape(1)

        def finish(lists, compact, collective_id, other):
            parts = walk(which, src_local, level_weight, lists, blocks=graph, vertices=vertex_count, scale=scale, compact=compact)
            summed = total(parts, src, graph, collective_id)
            rows = slab_rows // LANES

            def plain():
                return summed[:rows].reshape(2, -1, LANES).transpose(1, 0, 2).reshape(slab_rows)

            return lax.cond(summed[rows, 0] > 0, other, plain)

        def dense_path():
            return dense(adj_slab, src_local, level_weight, src, graph)

        def general_path():
            half = lax.axis_index("src").astype(jnp.int32).reshape(1)
            lists = share(extract(adj_slab, half, slab_rows // src), src, graph)
            return finish(lists.reshape(-1, SUB, LANES), False, 3, dense_path)

        return finish(collect(adj_slab, src, graph), True, 1, general_path)

    return jax.shard_map(device_program, mesh=mesh,
                         in_specs=(P(("batch", "graph"), None), P(("batch", "src")), P(None)),
                         out_specs=P(("batch", "graph")), check_vma=False)
```

```python
import functools

import jax
import jax.numpy as jnp
from jax import lax
from jax.experimental import pallas as pl
from jax.experimental.pallas import tpu as pltpu
from jax.sharding import PartitionSpec as P

MESH = pl.DeviceIdType.MESH
exact_precision = lax.Precision.HIGHEST
f32, bf16 = jnp.float32, jnp.bfloat16

LANES, SUB = 128, 8
WIDE = 256
DEG, FEW = 8, 4
EMPTY = -2.0
FULL = 32767.0
TURN = (((1,), (1,)), ((), ()))
BLOCK = 128
READS = 4
STEP = 32
HALF = 64
SLOTS = SUB
WINDOW = 48
SCAN = 32
CAP = 1024
TALLY = 96
PAIR = (0, 1)
BYTE = WIDE
MIB = 2 ** 20
GROUP = SUB
PEEL = 32
BASE, COUNT = 0, 1
FAULT, LENGTH, GOT, PARITY, AWAIT0, AWAIT1, REACHED, SHORT0, SHORT1 = ((2, n) for n in range(9))


def place_and_others(src, graph):
    y, g = lax.axis_index("src"), lax.axis_index("graph")
    steps = sorted(((i, k) for i in range(src) for k in range(graph)), key=lambda s: (-s[0], abs(s[1] - graph // 2)))
    return g * src + y, g, [((y + i) % src, (g + k) % graph) for i, k in steps if i + k]


def hello(peers):
    for y, g in peers:
        pl.semaphore_signal(pltpu.get_barrier_semaphore(), inc=1, device_id={"src": y, "graph": g}, device_id_type=MESH)


def await_hello(peers):
    pl.semaphore_wait(pltpu.get_barrier_semaphore(), len(peers))


def place(plane, lists):
    lists = list(lists)
    row_i = lax.broadcasted_iota(jnp.int32, (WIDE, WIDE), 0)
    col_i = lax.broadcasted_iota(jnp.int32, (WIDE, WIDE), 1)
    eye = jnp.where(row_i == col_i, float(WIDE), 0.0).astype(bf16)
    flipped = lax.dot_general(eye, plane, TURN, preferred_element_type=f32)
    lane_id = lax.broadcasted_iota(jnp.int32, (SUB, flipped.shape[1]), 0).astype(f32)
    for g in range(WIDE // SUB):
        x = flipped[g * SUB:(g + 1) * SUB] + (lane_id + float(g * SUB))
        for s in range(len(lists)):
            hi = jnp.maximum(lists[s], x)
            if s < len(lists) - 1:
                x = jnp.minimum(lists[s], x)
            lists[s] = hi
    return lists


def sort(lists):
    gap = len(lists) // 2
    while gap:
        for s in range(len(lists)):
            if not s & gap:
                lists[s], lists[s + gap] = jnp.maximum(lists[s], lists[s + gap]), jnp.minimum(lists[s], lists[s + gap])
        gap //= 2
    return lists


def over_sublanes(lists):
    size = len(lists)
    for shift in (4, 2, 1):
        other = [pltpu.roll(v, shift, 0) for v in lists]
        lists = sort([jnp.maximum(lists[s], other[size - 1 - s]) for s in range(size)])
    out = jnp.full(lists[0].shape, EMPTY, f32)
    sub = lax.broadcasted_iota(jnp.int32, out.shape, 0)
    for s in range(size):
        out = jnp.where(sub == s, jnp.where(lists[s] >= WIDE, lists[s] - WIDE, EMPTY), out)
    return out


def degree_of(seen):
    return lax.dot_general(jnp.ones((SUB, WIDE), bf16), seen, TURN, preferred_element_type=f32)


def collect_kernel(src, graph, a_ref, o_ref, bufs, tops, mine, sems, own_sem, send_sems, recv_sems):
    vertices = a_ref.shape[1]
    pairs, chunks = mine.shape[0], vertices // WIDE
    blocks = 2 * pairs
    me, _, others = place_and_others(src, graph)
    y = me % src
    height = 4 * SUB
    pieces = BLOCK // height

    def fetch(i, t):
        rows = pl.ds(pl.multiple_of((y * blocks + i) * BLOCK + t * height, height), height)
        here = pl.ds(pl.multiple_of(t * height, height), height)
        return pltpu.make_async_copy(a_ref.at[rows], bufs.at[i % READS, here], sems.at[i % READS, t])

    def send(n, first, count):
        py, pg = others[n]
        return pltpu.make_async_remote_copy(
            src_ref=mine.at[pl.ds(first, count)], dst_ref=o_ref.at[pl.ds(me * pairs + first, count)],
            send_sem=send_sems.at[n], recv_sem=recv_sems.at[n], device_id={"src": py, "graph": pg}, device_id_type=MESH)

    def send_pair(p):
        for n in range(len(others)):
            send(n, p, 1).start()

    for i in range(READS - 1):
        for t in range(pieces):
            fetch(i, t).start()
    hello(others)
    none = jnp.zeros((SUB, 2 * BLOCK), f32)

    def scan(i, first):
        @pl.when(i + READS - 1 < blocks)
        def _():
            for t in range(pieces):
                fetch(i + READS - 1, t).start()

        def scan_rows(t, carry):
            fetch(i, t).wait()
            here = pl.ds(pl.multiple_of(t * height, height), height)

            def scan_chunks(c, state):
                top, low, seen, sums, value = state
                for k in range(STEP):
                    a = bufs[i % READS, here, pl.ds(pl.multiple_of((c * STEP + k) * WIDE, WIDE), WIDE)]
                    x = a * value
                    low = jnp.maximum(low, jnp.minimum(top, x))
                    top = jnp.maximum(top, x)
                    seen = seen + a
                    sums = sums + x
                    value = value + 1
                return top, low, seen, sums, value

            zero = jnp.zeros((height, WIDE), bf16)
            top, low, seen, sums, _ = lax.fori_loop(0, chunks // STEP, scan_chunks, (zero,) * 4 + (zero + 1,))
            for n, v in enumerate((top, low, (sums - top) - low, seen)):
                tops[n, pl.ds(pl.multiple_of(first + t * height, height), height), :] = v
            return carry

        lax.fori_loop(0, pieces, scan_rows, 0)

    def pair_step(p, carry):
        for h in range(2):
            scan(2 * p + h, h * BLOCK)
        seen = tops[3]
        crowd = seen[:SUB]
        for k in range(1, 2 * BLOCK // SUB):
            crowd = jnp.maximum(crowd, seen[k * SUB:(k + 1) * SUB])
        crowd = jnp.max(crowd.astype(f32), axis=0, keepdims=True)
        a, b, c = place(tops[0], (none,) * 4), place(tops[1], (none,) * 2), place(tops[2], (none,))
        rest = [jnp.maximum(b[0], c[0]), jnp.minimum(b[0], c[0])]
        rest = [rest[0], jnp.maximum(b[1], rest[1]), jnp.minimum(b[1], rest[1])]
        lists = over_sublanes(sort([a[0]] + [jnp.maximum(a[s + 1], rest[2 - s]) for s in range(3)]))
        lists = jnp.where((crowd > 3) | (degree_of(seen) > 4), FULL, lists)
        even, odd = lists[:, :BLOCK], lists[:, BLOCK:]
        sub = lax.broadcasted_iota(jnp.int32, even.shape, 0)
        mine[p] = jnp.where(sub < 4, even, pltpu.roll(odd, 4, 0))

        @pl.when(p == 1)
        def _():
            await_hello(others)

        @pl.when(p > 0)
        def _():
            send_pair(p - 1)

        return carry

    lax.fori_loop(0, pairs, pair_step, 0)
    own = pltpu.make_async_copy(mine, o_ref.at[pl.ds(me * pairs, pairs)], own_sem)
    send_pair(pairs - 1)
    own.start()
    own.wait()
    for n in range(len(others)):
        send(n, 0, pairs).wait()


def collect(adj_slab, src, graph):
    rows, vertices = adj_slab.shape
    n = src * graph
    mine = (rows // src // (2 * BLOCK), SUB, BLOCK)
    return pl.pallas_call(
        functools.partial(collect_kernel, src, graph),
        in_specs=[pl.BlockSpec(memory_space=pl.ANY)],
        out_specs=pl.BlockSpec(memory_space=pltpu.VMEM),
        out_shape=jax.ShapeDtypeStruct((n * mine[0],) + mine[1:], f32),
        scratch_shapes=[pltpu.VMEM((READS, BLOCK, vertices), bf16), pltpu.VMEM((4, 2 * BLOCK, WIDE), bf16), pltpu.VMEM(mine, f32),
                        pltpu.SemaphoreType.DMA((READS, BLOCK // (4 * SUB))), pltpu.SemaphoreType.DMA,
                        pltpu.SemaphoreType.DMA((n - 1,)), pltpu.SemaphoreType.DMA((n - 1,))],
        compiler_params=pltpu.CompilerParams(collective_id=0, has_side_effects=True, vmem_limit_bytes=40 * MIB),
        name="collect",
    )(adj_slab)


def extract_kernel(half_ref, a_ref, o_ref, block, seen, planes, sem):
    vertices = a_ref.shape[1]

    def block_step(i, carry):
        copy = pltpu.make_async_copy(
            a_ref.at[pl.ds(pl.multiple_of((half_ref[0] * o_ref.shape[0] + i) * BLOCK, BLOCK), BLOCK)], block, sem)
        copy.start()
        copy.wait()
        planes[...] = jnp.zeros_like(planes)
        seen[...] = jnp.zeros_like(seen)

        def scan_chunk(c, carry):
            a = block[:, pl.ds(pl.multiple_of(c * WIDE, WIDE), WIDE)]
            seen[...] = seen[...] + a
            x = a.astype(f32) * (c + 1).astype(f32)
            for s in range(DEG):
                top = planes[s].astype(f32)
                planes[s] = jnp.maximum(top, x).astype(bf16)
                x = jnp.minimum(top, x)
            return carry

        lax.fori_loop(0, vertices // WIDE, scan_chunk, 0)
        lists = lax.fori_loop(0, DEG, lambda p, lists: tuple(place(planes[p], lists)), (jnp.zeros((SUB, BLOCK), f32),) * DEG)
        o_ref[i] = jnp.where(degree_of(seen[...]) > DEG, FULL, over_sublanes(list(lists)))
        return carry

    lax.fori_loop(0, o_ref.shape[0], block_step, 0)


def extract(adj_slab, half, rows):
    vertices = adj_slab.shape[1]
    return pl.pallas_call(
        extract_kernel,
        in_specs=[pl.BlockSpec(memory_space=pltpu.SMEM), pl.BlockSpec(memory_space=pl.ANY)],
        out_specs=pl.BlockSpec(memory_space=pltpu.VMEM),
        out_shape=jax.ShapeDtypeStruct((rows // BLOCK, DEG, BLOCK), f32),
        scratch_shapes=[pltpu.VMEM((BLOCK, vertices), bf16), pltpu.VMEM((BLOCK, WIDE), bf16),
                        pltpu.VMEM((DEG, BLOCK, WIDE), bf16), pltpu.SemaphoreType.DMA],
        name="extract",
    )(half, adj_slab)


def along(shape, axis=0):
    return lax.broadcasted_iota(jnp.int32, shape, axis)


def swap(x):
    return pltpu.roll(x, HALF, 1)


def digits(x, base):
    high = jnp.floor(x * (1.0 / base))
    return high, x - high * base


def walk_kernel(which_ref, src_ref, weight_ref, lists_ref, out_ref,
                table, queue, sigma, ratio, delta, cand, ids, now, dest, tail_ref, held, rowhot, colhot, bins,
                ids_a, ids_b, meta, sems, *, levels, vertices, scale, compact):
    pitch = vertices + SUB
    lane = along((SUB, LANES), 1)
    sub = along((SUB, LANES))
    upper = lane >= HALF
    lane_row = along((1, LANES), 1)
    group_odd = ((lane_row // 32) % 2) == 1
    lane32 = lane_row % 32
    rows_all = queue.shape[0]
    tile_bits = (vertices // lists_ref.shape[0]).bit_length() - 1
    high = vertices // WIDE

    def eight(row):
        return pl.ds(pl.multiple_of(row, SUB), SUB)

    def part(n):
        return pl.ds(n * SUB, SUB)

    def spread_row(ref, *index):
        return jnp.broadcast_to(ref[(*index[:-1], pl.ds(index[-1], 1), slice(None))], (SUB, LANES))

    def clear(t, carry):
        for k in range(SUB):
            rows = eight((t * SUB + k) * SUB)
            queue[rows, :] = jnp.full((SUB, LANES), -1.0, f32)
            sigma[rows, :] = jnp.zeros((SUB, LANES), f32)
        return carry

    def fetch(quad, row, buf):
        return pltpu.make_async_copy(ids.at[quad, eight(row)], buf[0], sems.at[buf[1]])

    def name(row, q):
        v = jnp.where(q < 0, vertices, q.astype(jnp.int32))
        ids[0, eight(row), :] = v
        if not compact:
            ids[1, eight(row), :] = v + pitch

    bufs = (ids_a, 0), (ids_b, 1)
    clear(0, 0)

    near_source = jnp.full((SUB, LANES), EMPTY, f32)
    source = along((SUB, LANES))
    for j in range(HALF):
        v = src_ref[which_ref[0] * HALF + j]
        near_source = jnp.where(lane == j, pltpu.roll(lists_ref[v >> tile_bits], (j - v) & (LANES - 1), 1), near_source)
        source = jnp.where(lane % HALF == j, v, source)
    if compact:
        near_source = jnp.where((source & LANES) > 0, pltpu.roll(near_source, FEW, 0), near_source)
    near_source = jnp.where(upper, swap(near_source), near_source)
    reached = near_source >= 0
    if compact:
        reached = reached & (sub < FEW)
    queue[0:1, :] = source[:1].astype(f32)
    queue[eight(SUB), :] = jnp.where(reached, near_source, -1.0)
    sigma[eight(SUB), :] = jnp.where(reached & jnp.logical_not(upper), 1.0, 0.0)
    for n in (1, 2):
        name(n * SUB, queue[eight(n * SUB), :])
    bins[...] = jnp.zeros_like(bins)
    fetch(0, SUB, bufs[0]).start()
    if compact:
        fetch(0, 2 * SUB, bufs[1]).start()
    eights = rows_all // (SUB * SUB)
    soon_clear = FEW if compact else eights
    lax.fori_loop(1, soon_clear, clear, 0)

    srow = along((2 * SUB, LANES))
    slane = along((2 * SUB, LANES), 1)

    def fill(halves, target):
        picks = [jnp.where((srow % SUB) == (slane // 32 + FEW * h), jnp.where(srow < SUB, float(LANES), 1.0), 0.0).astype(bf16)
                 for h in halves]

        def body(step, most):
            for k in range(GROUP):
                first = (GROUP * step + k) * SUB
                x = jnp.concatenate([lists_ref[first + n] for n in range(SUB)], axis=1)
                both = jnp.concatenate(digits(x, LANES), axis=0).astype(bf16)
                for h, pick in zip(halves, picks):
                    rows = lax.dot_general(both, pick, (((0,), (0,)), ((), ())), preferred_element_type=f32)
                    for n in range(SUB):
                        table[pl.ds(pl.multiple_of(target(h, first + n), SUB), LANES), :] = rows[n * LANES:(n + 1) * LANES]
                for n in range(SUB):
                    most = jnp.maximum(most, lists_ref[first + n])
            return most

        return lax.fori_loop(0, lists_ref.shape[0] // (GROUP * SUB), body, jnp.full((SUB, LANES), EMPTY, f32))

    table[vertices:pitch, :] = jnp.full((SUB, LANES), EMPTY, f32)
    if compact:
        most = fill(PAIR, lambda h, t: (2 * t + h) * LANES)
        quads = 1
    else:
        table[pitch + vertices:, :] = jnp.full((SUB, LANES), EMPTY, f32)
        most = fill((0,), lambda h, t: t * LANES)
        wide = jnp.max(jnp.where(sub >= FEW, most, EMPTY)) >= 0
        quads = jnp.where(wide, 2, 1)

        @pl.when(wide)
        def _():
            fill((1,), lambda h, t: pitch + t * LANES)

    bad = jnp.max(most) > vertices
    meta[FAULT] = bad.astype(jnp.int32)

    def gather(rows_of_ids):
        acc = [[jnp.full((1, LANES), EMPTY, f32)] * 2 for _ in rows_of_ids]
        for j in range(32):
            hit = lane32 == j
            for i, id_of in enumerate(rows_of_ids):
                for b in PAIR:
                    acc[i][b] = jnp.where(hit, table[pl.ds(id_of(b * 32 + j), 1), :], acc[i][b])
        return [(jnp.where(group_odd, b, a), pltpu.roll(jnp.where(group_odd, a, b), LANES - 32, 1)) for a, b in acc]

    def gather_slots(ids_s, slots=SLOTS):
        return gather([functools.partial(lambda i, j: ids_s[i, j], i) for i in range(slots)])

    def keep(rows, quad, row):
        for i, pair in enumerate(rows):
            for h in PAIR:
                cand[2 * quad + h, pl.ds(row + i, 1), :] = pair[h]

    def flag(x):
        return jnp.where(x, 1, 0)

    def at(unit, origin):
        return unit & (quads - 1), origin + (unit >> (quads - 1)) * SUB

    def level_step(level, carry):
        base, count = meta[BASE, level], meta[COUNT, level]
        following = base + (count + 7) // SUB * SUB
        batches = jnp.where(following <= CAP, (count + SLOTS - 1) // SLOTS, 0)
        units = batches * quads
        parity = meta[PARITY]

        def on_parity(n, f):
            for k in PAIR:
                @pl.when(n & 1 == k)
                def _():
                    f(bufs[k], bufs[1 - k])

        def unit_step(unit, other, to):
            quad, row = at(unit, base)
            x = [cand[2 * quad + h, eight(row), :] for h in PAIR]

            def search(first, count, marks):
                marks = list(marks)
                for k in range(count):
                    q = spread_row(queue, first + k)
                    for h in PAIR:
                        n = 2 * h + k % 2
                        marks[n] = jnp.where(x[h] == q, 1, marks[n])
                return tuple(marks)

            reach = following + meta[LENGTH] - PEEL
            marks = lax.fori_loop(0, (reach + SCAN - 1) // SCAN, lambda t, m: search(PEEL + t * SCAN, SCAN, m),
                                  (jnp.zeros((SUB, LANES), jnp.int32),) * 4)
            ahead = unit + 1 < units
            final_unit = unit + 1 == units
            soon = jnp.logical_and(final_unit, meta[AWAIT0] > 0)

            @pl.when(jnp.logical_or(ahead, soon))
            def _():
                fetch(0, base, to).wait()

            def insert(g):
                slots = [eight(following + g * WINDOW + SUB * t) for t in range(WINDOW // SUB)]
                qs = [queue[r, :] for r in slots]
                ss = [sigma[r, :] for r in slots]
                pos = [sub + (g * WINDOW + SUB * t) for t in range(WINDOW // SUB)]
                for h in PAIR:
                    for i in range(SUB):
                        d, e = spread_row(dest, SUB * h + i), spread_row(dest, SUB * (h + 2) + i)
                        v, w = spread_row(now, SUB * h + i), spread_row(now, SUB * (h + 2) + i)
                        for t in range(WINDOW // SUB):
                            qs[t] = jnp.where(pos[t] == d, v, jnp.where(pos[t] == e, w, qs[t]))
                for i in range(SUB):
                    v, w, sig = (spread_row(now, SUB * n + i) for n in (0, 1, 4))
                    for t in range(WINDOW // SUB):
                        ss[t] = ss[t] + jnp.where((qs[t] == v) | (qs[t] == w), sig, 0.0)
                for t, r in enumerate(slots):
                    queue[r, :] = qs[t]
                    sigma[r, :] = ss[t]
                return qs

            def core(looking):
                even, odd = x
                m, n, k, l = search(0, PEEL, marks)
                near_even, near_odd = m | n | flag(even < 0), k | l | flag(odd < 0)

                xr = [swap(v) for v in x]
                turns = [[[pltpu.roll(v, s, 0) if s else v for v in (x[h], xr[h])] for s in range(SUB)] for h in PAIR]
                for s, ((a, b), (c, d)) in enumerate(zip(*turns)):
                    near_odd = jnp.where((odd == a) | (odd == b), 1, near_odd)
                    if s:
                        after = sub >= s
                        near_even = jnp.where(((even == a) | (even == b)) & after, 1, near_even)
                        near_odd = jnp.where(((odd == c) | (odd == d)) & after, 1, near_odd)

                new = [1 - near_even, 1 - near_odd]
                packed = new[0] + BYTE * new[1]
                across = swap(packed)
                far = [across & (BYTE - 1), across >> SUB]
                both = packed + across
                run, whole = both, both
                for s in (1, 2, 4):
                    run = run + jnp.where(sub >= s, pltpu.roll(run, s, 0), 0)
                    whole = whole + pltpu.roll(whole, s, 0)
                run = run - both
                tail = tail_ref[...]
                evens = whole & (BYTE - 1)
                begin = [tail + (run & (BYTE - 1)), tail + evens + (run >> SUB)]
                for h in PAIR:
                    dest[part(h), :] = jnp.where(new[h] > 0, begin[h] + jnp.where(upper, far[h], 0), -1)
                    dest[part(h + 2), :] = jnp.where(far[h] > 0, begin[h] + jnp.where(upper, 0, new[h]), -1)
                    now[part(h), :] = x[h]
                    now[part(h + 2), :] = xr[h]
                now[part(4), :] = sigma[eight(row), :] + swap(sigma[eight(row), :])
                tail = tail + evens + (whole >> SUB)
                tail_ref[...] = tail
                passed = SLOTS * ((unit + 1) >> (quads - 1))
                second = SUB + SUB * (1 >> (quads - 1))
                need = jnp.where(sub == 1, SUB, second)
                short = (tail < need) & (held[...] > passed)
                most = jnp.max(jnp.where(sub == 0, tail, flag(short)).astype(f32), axis=1, keepdims=True)
                meta[REACHED] = most[0, 0].astype(jnp.int32)
                for n in PAIR:
                    meta[(SHORT0, SHORT1)[n]] = most[n + 1, 0].astype(jnp.int32)

                if looking:
                    quad2, row2 = at(unit + 1, base)
                    rows = gather_slots(to[0])
                qs = insert(0)
                for n in PAIR:
                    name(following + n * SUB, qs[n])
                if looking:
                    keep(rows, jnp.where(ahead, quad2, 0), jnp.where(ahead, row2, following))

            look = jnp.logical_or(ahead, soon)
            for looking in PAIR:
                @pl.when(look == (looking > 0))
                def _():
                    core(looking)

            length = meta[REACHED]
            ready = [meta[n] == 0 for n in (SHORT0, SHORT1)]

            @pl.when(unit + 3 < units)
            def _():
                fetch(*at(unit + 3, base), to).start()

            @pl.when(soon)
            def _():
                meta[GOT] = 1

            def first_of_next(n, when, buf):
                @pl.when(jnp.logical_and(when, meta[(AWAIT0, AWAIT1)[n]] == 0))
                def _():
                    fetch(*at(n, following), buf).start()
                    meta[(AWAIT0, AWAIT1)[n]] = 1

            first_of_next(0, jnp.logical_and(ready[0], unit + 3 == units), to)
            first_of_next(0, jnp.logical_and(ready[0], unit + 2 == units), other)
            first_of_next(1, jnp.logical_and(ready[1], unit + 2 == units), to)
            first_of_next(0, final_unit, to)
            first_of_next(1, final_unit, other)

            groups = (length + WINDOW - 1) // WINDOW
            fits = following + groups * WINDOW <= CAP + WINDOW
            meta[LENGTH] = jnp.where(fits, length, 0)

            @pl.when(jnp.logical_not(fits))
            def _():
                meta[FAULT] = 1

            def more(g, carry):
                insert(g)
                return carry

            lax.fori_loop(1, jnp.where(fits, groups, 0), more, 0)

        tail_ref[...] = jnp.zeros_like(tail_ref)
        meta[LENGTH] = 0

        def open_level(mine, other):
            @pl.when(jnp.logical_and(meta[GOT] == 0, meta[AWAIT0] > 0))
            def _():
                fetch(0, base, mine).wait()
                keep(gather_slots(mine[0]), 0, base)

            @pl.when(jnp.logical_and(units < 2, meta[AWAIT1] > 0))
            def _():
                fetch(0, base, other).wait()

            @pl.when(units > 2)
            def _():
                fetch(*at(2, base), mine).start()

        if compact:
            @pl.when(level == 2)
            def _():
                lax.fori_loop(soon_clear, eights, clear, 0)

        on_parity(parity, open_level)
        for place_ in (GOT, AWAIT0, AWAIT1):
            meta[place_] = 0

        def any_unit(unit, carry):
            on_parity(parity + unit, functools.partial(unit_step, unit))
            return carry

        lax.fori_loop(0, units, any_unit, 0)
        meta[PARITY] = parity + units

        @pl.when(following > CAP)
        def _():
            meta[FAULT] = 1

        found = jnp.where(meta[FAULT] == 0, meta[LENGTH], 0)
        meta[BASE, level + 1] = following
        meta[COUNT, level + 1] = found

        def names(t, carry):
            row = following + t * SUB
            name(row, queue[eight(row), :])
            return carry

        for t in range(2, WINDOW // SUB):
            names(t, carry)
        lax.fori_loop(WINDOW // SUB, (found + SUB - 1) // SUB, names, 0)
        held[...] = tail_ref[...]
        return carry

    for place_ in (GOT, PARITY):
        meta[place_] = 0

    @pl.when(jnp.logical_not(bad))
    def _():
        held[...] = jnp.full_like(held, FEW * quads)
        meta[BASE, 1] = SUB
        meta[COUNT, 1] = FEW * quads
        fetch(0, SUB, bufs[0]).wait()
        if compact:
            for h in PAIR:
                cand[h, eight(SUB), :] = jnp.full((SUB, LANES), EMPTY, f32)
        else:
            fetch(*at(1, SUB), bufs[1]).start()
        keep(gather_slots(ids_a, FEW if compact else SLOTS), 0, SUB)
        meta[GOT] = 1
        meta[AWAIT0] = 0
        meta[AWAIT1] = 1
        lax.fori_loop(1, levels, level_step, 0)

    @pl.when(bad)
    def _():
        fetch(0, SUB, bufs[0]).wait()
        meta[AWAIT0] = 0
        meta[AWAIT1] = int(compact)

    def drain(n, buf):
        @pl.when(meta[(AWAIT0, AWAIT1)[n]] > 0)
        def _():
            fetch(0, 0, buf).wait()

    for k in PAIR:
        @pl.when(meta[PARITY] & 1 == k)
        def _():
            @pl.when(meta[GOT] == 0)
            def _():
                drain(0, bufs[k])

            drain(1, bufs[1 - k])

    good = meta[FAULT] == 0

    @pl.when(good)
    def _():
        last = meta[BASE, levels]
        g_last = weight_ref[levels - 2]

        def seed(g, carry):
            for t in range(WINDOW // SUB):
                r = eight(last + g * WINDOW + SUB * t)
                s = sigma[r, :] + swap(sigma[r, :])
                ratio[r, :] = jnp.where(s > 0, g_last / jnp.where(s > 0, s, 1.0), 0.0)
            return carry

        lax.fori_loop(0, (meta[COUNT, levels] + WINDOW - 1) // WINDOW, seed, 0)

        def back_step(k, carry):
            level = levels - 1 - k
            base, count = meta[BASE, level], meta[COUNT, level]
            nbase, ncount = meta[BASE, level + 1], meta[COUNT, level + 1]
            g_here = weight_ref[jnp.maximum(level - 2, 0)]

            def pull_batch(bt, carry):
                here = eight(base + bt * SLOTS)

                def pull(quad, c, acc):
                    even, odd = cand[2 * quad, here, :], cand[2 * quad + 1, here, :]
                    acc = list(acc)
                    for n in range(WINDOW):
                        q = spread_row(queue, nbase + c * WINDOW + n)
                        w = spread_row(ratio, nbase + c * WINDOW + n)
                        acc[n % 2] = acc[n % 2] + jnp.where((even == q) | (odd == q), w, 0.0)
                    return tuple(acc)

                def pull_quad(quad, acc):
                    return lax.fori_loop(1, (ncount + WINDOW - 1) // WINDOW, functools.partial(pull, quad), pull(quad, 0, acc))

                acc = pull_quad(0, (jnp.zeros((SUB, LANES), f32),) * 2)
                if not compact:
                    acc = lax.fori_loop(1, quads, pull_quad, acc)
                delta[here, :] = acc[0] + acc[1]
                return carry

            lax.fori_loop(0, (count + SLOTS - 1) // SLOTS, pull_batch, 0)

            def finish(g, carry):
                slots = [eight(base + g * WINDOW + SUB * t) for t in range(WINDOW // SUB)]
                for t, r in enumerate(slots):
                    inside = g * WINDOW + SUB * t < count
                    part, s = (v + swap(v) for v in (delta[r, :], sigma[r, :]))
                    d = s * part
                    w = jnp.where(s > 0, (g_here + d) / jnp.where(s > 0, s, 1.0), 0.0)
                    delta[r, :] = jnp.where(inside, d, delta[r, :])
                    ratio[r, :] = jnp.where(inside, w, ratio[r, :])
                return carry

            lax.fori_loop(0, (count + WINDOW - 1) // WINDOW, finish, 0)
            return carry

        lax.fori_loop(0, levels - 1, back_step, 0)

        tall = along((WIDE, WIDE)).astype(f32).astype(bf16)
        zero = jnp.zeros((WIDE, WIDE), bf16)
        one = zero + 1
        start = meta[BASE, 1]

        def tally(t, carry):
            for u in range(TALLY // 16):
                a, b = eight(start + t * TALLY + u * 16), eight(start + t * TALLY + u * 16 + SUB)
                v = jnp.where(upper, queue[b, :], queue[a, :])
                d = jnp.where(upper, delta[b, :], delta[a, :])
                hi, lo = digits(v, WIDE)
                d_hi = d.astype(bf16).astype(f32)
                d_mid = (d - d_hi).astype(bf16).astype(f32)
                d_lo = d - d_hi - d_mid
                for p in range(0, SUB, 2):
                    cols = slice((u * SUB + p) * LANES, (u * SUB + p + 2) * LANES)

                    def pair(x):
                        return jnp.concatenate([x[p:p + 1], x[p + 1:p + 2]], axis=1).astype(bf16)

                    colhot[:, cols] = jnp.where(tall == pair(lo), one, zero)
                    match = tall[:high] == pair(hi)
                    for n, x in enumerate((d_hi, d_mid, d_lo)):
                        rowhot[n * high:(n + 1) * high, cols] = jnp.where(match, pair(x), zero[:high])
            bins[...] += lax.dot_general(rowhot[...], colhot[...], TURN, preferred_element_type=f32)
            return carry

        for t in range(TALLY // SUB):
            delta[eight(last + t * SUB), :] = jnp.zeros((SUB, LANES), f32)
        lax.fori_loop(0, (last - start + TALLY - 1) // TALLY, tally, 0)

    blocks = out_ref.shape[0]
    per = high // blocks
    total = (bins[:high] + bins[high:2 * high] + bins[2 * high:]) * scale
    fault = jnp.where(good, 0.0, 1.0)
    for b in range(blocks):
        for n in PAIR:
            out_ref[b, n * per:(n + 1) * per, :] = total[b * per:(b + 1) * per, n * LANES:(n + 1) * LANES]
        out_ref[b, 2 * per:, :] = jnp.full((1, LANES), fault, f32)


def walk(which, sources, weights, lists, *, blocks, vertices, scale, compact):
    levels = weights.shape[0] + 1
    rows = CAP + 4 * WINDOW
    high = LANES // blocks + 1
    vm = pltpu.VMEM
    queue = vm((rows, LANES), f32)
    parts = 3 * (vertices // WIDE)
    return pl.pallas_call(
        functools.partial(walk_kernel, levels=levels, vertices=vertices, scale=scale, compact=compact),
        in_specs=[pl.BlockSpec(memory_space=pltpu.SMEM)] * 3 + [pl.BlockSpec(memory_space=pltpu.VMEM)],
        out_specs=pl.BlockSpec(memory_space=pltpu.VMEM),
        out_shape=jax.ShapeDtypeStruct((blocks, high, LANES), f32),
        scratch_shapes=[
            vm(((1 if compact else 2) * (vertices + SUB), LANES), f32), queue, queue, queue, queue,
            vm((4, rows, LANES), f32), vm((2, rows, LANES), jnp.int32),
            vm((40, LANES), f32), vm((32, LANES), jnp.int32), vm((SUB, LANES), jnp.int32), vm((SUB, LANES), jnp.int32),
            vm((parts, TALLY // 2 * LANES), bf16), vm((WIDE, TALLY // 2 * LANES), bf16), vm((parts, WIDE), f32),
            pltpu.SMEM((SLOTS, LANES), jnp.int32), pltpu.SMEM((SLOTS, LANES), jnp.int32), pltpu.SMEM((3, 16), jnp.int32),
            pltpu.SemaphoreType.DMA((2,)),
        ],
        compiler_params=pltpu.CompilerParams(
            vmem_limit_bytes=48 * MIB),
        name="walk",
    )(which, sources, weights, lists)


def share_kernel(src, graph, x_ref, o_ref, own_sem, send_sem, recv_sem):
    mine, g, others = place_and_others(src, graph)
    hello(others)
    await_hello(others)
    own = pltpu.make_async_copy(x_ref, o_ref.at[mine], own_sem)
    own.start()
    copies = []
    for n, (py, pg) in enumerate(others):
        copies.append(pltpu.make_async_remote_copy(
            src_ref=x_ref, dst_ref=o_ref.at[mine], send_sem=send_sem.at[n], recv_sem=recv_sem.at[n],
            device_id={"src": py, "graph": pg}, device_id_type=MESH))
        copies[-1].start()
    own.wait()
    for c in copies:
        c.wait()


def share(x, src, graph):
    n = src * graph
    return pl.pallas_call(
        functools.partial(share_kernel, src, graph),
        in_specs=[pl.BlockSpec(memory_space=pltpu.VMEM)],
        out_specs=pl.BlockSpec(memory_space=pltpu.VMEM),
        out_shape=jax.ShapeDtypeStruct((n,) + x.shape, x.dtype),
        scratch_shapes=[pltpu.SemaphoreType.DMA, pltpu.SemaphoreType.DMA((n - 1,)), pltpu.SemaphoreType.DMA((n - 1,))],
        compiler_params=pltpu.CompilerParams(collective_id=2, has_side_effects=True),
        name="share",
    )(x)


def total_kernel(src, graph, x_ref, o_ref, got, own_sem, send_sem, recv_sem):
    mine, g, others = place_and_others(src, graph)
    hello(others)
    own = pltpu.make_async_copy(x_ref.at[g], got.at[mine], own_sem)
    own.start()
    await_hello(others)
    copies = []
    for n, (py, pg) in enumerate(others):
        copies.append(pltpu.make_async_remote_copy(
            src_ref=x_ref.at[pg], dst_ref=got.at[mine], send_sem=send_sem.at[n], recv_sem=recv_sem.at[n],
            device_id={"src": py, "graph": pg}, device_id_type=MESH))
        copies[-1].start()
    own.wait()
    for c in copies:
        c.wait()
    acc = got[0]
    for n in range(1, src * graph):
        acc = acc + got[n]
    o_ref[...] = acc


def total(x, src, graph, collective_id):
    n = src * graph
    return pl.pallas_call(
        functools.partial(total_kernel, src, graph),
        in_specs=[pl.BlockSpec(memory_space=pltpu.VMEM)],
        out_specs=pl.BlockSpec(memory_space=pltpu.VMEM),
        out_shape=jax.ShapeDtypeStruct(x.shape[1:], x.dtype),
        scratch_shapes=[pltpu.VMEM((n,) + x.shape[1:], x.dtype), pltpu.SemaphoreType.DMA,
                        pltpu.SemaphoreType.DMA((n - 1,)), pltpu.SemaphoreType.DMA((n - 1,))],
        compiler_params=pltpu.CompilerParams(collective_id=collective_id, has_side_effects=True),
        name="total",
    )(pltpu.with_memory_space_constraint(x, pltpu.VMEM))


def exchange(x, axis):
    return lax.all_to_all(x, axis, 0, 0)


def dense(adj_slab, src_local, level_weight, src, graph):
    slab_rows, vertex_count = adj_slab.shape
    src_count = src_local.shape[0]
    levels = level_weight.shape[0] + 1
    row_start = lax.axis_index("graph") * slab_rows
    vertex_ids = row_start + lax.broadcasted_iota(jnp.int32, (slab_rows, 1), 0)
    first = jnp.where(vertex_ids == src_local[None, :], 1.0, 0.0).astype(f32)

    def forward(carry, unused):
        sigma, seen = carry
        partial = jnp.einsum("uv,us->vs", adj_slab, sigma, preferred_element_type=f32, precision=exact_precision)
        parts = exchange(partial.reshape(graph, slab_rows, src_count), "graph")
        sigma = jnp.sum(parts, axis=0) * (1.0 - seen)
        seen = jnp.maximum(seen, jnp.where(sigma > 0, 1.0, 0.0))
        return (sigma, seen), sigma

    _, sigmas = lax.scan(forward, (first, first), None, length=levels)

    def backward(carry, xs):
        delta, acc = carry
        upper, lower, weight = xs
        reached = upper > 0
        ratio = jnp.where(reached, (weight + delta) / jnp.where(reached, upper, 1.0), 0.0)
        gathered = exchange(jnp.broadcast_to(ratio[None], (graph,) + ratio.shape), "graph")
        pulled = jnp.einsum("uv,vs->us", adj_slab, gathered.reshape(vertex_count, src_count),
                            preferred_element_type=f32, precision=exact_precision)
        delta = lower * pulled
        return (delta, acc + delta), None

    zero = jnp.zeros_like(first)
    (_, acc), _ = lax.scan(backward, (zero, zero), (sigmas[1:][::-1], sigmas[:-1][::-1], level_weight[::-1]))
    scale = vertex_count / (src_count * src * levels ** 3)
    mine = jnp.sum(acc, axis=1) * scale
    both = exchange(jnp.broadcast_to(mine.reshape(1, -1, LANES), (src, slab_rows // LANES, LANES)), "src")
    return jnp.sum(both, axis=0).reshape(slab_rows)


def solution(mesh):
    src, graph = mesh.shape["src"], mesh.shape["graph"]

    def device_program(adj_slab, src_local, level_weight):
        slab_rows, vertex_count = adj_slab.shape
        levels = level_weight.shape[0] + 1
        scale = vertex_count / (HALF * src * graph * levels ** 3)
        which = lax.axis_index("graph").astype(jnp.int32).reshape(1)

        def finish(lists, compact, collective_id, other):
            parts = walk(which, src_local, level_weight, lists, blocks=graph, vertices=vertex_count, scale=scale, compact=compact)
            summed = total(parts, src, graph, collective_id)
            rows = slab_rows // LANES

            def plain():
                return summed[:rows].reshape(2, -1, LANES).transpose(1, 0, 2).reshape(slab_rows)

            return lax.cond(summed[rows, 0] > 0, other, plain)

        def dense_path():
            return dense(adj_slab, src_local, level_weight, src, graph)

        def general_path():
            half = lax.axis_index("src").astype(jnp.int32).reshape(1)
            lists = share(extract(adj_slab, half, slab_rows // src), src, graph)
            return finish(lists.reshape(-1, SUB, LANES), False, 3, dense_path)

        return finish(collect(adj_slab, src, graph), True, 1, general_path)

    return jax.shard_map(device_program, mesh=mesh,
                         in_specs=(P(("batch", "graph"), None), P(("batch", "src")), P(None)),
                         out_specs=P(("batch", "graph")), check_vma=False)
```

```python
import functools

import jax
import jax.numpy as jnp
from jax import lax
from jax.experimental import pallas as pl
from jax.experimental.pallas import tpu as pltpu
from jax.sharding import PartitionSpec as P

MESH = pl.DeviceIdType.MESH
exact_precision = lax.Precision.HIGHEST
f32, bf16 = jnp.float32, jnp.bfloat16

LANES, SUB = 128, 8
WIDE = 256
DEG, FEW = 8, 4
EMPTY = -2.0
FULL = 32767.0
TURN = (((1,), (1,)), ((), ()))
BLOCK = 128
READS = 6
STEP = 32
HALF = 64
SLOTS = SUB
WINDOW = 48
SCAN = 32
CAP = 1024
TALLY = 96
PAIR = (0, 1)
BYTE = WIDE
MIB = 2 ** 20
GROUP = SUB
PEEL = 32
BASE, COUNT = 0, 1
FAULT, LENGTH, GOT, PARITY, AWAIT0, AWAIT1, REACHED, SHORT0, SHORT1 = ((2, n) for n in range(9))


def place_and_others(src, graph):
    y, g = lax.axis_index("src"), lax.axis_index("graph")
    steps = sorted(((i, k) for i in range(src) for k in range(graph)), key=lambda s: (-s[0], abs(s[1] - graph // 2)))
    return g * src + y, g, [((y + i) % src, (g + k) % graph) for i, k in steps if i + k]


def hello(peers):
    for y, g in peers:
        pl.semaphore_signal(pltpu.get_barrier_semaphore(), inc=1, device_id={"src": y, "graph": g}, device_id_type=MESH)


def await_hello(peers):
    pl.semaphore_wait(pltpu.get_barrier_semaphore(), len(peers))


def place(plane, lists):
    lists = list(lists)
    row_i = lax.broadcasted_iota(jnp.int32, (WIDE, WIDE), 0)
    col_i = lax.broadcasted_iota(jnp.int32, (WIDE, WIDE), 1)
    eye = jnp.where(row_i == col_i, float(WIDE), 0.0).astype(bf16)
    flipped = lax.dot_general(eye, plane, TURN, preferred_element_type=f32)
    lane_id = lax.broadcasted_iota(jnp.int32, (SUB, flipped.shape[1]), 0).astype(f32)
    for g in range(WIDE // SUB):
        x = flipped[g * SUB:(g + 1) * SUB] + (lane_id + float(g * SUB))
        for s in range(len(lists)):
            hi = jnp.maximum(lists[s], x)
            if s < len(lists) - 1:
                x = jnp.minimum(lists[s], x)
            lists[s] = hi
    return lists


def sort(lists):
    gap = len(lists) // 2
    while gap:
        for s in range(len(lists)):
            if not s & gap:
                lists[s], lists[s + gap] = jnp.maximum(lists[s], lists[s + gap]), jnp.minimum(lists[s], lists[s + gap])
        gap //= 2
    return lists


def over_sublanes(lists):
    size = len(lists)
    for shift in (4, 2, 1):
        other = [pltpu.roll(v, shift, 0) for v in lists]
        lists = sort([jnp.maximum(lists[s], other[size - 1 - s]) for s in range(size)])
    out = jnp.full(lists[0].shape, EMPTY, f32)
    sub = lax.broadcasted_iota(jnp.int32, out.shape, 0)
    for s in range(size):
        out = jnp.where(sub == s, jnp.where(lists[s] >= WIDE, lists[s] - WIDE, EMPTY), out)
    return out


def degree_of(seen):
    return lax.dot_general(jnp.ones((SUB, WIDE), bf16), seen, TURN, preferred_element_type=f32)


def collect_kernel(src, graph, a_ref, o_ref, bufs, tops, mine, sems, own_sem, send_sems, recv_sems):
    vertices = a_ref.shape[1]
    pairs, chunks = mine.shape[0], vertices // WIDE
    blocks = 2 * pairs
    me, _, others = place_and_others(src, graph)
    y = me % src
    height = 4 * SUB
    pieces = BLOCK // height

    def fetch(i, t):
        rows = pl.ds(pl.multiple_of((y * blocks + i) * BLOCK + t * height, height), height)
        here = pl.ds(pl.multiple_of(t * height, height), height)
        return pltpu.make_async_copy(a_ref.at[rows], bufs.at[i % READS, here], sems.at[i % READS, t])

    def send(n, first, count):
        py, pg = others[n]
        return pltpu.make_async_remote_copy(
            src_ref=mine.at[pl.ds(first, count)], dst_ref=o_ref.at[pl.ds(me * pairs + first, count)],
            send_sem=send_sems.at[n], recv_sem=recv_sems.at[n], device_id={"src": py, "graph": pg}, device_id_type=MESH)

    def send_pair(p):
        for n in range(len(others)):
            send(n, p, 1).start()

    for i in range(READS - 1):
        for t in range(pieces):
            fetch(i, t).start()
    hello(others)
    none = jnp.zeros((SUB, 2 * BLOCK), f32)

    def scan(i, first):
        @pl.when(i + READS - 1 < blocks)
        def _():
            for t in range(pieces):
                fetch(i + READS - 1, t).start()

        def scan_rows(t, carry):
            fetch(i, t).wait()
            here = pl.ds(pl.multiple_of(t * height, height), height)

            def scan_chunks(c, state):
                top, low, seen, sums, value = state
                for k in range(STEP):
                    a = bufs[i % READS, here, pl.ds(pl.multiple_of((c * STEP + k) * WIDE, WIDE), WIDE)]
                    x = a * value
                    low = jnp.maximum(low, jnp.minimum(top, x))
                    top = jnp.maximum(top, x)
                    seen = seen + a
                    sums = sums + x
                    value = value + 1
                return top, low, seen, sums, value

            zero = jnp.zeros((height, WIDE), bf16)
            top, low, seen, sums, _ = lax.fori_loop(0, chunks // STEP, scan_chunks, (zero,) * 4 + (zero + 1,))
            for n, v in enumerate((top, low, (sums - top) - low, seen)):
                tops[n, pl.ds(pl.multiple_of(first + t * height, height), height), :] = v
            return carry

        lax.fori_loop(0, pieces, scan_rows, 0)

    def pair_step(p, carry):
        for h in range(2):
            scan(2 * p + h, h * BLOCK)
        seen = tops[3]
        crowd = seen[:SUB]
        for k in range(1, 2 * BLOCK // SUB):
            crowd = jnp.maximum(crowd, seen[k * SUB:(k + 1) * SUB])
        crowd = jnp.max(crowd.astype(f32), axis=0, keepdims=True)
        a, b, c = place(tops[0], (none,) * 4), place(tops[1], (none,) * 2), place(tops[2], (none,))
        rest = [jnp.maximum(b[0], c[0]), jnp.minimum(b[0], c[0])]
        rest = [rest[0], jnp.maximum(b[1], rest[1]), jnp.minimum(b[1], rest[1])]
        lists = over_sublanes(sort([a[0]] + [jnp.maximum(a[s + 1], rest[2 - s]) for s in range(3)]))
        lists = jnp.where((crowd > 3) | (degree_of(seen) > 4), FULL, lists)
        even, odd = lists[:, :BLOCK], lists[:, BLOCK:]
        sub = lax.broadcasted_iota(jnp.int32, even.shape, 0)
        mine[p] = jnp.where(sub < 4, even, pltpu.roll(odd, 4, 0))

        @pl.when(p == 1)
        def _():
            await_hello(others)

        @pl.when(p > 0)
        def _():
            send_pair(p - 1)

        return carry

    lax.fori_loop(0, pairs, pair_step, 0)
    own = pltpu.make_async_copy(mine, o_ref.at[pl.ds(me * pairs, pairs)], own_sem)
    send_pair(pairs - 1)
    own.start()
    own.wait()
    for n in range(len(others)):
        send(n, 0, pairs).wait()


def collect(adj_slab, src, graph):
    rows, vertices = adj_slab.shape
    n = src * graph
    mine = (rows // src // (2 * BLOCK), SUB, BLOCK)
    return pl.pallas_call(
        functools.partial(collect_kernel, src, graph),
        in_specs=[pl.BlockSpec(memory_space=pl.ANY)],
        out_specs=pl.BlockSpec(memory_space=pltpu.VMEM),
        out_shape=jax.ShapeDtypeStruct((n * mine[0],) + mine[1:], f32),
        scratch_shapes=[pltpu.VMEM((READS, BLOCK, vertices), bf16), pltpu.VMEM((4, 2 * BLOCK, WIDE), bf16), pltpu.VMEM(mine, f32),
                        pltpu.SemaphoreType.DMA((READS, BLOCK // (4 * SUB))), pltpu.SemaphoreType.DMA,
                        pltpu.SemaphoreType.DMA((n - 1,)), pltpu.SemaphoreType.DMA((n - 1,))],
        compiler_params=pltpu.CompilerParams(collective_id=0, has_side_effects=True, vmem_limit_bytes=40 * MIB),
        name="collect",
    )(adj_slab)


def extract_kernel(half_ref, a_ref, o_ref, block, seen, planes, sem):
    vertices = a_ref.shape[1]

    def block_step(i, carry):
        copy = pltpu.make_async_copy(
            a_ref.at[pl.ds(pl.multiple_of((half_ref[0] * o_ref.shape[0] + i) * BLOCK, BLOCK), BLOCK)], block, sem)
        copy.start()
        copy.wait()
        planes[...] = jnp.zeros_like(planes)
        seen[...] = jnp.zeros_like(seen)

        def scan_chunk(c, carry):
            a = block[:, pl.ds(pl.multiple_of(c * WIDE, WIDE), WIDE)]
            seen[...] = seen[...] + a
            x = a.astype(f32) * (c + 1).astype(f32)
            for s in range(DEG):
                top = planes[s].astype(f32)
                planes[s] = jnp.maximum(top, x).astype(bf16)
                x = jnp.minimum(top, x)
            return carry

        lax.fori_loop(0, vertices // WIDE, scan_chunk, 0)
        lists = lax.fori_loop(0, DEG, lambda p, lists: tuple(place(planes[p], lists)), (jnp.zeros((SUB, BLOCK), f32),) * DEG)
        o_ref[i] = jnp.where(degree_of(seen[...]) > DEG, FULL, over_sublanes(list(lists)))
        return carry

    lax.fori_loop(0, o_ref.shape[0], block_step, 0)


def extract(adj_slab, half, rows):
    vertices = adj_slab.shape[1]
    return pl.pallas_call(
        extract_kernel,
        in_specs=[pl.BlockSpec(memory_space=pltpu.SMEM), pl.BlockSpec(memory_space=pl.ANY)],
        out_specs=pl.BlockSpec(memory_space=pltpu.VMEM),
        out_shape=jax.ShapeDtypeStruct((rows // BLOCK, DEG, BLOCK), f32),
        scratch_shapes=[pltpu.VMEM((BLOCK, vertices), bf16), pltpu.VMEM((BLOCK, WIDE), bf16),
                        pltpu.VMEM((DEG, BLOCK, WIDE), bf16), pltpu.SemaphoreType.DMA],
        name="extract",
    )(half, adj_slab)


def along(shape, axis=0):
    return lax.broadcasted_iota(jnp.int32, shape, axis)


def swap(x):
    return pltpu.roll(x, HALF, 1)


def digits(x, base):
    high = jnp.floor(x * (1.0 / base))
    return high, x - high * base


def walk_kernel(which_ref, src_ref, weight_ref, lists_ref, out_ref,
                table, queue, sigma, ratio, delta, cand, ids, now, dest, tail_ref, held, rowhot, colhot, bins,
                ids_a, ids_b, meta, sems, *, levels, vertices, scale, compact):
    pitch = vertices + SUB
    lane = along((SUB, LANES), 1)
    sub = along((SUB, LANES))
    upper = lane >= HALF
    lane_row = along((1, LANES), 1)
    group_odd = ((lane_row // 32) % 2) == 1
    lane32 = lane_row % 32
    rows_all = queue.shape[0]
    tile_bits = (vertices // lists_ref.shape[0]).bit_length() - 1
    high = vertices // WIDE

    def eight(row):
        return pl.ds(pl.multiple_of(row, SUB), SUB)

    def part(n):
        return pl.ds(n * SUB, SUB)

    def spread_row(ref, *index):
        return jnp.broadcast_to(ref[(*index[:-1], pl.ds(index[-1], 1), slice(None))], (SUB, LANES))

    def clear(t, carry):
        for k in range(SUB):
            rows = eight((t * SUB + k) * SUB)
            queue[rows, :] = jnp.full((SUB, LANES), -1.0, f32)
            sigma[rows, :] = jnp.zeros((SUB, LANES), f32)
        return carry

    def fetch(quad, row, buf):
        return pltpu.make_async_copy(ids.at[quad, eight(row)], buf[0], sems.at[buf[1]])

    def name(row, q):
        v = jnp.where(q < 0, vertices, q.astype(jnp.int32))
        ids[0, eight(row), :] = v
        if not compact:
            ids[1, eight(row), :] = v + pitch

    bufs = (ids_a, 0), (ids_b, 1)
    clear(0, 0)

    near_source = jnp.full((SUB, LANES), EMPTY, f32)
    source = along((SUB, LANES))
    for j in range(HALF):
        v = src_ref[which_ref[0] * HALF + j]
        near_source = jnp.where(lane == j, pltpu.roll(lists_ref[v >> tile_bits], (j - v) & (LANES - 1), 1), near_source)
        source = jnp.where(lane % HALF == j, v, source)
    if compact:
        near_source = jnp.where((source & LANES) > 0, pltpu.roll(near_source, FEW, 0), near_source)
    near_source = jnp.where(upper, swap(near_source), near_source)
    reached = near_source >= 0
    if compact:
        reached = reached & (sub < FEW)
    queue[0:1, :] = source[:1].astype(f32)
    queue[eight(SUB), :] = jnp.where(reached, near_source, -1.0)
    sigma[eight(SUB), :] = jnp.where(reached & jnp.logical_not(upper), 1.0, 0.0)
    for n in (1, 2):
        name(n * SUB, queue[eight(n * SUB), :])
    bins[...] = jnp.zeros_like(bins)
    fetch(0, SUB, bufs[0]).start()
    if compact:
        fetch(0, 2 * SUB, bufs[1]).start()
    eights = rows_all // (SUB * SUB)
    soon_clear = FEW if compact else eights
    lax.fori_loop(1, soon_clear, clear, 0)

    srow = along((2 * SUB, LANES))
    slane = along((2 * SUB, LANES), 1)

    def fill(halves, target):
        picks = [jnp.where((srow % SUB) == (slane // 32 + FEW * h), jnp.where(srow < SUB, float(LANES), 1.0), 0.0).astype(bf16)
                 for h in halves]

        def body(step, most):
            for k in range(GROUP):
                first = (GROUP * step + k) * SUB
                x = jnp.concatenate([lists_ref[first + n] for n in range(SUB)], axis=1)
                both = jnp.concatenate(digits(x, LANES), axis=0).astype(bf16)
                for h, pick in zip(halves, picks):
                    rows = lax.dot_general(both, pick, (((0,), (0,)), ((), ())), preferred_element_type=f32)
                    for n in range(SUB):
                        table[pl.ds(pl.multiple_of(target(h, first + n), SUB), LANES), :] = rows[n * LANES:(n + 1) * LANES]
                for n in range(SUB):
                    most = jnp.maximum(most, lists_ref[first + n])
            return most

        return lax.fori_loop(0, lists_ref.shape[0] // (GROUP * SUB), body, jnp.full((SUB, LANES), EMPTY, f32))

    table[vertices:pitch, :] = jnp.full((SUB, LANES), EMPTY, f32)
    if compact:
        most = fill(PAIR, lambda h, t: (2 * t + h) * LANES)
        quads = 1
    else:
        table[pitch + vertices:, :] = jnp.full((SUB, LANES), EMPTY, f32)
        most = fill((0,), lambda h, t: t * LANES)
        wide = jnp.max(jnp.where(sub >= FEW, most, EMPTY)) >= 0
        quads = jnp.where(wide, 2, 1)

        @pl.when(wide)
        def _():
            fill((1,), lambda h, t: pitch + t * LANES)

    bad = jnp.max(most) > vertices
    meta[FAULT] = bad.astype(jnp.int32)

    def gather(rows_of_ids):
        acc = [[jnp.full((1, LANES), EMPTY, f32)] * 2 for _ in rows_of_ids]
        for j in range(32):
            hit = lane32 == j
            for i, id_of in enumerate(rows_of_ids):
                for b in PAIR:
                    acc[i][b] = jnp.where(hit, table[pl.ds(id_of(b * 32 + j), 1), :], acc[i][b])
        return [(jnp.where(group_odd, b, a), pltpu.roll(jnp.where(group_odd, a, b), LANES - 32, 1)) for a, b in acc]

    def gather_slots(ids_s, slots=SLOTS):
        return gather([functools.partial(lambda i, j: ids_s[i, j], i) for i in range(slots)])

    def keep(rows, quad, row):
        for i, pair in enumerate(rows):
            for h in PAIR:
                cand[2 * quad + h, pl.ds(row + i, 1), :] = pair[h]

    def flag(x):
        return jnp.where(x, 1, 0)

    def at(unit, origin):
        return unit & (quads - 1), origin + (unit >> (quads - 1)) * SUB

    def level_step(level, carry):
        base, count = meta[BASE, level], meta[COUNT, level]
        following = base + (count + 7) // SUB * SUB
        batches = jnp.where(following <= CAP, (count + SLOTS - 1) // SLOTS, 0)
        units = batches * quads
        parity = meta[PARITY]

        def on_parity(n, f):
            for k in PAIR:
                @pl.when(n & 1 == k)
                def _():
                    f(bufs[k], bufs[1 - k])

        def unit_step(unit, other, to):
            quad, row = at(unit, base)
            x = [cand[2 * quad + h, eight(row), :] for h in PAIR]

            def search(first, count, marks):
                marks = list(marks)
                for k in range(count):
                    q = spread_row(queue, first + k)
                    for h in PAIR:
                        n = 2 * h + k % 2
                        marks[n] = jnp.where(x[h] == q, 1, marks[n])
                return tuple(marks)

            reach = following + meta[LENGTH] - PEEL
            marks = lax.fori_loop(0, (reach + SCAN - 1) // SCAN, lambda t, m: search(PEEL + t * SCAN, SCAN, m),
                                  (jnp.zeros((SUB, LANES), jnp.int32),) * 4)
            ahead = unit + 1 < units
            final_unit = unit + 1 == units
            soon = jnp.logical_and(final_unit, meta[AWAIT0] > 0)

            @pl.when(jnp.logical_or(ahead, soon))
            def _():
                fetch(0, base, to).wait()

            def insert(g):
                slots = [eight(following + g * WINDOW + SUB * t) for t in range(WINDOW // SUB)]
                qs = [queue[r, :] for r in slots]
                ss = [sigma[r, :] for r in slots]
                pos = [sub + (g * WINDOW + SUB * t) for t in range(WINDOW // SUB)]
                for h in PAIR:
                    for i in range(SUB):
                        d, e = spread_row(dest, SUB * h + i), spread_row(dest, SUB * (h + 2) + i)
                        v, w = spread_row(now, SUB * h + i), spread_row(now, SUB * (h + 2) + i)
                        for t in range(WINDOW // SUB):
                            qs[t] = jnp.where(pos[t] == d, v, jnp.where(pos[t] == e, w, qs[t]))
                for i in range(SUB):
                    v, w, sig = (spread_row(now, SUB * n + i) for n in (0, 1, 4))
                    for t in range(WINDOW // SUB):
                        ss[t] = ss[t] + jnp.where((qs[t] == v) | (qs[t] == w), sig, 0.0)
                for t, r in enumerate(slots):
                    queue[r, :] = qs[t]
                    sigma[r, :] = ss[t]
                return qs

            def core(looking):
                even, odd = x
                m, n, k, l = search(0, PEEL, marks)
                near_even, near_odd = m | n | flag(even < 0), k | l | flag(odd < 0)

                xr = [swap(v) for v in x]
                turns = [[[pltpu.roll(v, s, 0) if s else v for v in (x[h], xr[h])] for s in range(SUB)] for h in PAIR]
                for s, ((a, b), (c, d)) in enumerate(zip(*turns)):
                    near_odd = jnp.where((odd == a) | (odd == b), 1, near_odd)
                    if s:
                        after = sub >= s
                        near_even = jnp.where(((even == a) | (even == b)) & after, 1, near_even)
                        near_odd = jnp.where(((odd == c) | (odd == d)) & after, 1, near_odd)

                new = [1 - near_even, 1 - near_odd]
                packed = new[0] + BYTE * new[1]
                across = swap(packed)
                far = [across & (BYTE - 1), across >> SUB]
                both = packed + across
                run, whole = both, both
                for s in (1, 2, 4):
                    run = run + jnp.where(sub >= s, pltpu.roll(run, s, 0), 0)
                    whole = whole + pltpu.roll(whole, s, 0)
                run = run - both
                tail = tail_ref[...]
                evens = whole & (BYTE - 1)
                begin = [tail + (run & (BYTE - 1)), tail + evens + (run >> SUB)]
                for h in PAIR:
                    dest[part(h), :] = jnp.where(new[h] > 0, begin[h] + jnp.where(upper, far[h], 0), -1)
                    dest[part(h + 2), :] = jnp.where(far[h] > 0, begin[h] + jnp.where(upper, 0, new[h]), -1)
                    now[part(h), :] = x[h]
                    now[part(h + 2), :] = xr[h]
                now[part(4), :] = sigma[eight(row), :] + swap(sigma[eight(row), :])
                tail = tail + evens + (whole >> SUB)
                tail_ref[...] = tail
                passed = SLOTS * ((unit + 1) >> (quads - 1))
                second = SUB + SUB * (1 >> (quads - 1))
                need = jnp.where(sub == 1, SUB, second)
                short = (tail < need) & (held[...] > passed)
                most = jnp.max(jnp.where(sub == 0, tail, flag(short)).astype(f32), axis=1, keepdims=True)
                meta[REACHED] = most[0, 0].astype(jnp.int32)
                for n in PAIR:
                    meta[(SHORT0, SHORT1)[n]] = most[n + 1, 0].astype(jnp.int32)

                if looking:
                    quad2, row2 = at(unit + 1, base)
                    rows = gather_slots(to[0])
                qs = insert(0)
                for n in PAIR:
                    name(following + n * SUB, qs[n])
                if looking:
                    keep(rows, jnp.where(ahead, quad2, 0), jnp.where(ahead, row2, following))

            look = jnp.logical_or(ahead, soon)
            for looking in PAIR:
                @pl.when(look == (looking > 0))
                def _():
                    core(looking)

            length = meta[REACHED]
            ready = [meta[n] == 0 for n in (SHORT0, SHORT1)]

            @pl.when(unit + 3 < units)
            def _():
                fetch(*at(unit + 3, base), to).start()

            @pl.when(soon)
            def _():
                meta[GOT] = 1

            def first_of_next(n, when, buf):
                @pl.when(jnp.logical_and(when, meta[(AWAIT0, AWAIT1)[n]] == 0))
                def _():
                    fetch(*at(n, following), buf).start()
                    meta[(AWAIT0, AWAIT1)[n]] = 1

            first_of_next(0, jnp.logical_and(ready[0], unit + 3 == units), to)
            first_of_next(0, jnp.logical_and(ready[0], unit + 2 == units), other)
            first_of_next(1, jnp.logical_and(ready[1], unit + 2 == units), to)
            first_of_next(0, final_unit, to)
            first_of_next(1, final_unit, other)

            groups = (length + WINDOW - 1) // WINDOW
            fits = following + groups * WINDOW <= CAP + WINDOW
            meta[LENGTH] = jnp.where(fits, length, 0)

            @pl.when(jnp.logical_not(fits))
            def _():
                meta[FAULT] = 1

            def more(g, carry):
                insert(g)
                return carry

            lax.fori_loop(1, jnp.where(fits, groups, 0), more, 0)

        tail_ref[...] = jnp.zeros_like(tail_ref)
        meta[LENGTH] = 0

        def open_level(mine, other):
            @pl.when(jnp.logical_and(meta[GOT] == 0, meta[AWAIT0] > 0))
            def _():
                fetch(0, base, mine).wait()
                keep(gather_slots(mine[0]), 0, base)

            @pl.when(jnp.logical_and(units < 2, meta[AWAIT1] > 0))
            def _():
                fetch(0, base, other).wait()

            @pl.when(units > 2)
            def _():
                fetch(*at(2, base), mine).start()

        if compact:
            @pl.when(level == 2)
            def _():
                lax.fori_loop(soon_clear, eights, clear, 0)

        on_parity(parity, open_level)
        for place_ in (GOT, AWAIT0, AWAIT1):
            meta[place_] = 0

        def any_unit(unit, carry):
            on_parity(parity + unit, functools.partial(unit_step, unit))
            return carry

        lax.fori_loop(0, units, any_unit, 0)
        meta[PARITY] = parity + units

        @pl.when(following > CAP)
        def _():
            meta[FAULT] = 1

        found = jnp.where(meta[FAULT] == 0, meta[LENGTH], 0)
        meta[BASE, level + 1] = following
        meta[COUNT, level + 1] = found

        def names(t, carry):
            row = following + t * SUB
            name(row, queue[eight(row), :])
            return carry

        for t in range(2, WINDOW // SUB):
            names(t, carry)
        lax.fori_loop(WINDOW // SUB, (found + SUB - 1) // SUB, names, 0)
        held[...] = tail_ref[...]
        return carry

    for place_ in (GOT, PARITY):
        meta[place_] = 0

    @pl.when(jnp.logical_not(bad))
    def _():
        held[...] = jnp.full_like(held, FEW * quads)
        meta[BASE, 1] = SUB
        meta[COUNT, 1] = FEW * quads
        fetch(0, SUB, bufs[0]).wait()
        if compact:
            for h in PAIR:
                cand[h, eight(SUB), :] = jnp.full((SUB, LANES), EMPTY, f32)
        else:
            fetch(*at(1, SUB), bufs[1]).start()
        keep(gather_slots(ids_a, FEW if compact else SLOTS), 0, SUB)
        meta[GOT] = 1
        meta[AWAIT0] = 0
        meta[AWAIT1] = 1
        lax.fori_loop(1, levels, level_step, 0)

    @pl.when(bad)
    def _():
        fetch(0, SUB, bufs[0]).wait()
        meta[AWAIT0] = 0
        meta[AWAIT1] = int(compact)

    def drain(n, buf):
        @pl.when(meta[(AWAIT0, AWAIT1)[n]] > 0)
        def _():
            fetch(0, 0, buf).wait()

    for k in PAIR:
        @pl.when(meta[PARITY] & 1 == k)
        def _():
            @pl.when(meta[GOT] == 0)
            def _():
                drain(0, bufs[k])

            drain(1, bufs[1 - k])

    good = meta[FAULT] == 0

    @pl.when(good)
    def _():
        last = meta[BASE, levels]
        g_last = weight_ref[levels - 2]

        def seed(g, carry):
            for t in range(WINDOW // SUB):
                r = eight(last + g * WINDOW + SUB * t)
                s = sigma[r, :] + swap(sigma[r, :])
                ratio[r, :] = jnp.where(s > 0, g_last / jnp.where(s > 0, s, 1.0), 0.0)
            return carry

        lax.fori_loop(0, (meta[COUNT, levels] + WINDOW - 1) // WINDOW, seed, 0)

        def back_step(k, carry):
            level = levels - 1 - k
            base, count = meta[BASE, level], meta[COUNT, level]
            nbase, ncount = meta[BASE, level + 1], meta[COUNT, level + 1]
            g_here = weight_ref[jnp.maximum(level - 2, 0)]

            def pull_batch(bt, carry):
                here = eight(base + bt * SLOTS)

                def pull(quad, c, acc):
                    even, odd = cand[2 * quad, here, :], cand[2 * quad + 1, here, :]
                    acc = list(acc)
                    for n in range(WINDOW):
                        q = spread_row(queue, nbase + c * WINDOW + n)
                        w = spread_row(ratio, nbase + c * WINDOW + n)
                        acc[n % 2] = acc[n % 2] + jnp.where((even == q) | (odd == q), w, 0.0)
                    return tuple(acc)

                def pull_quad(quad, acc):
                    return lax.fori_loop(1, (ncount + WINDOW - 1) // WINDOW, functools.partial(pull, quad), pull(quad, 0, acc))

                acc = pull_quad(0, (jnp.zeros((SUB, LANES), f32),) * 2)
                if not compact:
                    acc = lax.fori_loop(1, quads, pull_quad, acc)
                delta[here, :] = acc[0] + acc[1]
                return carry

            lax.fori_loop(0, (count + SLOTS - 1) // SLOTS, pull_batch, 0)

            def finish(g, carry):
                slots = [eight(base + g * WINDOW + SUB * t) for t in range(WINDOW // SUB)]
                for t, r in enumerate(slots):
                    inside = g * WINDOW + SUB * t < count
                    part, s = (v + swap(v) for v in (delta[r, :], sigma[r, :]))
                    d = s * part
                    w = jnp.where(s > 0, (g_here + d) / jnp.where(s > 0, s, 1.0), 0.0)
                    delta[r, :] = jnp.where(inside, d, delta[r, :])
                    ratio[r, :] = jnp.where(inside, w, ratio[r, :])
                return carry

            lax.fori_loop(0, (count + WINDOW - 1) // WINDOW, finish, 0)
            return carry

        lax.fori_loop(0, levels - 1, back_step, 0)

        tall = along((WIDE, WIDE)).astype(f32).astype(bf16)
        zero = jnp.zeros((WIDE, WIDE), bf16)
        one = zero + 1
        start = meta[BASE, 1]

        def tally(t, carry):
            for u in range(TALLY // 16):
                a, b = eight(start + t * TALLY + u * 16), eight(start + t * TALLY + u * 16 + SUB)
                v = jnp.where(upper, queue[b, :], queue[a, :])
                d = jnp.where(upper, delta[b, :], delta[a, :])
                hi, lo = digits(v, WIDE)
                d_hi = d.astype(bf16).astype(f32)
                d_mid = (d - d_hi).astype(bf16).astype(f32)
                d_lo = d - d_hi - d_mid
                for p in range(0, SUB, 2):
                    cols = slice((u * SUB + p) * LANES, (u * SUB + p + 2) * LANES)

                    def pair(x):
                        return jnp.concatenate([x[p:p + 1], x[p + 1:p + 2]], axis=1).astype(bf16)

                    colhot[:, cols] = jnp.where(tall == pair(lo), one, zero)
                    match = tall[:high] == pair(hi)
                    for n, x in enumerate((d_hi, d_mid, d_lo)):
                        rowhot[n * high:(n + 1) * high, cols] = jnp.where(match, pair(x), zero[:high])
            bins[...] += lax.dot_general(rowhot[...], colhot[...], TURN, preferred_element_type=f32)
            return carry

        for t in range(TALLY // SUB):
            delta[eight(last + t * SUB), :] = jnp.zeros((SUB, LANES), f32)
        lax.fori_loop(0, (last - start + TALLY - 1) // TALLY, tally, 0)

    blocks = out_ref.shape[0]
    per = high // blocks
    total = (bins[:high] + bins[high:2 * high] + bins[2 * high:]) * scale
    fault = jnp.where(good, 0.0, 1.0)
    for b in range(blocks):
        for n in PAIR:
            out_ref[b, n * per:(n + 1) * per, :] = total[b * per:(b + 1) * per, n * LANES:(n + 1) * LANES]
        out_ref[b, 2 * per:, :] = jnp.full((1, LANES), fault, f32)


def walk(which, sources, weights, lists, *, blocks, vertices, scale, compact):
    levels = weights.shape[0] + 1
    rows = CAP + 4 * WINDOW
    high = LANES // blocks + 1
    vm = pltpu.VMEM
    queue = vm((rows, LANES), f32)
    parts = 3 * (vertices // WIDE)
    return pl.pallas_call(
        functools.partial(walk_kernel, levels=levels, vertices=vertices, scale=scale, compact=compact),
        in_specs=[pl.BlockSpec(memory_space=pltpu.SMEM)] * 3 + [pl.BlockSpec(memory_space=pltpu.VMEM)],
        out_specs=pl.BlockSpec(memory_space=pltpu.VMEM),
        out_shape=jax.ShapeDtypeStruct((blocks, high, LANES), f32),
        scratch_shapes=[
            vm(((1 if compact else 2) * (vertices + SUB), LANES), f32), queue, queue, queue, queue,
            vm((4, rows, LANES), f32), vm((2, rows, LANES), jnp.int32),
            vm((40, LANES), f32), vm((32, LANES), jnp.int32), vm((SUB, LANES), jnp.int32), vm((SUB, LANES), jnp.int32),
            vm((parts, TALLY // 2 * LANES), bf16), vm((WIDE, TALLY // 2 * LANES), bf16), vm((parts, WIDE), f32),
            pltpu.SMEM((SLOTS, LANES), jnp.int32), pltpu.SMEM((SLOTS, LANES), jnp.int32), pltpu.SMEM((3, 16), jnp.int32),
            pltpu.SemaphoreType.DMA((2,)),
        ],
        compiler_params=pltpu.CompilerParams(
            vmem_limit_bytes=48 * MIB),
        name="walk",
    )(which, sources, weights, lists)


def share_kernel(src, graph, x_ref, o_ref, own_sem, send_sem, recv_sem):
    mine, g, others = place_and_others(src, graph)
    hello(others)
    await_hello(others)
    own = pltpu.make_async_copy(x_ref, o_ref.at[mine], own_sem)
    own.start()
    copies = []
    for n, (py, pg) in enumerate(others):
        copies.append(pltpu.make_async_remote_copy(
            src_ref=x_ref, dst_ref=o_ref.at[mine], send_sem=send_sem.at[n], recv_sem=recv_sem.at[n],
            device_id={"src": py, "graph": pg}, device_id_type=MESH))
        copies[-1].start()
    own.wait()
    for c in copies:
        c.wait()


def share(x, src, graph):
    n = src * graph
    return pl.pallas_call(
        functools.partial(share_kernel, src, graph),
        in_specs=[pl.BlockSpec(memory_space=pltpu.VMEM)],
        out_specs=pl.BlockSpec(memory_space=pltpu.VMEM),
        out_shape=jax.ShapeDtypeStruct((n,) + x.shape, x.dtype),
        scratch_shapes=[pltpu.SemaphoreType.DMA, pltpu.SemaphoreType.DMA((n - 1,)), pltpu.SemaphoreType.DMA((n - 1,))],
        compiler_params=pltpu.CompilerParams(collective_id=2, has_side_effects=True),
        name="share",
    )(x)


def total_kernel(src, graph, x_ref, o_ref, got, own_sem, send_sem, recv_sem):
    mine, g, others = place_and_others(src, graph)
    hello(others)
    own = pltpu.make_async_copy(x_ref.at[g], got.at[mine], own_sem)
    own.start()
    await_hello(others)
    copies = []
    for n, (py, pg) in enumerate(others):
        copies.append(pltpu.make_async_remote_copy(
            src_ref=x_ref.at[pg], dst_ref=got.at[mine], send_sem=send_sem.at[n], recv_sem=recv_sem.at[n],
            device_id={"src": py, "graph": pg}, device_id_type=MESH))
        copies[-1].start()
    own.wait()
    for c in copies:
        c.wait()
    acc = got[0]
    for n in range(1, src * graph):
        acc = acc + got[n]
    o_ref[...] = acc


def total(x, src, graph, collective_id):
    n = src * graph
    return pl.pallas_call(
        functools.partial(total_kernel, src, graph),
        in_specs=[pl.BlockSpec(memory_space=pltpu.VMEM)],
        out_specs=pl.BlockSpec(memory_space=pltpu.VMEM),
        out_shape=jax.ShapeDtypeStruct(x.shape[1:], x.dtype),
        scratch_shapes=[pltpu.VMEM((n,) + x.shape[1:], x.dtype), pltpu.SemaphoreType.DMA,
                        pltpu.SemaphoreType.DMA((n - 1,)), pltpu.SemaphoreType.DMA((n - 1,))],
        compiler_params=pltpu.CompilerParams(collective_id=collective_id, has_side_effects=True),
        name="total",
    )(pltpu.with_memory_space_constraint(x, pltpu.VMEM))


def exchange(x, axis):
    return lax.all_to_all(x, axis, 0, 0)


def dense(adj_slab, src_local, level_weight, src, graph):
    slab_rows, vertex_count = adj_slab.shape
    src_count = src_local.shape[0]
    levels = level_weight.shape[0] + 1
    row_start = lax.axis_index("graph") * slab_rows
    vertex_ids = row_start + lax.broadcasted_iota(jnp.int32, (slab_rows, 1), 0)
    first = jnp.where(vertex_ids == src_local[None, :], 1.0, 0.0).astype(f32)

    def forward(carry, unused):
        sigma, seen = carry
        partial = jnp.einsum("uv,us->vs", adj_slab, sigma, preferred_element_type=f32, precision=exact_precision)
        parts = exchange(partial.reshape(graph, slab_rows, src_count), "graph")
        sigma = jnp.sum(parts, axis=0) * (1.0 - seen)
        seen = jnp.maximum(seen, jnp.where(sigma > 0, 1.0, 0.0))
        return (sigma, seen), sigma

    _, sigmas = lax.scan(forward, (first, first), None, length=levels)

    def backward(carry, xs):
        delta, acc = carry
        upper, lower, weight = xs
        reached = upper > 0
        ratio = jnp.where(reached, (weight + delta) / jnp.where(reached, upper, 1.0), 0.0)
        gathered = exchange(jnp.broadcast_to(ratio[None], (graph,) + ratio.shape), "graph")
        pulled = jnp.einsum("uv,vs->us", adj_slab, gathered.reshape(vertex_count, src_count),
                            preferred_element_type=f32, precision=exact_precision)
        delta = lower * pulled
        return (delta, acc + delta), None

    zero = jnp.zeros_like(first)
    (_, acc), _ = lax.scan(backward, (zero, zero), (sigmas[1:][::-1], sigmas[:-1][::-1], level_weight[::-1]))
    scale = vertex_count / (src_count * src * levels ** 3)
    mine = jnp.sum(acc, axis=1) * scale
    both = exchange(jnp.broadcast_to(mine.reshape(1, -1, LANES), (src, slab_rows // LANES, LANES)), "src")
    return jnp.sum(both, axis=0).reshape(slab_rows)


def solution(mesh):
    src, graph = mesh.shape["src"], mesh.shape["graph"]

    def device_program(adj_slab, src_local, level_weight):
        slab_rows, vertex_count = adj_slab.shape
        levels = level_weight.shape[0] + 1
        scale = vertex_count / (HALF * src * graph * levels ** 3)
        which = lax.axis_index("graph").astype(jnp.int32).reshape(1)

        def finish(lists, compact, collective_id, other):
            parts = walk(which, src_local, level_weight, lists, blocks=graph, vertices=vertex_count, scale=scale, compact=compact)
            summed = total(parts, src, graph, collective_id)
            rows = slab_rows // LANES

            def plain():
                return summed[:rows].reshape(2, -1, LANES).transpose(1, 0, 2).reshape(slab_rows)

            return lax.cond(summed[rows, 0] > 0, other, plain)

        def dense_path():
            return dense(adj_slab, src_local, level_weight, src, graph)

        def general_path():
            half = lax.axis_index("src").astype(jnp.int32).reshape(1)
            lists = share(extract(adj_slab, half, slab_rows // src), src, graph)
            return finish(lists.reshape(-1, SUB, LANES), False, 3, dense_path)

        return finish(collect(adj_slab, src, graph), True, 1, general_path)

    return jax.shard_map(device_program, mesh=mesh,
                         in_specs=(P(("batch", "graph"), None), P(("batch", "src")), P(None)),
                         out_specs=P(("batch", "graph")), check_vma=False)
```
